32 devices in a mesh: fsdp: 4 (over y, x), expert: 8 (over z, core).
Axes of the slice: x: 2, y: 2, z: 4, core: 2. Of those that a mesh axis runs over, the one named last changes fastest.
Arguments:
- block_input: bfloat16 [8, 512, 2048], P('expert', 'fsdp'), may hold values from -6 to 6
- cotangent: bfloat16 [8, 512, 2048], P('expert', 'fsdp'), may hold values from -6 to 6
- w_query: bfloat16 [2048, 2048], P(None, 'fsdp'), may hold values from -0.125 to 0.125
- w_key: bfloat16 [2048, 2048], P(None, 'fsdp'), may hold values from -0.125 to 0.125
- w_value: bfloat16 [2048, 2048], P(None, 'fsdp'), may hold values from -0.125 to 0.125
- w_output: bfloat16 [2048, 2048], P('fsdp'), may hold values from -0.75 to 0.75
- q_gain: float32 [2048], P('fsdp'), may hold values from 0.7 to 1.3
- k_gain: float32 [2048], P('fsdp'), may hold values from 0.7 to 1.3
- attn_gain: float32 [2048], replicated, may hold values from 0.1 to 1.9
- mlp_gain: float32 [2048], replicated, may hold values from 0.1 to 1.9
- w_router: bfloat16 [2048, 16], replicated, may hold values from -0.125 to 0.125
- w_gate: bfloat16 [16, 2048, 1024], P('expert', None, 'fsdp'), may hold values from -0.125 to 0.125
- w_up: bfloat16 [16, 2048, 1024], P('expert', None, 'fsdp'), may hold values from -0.125 to 0.125
- w_down: bfloat16 [16, 1024, 2048], P('expert', 'fsdp'), may hold values from -0.5 to 0.5
- segments: int32 [8, 512], P('expert', 'fsdp'), may hold values from 0 to 1, as said below
- routes: int32 [8, 512, 8], P('expert', 'fsdp'), may hold values from 0 to 15, all different within a row; in each aligned block of 128 rows (0 to 127, 128 to 255, ..., all dimensions but the last counted through in order) at most 96 rows name the same one
- capacity: int32 [16], replicated, may hold values from 48 to 96
Outputs:
- block_output: bfloat16 [8, 512, 2048], P('expert', 'fsdp')
- grad_input: float32 [8, 512, 2048], P('expert', 'fsdp')
- grad_query: float32 [2048, 2048], P(None, 'fsdp')
- grad_key: float32 [2048, 2048], P(None, 'fsdp')
- grad_value: float32 [2048, 2048], P(None, 'fsdp')
- grad_w_output: float32 [2048, 2048], P('fsdp')
- grad_q_gain: float32 [2048], P('fsdp')
- grad_k_gain: float32 [2048], P('fsdp')
- grad_attn_gain: float32 [2048], replicated
- grad_mlp_gain: float32 [2048], replicated
- grad_router: float32 [2048, 16], replicated
- grad_gate: float32 [16, 2048, 1024], P('expert', None, 'fsdp')
- grad_up: float32 [16, 2048, 1024], P('expert', None, 'fsdp')
- grad_down: float32 [16, 1024, 2048], P('expert', 'fsdp')
The draws below stay inside these ranges and needn't reach their ends.
Inputs may be any that keep to these rules, and one draw needn't show every extreme that they name: `segments`: segment ids start at 0 and never fall along the rows of a group; each group holds exactly 2 sequences. `routes`: each token names 8 different experts; among the tokens of one device no expert is named more than 96 times.
All inputs are finite; a program needn't handle non-finite values.
Results may differ from the reference program's by a relative error of at most 0.017.
Values may be sent and summed in bfloat16 or wider, within the bound.
A program may use at most 384 MiB of HBM per device.

```python
import math
import jax
import jax.numpy as jnp
import numpy as np
from jax import lax

D = 2048
HEADS = 16
HEAD_DIM = 128
FF = 1024
TOP = 8
TOK_DEV = 128
EXPERTS = 16
GROUPS = 8
GROUP_TOK = 512
SLOT = 96


def head_gains(key):
    return jax.random.uniform(jax.random.fold_in(key, 1), (D,), jnp.float32, 0.7, 1.3)


def draw_q_gain(key, part):
    return head_gains(jax.random.fold_in(key, 5))


def draw_k_gain(key, part):
    return head_gains(jax.random.fold_in(key, 6))


def group_segments(key):
    cut_point = jax.random.randint(key, (), 1, GROUP_TOK)
    position = jnp.arange(GROUP_TOK, dtype=jnp.int32)
    return (position >= cut_point).astype(jnp.int32)


def draw_segments(key, part):
    group_keys = jax.random.split(jax.random.fold_in(key, 41), GROUPS)
    return jax.vmap(group_segments)(group_keys).astype(jnp.int32)


def draw_capacity(key, part):
    levels = jax.random.randint(jax.random.fold_in(key, 51), (EXPERTS,), SLOT // 2, SLOT + 1)
    fullest = jax.random.randint(jax.random.fold_in(key, 52), (), 0, EXPERTS)
    return levels.at[fullest].set(SLOT).astype(jnp.int32)


def steps_of(rng, extent, cuts, least, high):
    level = 1.0
    for axis_at, shards_of in cuts:
        draws = jax.random.uniform(jax.random.fold_in(jax.random.fold_in(rng, 6), axis_at), (shards_of,), jnp.float32, least / len(cuts), high / len(cuts))
        level = level * jnp.repeat(jnp.exp(draws), extent[axis_at] // shards_of).reshape((-1,) + (1,) * (len(extent) - 1 - axis_at))
    return level


def shared_out(key, own, number, rows, count, top, bound, skew):
    sequence = jax.random.permutation(key, count)
    crowded, common = portions_of(count, rows * top, bound, skew, True), portions_of(count, rows * top, bound, skew, False)
    places = jnp.arange(count)

    def named(sizes, offset_by):
        used = int((sizes > 0).sum())
        fixed = max(1, used // 4)
        shifted = fixed + (places - fixed + offset_by * (used - fixed)) % max(1, count - fixed)
        return jnp.zeros((count,), jnp.int32).at[sequence[jnp.where(places < fixed, places, shifted)]].set(jnp.asarray(sizes, jnp.int32))

    sizes = jnp.where(number % 4 == 0, named(crowded, number // 4), named(common, number - number // 4 - 1))
    mixed = jax.random.permutation(jax.random.fold_in(own, 3), count)
    source_of, taker = mixed[0:count // 2 * 2:2], mixed[1:count // 2 * 2:2]
    room = jnp.minimum(sizes[source_of] - 1, bound - sizes[taker]) // 2
    room = jnp.where((source_of == sequence[0]) | (taker == sequence[0]) | (sizes[taker] == 0), 0, jnp.maximum(room, 0))
    shifted = jax.random.randint(jax.random.fold_in(own, 4), (count // 2,), 0, 1 << 20) % (room + 1)
    sizes = sizes.at[source_of].add(-shifted).at[taker].add(shifted)
    labels = jnp.searchsorted(jnp.cumsum(sizes), jnp.arange(rows * top), side="right").astype(jnp.int32)
    listing = labels.reshape(top, rows).T
    listing = listing[jax.random.permutation(jax.random.fold_in(own, 1), rows)]
    offset_by = jax.random.randint(jax.random.fold_in(own, 2), (rows, 1), 0, top)
    return jnp.take_along_axis(listing, (jnp.arange(top)[None, :] + offset_by) % top, axis=1)


def portions_of(count, total, bound, skew, full):
    weights = [(1 << 20) // math.isqrt(standing ** skew) + 1 for standing in range(1, count + 1)]
    largest = bound if full else min(bound, max(-(-total // count), total * weights[0] // sum(weights)))
    least = 1 if total - largest >= count - 1 else 0
    given, surplus = [largest] + [least] * (count - 1), total - largest - least * (count - 1)
    while surplus > 0:
        candidates = [i for i in range(1, count) if given[i] < largest] or [i for i in range(1, count) if given[i] < bound]
        pool, remaining = sum([weights[i] for i in candidates]), surplus
        for i in candidates:
            extra = min(bound - given[i], max(1, remaining * weights[i] // pool), surplus)
            given[i] = given[i] + extra
            surplus = surplus - extra
    return np.array(given)


def scatter_about(own_key, shape, deviation, most, cuts=(), kind=jnp.bfloat16):
    drawn = jax.random.normal(own_key, shape, jnp.float32) * deviation
    if len(cuts) > 0:
        drawn = steps_of(own_key, shape, cuts, -0.22, 0.18) * drawn
    return jnp.clip(drawn, min=-most, max=most).astype(kind)


def setup_inputs(seed: int = 0) -> dict:
    seeds = jax.random.split(jax.random.key(seed), 18)
    block_input = scatter_about(seeds[0], (GROUPS, GROUP_TOK, D), 1.0, 6.0, ((0, 8), (1, 4)))
    cotangent = scatter_about(seeds[1], (GROUPS, GROUP_TOK, D), 1.0, 6.0, ((0, 8), (1, 4)))
    w_query = scatter_about(seeds[2], (D, D), D ** -0.5, 0.125, ((1, 4),))
    w_key = scatter_about(seeds[3], (D, D), D ** -0.5, 0.125, ((1, 4),))
    w_value = scatter_about(seeds[4], (D, D), D ** -0.5, 0.125, ((1, 4),))
    w_output = scatter_about(seeds[5], (D, D), (D // 32) ** -0.5, 0.75, ((0, 4),))
    q_gain = draw_q_gain(jax.random.fold_in(seeds[17], 71), 0)
    k_gain = draw_k_gain(jax.random.fold_in(seeds[17], 71), 0)
    attn_gain = jnp.clip(1.0 + 0.18 * jax.random.normal(seeds[8], (D,), jnp.float32), 0.1, 1.9)
    mlp_gain = jnp.clip(1.0 + 0.18 * jax.random.normal(seeds[9], (D,), jnp.float32), 0.1, 1.9)
    w_router = scatter_about(seeds[10], (D, EXPERTS), D ** -0.5, 0.125)
    w_gate = scatter_about(seeds[11], (EXPERTS, D, FF), D ** -0.5, 0.125, ((0, 8), (2, 4)))
    w_up = scatter_about(seeds[12], (EXPERTS, D, FF), D ** -0.5, 0.125, ((0, 8), (2, 4)))
    w_down = scatter_about(seeds[13], (EXPERTS, FF, D), (FF // 8) ** -0.5, 0.5, ((0, 8), (1, 4)))
    segments = draw_segments(jax.random.fold_in(seeds[17], 71), 0)
    routes_keys = jax.random.split(jax.random.fold_in(seeds[15], 1), GROUPS * GROUP_TOK // TOK_DEV)
    routes_turns = jax.random.permutation(jax.random.fold_in(seeds[15], 3), GROUPS * GROUP_TOK // TOK_DEV)
    routes = jax.vmap(lambda own, number: shared_out(jax.random.fold_in(seeds[15], 2), own, number, TOK_DEV, EXPERTS, TOP, SLOT, 2))(routes_keys, routes_turns).reshape((GROUPS, GROUP_TOK, TOP))
    capacity = draw_capacity(jax.random.fold_in(seeds[17], 71), 0)
    return {"block_input": block_input, "cotangent": cotangent, "w_query": w_query, "w_key": w_key, "w_value": w_value, "w_output": w_output, "q_gain": q_gain, "k_gain": k_gain, "attn_gain": attn_gain, "mlp_gain": mlp_gain, "w_router": w_router, "w_gate": w_gate, "w_up": w_up, "w_down": w_down, "segments": segments, "routes": routes, "capacity": capacity}


@jax.custom_vjp
def low(v):
    return lax.optimization_barrier(v.astype(jnp.bfloat16)).astype(jnp.float32)

@jax.custom_vjp
def low_back(v):
    return v

def low_keep(v):
    return (low(v), None)

def low_pass(kept, grad):
    return (grad,)

def back_keep(v):
    return (v, None)

def back_low(kept, grad):
    return (low(grad),)
low.defvjp(low_keep, low_pass)
low_back.defvjp(back_keep, back_low)
epsilon = 1e-05
rope_base = 10000.0
precise = lax.Precision.HIGHEST

def matmul(left, right):
    return jnp.dot(left, right, precision=precise, preferred_element_type=jnp.float32)

def rms_normed(values):
    return values * lax.rsqrt(lax.optimization_barrier(jnp.mean(values * values, axis=-1, keepdims=True)) + epsilon)

def rope_tables(seg_ids, head_dim):
    length = seg_ids.shape[0]
    ordinal = lax.iota(jnp.int32, length)
    earlier = (seg_ids[:, None] == seg_ids[None, :]) & (ordinal[None, :] < ordinal[:, None])
    places = lax.optimization_barrier(jnp.sum(earlier.astype(jnp.int32), axis=1)).astype(jnp.float32)
    half_dim = head_dim // 2
    inv_freq = rope_base ** (-(lax.iota(jnp.int32, half_dim).astype(jnp.float32) * (2.0 / head_dim)))
    angles = places[:, None] * inv_freq[None, :]
    angles = jnp.concatenate([angles, angles], axis=1)
    return (jnp.cos(angles), jnp.sin(angles))

def rotate_half(values):
    half_dim = values.shape[-1] // 2
    return jnp.concatenate([-values[..., half_dim:], values[..., :half_dim]], axis=-1)

def apply_rope(values, cosine, sine_table):
    return values * cosine[:, None, :] + rotate_half(values) * sine_table[:, None, :]

def attend(pieces):
    q_heads, k_heads, v_heads, seg_ids = pieces
    length = seg_ids.shape[0]
    ordinal = lax.iota(jnp.int32, length)
    allowed = (seg_ids[:, None] == seg_ids[None, :]) & (ordinal[None, :] <= ordinal[:, None])
    scores = jnp.einsum('thd,shd->hts', q_heads, k_heads, precision=precise) * HEAD_DIM ** (-0.5)
    scores = low_back(scores)
    scores = jnp.where(allowed[None], scores, -1e+30)
    weights_attn = low(jax.nn.softmax(scores, axis=2))
    return jnp.einsum('hts,shd->thd', weights_attn, v_heads, precision=precise)

def seg_tables(seg_ids):
    return rope_tables(seg_ids, HEAD_DIM)

def reference(block_input, cotangent, w_query, w_key, w_value, w_output, q_gain, k_gain, attn_gain, mlp_gain, w_router, w_gate, w_up, w_down, segments, routes, capacity):
    tokens = GROUPS * GROUP_TOK
    blocks = tokens // TOK_DEV
    pair_count = TOK_DEV * TOP
    cosine, sine_table = jax.vmap(seg_tables)(segments)
    cosine = cosine.reshape(tokens, HEAD_DIM)
    sine_table = sine_table.reshape(tokens, HEAD_DIM)
    flat_routes = routes.reshape(tokens, TOP)
    per_block = routes.reshape(blocks, pair_count)
    chosen_hot = (per_block[:, :, None] == lax.iota(jnp.int32, EXPERTS)[None, None, :]).astype(jnp.int32)
    before = jnp.cumsum(chosen_hot, axis=1) - chosen_hot
    ranking = lax.optimization_barrier(jnp.sum(before * chosen_hot, axis=2))
    cap_pair = capacity[per_block]
    is_kept = ranking < cap_pair
    slot_rank = jnp.where(is_kept, ranking, SLOT).astype(jnp.int32)
    block_ids = jnp.broadcast_to(lax.iota(jnp.int32, blocks)[:, None], (blocks, pair_count))
    token_ids = block_ids * TOK_DEV + lax.iota(jnp.int32, pair_count)[None, :] // TOP
    slot_token = jnp.full((EXPERTS, blocks, SLOT), tokens, jnp.int32).at[per_block, block_ids, slot_rank].set(token_ids, mode='drop')
    shaped = (GROUPS, GROUP_TOK, HEADS, HEAD_DIM)

    def forward(flat_x, query_w, key_w, value_w, output_w, gain_q, gain_k, gain_a, gain_m, router_w, gate_w, up_w, down_w):
        first_rows = low(rms_normed(flat_x) * gain_a)
        query_rows = low_back(matmul(first_rows, query_w))
        key_rows = low_back(matmul(first_rows, key_w))
        values = low(low_back(matmul(first_rows, value_w)))
        q_heads = low(apply_rope((rms_normed(query_rows) * gain_q).reshape(tokens, HEADS, HEAD_DIM), cosine, sine_table))
        k_heads = low(apply_rope((rms_normed(key_rows) * gain_k).reshape(tokens, HEADS, HEAD_DIM), cosine, sine_table))
        mixed_heads = lax.map(jax.checkpoint(attend), (q_heads.reshape(shaped), k_heads.reshape(shaped), values.reshape(shaped), segments))
        attn_rows = low_back(low(mixed_heads.reshape(tokens, D)))
        second_in = flat_x + low_back(matmul(attn_rows, output_w))
        second_rows = low(rms_normed(second_in) * gain_m)
        logits = matmul(second_rows, router_w)
        routed = jnp.take_along_axis(logits, flat_routes, axis=1)
        gate_wts = jax.nn.softmax(routed, axis=1)
        slot_weight = jnp.zeros((EXPERTS, blocks, SLOT), jnp.float32).at[per_block, block_ids, slot_rank].add(gate_wts.reshape(blocks, pair_count), mode='drop')
        padded = jnp.concatenate([second_rows, jnp.zeros((1, D), jnp.float32)], axis=0)

        def expert_step(running, pieces):
            slot_ids, weight_slots, gate_e, up_e, down_e = pieces
            flat_ids = slot_ids.reshape(blocks * SLOT)
            rows_in = low_back(padded[flat_ids])
            gate_act = low_back(matmul(rows_in, gate_e))
            up_act = low_back(matmul(rows_in, up_e))
            hidden = low(jax.nn.silu(gate_act) * up_act)
            produced = low_back(low(matmul(hidden, down_e)))
            running = running.at[flat_ids].add(weight_slots.reshape(blocks * SLOT)[:, None] * produced)
            return (running, None)
        moe_rows, unused = lax.scan(expert_step, jnp.zeros((tokens + 1, D), jnp.float32), (slot_token, slot_weight, gate_w, up_w, down_w))
        return second_in + moe_rows[:tokens]
    result, pullback = jax.vjp(forward, block_input.reshape(tokens, D).astype(jnp.float32), w_query.astype(jnp.float32), w_key.astype(jnp.float32), w_value.astype(jnp.float32), w_output.astype(jnp.float32), q_gain, k_gain, attn_gain, mlp_gain, w_router.astype(jnp.float32), w_gate.astype(jnp.float32), w_up.astype(jnp.float32), w_down.astype(jnp.float32))
    gradients = pullback(cotangent.reshape(tokens, D).astype(jnp.float32))
    return (result.astype(jnp.bfloat16).reshape(GROUPS, GROUP_TOK, D), gradients[0].reshape(GROUPS, GROUP_TOK, D), gradients[1], gradients[2], gradients[3], gradients[4], gradients[5], gradients[6], gradients[7], gradients[8], gradients[9], gradients[10], gradients[11], gradients[12])
```

```python
import jax
import jax.numpy as jnp
from jax import lax
from jax.sharding import PartitionSpec as P

HEAD_DIM = 128
TOP = 8


epsilon = 1e-05
rope_base = 10000.0
precise = lax.Precision.HIGHEST


def rope_tables(seg_ids, head_dim):
    length = seg_ids.shape[0]
    ordinal = lax.iota(jnp.int32, length)
    earlier = (seg_ids[:, None] == seg_ids[None, :]) & (ordinal[None, :] < ordinal[:, None])
    places = jnp.sum(earlier.astype(jnp.int32), axis=1).astype(jnp.float32)
    half_dim = head_dim // 2
    inv_freq = rope_base ** (
        -(lax.iota(jnp.int32, half_dim).astype(jnp.float32) * (2.0 / head_dim))
    )
    angles = places[:, None] * inv_freq[None, :]
    angles = jnp.concatenate([angles, angles], axis=1)
    return (jnp.cos(angles), jnp.sin(angles))


def rotate_half(values):
    half_dim = values.shape[-1] // 2
    return jnp.concatenate([-values[..., half_dim:], values[..., :half_dim]], axis=-1)


def rotate_back(values):
    half_dim = values.shape[-1] // 2
    return jnp.concatenate([values[..., half_dim:], -values[..., :half_dim]], axis=-1)


def apply_rope(values, cosine, sine_table):
    return values * cosine[:, None, :] + rotate_half(values) * sine_table[:, None, :]


def rope_grad(grads_in, cosine, sine_table):
    return grads_in * cosine[:, None, :] + rotate_back(grads_in * sine_table[:, None, :])


def across_heads(pair_sums):
    return lax.psum((pair_sums[0], pair_sums[1]), "fsdp")


def share_rows(term_fn, own_rows):
    return lax.psum_scatter(
        term_fn(jnp.int32(0), own_rows * lax.axis_size("fsdp")),
        "fsdp",
        scatter_dimension=0,
        tiled=True,
    )


def to_owner(block_rows):
    return lax.all_to_all(block_rows, "expert", split_axis=0, concat_axis=0, tiled=True)


def from_owner(block_rows):
    return lax.all_to_all(block_rows, "expert", split_axis=0, concat_axis=0, tiled=True)


def shard_gather(block_rows):
    return lax.all_gather(block_rows, "fsdp", axis=0, tiled=True)


def owner_sum(term_fn, sources):
    own_rows = sources // lax.axis_size("fsdp")
    return lax.psum_scatter(
        term_fn(jnp.int32(0), own_rows * lax.axis_size("fsdp")),
        "fsdp",
        scatter_dimension=0,
        tiled=True,
    )


def head_scores(q_heads, k_heads, allowed):
    scores = jnp.einsum(
        "thd,shd->hts", q_heads, k_heads, preferred_element_type=jnp.float32
    ) * HEAD_DIM ** (-0.5)
    return jnp.where(allowed[None], scores, -1e30)


def experts_by_slot(
    second_in, second_rows, cotangent, routes, capacity, w_router, w_gate, w_up, w_down
):
    tok_count, model_width = second_rows.shape
    experts = w_router.shape[1]
    local_experts = w_gate.shape[0]
    slot_count = tok_count * TOP * 3 // (2 * experts)
    pair_count = tok_count * TOP
    zero_row = jnp.zeros((1, model_width), jnp.bfloat16)
    logits = jnp.dot(second_rows, w_router, preferred_element_type=jnp.float32)
    chosen = routes
    expert_ids = lax.iota(jnp.int32, experts)
    chosen_hot = (chosen[:, :, None] == expert_ids[None, None, :]).astype(jnp.float32)
    routed = jnp.sum(chosen_hot * logits[:, None, :], axis=2)
    gate_wts = jax.nn.softmax(routed, axis=1)
    pair_hot = chosen_hot.reshape(pair_count, experts).astype(jnp.int32)
    earlier_hits = jnp.cumsum(pair_hot, axis=0) - pair_hot
    ranking = jnp.sum(earlier_hits * pair_hot, axis=1)
    cap_pair = jnp.sum(pair_hot * capacity[None, :], axis=1)
    is_kept = ranking < cap_pair
    pair_route = chosen.reshape(pair_count)
    slot_place = jnp.where(is_kept, pair_route * slot_count + ranking, experts * slot_count)
    pair_ids = lax.iota(jnp.int32, pair_count)
    slot_pair = (
        jnp.full((experts * slot_count,), pair_count, jnp.int32)
        .at[slot_place]
        .set(pair_ids, mode="drop")
    )
    padded = jnp.concatenate([second_rows, zero_row], axis=0)
    outgoing = padded[slot_pair // TOP].reshape(experts, slot_count, model_width)
    arrived = shard_gather(to_owner(outgoing))
    gate_w, up_w, down_w = (w_gate, w_up, w_down)
    owner_rows = arrived.reshape(-1, local_experts, slot_count, model_width)
    sources = owner_rows.shape[0]
    gate_act = jnp.einsum("sjcd,jdh->sjch", owner_rows, gate_w, preferred_element_type=jnp.float32)
    up_act = jnp.einsum("sjcd,jdh->sjch", owner_rows, up_w, preferred_element_type=jnp.float32)
    sig_gate = jax.nn.sigmoid(gate_act)
    silu_gate = gate_act * sig_gate
    hidden = (silu_gate * up_act).astype(jnp.bfloat16)

    def down_term(start, length):
        return jnp.einsum("sjch,jhd->sjcd", hidden, down_w, preferred_element_type=jnp.float32)

    produced = owner_sum(down_term, sources)
    returned = from_owner(produced.astype(jnp.bfloat16).reshape(-1, slot_count, model_width))
    slot_rows = jnp.concatenate(
        [returned.reshape(experts * slot_count, model_width), zero_row], axis=0
    )
    pair_rows = slot_rows[slot_place].reshape(tok_count, TOP, model_width).astype(jnp.float32)
    kept_mask = is_kept.reshape(tok_count, TOP).astype(jnp.float32)
    gate_kept = gate_wts * kept_mask
    moe_rows = jnp.sum(gate_kept[:, :, None] * pair_rows, axis=1)
    final_rows = second_in + moe_rows
    block_output = final_rows.astype(jnp.bfloat16)
    grad_out = cotangent.astype(jnp.float32)
    grad_gate_k = jnp.sum(pair_rows * grad_out[:, None, :], axis=2) * kept_mask
    grad_routed = gate_wts * (grad_gate_k - jnp.sum(gate_wts * grad_gate_k, axis=1, keepdims=True))
    grad_logits = jnp.sum(chosen_hot * grad_routed[:, :, None], axis=1)
    router_grad = jnp.dot(second_rows.astype(jnp.float32).T, grad_logits, precision=precise)
    grad_second = jnp.dot(grad_logits, w_router.astype(jnp.float32).T, precision=precise)
    pair_grads = (
        (gate_kept[:, :, None] * grad_out[:, None, :])
        .astype(jnp.bfloat16)
        .reshape(pair_count, model_width)
    )
    pair_grads = jnp.concatenate([pair_grads, zero_row], axis=0)
    slot_grads = pair_grads[slot_pair].reshape(experts, slot_count, model_width)
    grad_blocks = shard_gather(to_owner(slot_grads)).reshape(
        -1, local_experts, slot_count, model_width
    )
    grad_hidden = jnp.einsum(
        "sjcd,jhd->sjch", grad_blocks, down_w, preferred_element_type=jnp.float32
    )
    grad_down_w = jnp.einsum(
        "sjch,sjcd->jhd", hidden, grad_blocks, preferred_element_type=jnp.float32
    )
    grad_gate_in = (grad_hidden * up_act * sig_gate * (1.0 + gate_act * (1.0 - sig_gate))).astype(
        jnp.bfloat16
    )
    grad_up_in = (grad_hidden * silu_gate).astype(jnp.bfloat16)
    grad_gate_w = jnp.einsum(
        "sjcd,sjch->jdh", owner_rows, grad_gate_in, preferred_element_type=jnp.float32
    )
    grad_up_w = jnp.einsum(
        "sjcd,sjch->jdh", owner_rows, grad_up_in, preferred_element_type=jnp.float32
    )

    def back_term(start, length):
        from_gate = jnp.einsum(
            "sjch,jdh->sjcd", grad_gate_in, gate_w, preferred_element_type=jnp.float32
        )
        from_up = jnp.einsum("sjch,jdh->sjcd", grad_up_in, up_w, preferred_element_type=jnp.float32)
        return from_gate + from_up

    grad_slots = from_owner(
        owner_sum(back_term, sources).astype(jnp.bfloat16).reshape(-1, slot_count, model_width)
    )
    back_rows = jnp.concatenate(
        [grad_slots.reshape(experts * slot_count, model_width), zero_row], axis=0
    )
    grad_second = grad_second + jnp.sum(
        back_rows[slot_place].reshape(tok_count, TOP, model_width).astype(jnp.float32), axis=1
    )
    return block_output[None], grad_second, router_grad.T, (grad_gate_w, grad_up_w, grad_down_w)


def experts_dense(
    second_in, second_rows, cotangent, routes, capacity, w_router, w_gate, w_up, w_down
):
    tok_count = second_rows.shape[0]
    experts = w_router.shape[1]
    local_experts, model_width, hidden_here = w_gate.shape
    shards = lax.axis_size("fsdp")
    owners = lax.axis_size("expert")
    wide = local_experts * hidden_here
    logits = jnp.dot(second_rows, w_router, preferred_element_type=jnp.float32)
    expert_ids = lax.iota(jnp.int32, experts)
    named = jnp.any(routes[:, :, None] == expert_ids[None, None, :], axis=1)
    before = lax.iota(jnp.int32, tok_count)[None, :] < lax.iota(jnp.int32, tok_count)[:, None]
    ranking = jnp.dot(
        before.astype(jnp.bfloat16), named.astype(jnp.bfloat16), preferred_element_type=jnp.float32
    )
    kept = named & (ranking < capacity.astype(jnp.float32)[None, :])
    kept_mask = kept.astype(jnp.float32)
    top_logit = jnp.max(jnp.where(named, logits, -jnp.inf), axis=1, keepdims=True)
    powers = jnp.where(named, jnp.exp(jnp.where(named, logits - top_logit, 0.0)), 0.0)
    gate_wts = powers / jnp.sum(powers, axis=1, keepdims=True)
    gate_kept = gate_wts * kept_mask

    grad_all = lax.all_gather(cotangent, ("fsdp", "expert"), axis=0, tiled=True)
    rows_all = lax.all_gather(second_rows, ("fsdp", "expert"), axis=0, tiled=True)
    kept_all = lax.all_gather(gate_kept, ("fsdp", "expert"), axis=0, tiled=True)
    first_expert = lax.axis_index("expert") * local_experts
    gate_here = lax.dynamic_slice_in_dim(kept_all, first_expert, local_experts, axis=1)
    gate_cols = jnp.repeat(gate_here, hidden_here, axis=1)
    tokens = rows_all.shape[0]

    gate_w = jnp.transpose(w_gate, (1, 0, 2)).reshape(model_width, wide)
    up_w = jnp.transpose(w_up, (1, 0, 2)).reshape(model_width, wide)
    down_w = w_down.reshape(wide, model_width)
    grad_hid = jnp.einsum("td,hd->th", grad_all, down_w, preferred_element_type=jnp.float32)
    gate_act = jnp.dot(rows_all, gate_w, preferred_element_type=jnp.float32)
    up_act = jnp.dot(rows_all, up_w, preferred_element_type=jnp.float32)
    sig_gate = jax.nn.sigmoid(gate_act)
    silu_gate = gate_act * sig_gate
    hidden = silu_gate * up_act
    gate_terms = jnp.sum((hidden * grad_hid).reshape(tokens, local_experts, hidden_here), axis=2)
    weighted = (hidden * gate_cols).astype(jnp.bfloat16)
    grad_hid = grad_hid * gate_cols
    grad_gate_in = (grad_hid * up_act * sig_gate * (1.0 + gate_act * (1.0 - sig_gate))).astype(
        jnp.bfloat16
    )
    grad_up_in = (grad_hid * silu_gate).astype(jnp.bfloat16)
    back = (
        jnp.einsum("th,dh->td", grad_gate_in, gate_w, preferred_element_type=jnp.float32)
        + jnp.einsum("th,dh->td", grad_up_in, up_w, preferred_element_type=jnp.float32)
    ).astype(jnp.bfloat16)
    back_rows = lax.psum_scatter(back, "fsdp", scatter_dimension=0, tiled=True)
    back_rows = lax.psum_scatter(back_rows, "expert", scatter_dimension=0, tiled=True)
    terms = lax.psum_scatter(
        gate_terms.reshape(shards, owners * tok_count, local_experts), "fsdp", scatter_dimension=0, tiled=True
    ).reshape(owners, tok_count, local_experts)
    terms = lax.all_to_all(terms, "expert", split_axis=0, concat_axis=0, tiled=True)
    grad_gate_k = jnp.transpose(terms, (1, 0, 2)).reshape(tok_count, experts) * kept_mask
    forward = jnp.dot(weighted, down_w, preferred_element_type=jnp.float32).astype(jnp.bfloat16)
    forward_rows = lax.psum_scatter(forward, "fsdp", scatter_dimension=0, tiled=True)
    forward_rows = lax.psum_scatter(forward_rows, "expert", scatter_dimension=0, tiled=True)
    block_output = (second_in + forward_rows.astype(jnp.float32)).astype(jnp.bfloat16)[None]
    grad_logits = gate_wts * (grad_gate_k - jnp.sum(gate_wts * grad_gate_k, axis=1, keepdims=True))
    router_grad = jnp.dot(grad_logits.T, second_rows.astype(jnp.float32), precision=precise)
    grad_second = jnp.dot(grad_logits, w_router.astype(jnp.float32).T, precision=precise)
    grad_second = grad_second + back_rows.astype(jnp.float32)

    def by_expert(left, right):
        return jnp.dot(left.T, right, preferred_element_type=jnp.float32)

    parts = [slice(j * hidden_here, (j + 1) * hidden_here) for j in range(local_experts)]
    grad_gate_w = jnp.stack([by_expert(rows_all, grad_gate_in[:, p]) for p in parts])
    grad_up_w = jnp.stack([by_expert(rows_all, grad_up_in[:, p]) for p in parts])
    grad_down_w = by_expert(weighted, grad_all).reshape(local_experts, hidden_here, model_width)
    return block_output, grad_second, router_grad, (grad_gate_w, grad_up_w, grad_down_w)


def on_device(
    block_input,
    cotangent,
    w_query,
    w_key,
    w_value,
    w_output,
    q_gain,
    k_gain,
    attn_gain,
    mlp_gain,
    w_router,
    w_gate,
    w_up,
    w_down,
    segments,
    routes,
    capacity,
):
    tok_count = block_input.shape[1]
    model_width = block_input.shape[2]
    flat_in = block_input[0].astype(jnp.float32)
    scale_one = lax.rsqrt(jnp.mean(flat_in * flat_in, axis=1, keepdims=True) + epsilon)
    normed_one = flat_in * scale_one
    first_rows = (normed_one * attn_gain).astype(jnp.bfloat16)
    group_rows, group_segs = (
        lax.all_gather(first_rows, "fsdp", axis=0, tiled=True),
        lax.all_gather(segments[0], "fsdp", axis=0, tiled=True),
    )
    group_len = group_rows.shape[0]
    heads_here = w_query.shape[1] // HEAD_DIM
    query_rows = jnp.dot(group_rows, w_query, preferred_element_type=jnp.float32)
    key_rows = jnp.dot(group_rows, w_key, preferred_element_type=jnp.float32)
    value_rows = jnp.dot(group_rows, w_value, preferred_element_type=jnp.float32).astype(
        jnp.bfloat16
    )
    square_sums = across_heads(
        (jnp.sum(query_rows * query_rows, axis=1), jnp.sum(key_rows * key_rows, axis=1))
    )
    q_scale = lax.rsqrt(square_sums[0][:, None] / model_width + epsilon)
    k_scale = lax.rsqrt(square_sums[1][:, None] / model_width + epsilon)
    cosine, sine_table = rope_tables(group_segs, HEAD_DIM)
    head_shape = (group_len, heads_here, HEAD_DIM)
    q_heads = apply_rope(
        (query_rows * q_scale * q_gain).reshape(head_shape), cosine, sine_table
    ).astype(jnp.bfloat16)
    k_heads = apply_rope(
        (key_rows * k_scale * k_gain).reshape(head_shape), cosine, sine_table
    ).astype(jnp.bfloat16)
    v_heads = value_rows.reshape(head_shape)
    ordinal = lax.iota(jnp.int32, group_len)
    allowed = (group_segs[:, None] == group_segs[None, :]) & (ordinal[None, :] <= ordinal[:, None])
    scores = head_scores(q_heads, k_heads, allowed)
    row_top = jnp.max(scores, axis=2, keepdims=True)
    log_total = row_top + jnp.log(jnp.sum(jnp.exp(scores - row_top), axis=2, keepdims=True))
    attn_weights = jnp.exp(scores - log_total)
    mixed_heads = jnp.einsum(
        "hts,shd->thd",
        attn_weights.astype(jnp.bfloat16),
        v_heads,
        preferred_element_type=jnp.float32,
    )
    attn_rows = mixed_heads.reshape(group_len, heads_here * HEAD_DIM).astype(jnp.bfloat16)

    def mixed_term(start, length):
        return jnp.dot(attn_rows, w_output, preferred_element_type=jnp.float32).astype(jnp.bfloat16)

    mixed_rows = share_rows(mixed_term, tok_count).astype(jnp.float32)
    second_in = flat_in + mixed_rows
    scale_two = lax.rsqrt(jnp.mean(second_in * second_in, axis=1, keepdims=True) + epsilon)
    normed_two = second_in * scale_two
    second_rows = (normed_two * mlp_gain).astype(jnp.bfloat16)
    experts = w_router.shape[1]
    if TOP * 2 >= experts:
        block_output, grad_second, router_grad, expert_grads = experts_dense(
            second_in, second_rows, cotangent[0], routes[0], capacity, w_router, w_gate, w_up, w_down
        )
    else:
        block_output, grad_second, router_grad, expert_grads = experts_by_slot(
            second_in, second_rows, cotangent[0], routes[0], capacity, w_router, w_gate, w_up, w_down
        )
    grad_gate_w, grad_up_w, grad_down_w = expert_grads
    grad_out = cotangent[0].astype(jnp.float32)
    mlp_gain_grad = jnp.sum(grad_second * normed_two, axis=0)
    grad_normed_two = grad_second * mlp_gain
    grad_mid = grad_out + scale_two * (
        grad_normed_two - normed_two * jnp.mean(grad_normed_two * normed_two, axis=1, keepdims=True)
    )
    group_grad = lax.all_gather(grad_mid.astype(jnp.bfloat16), "fsdp", axis=0, tiled=True)
    out_grad = jnp.einsum("ti,td->id", attn_rows, group_grad, preferred_element_type=jnp.float32)
    grad_attn = (
        jnp.einsum("td,id->ti", group_grad, w_output, preferred_element_type=jnp.float32)
        .astype(jnp.bfloat16)
        .reshape(head_shape)
    )
    scores_again = head_scores(q_heads, k_heads, allowed)
    weights_again = jnp.exp(scores_again - log_total)
    grad_values = jnp.einsum(
        "hts,thd->shd",
        weights_again.astype(jnp.bfloat16),
        grad_attn,
        preferred_element_type=jnp.float32,
    )
    grad_weights = jnp.einsum(
        "thd,shd->hts", grad_attn, v_heads, preferred_element_type=jnp.float32
    )
    inner_sum = jnp.sum(weights_again * grad_weights, axis=2, keepdims=True)
    grad_scores = (weights_again * (grad_weights - inner_sum)).astype(jnp.bfloat16)
    grad_q_heads = jnp.einsum(
        "hts,shd->thd", grad_scores, k_heads, preferred_element_type=jnp.float32
    ) * HEAD_DIM ** (-0.5)
    grad_k_heads = jnp.einsum(
        "hts,thd->shd", grad_scores, q_heads, preferred_element_type=jnp.float32
    ) * HEAD_DIM ** (-0.5)
    grad_q_normed = rope_grad(grad_q_heads, cosine, sine_table).reshape(group_len, -1)
    grad_k_normed = rope_grad(grad_k_heads, cosine, sine_table).reshape(group_len, -1)
    q_gain_grad = jnp.sum(grad_q_normed * query_rows * q_scale, axis=0)
    k_gain_grad = jnp.sum(grad_k_normed * key_rows * k_scale, axis=0)
    inner_q = grad_q_normed * q_gain
    inner_k = grad_k_normed * k_gain
    inner_sums = across_heads(
        (jnp.sum(inner_q * query_rows, axis=1), jnp.sum(inner_k * key_rows, axis=1))
    )
    grad_query_rows = (
        q_scale
        * (inner_q - query_rows * q_scale * q_scale * (inner_sums[0][:, None] / model_width))
    ).astype(jnp.bfloat16)
    grad_key_rows = (
        k_scale * (inner_k - key_rows * k_scale * k_scale * (inner_sums[1][:, None] / model_width))
    ).astype(jnp.bfloat16)
    grad_value_rows = grad_values.reshape(group_len, -1).astype(jnp.bfloat16)
    query_grad = jnp.einsum(
        "td,ti->di", group_rows, grad_query_rows, preferred_element_type=jnp.float32
    )
    key_grad = jnp.einsum(
        "td,ti->di", group_rows, grad_key_rows, preferred_element_type=jnp.float32
    )
    value_grad = jnp.einsum(
        "td,ti->di", group_rows, grad_value_rows, preferred_element_type=jnp.float32
    )

    def input_term(start, length):
        from_q = jnp.einsum(
            "ti,di->td", grad_query_rows, w_query, preferred_element_type=jnp.float32
        )
        from_k = jnp.einsum("ti,di->td", grad_key_rows, w_key, preferred_element_type=jnp.float32)
        from_v = jnp.einsum(
            "ti,di->td", grad_value_rows, w_value, preferred_element_type=jnp.float32
        )
        return (from_q + from_k + from_v).astype(jnp.bfloat16)

    grad_first = share_rows(input_term, tok_count).astype(jnp.float32)
    attn_gain_grad = jnp.sum(grad_first * normed_one, axis=0)
    grad_normed_one = grad_first * attn_gain
    grad_x = grad_mid + scale_one * (
        grad_normed_one - normed_one * jnp.mean(grad_normed_one * normed_one, axis=1, keepdims=True)
    )
    narrow = tuple(g.astype(jnp.bfloat16) for g in (query_grad, key_grad, value_grad, out_grad))
    mixer = tuple(g.astype(jnp.float32) for g in lax.psum(narrow, "expert"))
    mixer = mixer + lax.psum((q_gain_grad, k_gain_grad), "expert")
    shared = lax.psum(
        jnp.concatenate([attn_gain_grad[None], mlp_gain_grad[None], router_grad], axis=0),
        ("fsdp", "expert"),
    )
    return (
        block_output,
        grad_x[None],
        mixer[0],
        mixer[1],
        mixer[2],
        mixer[3],
        mixer[4],
        mixer[5],
        shared[0],
        shared[1],
        shared[2:].T,
        grad_gate_w,
        grad_up_w,
        grad_down_w,
    )


def solution(mesh):
    placed = (
        P("expert", "fsdp", None),
        P("expert", "fsdp", None),
        P(None, "fsdp"),
        P(None, "fsdp"),
        P(None, "fsdp"),
        P("fsdp", None),
        P("fsdp"),
        P("fsdp"),
        P(),
        P(),
        P(),
        P("expert", None, "fsdp"),
        P("expert", None, "fsdp"),
        P("expert", "fsdp", None),
        P("expert", "fsdp"),
        P("expert", "fsdp", None),
        P(),
    )
    return jax.shard_map(
        on_device,
        mesh=mesh,
        in_specs=placed,
        out_specs=(
            P("expert", "fsdp", None),
            P("expert", "fsdp", None),
            P(None, "fsdp"),
            P(None, "fsdp"),
            P(None, "fsdp"),
            P("fsdp", None),
            P("fsdp"),
            P("fsdp"),
            P(),
            P(),
            P(),
            P("expert", None, "fsdp"),
            P("expert", None, "fsdp"),
            P("expert", "fsdp", None),
        ),
        check_vma=False,
    )
```

```python
import functools

import jax
import jax.numpy as jnp
from jax import lax
from jax.experimental import pallas as pl
from jax.experimental.pallas import tpu as pltpu
from jax.sharding import PartitionSpec as P

HEAD_DIM = 128
TOP = 8


epsilon = 1e-05
rope_base = 10000.0
precise = lax.Precision.HIGHEST


MESH = pl.DeviceIdType.MESH
DMA = pltpu.SemaphoreType.DMA


class Place:
    def __init__(self):
        self.f, self.e = lax.axis_index("fsdp"), lax.axis_index("expert")
        self.c, self.z = self.e % 2, self.e // 2
        self.fx = self.f + 1 - 2 * (self.f % 2)
        self.fy = (self.f + 2) % 4
        self.fd = 3 - self.f
        self.pe = self.e + 1 - 2 * self.c


def send(src, dst, send_sem, recv_sem, f, e):
    return pltpu.make_async_remote_copy(
        src_ref=src,
        dst_ref=dst,
        send_sem=send_sem,
        recv_sem=recv_sem,
        device_id={"fsdp": f, "expert": e},
        device_id_type=MESH,
    )


def greet(peers, line=None):
    barrier = pltpu.get_barrier_semaphore()

    def hello(f, e):
        pl.semaphore_signal(
            barrier, inc=1, device_id={"fsdp": f, "expert": e}, device_id_type=MESH
        )

    for f, e in peers:
        hello(f, e)
    if line is not None:
        at, nz = line
        for step in range(1, nz):
            hello(at.f, 2 * ((at.z + step) % nz) + at.c)
        pl.semaphore_wait(barrier, len(peers) + nz - 1)
    else:
        pl.semaphore_wait(barrier, len(peers))


class SmallGather:
    sems = staticmethod(
        lambda nz: [DMA((nz,)), DMA((nz,)), DMA((4,)), DMA((4,))]
    )

    def __init__(self, at, nz, own, out, sems):
        self.at, self.nz, self.own, self.out = at, nz, own, out
        self.ls, self.lr, self.ss, self.sr = sems

    def line(self, step):
        at = self.at
        z = (at.z + step) % self.nz
        back = (at.z + self.nz - step) % self.nz
        slot = self.out.at[at.c, at.f]
        to = send(self.own, slot.at[at.z], self.ls.at[step], self.lr.at[step], at.f, 2 * z + at.c)
        come = send(self.own, slot.at[back], self.ls.at[step], self.lr.at[step], at.f, 2 * z + at.c)
        return to, come

    def plane(self, i):
        at, out = self.at, self.out
        f, to_f = ((at.f, at.fx), (at.f, at.fy), (at.fx, at.fy))[i]
        slot = out.at[at.c, f]
        return send(slot, slot, self.ss.at[i], self.sr.at[i], to_f, at.e)

    def pair(self):
        at = self.at
        slot = self.out.at[at.c]
        return send(slot, slot, self.ss.at[3], self.sr.at[3], at.f, at.pe)

    def stage(self, i):
        at = self.at
        if i == 0:
            for step in range(1, self.nz):
                self.line(step)[0].start()
            self.out[at.c, at.f, at.z] = self.own[...]
        elif i == 1:
            for step in range(1, self.nz):
                self.line(step)[1].wait_recv()
            self.plane(0).start()
            self.plane(1).start()
        elif i == 2:
            self.plane(0).wait_recv()
            self.plane(2).start()
        elif i == 3:
            self.plane(1).wait_recv()
            self.plane(2).wait_recv()
            self.pair().start()
        elif i == 4:
            self.pair().wait_recv()
            self.pair().wait_send()
            for step in range(1, self.nz):
                self.line(step)[0].wait_send()
            for k in range(3):
                self.plane(k).wait_send()


class SmallScatter:
    sems = staticmethod(lambda nz: [DMA((nz,)), DMA((nz,)), DMA((4,)), DMA((4,))])
    scratch = staticmethod(
        lambda nz, shape: [
            pltpu.VMEM((4, nz, *shape), jnp.float32),
            pltpu.VMEM((4, nz, *shape), jnp.float32),
            pltpu.VMEM((3, nz, *shape), jnp.float32),
            pltpu.VMEM((nz, *shape), jnp.float32),
        ]
    )

    def __init__(self, at, nz, part, out, scratch, sems):
        self.at, self.nz, self.part, self.out = at, nz, part, out
        self.acc, self.pb, self.xy, self.zb = scratch
        self.ls, self.lr, self.ss, self.sr = sems

    def pair(self):
        at = self.at
        return send(
            self.part.at[1 - at.c], self.pb, self.ss.at[0], self.sr.at[0], at.f, at.pe
        )

    def plane(self, i):
        at = self.at
        f, to_f = ((at.fx, at.fx), (at.fd, at.fx), (at.fy, at.fy))[i]
        return send(
            self.acc.at[f], self.xy.at[i], self.ss.at[1 + i], self.sr.at[1 + i], to_f, at.e
        )

    def line(self, step):
        at = self.at
        z = (at.z + step) % self.nz
        return send(
            self.acc.at[at.f, z], self.zb.at[step], self.ls.at[step], self.lr.at[step], at.f, 2 * z + at.c
        )

    def stage(self, i):
        at, acc, xy = self.at, self.acc, self.xy
        if i == 0:
            self.pair().start()
        elif i == 1:
            self.pair().wait_recv()
            acc[...] = self.part[at.c] + self.pb[...]
            self.plane(0).start()
            self.plane(1).start()
        elif i == 2:
            self.plane(0).wait_recv()
            self.plane(1).wait_recv()
            acc[at.fy] = acc[at.fy] + xy[1]
            self.plane(2).start()
            acc[at.f] = acc[at.f] + xy[0]
        elif i == 3:
            self.plane(2).wait_recv()
            acc[at.f] = acc[at.f] + xy[2]
            for step in range(1, self.nz):
                self.line(step).start()
        elif i == 4:
            total = acc[at.f, at.z]
            for step in range(1, self.nz):
                self.line(step).wait_recv()
                total = total + self.zb[step]
            self.out[...] = total
            self.pair().wait_send()
            for k in range(3):
                self.plane(k).wait_send()
            for step in range(1, self.nz):
                self.line(step).wait_send()


def take(sequence, count):
    return [next(sequence) for _ in range(count)]


def gather_kernel(nz, own, own_small, out, out_small, own_sem, zr, zs, xr, xs, yr, ys, dr, xf, yf, pr, ps, *small_sems):
    at = Place()
    half = own.shape[0] // 2
    halves = (pl.ds(0, half), pl.ds(half, half))
    small = SmallGather(at, nz, own_small, out_small, small_sems)
    greet([(at.fx, at.e), (at.fy, at.e), (at.f, at.pe)], (at, nz))
    keep = pltpu.make_async_copy(own, out.at[at.f, at.e], own_sem)
    keep.start()
    small.stage(0)

    def up(z, slot):
        return send(slot, slot, zs.at[0, z], zr.at[z], at.f, at.e + 2)

    def down(z, slot):
        return send(slot, slot, zs.at[1, z], zr.at[z], at.f, at.e - 2)

    def to_x(z, h):
        ref = out.at[at.f, 2 * z + at.c, halves[h]]
        return send(ref, ref, xs.at[h, z], xr.at[h, z], at.fx, at.e)

    def to_y(z, h):
        ref = out.at[at.f, 2 * z + at.c, halves[h]]
        return send(ref, ref, ys.at[h, z], yr.at[h, z], at.fy, at.e)

    def x_on(z):
        ref = out.at[at.fx, 2 * z + at.c, halves[0]]
        return send(ref, ref, yf.at[z], dr.at[0, z], at.fy, at.e)

    def y_on(z):
        ref = out.at[at.fy, 2 * z + at.c, halves[1]]
        return send(ref, ref, xf.at[z], dr.at[1, z], at.fx, at.e)

    def to_p(f, z, h):
        ref = out.at[f, 2 * z + at.c, halves[h]]
        return send(ref, ref, ps.at[f, z, h], pr.at[f, z, h], at.f, at.pe)

    def order(i):
        return at.z + (i + 1) // 2 * (1 - 2 * (i % 2))

    def on_line(i, run):
        z = order(i)
        pl.when((z >= 0) & (z < nz))(lambda: run(z))

    def line_step(z):
        slot = out.at[at.f, 2 * z + at.c]

        @pl.when(z != at.z)
        def _():
            up(z, slot).wait_recv()

        @pl.when((z <= at.z) & (at.z < nz - 1))
        def _():
            up(z, slot).start()

        @pl.when((z >= at.z) & (at.z > 0))
        def _():
            down(z, slot).start()

        to_x(z, 0).start()
        to_y(z, 1).start()
        to_x(z, 1).start()
        to_y(z, 0).start()
        for h in range(2):
            to_p(at.f, z, h).start()

    def plane_step(z):
        to_x(z, 0).wait_recv()
        x_on(z).start()
        to_y(z, 1).wait_recv()
        y_on(z).start()
        to_p(at.fx, z, 0).start()
        to_p(at.fy, z, 1).start()
        to_x(z, 1).wait_recv()
        to_p(at.fx, z, 1).start()
        to_y(z, 0).wait_recv()
        to_p(at.fy, z, 0).start()

    def diag_step(z):
        x_on(z).wait_recv()
        to_p(at.fd, z, 0).start()
        y_on(z).wait_recv()
        to_p(at.fd, z, 1).start()

    keep.wait()
    steps = 2 * nz - 1

    def body(i, carry):
        pl.when(i < steps)(lambda: on_line(i, line_step))
        pl.when((i >= 1) & (i < steps + 1))(lambda: on_line(i - 1, plane_step))
        pl.when(i >= 2)(lambda: on_line(i - 2, diag_step))
        for k in range(1, 5):
            pl.when(i == k)(functools.partial(small.stage, k))
        return carry

    lax.fori_loop(0, steps + 2, body, 0)

    def finish(z, carry):
        slot = out.at[at.f, 2 * z + at.c]

        @pl.when((z <= at.z) & (at.z < nz - 1))
        def _():
            up(z, slot).wait_send()

        @pl.when((z >= at.z) & (at.z > 0))
        def _():
            down(z, slot).wait_send()

        for h in range(2):
            to_x(z, h).wait_send()
            to_y(z, h).wait_send()
        x_on(z).wait_send()
        y_on(z).wait_send()
        for f in range(4):
            for h in range(2):
                to_p(f, z, h).wait_send()
                to_p(f, z, h).wait_recv()
        return carry

    lax.fori_loop(0, nz, finish, 0)


def gather_all(rows, small, nz, cid):
    r, c = rows.shape
    return pl.pallas_call(
        functools.partial(gather_kernel, nz),
        out_shape=(
            jax.ShapeDtypeStruct((4, 2 * nz, r, c), rows.dtype),
            jax.ShapeDtypeStruct((2, 4, nz, *small.shape), jnp.float32),
        ),
        in_specs=[pl.BlockSpec(memory_space=pltpu.VMEM)] * 2,
        out_specs=(pl.BlockSpec(memory_space=pl.ANY), pl.BlockSpec(memory_space=pltpu.VMEM)),
        scratch_shapes=[
            DMA(()), DMA((nz,)), DMA((2, nz)), DMA((2, nz)), DMA((2, nz)), DMA((2, nz)), DMA((2, nz)),
            DMA((2, nz)), DMA((nz,)), DMA((nz,)), DMA((4, nz, 2)), DMA((4, nz, 2)),
            *SmallGather.sems(nz),
        ],
        compiler_params=pltpu.CompilerParams(collective_id=cid, has_side_effects=True),
        cost_estimate=pl.CostEstimate(flops=0, bytes_accessed=240 << 20, transcendentals=0),
        name="gather_all",
    )(rows, small)


def add_rows(dst, dst_rows, parts):
    start, count = dst_rows

    def body(i, carry):
        r = pl.multiple_of(i * 16, 16)
        total = None
        for ref, offset in parts:
            piece = ref[pl.ds(offset + r, 16), :].astype(jnp.float32)
            total = piece if total is None else total + piece
        dst[pl.ds(start + r, 16), :] = total.astype(dst.dtype)
        return carry

    lax.fori_loop(0, count // 16, body, 0)


def scatter_kernel(nz, part, part_small, out, out_small, acc, pb, xh, yh, xf, yf, zu, zd, ls, pr, ps, xhs, xhr, yhs, yhr, xs, xr, ys, yr, us, ur, ds_, dr, *small_refs):
    at = Place()
    rows = out.shape[0]
    half = rows // 2
    lo, hi = pl.ds(0, half), pl.ds(half, half)
    small = SmallScatter(at, nz, part_small, out_small, small_refs[:4], small_refs[4:])
    greet([(at.fx, at.e), (at.fy, at.e), (at.f, at.pe)], (at, nz))
    steps = 2 * nz - 1
    small.stage(0)

    def order(i):
        return at.z + (nz - 1 - i // 2) * (2 * (i % 2) - 1)

    def on_line(i, run):
        z = order(i)
        pl.when((z >= 0) & (z < nz))(lambda: run(z))

    def load(f, z):
        return pltpu.make_async_copy(part.at[f, 2 * z + at.c], acc.at[f, z], ls.at[f, z])

    def to_p(f, z):
        return send(part.at[f, 2 * z + 1 - at.c], pb.at[f, z], ps.at[f, z], pr.at[f, z], at.f, at.pe)

    def start_step(z):
        for f in (at.fd, at.fx, at.fy, at.f):
            load(f, z).start()
            to_p(f, z).start()

    def start(i, carry):
        on_line(i, start_step)
        return carry

    lax.fori_loop(0, steps, start, 0)

    def half_x(z):
        return send(acc.at[at.fd, z, lo], xh.at[z], xhs.at[z], xhr.at[z], at.fx, at.e)

    def half_y(z):
        return send(acc.at[at.fd, z, hi], yh.at[z], yhs.at[z], yhr.at[z], at.fy, at.e)

    def full_x(z):
        return send(acc.at[at.fx, z], xf.at[z], xs.at[z], xr.at[z], at.fx, at.e)

    def full_y(z):
        return send(acc.at[at.fy, z], yf.at[z], ys.at[z], yr.at[z], at.fy, at.e)

    def go_up(z):
        return send(acc.at[at.f, z], zu.at[z], us.at[z], ur.at[z], at.f, at.e + 2)

    def go_down(z):
        return send(acc.at[at.f, z], zd.at[z], ds_.at[z], dr.at[z], at.f, at.e - 2)

    def diag_step(z):
        load(at.fd, z).wait()
        to_p(at.fd, z).wait_recv()
        a, b = acc.at[at.fd, z], pb.at[at.fd, z]
        add_rows(a, (0, half), [(a, 0), (b, 0)])
        half_x(z).start()
        add_rows(a, (half, half), [(a, half), (b, half)])
        half_y(z).start()

    def plane_step(z):
        load(at.fx, z).wait()
        to_p(at.fx, z).wait_recv()
        a, b = acc.at[at.fx, z], pb.at[at.fx, z]
        half_y(z).wait_recv()
        add_rows(a, (0, half), [(a, 0), (b, 0)])
        add_rows(a, (half, half), [(a, half), (b, half), (yh.at[z], 0)])
        full_x(z).start()
        load(at.fy, z).wait()
        to_p(at.fy, z).wait_recv()
        half_x(z).wait_recv()
        a, b = acc.at[at.fy, z], pb.at[at.fy, z]
        add_rows(a, (0, half), [(a, 0), (b, 0), (xh.at[z], 0)])
        add_rows(a, (half, half), [(a, half), (b, half)])
        full_y(z).start()

    def line_step(z):
        load(at.f, z).wait()
        to_p(at.f, z).wait_recv()
        full_x(z).wait_recv()
        full_y(z).wait_recv()
        a = acc.at[at.f, z]
        four = [(a, 0), (pb.at[at.f, z], 0), (xf.at[z], 0), (yf.at[z], 0)]

        @pl.when(z > at.z)
        def _():
            @pl.when(at.z > 0)
            def _():
                go_up(z).wait_recv()
                add_rows(a, (0, rows), four + [(zu.at[z], 0)])

            pl.when(at.z == 0)(lambda: add_rows(a, (0, rows), four))
            go_up(z).start()

        @pl.when(z < at.z)
        def _():
            @pl.when(at.z < nz - 1)
            def _():
                go_down(z).wait_recv()
                add_rows(a, (0, rows), four + [(zd.at[z], 0)])

            pl.when(at.z == nz - 1)(lambda: add_rows(a, (0, rows), four))
            go_down(z).start()

        @pl.when(z == at.z)
        def _():
            add_rows(out, (0, rows), four)

            @pl.when(at.z > 0)
            def _():
                go_up(z).wait_recv()
                add_rows(out, (0, rows), [(out, 0), (zu.at[z], 0)])

            @pl.when(at.z < nz - 1)
            def _():
                go_down(z).wait_recv()
                add_rows(out, (0, rows), [(out, 0), (zd.at[z], 0)])

    def body(i, carry):
        pl.when(i < steps)(lambda: on_line(i, diag_step))
        pl.when((i >= 1) & (i < steps + 1))(lambda: on_line(i - 1, plane_step))
        pl.when(i >= 2)(lambda: on_line(i - 2, line_step))
        for k in range(1, 5):
            pl.when(i == k)(functools.partial(small.stage, k))
        return carry

    lax.fori_loop(0, steps + 2, body, 0)

    def finish(z, carry):
        for f in range(4):
            to_p(f, z).wait_send()
        half_x(z).wait_send()
        half_y(z).wait_send()
        full_x(z).wait_send()
        full_y(z).wait_send()
        pl.when(z > at.z)(lambda: go_up(z).wait_send())
        pl.when(z < at.z)(lambda: go_down(z).wait_send())
        return carry

    lax.fori_loop(0, nz, finish, 0)


def scatter_all(parts, small, nz, cid):
    _, _, r, c = parts.shape

    def buf(*n):
        return pltpu.VMEM((*n, c), parts.dtype)

    return pl.pallas_call(
        functools.partial(scatter_kernel, nz),
        out_shape=(
            jax.ShapeDtypeStruct((r, c), jnp.float32),
            jax.ShapeDtypeStruct(small.shape[-2:], jnp.float32),
        ),
        in_specs=[pl.BlockSpec(memory_space=pl.ANY), pl.BlockSpec(memory_space=pltpu.VMEM)],
        out_specs=(pl.BlockSpec(memory_space=pltpu.VMEM),) * 2,
        scratch_shapes=[
            buf(4, nz, r), buf(4, nz, r), buf(nz, r // 2), buf(nz, r // 2),
            buf(nz, r), buf(nz, r), buf(nz, r), buf(nz, r),
            DMA((4, nz)), DMA((4, nz)), DMA((4, nz)),
            *[DMA((nz,))] * 12,
            *SmallScatter.scratch(nz, small.shape[-2:]),
            *SmallScatter.sems(nz),
        ],
        compiler_params=pltpu.CompilerParams(
            collective_id=cid, has_side_effects=True, vmem_limit_bytes=50 << 20
        ),
        cost_estimate=pl.CostEstimate(flops=0, bytes_accessed=240 << 20, transcendentals=0),
        name="scatter_all",
    )(parts, small)


def square_gather_kernel(own, ids, out, out_ids, xs, xr, ys, yr, fs, fr, js, jr):
    at = Place()
    half = own.shape[0] // 2
    halves = (pl.ds(0, half), pl.ds(half, half))
    peers = [(at.fx, at.e), (at.fy, at.e), (at.fd, at.e)]
    greet(peers)

    def to_x(h):
        return send(own.at[halves[h]], out.at[at.f, halves[h]], xs.at[h], xr.at[h], at.fx, at.e)

    def to_y(h):
        return send(own.at[halves[h]], out.at[at.f, halves[h]], ys.at[h], yr.at[h], at.fy, at.e)

    x_ref, y_ref = out.at[at.fx, halves[0]], out.at[at.fy, halves[1]]
    x_on = send(x_ref, x_ref, fs.at[0], fr.at[0], at.fy, at.e)
    y_on = send(y_ref, y_ref, fs.at[1], fr.at[1], at.fx, at.e)
    notes = [
        send(ids, out_ids.at[at.f], js.at[k], jr.at[k], f, e) for k, (f, e) in enumerate(peers)
    ]
    to_x(0).start()
    to_y(1).start()
    for note in notes:
        note.start()
    to_x(1).start()
    to_y(0).start()
    out[at.f] = own[...]
    out_ids[at.f] = ids[...]
    to_x(0).wait_recv()
    x_on.start()
    to_y(1).wait_recv()
    y_on.start()
    to_x(1).wait()
    to_y(0).wait()
    for note in notes:
        note.wait()
    to_x(0).wait_send()
    to_y(1).wait_send()
    x_on.wait()
    y_on.wait()


def square_gather(rows, ids, cid):
    r, c = rows.shape
    vmem = pl.BlockSpec(memory_space=pltpu.VMEM)
    return pl.pallas_call(
        square_gather_kernel,
        out_shape=(
            jax.ShapeDtypeStruct((4, r, c), rows.dtype),
            jax.ShapeDtypeStruct((4, *ids.shape), ids.dtype),
        ),
        in_specs=[vmem] * 2,
        out_specs=(vmem,) * 2,
        scratch_shapes=[DMA((2,))] * 6 + [DMA((3,))] * 2,
        compiler_params=pltpu.CompilerParams(collective_id=cid, has_side_effects=True),
        cost_estimate=pl.CostEstimate(flops=0, bytes_accessed=60 << 20, transcendentals=0),
        name="square_gather",
    )(rows, ids)


def square_scatter_kernel(part, out, xh, yh, xf, yf, ss, rs):
    at = Place()
    rows = out.shape[0]
    half = rows // 2
    lo, hi = pl.ds(0, half), pl.ds(half, half)
    greet([(at.fx, at.e), (at.fy, at.e)])

    def to_x(k, src, dst):
        return send(src, dst, ss.at[k], rs.at[k], at.fx, at.e)

    def to_y(k, src, dst):
        return send(src, dst, ss.at[k], rs.at[k], at.fy, at.e)

    copies = [
        to_x(0, part.at[at.fd, lo], xh),
        to_y(1, part.at[at.fd, hi], yh),
        to_x(2, part.at[at.fx, lo], xf.at[lo]),
        to_y(3, part.at[at.fy, hi], yf.at[hi]),
        to_x(4, yh, xf.at[hi]),
        to_y(5, xh, yf.at[lo]),
    ]
    for copy in copies[:4]:
        copy.start()
    copies[1].wait_recv()
    add_rows(yh, (0, half), [(yh, 0), (part.at[at.fx], half)])
    copies[4].start()
    copies[0].wait_recv()
    add_rows(xh, (0, half), [(xh, 0), (part.at[at.fy], 0)])
    copies[5].start()
    copies[2].wait_recv()
    copies[5].wait_recv()
    copies[3].wait_recv()
    copies[4].wait_recv()
    add_rows(out, (0, rows), [(part.at[at.f], 0), (xf, 0), (yf, 0)])
    for copy in copies:
        copy.wait_send()


def square_scatter(parts, cid):
    _, r, c = parts.shape
    vmem = pl.BlockSpec(memory_space=pltpu.VMEM)

    def buf(n):
        return pltpu.VMEM((n, c), parts.dtype)

    return pl.pallas_call(
        square_scatter_kernel,
        out_shape=jax.ShapeDtypeStruct((r, c), jnp.float32),
        in_specs=[vmem],
        out_specs=vmem,
        scratch_shapes=[buf(r // 2), buf(r // 2), buf(r), buf(r), DMA((6,)), DMA((6,))],
        compiler_params=pltpu.CompilerParams(collective_id=cid, has_side_effects=True),
        cost_estimate=pl.CostEstimate(flops=0, bytes_accessed=60 << 20, transcendentals=0),
        name="square_scatter",
    )(parts)


def square_sum_kernel(own, out, got, ss, rs):
    at = Place()
    peers = [(at.fx, at.e), (at.fy, at.e), (at.fd, at.e)]
    greet(peers)
    copies = [send(own, got.at[k], ss.at[k], rs.at[k], f, e) for k, (f, e) in enumerate(peers)]
    for copy in copies:
        copy.start()
    for copy in copies:
        copy.wait()
    out[...] = (own[...] + got[0]) + (got[1] + got[2])


def square_sum(values, cid):
    flat = values.reshape(8, -1)
    vmem = pl.BlockSpec(memory_space=pltpu.VMEM)
    return pl.pallas_call(
        square_sum_kernel,
        out_shape=jax.ShapeDtypeStruct(flat.shape, jnp.float32),
        in_specs=[vmem],
        out_specs=vmem,
        scratch_shapes=[pltpu.VMEM((3, *flat.shape), jnp.float32), DMA((3,)), DMA((3,))],
        compiler_params=pltpu.CompilerParams(collective_id=cid, has_side_effects=True),
        cost_estimate=pl.CostEstimate(flops=0, bytes_accessed=10 << 20, transcendentals=0),
        name="square_sum",
    )(flat).reshape(values.shape)


def line_sum_kernel(nz, counts, *refs):
    at = Place()
    refs = iter(refs)
    n = len(counts)
    parts, part_small, outs, out_small = take(refs, n), next(refs), take(refs, n), next(refs)
    bufs = [take(refs, 5) for _ in range(n)]
    sems = [take(refs, 12) for _ in range(n)]
    own_small = next(refs)
    scatter_small = SmallScatter(at, nz, part_small, own_small, take(refs, 4), take(refs, 4))
    gather_small = SmallGather(at, nz, own_small, out_small, take(refs, 4))
    greet([(at.fx, at.e), (at.fy, at.e), (at.f, at.pe)], (at, nz))
    scatter_small.stage(0)
    total = sum(counts)
    last = nz - 1

    class Piece:
        def __init__(self, k, p):
            self.p, self.part, self.out = p, parts[k], outs[k]
            self.acc, self.pb, self.zu, self.zd, self.mine = bufs[k]
            self.sems = sems[k]
            self.r = self.acc.shape[2]

        def load(self):
            p = self.p
            return pltpu.make_async_copy(self.part.at[p, at.c], self.acc.at[p], self.sems[0].at[p])

        def to_p(self):
            p, (_, s, r, *_rest) = self.p, self.sems
            return send(self.part.at[p, 1 - at.c], self.pb.at[p], s.at[p], r.at[p], at.f, at.pe)

        def go_up(self, z):
            p, s, r = self.p, self.sems[3], self.sems[4]
            return send(self.acc.at[p, z], self.zu.at[p, z], s.at[p, z], r.at[p, z], at.f, at.e + 2)

        def go_down(self, z):
            p, s, r = self.p, self.sems[5], self.sems[6]
            return send(self.acc.at[p, z], self.zd.at[p, z], s.at[p, z], r.at[p, z], at.f, at.e - 2)

        def res(self, z, way):
            p, s, r = self.p, self.sems[7], self.sems[8]
            ref = self.out.at[p, at.c, z]
            return send(ref, ref, s.at[way, p, z], r.at[p, z], at.f, at.e + 2 - 4 * way)

        def res_p(self, z):
            p, s, r = self.p, self.sems[9], self.sems[10]
            ref = self.out.at[p, at.c, z]
            return send(ref, ref, s.at[p, z], r.at[p, z], at.f, at.pe)

        def keep(self):
            p = self.p
            return pltpu.make_async_copy(self.mine.at[p], self.out.at[p, at.c, at.z], self.sems[11].at[p])

    def piece(q, run, when=True):
        low = 0
        for k, count in enumerate(counts):
            @pl.when((q >= low) & (q < low + count) & when)
            def _(k=k, low=low):
                run(Piece(k, q - low))

            low += count

    def start(q, carry):
        def run(it):
            it.load().start()
            it.to_p().start()

        piece(q, run)
        return carry

    lax.fori_loop(0, total, start, 0)

    def halve(it):
        it.load().wait()
        it.to_p().wait_recv()
        p = it.p

        def body(z, carry):
            a = it.acc.at[p, z]
            add_rows(a, (0, it.r), [(a, 0), (it.pb.at[p, z], 0)])
            return carry

        lax.fori_loop(0, nz, body, 0)

    def rise(it):
        p = it.p

        def body(i, carry):
            z = last - i

            @pl.when(z > at.z)
            def _():
                a = it.acc.at[p, z]

                @pl.when(at.z > 0)
                def _():
                    it.go_up(z).wait_recv()
                    add_rows(a, (0, it.r), [(a, 0), (it.zu.at[p, z], 0)])

                it.go_up(z).start()

            return carry

        lax.fori_loop(0, last, body, 0)

    def sink(it):
        p = it.p

        def body(z, carry):
            @pl.when(z < at.z)
            def _():
                a = it.acc.at[p, z]

                @pl.when(at.z < last)
                def _():
                    it.go_down(z).wait_recv()
                    add_rows(a, (0, it.r), [(a, 0), (it.zd.at[p, z], 0)])

                it.go_down(z).start()

            return carry

        lax.fori_loop(0, last, body, 0)

    def settle(it):
        p, z = it.p, at.z
        pl.when(z > 0)(lambda: it.go_up(z).wait_recv())
        pl.when(z < last)(lambda: it.go_down(z).wait_recv())
        a, dst = (it.acc.at[p, z], 0), it.mine.at[p]
        up, down = (it.zu.at[p, z], 0), (it.zd.at[p, z], 0)
        pl.when((z > 0) & (z < last))(lambda: add_rows(dst, (0, it.r), [a, up, down]))
        pl.when(z == 0)(lambda: add_rows(dst, (0, it.r), [a, down]))
        pl.when(z == last)(lambda: add_rows(dst, (0, it.r), [a, up]))
        it.keep().start()

    def tell(it):
        z = at.z
        it.keep().wait()
        pl.when(z < last)(lambda: it.res(z, 0).start())
        pl.when(z > 0)(lambda: it.res(z, 1).start())
        it.res_p(z).start()

    def pass_up(it, z):
        it.res(z, 0).wait_recv()
        pl.when(at.z < last)(lambda: it.res(z, 0).start())
        it.res_p(z).start()

    def pass_down(it, z):
        it.res(z, 0).wait_recv()
        pl.when(at.z > 0)(lambda: it.res(z, 1).start())
        it.res_p(z).start()

    def body(i, carry):
        piece(i, halve)
        piece(i - at.z, rise, at.z < last)
        piece(i - (last - at.z), sink, at.z > 0)
        piece(i - nz, settle)
        piece(i - nz, tell)
        for d in range(1, nz):
            piece(i - nz - d, functools.partial(pass_up, z=at.z - d), at.z >= d)
            piece(i - nz - d, functools.partial(pass_down, z=at.z + d), at.z + d <= last)
        for s in range(1, 5):
            pl.when(i == s)(functools.partial(scatter_small.stage, s))
        for s in range(5):
            pl.when(i == 5 + s)(functools.partial(gather_small.stage, s))
        return carry

    lax.fori_loop(0, total + 2 * nz - 1, body, 0)

    def finish(q, carry):
        def run(it):
            it.to_p().wait_send()

            def one(z, carry):
                pl.when(z > at.z)(lambda: it.go_up(z).wait_send())
                pl.when(z < at.z)(lambda: it.go_down(z).wait_send())
                pl.when((z <= at.z) & (at.z < last))(lambda: it.res(z, 0).wait_send())
                pl.when((z >= at.z) & (at.z > 0))(lambda: it.res(z, 1).wait_send())
                it.res_p(z).wait_send()
                it.res_p(z).wait_recv()
                return carry

            lax.fori_loop(0, nz, one, 0)

        piece(q, run)
        return carry

    lax.fori_loop(0, total, finish, 0)


def line_sum(parts, small, nz, cid):
    counts = tuple(p.shape[0] for p in parts)
    scratch, sems = [], []
    for p in parts:
        n, _, _, r, c = p.shape

        def buf(*lead):
            return pltpu.VMEM((*lead, r, c), p.dtype)

        scratch += [buf(n, nz), buf(n, nz), buf(n, nz), buf(n, nz), buf(n)]
        each, line = DMA((n,)), DMA((n, nz))
        sems += [each, each, each, line, line, line, line, DMA((2, n, nz)), line, line, line, each]
    hbm, vmem = pl.BlockSpec(memory_space=pl.ANY), pl.BlockSpec(memory_space=pltpu.VMEM)
    return pl.pallas_call(
        functools.partial(line_sum_kernel, nz, counts),
        out_shape=(
            *(jax.ShapeDtypeStruct(p.shape, p.dtype) for p in parts),
            jax.ShapeDtypeStruct(small.shape, jnp.float32),
        ),
        in_specs=[hbm] * len(parts) + [vmem],
        out_specs=(*[hbm] * len(parts), vmem),
        scratch_shapes=[
            *scratch, *sems, pltpu.VMEM(small.shape[-2:], jnp.float32),
            *SmallScatter.scratch(nz, small.shape[-2:]), *SmallScatter.sems(nz), *SmallGather.sems(nz),
        ],
        compiler_params=pltpu.CompilerParams(
            collective_id=cid, has_side_effects=True, vmem_limit_bytes=50 << 20
        ),
        cost_estimate=pl.CostEstimate(flops=0, bytes_accessed=300 << 20, transcendentals=0),
        name="line_sum",
    )(*parts, small)


def rope_tables(seg_ids, head_dim):
    length = seg_ids.shape[0]
    ordinal = lax.iota(jnp.int32, length)
    earlier = (seg_ids[:, None] == seg_ids[None, :]) & (ordinal[None, :] < ordinal[:, None])
    places = jnp.sum(earlier.astype(jnp.int32), axis=1).astype(jnp.float32)
    half_dim = head_dim // 2
    inv_freq = rope_base ** (
        -(lax.iota(jnp.int32, half_dim).astype(jnp.float32) * (2.0 / head_dim))
    )
    angles = places[:, None] * inv_freq[None, :]
    angles = jnp.concatenate([angles, angles], axis=1)
    return (jnp.cos(angles), jnp.sin(angles))


def rotate_half(values):
    half_dim = values.shape[-1] // 2
    return jnp.concatenate([-values[..., half_dim:], values[..., :half_dim]], axis=-1)


def rotate_back(values):
    half_dim = values.shape[-1] // 2
    return jnp.concatenate([values[..., half_dim:], -values[..., :half_dim]], axis=-1)


def apply_rope(values, cosine, sine_table):
    return values * cosine[:, None, :] + rotate_half(values) * sine_table[:, None, :]


def rope_grad(grads_in, cosine, sine_table):
    return grads_in * cosine[:, None, :] + rotate_back(grads_in * sine_table[:, None, :])


def across_heads(kernel, pair_sums):
    if kernel:
        return square_sum(jnp.stack(pair_sums), kernel)
    return lax.psum((pair_sums[0], pair_sums[1]), "fsdp")


def share_rows(kernel, term_fn, own_rows):
    if kernel:
        parts = term_fn(jnp.int32(0), own_rows * lax.axis_size("fsdp"))
        return square_scatter(parts.reshape(-1, own_rows, parts.shape[1]), kernel)
    return lax.psum_scatter(
        term_fn(jnp.int32(0), own_rows * lax.axis_size("fsdp")),
        "fsdp",
        scatter_dimension=0,
        tiled=True,
    )


def to_owner(block_rows):
    return lax.all_to_all(block_rows, "expert", split_axis=0, concat_axis=0, tiled=True)


def from_owner(block_rows):
    return lax.all_to_all(block_rows, "expert", split_axis=0, concat_axis=0, tiled=True)


def shard_gather(block_rows):
    return lax.all_gather(block_rows, "fsdp", axis=0, tiled=True)


def owner_sum(term_fn, sources):
    own_rows = sources // lax.axis_size("fsdp")
    return lax.psum_scatter(
        term_fn(jnp.int32(0), own_rows * lax.axis_size("fsdp")),
        "fsdp",
        scatter_dimension=0,
        tiled=True,
    )


def head_scores(q_heads, k_heads, allowed):
    scores = jnp.einsum(
        "thd,shd->hts", q_heads, k_heads, preferred_element_type=jnp.float32
    ) * HEAD_DIM ** (-0.5)
    return jnp.where(allowed[None], scores, -1e30)


def experts_by_slot(
    second_in, second_rows, cotangent, routes, capacity, w_router, w_gate, w_up, w_down
):
    tok_count, model_width = second_rows.shape
    experts = w_router.shape[1]
    local_experts = w_gate.shape[0]
    slot_count = tok_count * TOP * 3 // (2 * experts)
    pair_count = tok_count * TOP
    zero_row = jnp.zeros((1, model_width), jnp.bfloat16)
    logits = jnp.dot(second_rows, w_router, preferred_element_type=jnp.float32)
    chosen = routes
    expert_ids = lax.iota(jnp.int32, experts)
    chosen_hot = (chosen[:, :, None] == expert_ids[None, None, :]).astype(jnp.float32)
    routed = jnp.sum(chosen_hot * logits[:, None, :], axis=2)
    gate_wts = jax.nn.softmax(routed, axis=1)
    pair_hot = chosen_hot.reshape(pair_count, experts).astype(jnp.int32)
    earlier_hits = jnp.cumsum(pair_hot, axis=0) - pair_hot
    ranking = jnp.sum(earlier_hits * pair_hot, axis=1)
    cap_pair = jnp.sum(pair_hot * capacity[None, :], axis=1)
    is_kept = ranking < cap_pair
    pair_route = chosen.reshape(pair_count)
    slot_place = jnp.where(is_kept, pair_route * slot_count + ranking, experts * slot_count)
    pair_ids = lax.iota(jnp.int32, pair_count)
    slot_pair = (
        jnp.full((experts * slot_count,), pair_count, jnp.int32)
        .at[slot_place]
        .set(pair_ids, mode="drop")
    )
    padded = jnp.concatenate([second_rows, zero_row], axis=0)
    outgoing = padded[slot_pair // TOP].reshape(experts, slot_count, model_width)
    arrived = shard_gather(to_owner(outgoing))
    gate_w, up_w, down_w = (w_gate, w_up, w_down)
    owner_rows = arrived.reshape(-1, local_experts, slot_count, model_width)
    sources = owner_rows.shape[0]
    gate_act = jnp.einsum("sjcd,jdh->sjch", owner_rows, gate_w, preferred_element_type=jnp.float32)
    up_act = jnp.einsum("sjcd,jdh->sjch", owner_rows, up_w, preferred_element_type=jnp.float32)
    sig_gate = jax.nn.sigmoid(gate_act)
    silu_gate = gate_act * sig_gate
    hidden = (silu_gate * up_act).astype(jnp.bfloat16)

    def down_term(start, length):
        return jnp.einsum("sjch,jhd->sjcd", hidden, down_w, preferred_element_type=jnp.float32)

    produced = owner_sum(down_term, sources)
    returned = from_owner(produced.astype(jnp.bfloat16).reshape(-1, slot_count, model_width))
    slot_rows = jnp.concatenate(
        [returned.reshape(experts * slot_count, model_width), zero_row], axis=0
    )
    pair_rows = slot_rows[slot_place].reshape(tok_count, TOP, model_width).astype(jnp.float32)
    kept_mask = is_kept.reshape(tok_count, TOP).astype(jnp.float32)
    gate_kept = gate_wts * kept_mask
    moe_rows = jnp.sum(gate_kept[:, :, None] * pair_rows, axis=1)
    final_rows = second_in + moe_rows
    block_output = final_rows.astype(jnp.bfloat16)
    grad_out = cotangent.astype(jnp.float32)
    grad_gate_k = jnp.sum(pair_rows * grad_out[:, None, :], axis=2) * kept_mask
    grad_routed = gate_wts * (grad_gate_k - jnp.sum(gate_wts * grad_gate_k, axis=1, keepdims=True))
    grad_logits = jnp.sum(chosen_hot * grad_routed[:, :, None], axis=1)
    router_grad = jnp.dot(second_rows.astype(jnp.float32).T, grad_logits, precision=precise)
    grad_second = jnp.dot(grad_logits, w_router.astype(jnp.float32).T, precision=precise)
    pair_grads = (
        (gate_kept[:, :, None] * grad_out[:, None, :])
        .astype(jnp.bfloat16)
        .reshape(pair_count, model_width)
    )
    pair_grads = jnp.concatenate([pair_grads, zero_row], axis=0)
    slot_grads = pair_grads[slot_pair].reshape(experts, slot_count, model_width)
    grad_blocks = shard_gather(to_owner(slot_grads)).reshape(
        -1, local_experts, slot_count, model_width
    )
    grad_hidden = jnp.einsum(
        "sjcd,jhd->sjch", grad_blocks, down_w, preferred_element_type=jnp.float32
    )
    grad_down_w = jnp.einsum(
        "sjch,sjcd->jhd", hidden, grad_blocks, preferred_element_type=jnp.float32
    )
    grad_gate_in = (grad_hidden * up_act * sig_gate * (1.0 + gate_act * (1.0 - sig_gate))).astype(
        jnp.bfloat16
    )
    grad_up_in = (grad_hidden * silu_gate).astype(jnp.bfloat16)
    grad_gate_w = jnp.einsum(
        "sjcd,sjch->jdh", owner_rows, grad_gate_in, preferred_element_type=jnp.float32
    )
    grad_up_w = jnp.einsum(
        "sjcd,sjch->jdh", owner_rows, grad_up_in, preferred_element_type=jnp.float32
    )

    def back_term(start, length):
        from_gate = jnp.einsum(
            "sjch,jdh->sjcd", grad_gate_in, gate_w, preferred_element_type=jnp.float32
        )
        from_up = jnp.einsum("sjch,jdh->sjcd", grad_up_in, up_w, preferred_element_type=jnp.float32)
        return from_gate + from_up

    grad_slots = from_owner(
        owner_sum(back_term, sources).astype(jnp.bfloat16).reshape(-1, slot_count, model_width)
    )
    back_rows = jnp.concatenate(
        [grad_slots.reshape(experts * slot_count, model_width), zero_row], axis=0
    )
    grad_second = grad_second + jnp.sum(
        back_rows[slot_place].reshape(tok_count, TOP, model_width).astype(jnp.float32), axis=1
    )
    return block_output[None], grad_second, router_grad.T, (grad_gate_w, grad_up_w, grad_down_w)


def experts_dense(
    second_in, second_rows, cotangent, routes, capacity, w_router, w_gate, w_up, w_down
):
    tok_count = second_rows.shape[0]
    experts = w_router.shape[1]
    local_experts, model_width, hidden_here = w_gate.shape
    shards = lax.axis_size("fsdp")
    owners = lax.axis_size("expert")
    wide = local_experts * hidden_here
    logits = jnp.dot(second_rows, w_router, preferred_element_type=jnp.float32)
    expert_ids = lax.iota(jnp.int32, experts)
    named = jnp.any(routes[:, :, None] == expert_ids[None, None, :], axis=1)
    before = lax.iota(jnp.int32, tok_count)[None, :] < lax.iota(jnp.int32, tok_count)[:, None]
    ranking = jnp.dot(
        before.astype(jnp.bfloat16), named.astype(jnp.bfloat16), preferred_element_type=jnp.float32
    )
    kept = named & (ranking < capacity.astype(jnp.float32)[None, :])
    kept_mask = kept.astype(jnp.float32)
    top_logit = jnp.max(jnp.where(named, logits, -jnp.inf), axis=1, keepdims=True)
    powers = jnp.where(named, jnp.exp(jnp.where(named, logits - top_logit, 0.0)), 0.0)
    gate_wts = powers / jnp.sum(powers, axis=1, keepdims=True)
    gate_kept = gate_wts * kept_mask

    grad_all = lax.all_gather(cotangent, ("fsdp", "expert"), axis=0, tiled=True)
    nz = owners // 2
    rows_all, kept_all = gather_all(second_rows, gate_kept.T, nz, 7)
    rows_all = rows_all.reshape(-1, model_width)
    first_expert = lax.axis_index("expert") * local_experts
    gate_here = lax.dynamic_slice_in_dim(kept_all, first_expert, local_experts, axis=3)
    gate_here = jnp.transpose(gate_here, (1, 2, 0, 4, 3)).reshape(-1, local_experts)
    gate_cols = jnp.repeat(gate_here, hidden_here, axis=1)
    tokens = rows_all.shape[0]

    gate_w = jnp.transpose(w_gate, (1, 0, 2)).reshape(model_width, wide)
    up_w = jnp.transpose(w_up, (1, 0, 2)).reshape(model_width, wide)
    down_w = w_down.reshape(wide, model_width)
    grad_hid = jnp.einsum("td,hd->th", grad_all, down_w, preferred_element_type=jnp.float32)
    gate_act = jnp.dot(rows_all, gate_w, preferred_element_type=jnp.float32)
    up_act = jnp.dot(rows_all, up_w, preferred_element_type=jnp.float32)
    sig_gate = jax.nn.sigmoid(gate_act)
    silu_gate = gate_act * sig_gate
    hidden = silu_gate * up_act
    gate_terms = jnp.sum((hidden * grad_hid).reshape(tokens, local_experts, hidden_here), axis=2)
    weighted = (hidden * gate_cols).astype(jnp.bfloat16)
    grad_hid = grad_hid * gate_cols
    grad_gate_in = (grad_hid * up_act * sig_gate * (1.0 + gate_act * (1.0 - sig_gate))).astype(
        jnp.bfloat16
    )
    grad_up_in = (grad_hid * silu_gate).astype(jnp.bfloat16)
    back = (
        jnp.einsum("th,dh->td", grad_gate_in, gate_w, preferred_element_type=jnp.float32)
        + jnp.einsum("th,dh->td", grad_up_in, up_w, preferred_element_type=jnp.float32)
    ).astype(jnp.bfloat16)
    terms = jnp.transpose(
        gate_terms.reshape(shards, nz, 2, tok_count, local_experts), (2, 0, 1, 4, 3)
    )
    terms = lax.dynamic_update_slice_in_dim(
        jnp.zeros((2, shards, nz, experts, tok_count), jnp.float32), terms, first_expert, axis=3
    )
    back = back.reshape(shards, owners, tok_count, model_width)
    back_rows, terms = scatter_all(back, terms, nz, 8)
    grad_gate_k = terms.T * kept_mask
    forward = jnp.dot(weighted, down_w, preferred_element_type=jnp.float32).astype(jnp.bfloat16)
    forward_rows = lax.psum_scatter(forward, "fsdp", scatter_dimension=0, tiled=True)
    forward_rows = lax.psum_scatter(forward_rows, "expert", scatter_dimension=0, tiled=True)
    block_output = (second_in + forward_rows.astype(jnp.float32)).astype(jnp.bfloat16)[None]
    grad_logits = gate_wts * (grad_gate_k - jnp.sum(gate_wts * grad_gate_k, axis=1, keepdims=True))
    router_grad = jnp.dot(grad_logits.T, second_rows.astype(jnp.float32), precision=precise)
    grad_second = jnp.dot(grad_logits, w_router.astype(jnp.float32).T, precision=precise)
    grad_second = grad_second + back_rows

    def by_expert(left, right):
        return jnp.dot(left.T, right, preferred_element_type=jnp.float32)

    parts = [slice(j * hidden_here, (j + 1) * hidden_here) for j in range(local_experts)]
    grad_gate_w = jnp.stack([by_expert(rows_all, grad_gate_in[:, p]) for p in parts])
    grad_up_w = jnp.stack([by_expert(rows_all, grad_up_in[:, p]) for p in parts])
    grad_down_w = by_expert(weighted, grad_all).reshape(local_experts, hidden_here, model_width)
    return block_output, grad_second, router_grad, (grad_gate_w, grad_up_w, grad_down_w)


def sum_grads(narrow, gains, head_gains, nz):
    shards, width = lax.axis_size("fsdp"), gains.shape[1]
    mine = lax.iota(jnp.int32, shards) == lax.axis_index("fsdp")
    heads_flat = jnp.pad(head_gains.reshape(-1), (0, width - head_gains.size))
    rows = jnp.concatenate([gains, jnp.where(mine[:, None], heads_flat[None], 0.0)], axis=0)
    share = -(-rows.size // (2 * shards * nz * 1024)) * 8
    small = jnp.pad(rows.reshape(-1), (0, 2 * shards * nz * share * 128 - rows.size))
    small = small.reshape(2, shards, nz, share, 128)
    parts = [g.reshape(-1, 2, nz, 16, g.shape[1]) for g in narrow]
    *sums, small = line_sum(parts, small, nz, 9)
    small = small.reshape(-1)[: rows.size].reshape(rows.shape)
    own = lax.dynamic_slice_in_dim(small, gains.shape[0] + lax.axis_index("fsdp"), 1, axis=0)
    head_gains = own[0, : head_gains.size].reshape(head_gains.shape)
    return [s.reshape(g.shape) for s, g in zip(sums, narrow)], small[: gains.shape[0]], head_gains


def on_device(
    block_input,
    cotangent,
    w_query,
    w_key,
    w_value,
    w_output,
    q_gain,
    k_gain,
    attn_gain,
    mlp_gain,
    w_router,
    w_gate,
    w_up,
    w_down,
    segments,
    routes,
    capacity,
):
    tok_count = block_input.shape[1]
    model_width = block_input.shape[2]
    experts = w_router.shape[1]
    nz = lax.axis_size("expert") // 2
    dense = 2 * TOP >= experts and lax.axis_size("fsdp") == 4
    flat_in = block_input[0].astype(jnp.float32)
    scale_one = lax.rsqrt(jnp.mean(flat_in * flat_in, axis=1, keepdims=True) + epsilon)
    normed_one = flat_in * scale_one
    first_rows = (normed_one * attn_gain).astype(jnp.bfloat16)
    if dense:
        group_rows, group_segs = square_gather(first_rows, jnp.tile(segments, (8, 1)), 1)
        group_rows = group_rows.reshape(-1, model_width)
        group_segs = group_segs[:, 0].reshape(-1)
    else:
        group_rows, group_segs = (
            lax.all_gather(first_rows, "fsdp", axis=0, tiled=True),
            lax.all_gather(segments[0], "fsdp", axis=0, tiled=True),
        )
    group_len = group_rows.shape[0]
    heads_here = w_query.shape[1] // HEAD_DIM
    query_rows = jnp.dot(group_rows, w_query, preferred_element_type=jnp.float32)
    key_rows = jnp.dot(group_rows, w_key, preferred_element_type=jnp.float32)
    value_rows = jnp.dot(group_rows, w_value, preferred_element_type=jnp.float32).astype(
        jnp.bfloat16
    )
    square_sums = across_heads(
        dense and 2,
        (jnp.sum(query_rows * query_rows, axis=1), jnp.sum(key_rows * key_rows, axis=1))
    )
    q_scale = lax.rsqrt(square_sums[0][:, None] / model_width + epsilon)
    k_scale = lax.rsqrt(square_sums[1][:, None] / model_width + epsilon)
    cosine, sine_table = rope_tables(group_segs, HEAD_DIM)
    head_shape = (group_len, heads_here, HEAD_DIM)
    q_heads = apply_rope(
        (query_rows * q_scale * q_gain).reshape(head_shape), cosine, sine_table
    ).astype(jnp.bfloat16)
    k_heads = apply_rope(
        (key_rows * k_scale * k_gain).reshape(head_shape), cosine, sine_table
    ).astype(jnp.bfloat16)
    v_heads = value_rows.reshape(head_shape)
    ordinal = lax.iota(jnp.int32, group_len)
    allowed = (group_segs[:, None] == group_segs[None, :]) & (ordinal[None, :] <= ordinal[:, None])
    scores = head_scores(q_heads, k_heads, allowed)
    row_top = jnp.max(scores, axis=2, keepdims=True)
    log_total = row_top + jnp.log(jnp.sum(jnp.exp(scores - row_top), axis=2, keepdims=True))
    attn_weights = jnp.exp(scores - log_total)
    mixed_heads = jnp.einsum(
        "hts,shd->thd",
        attn_weights.astype(jnp.bfloat16),
        v_heads,
        preferred_element_type=jnp.float32,
    )
    attn_rows = mixed_heads.reshape(group_len, heads_here * HEAD_DIM).astype(jnp.bfloat16)

    def mixed_term(start, length):
        return jnp.dot(attn_rows, w_output, preferred_element_type=jnp.float32).astype(jnp.bfloat16)

    mixed_rows = share_rows(dense and 4, mixed_term, tok_count).astype(jnp.float32)
    second_in = flat_in + mixed_rows
    scale_two = lax.rsqrt(jnp.mean(second_in * second_in, axis=1, keepdims=True) + epsilon)
    normed_two = second_in * scale_two
    second_rows = (normed_two * mlp_gain).astype(jnp.bfloat16)
    if dense:
        block_output, grad_second, router_grad, expert_grads = experts_dense(
            second_in, second_rows, cotangent[0], routes[0], capacity, w_router, w_gate, w_up, w_down
        )
    else:
        block_output, grad_second, router_grad, expert_grads = experts_by_slot(
            second_in, second_rows, cotangent[0], routes[0], capacity, w_router, w_gate, w_up, w_down
        )
    grad_gate_w, grad_up_w, grad_down_w = expert_grads
    grad_out = cotangent[0].astype(jnp.float32)
    mlp_gain_grad = jnp.sum(grad_second * normed_two, axis=0)
    grad_normed_two = grad_second * mlp_gain
    grad_mid = grad_out + scale_two * (
        grad_normed_two - normed_two * jnp.mean(grad_normed_two * normed_two, axis=1, keepdims=True)
    )
    if dense:
        group_grad, _ = square_gather(grad_mid.astype(jnp.bfloat16), jnp.tile(segments, (8, 1)), 6)
        group_grad = group_grad.reshape(-1, model_width)
    else:
        group_grad = lax.all_gather(grad_mid.astype(jnp.bfloat16), "fsdp", axis=0, tiled=True)
    out_grad = jnp.einsum("ti,td->id", attn_rows, group_grad, preferred_element_type=jnp.float32)
    grad_attn = (
        jnp.einsum("td,id->ti", group_grad, w_output, preferred_element_type=jnp.float32)
        .astype(jnp.bfloat16)
        .reshape(head_shape)
    )
    scores_again = head_scores(q_heads, k_heads, allowed)
    weights_again = jnp.exp(scores_again - log_total)
    grad_values = jnp.einsum(
        "hts,thd->shd",
        weights_again.astype(jnp.bfloat16),
        grad_attn,
        preferred_element_type=jnp.float32,
    )
    grad_weights = jnp.einsum(
        "thd,shd->hts", grad_attn, v_heads, preferred_element_type=jnp.float32
    )
    inner_sum = jnp.sum(weights_again * grad_weights, axis=2, keepdims=True)
    grad_scores = (weights_again * (grad_weights - inner_sum)).astype(jnp.bfloat16)
    grad_q_heads = jnp.einsum(
        "hts,shd->thd", grad_scores, k_heads, preferred_element_type=jnp.float32
    ) * HEAD_DIM ** (-0.5)
    grad_k_heads = jnp.einsum(
        "hts,thd->shd", grad_scores, q_heads, preferred_element_type=jnp.float32
    ) * HEAD_DIM ** (-0.5)
    grad_q_normed = rope_grad(grad_q_heads, cosine, sine_table).reshape(group_len, -1)
    grad_k_normed = rope_grad(grad_k_heads, cosine, sine_table).reshape(group_len, -1)
    q_gain_grad = jnp.sum(grad_q_normed * query_rows * q_scale, axis=0)
    k_gain_grad = jnp.sum(grad_k_normed * key_rows * k_scale, axis=0)
    inner_q = grad_q_normed * q_gain
    inner_k = grad_k_normed * k_gain
    inner_sums = across_heads(
        dense and 3,
        (jnp.sum(inner_q * query_rows, axis=1), jnp.sum(inner_k * key_rows, axis=1))
    )
    grad_query_rows = (
        q_scale
        * (inner_q - query_rows * q_scale * q_scale * (inner_sums[0][:, None] / model_width))
    ).astype(jnp.bfloat16)
    grad_key_rows = (
        k_scale * (inner_k - key_rows * k_scale * k_scale * (inner_sums[1][:, None] / model_width))
    ).astype(jnp.bfloat16)
    grad_value_rows = grad_values.reshape(group_len, -1).astype(jnp.bfloat16)
    head_grads = jnp.concatenate([grad_query_rows, grad_key_rows, grad_value_rows], axis=1)
    mixer_grad = jnp.einsum(
        "td,ti->di", group_rows, head_grads, preferred_element_type=jnp.float32
    ).astype(jnp.bfloat16)

    def input_term(start, length):
        from_q = jnp.einsum(
            "ti,di->td", grad_query_rows, w_query, preferred_element_type=jnp.float32
        )
        from_k = jnp.einsum("ti,di->td", grad_key_rows, w_key, preferred_element_type=jnp.float32)
        from_v = jnp.einsum(
            "ti,di->td", grad_value_rows, w_value, preferred_element_type=jnp.float32
        )
        return (from_q + from_k + from_v).astype(jnp.bfloat16)

    grad_first = share_rows(dense and 5, input_term, tok_count).astype(jnp.float32)
    attn_gain_grad = jnp.sum(grad_first * normed_one, axis=0)
    grad_normed_one = grad_first * attn_gain
    grad_x = grad_mid + scale_one * (
        grad_normed_one - normed_one * jnp.mean(grad_normed_one * normed_one, axis=1, keepdims=True)
    )
    narrow = (mixer_grad, out_grad.astype(jnp.bfloat16))
    gains = jnp.concatenate([attn_gain_grad[None], mlp_gain_grad[None], router_grad], axis=0)
    head_gains = jnp.stack([q_gain_grad, k_gain_grad])
    if dense:
        narrow, gains, head_gains = sum_grads(narrow, gains, head_gains, nz)
    else:
        narrow = lax.psum(narrow, "expert")
        head_gains = lax.psum(head_gains, "expert")
        gains = lax.psum(gains, ("fsdp", "expert"))
    wide = tuple(jnp.split(narrow[0], 3, axis=1)) + (narrow[1],)
    mixer = tuple(g.astype(jnp.float32) for g in wide) + (head_gains[0], head_gains[1])
    return (
        block_output,
        grad_x[None],
        mixer[0],
        mixer[1],
        mixer[2],
        mixer[3],
        mixer[4],
        mixer[5],
        gains[0],
        gains[1],
        gains[2:].T,
        grad_gate_w,
        grad_up_w,
        grad_down_w,
    )


def solution(mesh):
    placed = (
        P("expert", "fsdp", None),
        P("expert", "fsdp", None),
        P(None, "fsdp"),
        P(None, "fsdp"),
        P(None, "fsdp"),
        P("fsdp", None),
        P("fsdp"),
        P("fsdp"),
        P(),
        P(),
        P(),
        P("expert", None, "fsdp"),
        P("expert", None, "fsdp"),
        P("expert", "fsdp", None),
        P("expert", "fsdp"),
        P("expert", "fsdp", None),
        P(),
    )
    return jax.shard_map(
        on_device,
        mesh=mesh,
        in_specs=placed,
        out_specs=(
            P("expert", "fsdp", None),
            P("expert", "fsdp", None),
            P(None, "fsdp"),
            P(None, "fsdp"),
            P(None, "fsdp"),
            P("fsdp", None),
            P("fsdp"),
            P("fsdp"),
            P(),
            P(),
            P(),
            P("expert", None, "fsdp"),
            P("expert", None, "fsdp"),
            P("expert", "fsdp", None),
        ),
        check_vma=False,
    )
```

```python
import functools

import jax
import jax.numpy as jnp
from jax import lax
from jax.experimental import pallas as pl
from jax.experimental.pallas import tpu as pltpu
from jax.sharding import PartitionSpec as P

HEAD_DIM = 128
TOP = 8


epsilon = 1e-05
rope_base = 10000.0
precise = lax.Precision.HIGHEST


MESH = pl.DeviceIdType.MESH
DMA = pltpu.SemaphoreType.DMA


class Place:
    def __init__(self):
        self.f, self.e = lax.axis_index("fsdp"), lax.axis_index("expert")
        self.c, self.z = self.e % 2, self.e // 2
        self.fx = self.f + 1 - 2 * (self.f % 2)
        self.fy = (self.f + 2) % 4
        self.fd = 3 - self.f
        self.pe = self.e + 1 - 2 * self.c


def send(src, dst, send_sem, recv_sem, f, e):
    return pltpu.make_async_remote_copy(
        src_ref=src,
        dst_ref=dst,
        send_sem=send_sem,
        recv_sem=recv_sem,
        device_id={"fsdp": f, "expert": e},
        device_id_type=MESH,
    )


def greet(peers, line=None):
    barrier = pltpu.get_barrier_semaphore()

    def hello(f, e):
        pl.semaphore_signal(
            barrier, inc=1, device_id={"fsdp": f, "expert": e}, device_id_type=MESH
        )

    for f, e in peers:
        hello(f, e)
    if line is not None:
        at, nz = line
        for step in range(1, nz):
            hello(at.f, 2 * ((at.z + step) % nz) + at.c)
        pl.semaphore_wait(barrier, len(peers) + nz - 1)
    else:
        pl.semaphore_wait(barrier, len(peers))


class SmallGather:
    sems = staticmethod(
        lambda nz: [DMA((nz,)), DMA((nz,)), DMA((4,)), DMA((4,))]
    )

    def __init__(self, at, nz, own, out, sems):
        self.at, self.nz, self.own, self.out = at, nz, own, out
        self.ls, self.lr, self.ss, self.sr = sems

    def line(self, step):
        at = self.at
        z = (at.z + step) % self.nz
        back = (at.z + self.nz - step) % self.nz
        slot = self.out.at[at.c, at.f]
        to = send(self.own, slot.at[at.z], self.ls.at[step], self.lr.at[step], at.f, 2 * z + at.c)
        come = send(self.own, slot.at[back], self.ls.at[step], self.lr.at[step], at.f, 2 * z + at.c)
        return to, come

    def plane(self, i):
        at, out = self.at, self.out
        f, to_f = ((at.f, at.fx), (at.f, at.fy), (at.fx, at.fy))[i]
        slot = out.at[at.c, f]
        return send(slot, slot, self.ss.at[i], self.sr.at[i], to_f, at.e)

    def pair(self):
        at = self.at
        slot = self.out.at[at.c]
        return send(slot, slot, self.ss.at[3], self.sr.at[3], at.f, at.pe)

    def stage(self, i):
        at = self.at
        if i == 0:
            for step in range(1, self.nz):
                self.line(step)[0].start()
            self.out[at.c, at.f, at.z] = self.own[...]
        elif i == 1:
            for step in range(1, self.nz):
                self.line(step)[1].wait_recv()
            self.plane(0).start()
            self.plane(1).start()
        elif i == 2:
            self.plane(0).wait_recv()
            self.plane(2).start()
        elif i == 3:
            self.plane(1).wait_recv()
            self.plane(2).wait_recv()
            self.pair().start()
        elif i == 4:
            self.pair().wait_recv()
            self.pair().wait_send()
            for step in range(1, self.nz):
                self.line(step)[0].wait_send()
            for k in range(3):
                self.plane(k).wait_send()


class SmallScatter:
    sems = staticmethod(lambda nz: [DMA((nz,)), DMA((nz,)), DMA((4,)), DMA((4,))])
    scratch = staticmethod(
        lambda nz, shape: [
            pltpu.VMEM((4, nz, *shape), jnp.float32),
            pltpu.VMEM((4, nz, *shape), jnp.float32),
            pltpu.VMEM((3, nz, *shape), jnp.float32),
            pltpu.VMEM((nz, *shape), jnp.float32),
        ]
    )

    def __init__(self, at, nz, part, out, scratch, sems):
        self.at, self.nz, self.part, self.out = at, nz, part, out
        self.acc, self.pb, self.xy, self.zb = scratch
        self.ls, self.lr, self.ss, self.sr = sems

    def pair(self):
        at = self.at
        return send(
            self.part.at[1 - at.c], self.pb, self.ss.at[0], self.sr.at[0], at.f, at.pe
        )

    def plane(self, i):
        at = self.at
        f, to_f = ((at.fx, at.fx), (at.fd, at.fx), (at.fy, at.fy))[i]
        return send(
            self.acc.at[f], self.xy.at[i], self.ss.at[1 + i], self.sr.at[1 + i], to_f, at.e
        )

    def line(self, step):
        at = self.at
        z = (at.z + step) % self.nz
        return send(
            self.acc.at[at.f, z], self.zb.at[step], self.ls.at[step], self.lr.at[step], at.f, 2 * z + at.c
        )

    def stage(self, i):
        at, acc, xy = self.at, self.acc, self.xy
        if i == 0:
            self.pair().start()
        elif i == 1:
            self.pair().wait_recv()
            acc[...] = self.part[at.c] + self.pb[...]
            self.plane(0).start()
            self.plane(1).start()
        elif i == 2:
            self.plane(0).wait_recv()
            self.plane(1).wait_recv()
            acc[at.fy] = acc[at.fy] + xy[1]
            self.plane(2).start()
            acc[at.f] = acc[at.f] + xy[0]
        elif i == 3:
            self.plane(2).wait_recv()
            acc[at.f] = acc[at.f] + xy[2]
            for step in range(1, self.nz):
                self.line(step).start()
        elif i == 4:
            total = acc[at.f, at.z]
            for step in range(1, self.nz):
                self.line(step).wait_recv()
                total = total + self.zb[step]
            self.out[...] = total
            self.pair().wait_send()
            for k in range(3):
                self.plane(k).wait_send()
            for step in range(1, self.nz):
                self.line(step).wait_send()


def take(sequence, count):
    return [next(sequence) for _ in range(count)]


NT = (((1,), (1,)), ((), ()))
TN = (((0,), (0,)), ((), ()))


def above(a, b):
    return (a - b + 63) // 64


def near_first(at, nz, s):
    right = above(2 * at.z, nz - 1)
    alternate = at.z - right * (2 * at.z - (nz - 1))
    turn = at.z + (s + 1) // 2 * (1 - 2 * (s % 2))
    rest = s + right * (nz - 1 - 2 * s)
    return turn + above(s, 2 * alternate) * (rest - turn)


def gather_act_kernel(nz, own, own_small, w_gate, w_up, w_down, grads, out, acts, terms, gates, xb, cb, ab, load_x, load_c, store, own_sem, zr, zs, xr, xs, yr, ys, dr, xf, yf, pr, ps, *small_sems):
    at = Place()
    rows, width = own.shape
    experts = own_small.shape[0]
    local, _, hidden = w_gate.shape
    half = rows // 2
    halves = (pl.ds(0, half), pl.ds(half, half))
    small = SmallGather(at, nz, own_small, gates, small_sems)
    greet([(at.fx, at.e), (at.fy, at.e), (at.f, at.pe)], (at, nz))
    keep = pltpu.make_async_copy(own, out.at[at.f, at.e], own_sem)
    keep.start()
    small.stage(0)
    places = (at.f, at.fx, at.fy, at.fd)

    def up(z):
        ref = out.at[at.f, 2 * z + at.c]
        return send(ref, ref, zs.at[0, z], zr.at[z], at.f, at.e + 2)

    def down(z):
        ref = out.at[at.f, 2 * z + at.c]
        return send(ref, ref, zs.at[1, z], zr.at[z], at.f, at.e - 2)

    def to_x(z, h):
        ref = out.at[at.f, 2 * z + at.c, halves[h]]
        return send(ref, ref, xs.at[h, z], xr.at[h, z], at.fx, at.e)

    def to_y(z, h):
        ref = out.at[at.f, 2 * z + at.c, halves[h]]
        return send(ref, ref, ys.at[h, z], yr.at[h, z], at.fy, at.e)

    def x_on(z):
        ref = out.at[at.fx, 2 * z + at.c, halves[0]]
        return send(ref, ref, yf.at[z], dr.at[0, z], at.fy, at.e)

    def y_on(z):
        ref = out.at[at.fy, 2 * z + at.c, halves[1]]
        return send(ref, ref, xf.at[z], dr.at[1, z], at.fx, at.e)

    def to_p(f, z, h):
        ref = out.at[f, 2 * z + at.c, halves[h]]
        return send(ref, ref, ps.at[f, z, h], pr.at[f, z, h], at.f, at.pe)

    def line_step(z):
        pl.when(z != at.z)(lambda: up(z).wait_recv())
        pl.when((z <= at.z) & (at.z < nz - 1))(lambda: up(z).start())
        pl.when((z >= at.z) & (at.z > 0))(lambda: down(z).start())
        to_x(z, 0).start()
        to_y(z, 1).start()
        to_x(z, 1).start()
        to_y(z, 0).start()
        for h in range(2):
            to_p(at.f, z, h).start()

    def plane_step(z):
        to_x(z, 0).wait_recv()
        x_on(z).start()
        to_y(z, 1).wait_recv()
        y_on(z).start()
        to_p(at.fx, z, 0).start()
        to_p(at.fy, z, 1).start()
        to_x(z, 1).wait_recv()
        to_p(at.fx, z, 1).start()
        to_y(z, 0).wait_recv()
        to_p(at.fy, z, 0).start()

    def diag_step(z):
        x_on(z).wait_recv()
        to_p(at.fd, z, 0).start()
        y_on(z).wait_recv()
        to_p(at.fd, z, 1).start()

    def loads(q, z):
        pair = pl.ds(2 * z, 2)
        return (
            pltpu.make_async_copy(out.at[places[q], pair], xb.at[q], load_x.at[q]),
            pltpu.make_async_copy(grads.at[places[q], pair], cb.at[q], load_c.at[q]),
        )

    def stores(q, z):
        pair = pl.ds(2 * z, 2)
        return [
            pltpu.make_async_copy(ab.at[q, k], acts.at[k, places[q], pair], store.at[q, k])
            for k in range(3)
        ]

    def fetch(q, z):
        for h in range(2):
            to_p(places[q], z, h).wait_recv()
        for copy in loads(q, z):
            copy.start()

    first = at.e * local
    expert_row = lax.broadcasted_iota(jnp.int32, (experts, hidden), 0)

    def work(q, z):
        for copy in loads(q, z):
            copy.wait()
        f = places[q]
        sums = [None, None]
        x = xb[q].reshape(2 * rows, width)
        c = cb[q].reshape(2 * rows, width)
        for j in range(local):
            pick = (expert_row == first + j).astype(jnp.float32)
            cols = pl.ds(j * hidden, hidden)
            g = jnp.dot(x, w_gate[j], preferred_element_type=jnp.float32)
            u = jnp.dot(x, w_up[j], preferred_element_type=jnp.float32)
            dh = lax.dot_general(c, w_down[j], NT, preferred_element_type=jnp.float32)
            sig = 1.0 / (1.0 + jnp.exp(-g))
            silu = g * sig
            h = silu * u
            prod = h * dh
            for t in range(2):
                part = slice(t * rows, (t + 1) * rows)
                gate = lax.dot_general(
                    gates[t, f, z], pick, TN, precision=precise, preferred_element_type=jnp.float32
                )
                mine = lax.dot_general(
                    pick, prod[part], NT, precision=precise, preferred_element_type=jnp.float32
                )
                sums[t] = mine if sums[t] is None else sums[t] + mine
                d = dh[part] * gate
                ab[q, 0, t, :, cols] = (
                    d * u[part] * sig[part] * (1.0 + g[part] * (1.0 - sig[part]))
                ).astype(jnp.bfloat16)
                ab[q, 1, t, :, cols] = (d * silu[part]).astype(jnp.bfloat16)
                ab[q, 2, t, :, cols] = (h[part] * gate).astype(jnp.bfloat16)
        for t in range(2):
            terms[t, f, z] = sums[t]
        for copy in stores(q, z):
            copy.start()

    keep.wait()

    def body(s, carry):
        def at_step(lag, run):
            pl.when((s >= lag) & (s < nz + lag))(lambda: run(near_first(at, nz, s - lag)))

        def free(q, lag):
            def run(z):
                for copy in stores(q, z):
                    copy.wait()

            at_step(lag + 1, run)

        at_step(0, line_step)
        for k in range(1, 5):
            pl.when(s == 0)(functools.partial(small.stage, k))
        at_step(1, lambda z: fetch(0, z))
        free(3, 4)
        at_step(4, lambda z: work(3, z))
        at_step(1, plane_step)
        at_step(2, lambda z: fetch(1, z))
        free(0, 1)
        at_step(1, lambda z: work(0, z))
        at_step(2, diag_step)
        at_step(2, lambda z: fetch(2, z))
        free(1, 2)
        at_step(2, lambda z: work(1, z))
        at_step(3, lambda z: fetch(3, z))
        free(2, 2)
        at_step(2, lambda z: work(2, z))
        return carry

    lax.fori_loop(0, nz + 5, body, 0)

    def finish(z, carry):
        pl.when((z <= at.z) & (at.z < nz - 1))(lambda: up(z).wait_send())
        pl.when((z >= at.z) & (at.z > 0))(lambda: down(z).wait_send())
        for h in range(2):
            to_x(z, h).wait_send()
            to_y(z, h).wait_send()
        x_on(z).wait_send()
        y_on(z).wait_send()
        for f in range(4):
            for h in range(2):
                to_p(f, z, h).wait_send()
        return carry

    lax.fori_loop(0, nz, finish, 0)


def gather_act(rows, small, w_gate, w_up, w_down, grads, nz, cid):
    r, c = rows.shape
    local, _, hidden = w_gate.shape
    wide = local * hidden
    hbm, vmem = pl.BlockSpec(memory_space=pl.ANY), pl.BlockSpec(memory_space=pltpu.VMEM)
    bf16 = jnp.bfloat16
    return pl.pallas_call(
        functools.partial(gather_act_kernel, nz),
        out_shape=(
            jax.ShapeDtypeStruct((4, 2 * nz, r, c), bf16),
            jax.ShapeDtypeStruct((3, 4, 2 * nz, r, wide), bf16),
            jax.ShapeDtypeStruct((2, 4, nz, *small.shape), jnp.float32),
        ),
        in_specs=[vmem] * 5 + [hbm],
        out_specs=(hbm, hbm, vmem),
        scratch_shapes=[
            pltpu.VMEM((2, 4, nz, *small.shape), jnp.float32),
            pltpu.VMEM((4, 2, r, c), bf16),
            pltpu.VMEM((4, 2, r, c), bf16),
            pltpu.VMEM((4, 3, 2, r, wide), bf16),
            DMA((4,)), DMA((4,)), DMA((4, 3)),
            DMA(()), DMA((nz,)), DMA((2, nz)), DMA((2, nz)), DMA((2, nz)), DMA((2, nz)), DMA((2, nz)),
            DMA((2, nz)), DMA((nz,)), DMA((nz,)), DMA((4, nz, 2)), DMA((4, nz, 2)),
            *SmallGather.sems(nz),
        ],
        compiler_params=pltpu.CompilerParams(
            collective_id=cid, has_side_effects=True, vmem_limit_bytes=50 << 20
        ),
        cost_estimate=pl.CostEstimate(flops=0, bytes_accessed=240 << 20, transcendentals=0),
        name="gather_act",
    )(rows, small, w_gate, w_up, w_down, grads)


def add_rows(dst, dst_rows, parts):
    start, count = dst_rows

    def body(i, carry):
        r = pl.multiple_of(i * 16, 16)
        total = None
        for ref, offset in parts:
            piece = ref[pl.ds(offset + r, 16), :].astype(jnp.float32)
            total = piece if total is None else total + piece
        dst[pl.ds(start + r, 16), :] = total.astype(dst.dtype)
        return carry

    lax.fori_loop(0, count // 16, body, 0)


def scatter_plan(at, nz, part, out, refs):
    acc, pb, xh, yh, xf, yf, zu, zd, ls, pr, ps, xhs, xhr, yhs, yhr, xs, xr, ys, yr, us, ur, ds_, dr = refs
    rows = out.shape[0]
    half = rows // 2
    lo, hi = pl.ds(0, half), pl.ds(half, half)

    def place(s):
        return near_first(at, nz, nz - 1 - s)

    def load(f, z):
        return pltpu.make_async_copy(part.at[f, 2 * z + at.c], acc.at[f, z], ls.at[f, z])

    def to_p(f, z):
        return send(part.at[f, 2 * z + 1 - at.c], pb.at[f, z], ps.at[f, z], pr.at[f, z], at.f, at.pe)

    def start_step(s):
        z = place(s)
        for f in (at.fd, at.fx, at.fy, at.f):
            load(f, z).start()
            to_p(f, z).start()

    def half_x(z):
        return send(acc.at[at.fd, z, lo], xh.at[z], xhs.at[z], xhr.at[z], at.fx, at.e)

    def half_y(z):
        return send(acc.at[at.fd, z, hi], yh.at[z], yhs.at[z], yhr.at[z], at.fy, at.e)

    def full_x(z):
        return send(acc.at[at.fx, z], xf.at[z], xs.at[z], xr.at[z], at.fx, at.e)

    def full_y(z):
        return send(acc.at[at.fy, z], yf.at[z], ys.at[z], yr.at[z], at.fy, at.e)

    def go_up(z):
        return send(acc.at[at.f, z], zu.at[z], us.at[z], ur.at[z], at.f, at.e + 2)

    def go_down(z):
        return send(acc.at[at.f, z], zd.at[z], ds_.at[z], dr.at[z], at.f, at.e - 2)

    def diag_step(s):
        z = place(s)
        load(at.fd, z).wait()
        to_p(at.fd, z).wait_recv()
        a, b = acc.at[at.fd, z], pb.at[at.fd, z]
        add_rows(a, (0, half), [(a, 0), (b, 0)])
        half_x(z).start()
        add_rows(a, (half, half), [(a, half), (b, half)])
        half_y(z).start()

    def plane_step(s):
        z = place(s)
        load(at.fx, z).wait()
        to_p(at.fx, z).wait_recv()
        a, b = acc.at[at.fx, z], pb.at[at.fx, z]
        half_y(z).wait_recv()
        add_rows(a, (0, half), [(a, 0), (b, 0)])
        add_rows(a, (half, half), [(a, half), (b, half), (yh.at[z], 0)])
        full_x(z).start()
        load(at.fy, z).wait()
        to_p(at.fy, z).wait_recv()
        half_x(z).wait_recv()
        a, b = acc.at[at.fy, z], pb.at[at.fy, z]
        add_rows(a, (0, half), [(a, 0), (b, 0), (xh.at[z], 0)])
        add_rows(a, (half, half), [(a, half), (b, half)])
        full_y(z).start()

    def line_step(s):
        z = place(s)
        load(at.f, z).wait()
        to_p(at.f, z).wait_recv()
        full_x(z).wait_recv()
        full_y(z).wait_recv()
        a = acc.at[at.f, z]
        four = [(a, 0), (pb.at[at.f, z], 0), (xf.at[z], 0), (yf.at[z], 0)]

        @pl.when(z > at.z)
        def _():
            @pl.when(at.z > 0)
            def _():
                go_up(z).wait_recv()
                add_rows(a, (0, rows), four + [(zu.at[z], 0)])

            pl.when(at.z == 0)(lambda: add_rows(a, (0, rows), four))
            go_up(z).start()

        @pl.when(z < at.z)
        def _():
            @pl.when(at.z < nz - 1)
            def _():
                go_down(z).wait_recv()
                add_rows(a, (0, rows), four + [(zd.at[z], 0)])

            pl.when(at.z == nz - 1)(lambda: add_rows(a, (0, rows), four))
            go_down(z).start()

        @pl.when(z == at.z)
        def _():
            add_rows(out, (0, rows), four)

            @pl.when(at.z > 0)
            def _():
                go_up(z).wait_recv()
                add_rows(out, (0, rows), [(out, 0), (zu.at[z], 0)])

            @pl.when(at.z < nz - 1)
            def _():
                go_down(z).wait_recv()
                add_rows(out, (0, rows), [(out, 0), (zd.at[z], 0)])

    def finish():
        def body(z, carry):
            for f in range(4):
                to_p(f, z).wait_send()
            half_x(z).wait_send()
            half_y(z).wait_send()
            full_x(z).wait_send()
            full_y(z).wait_send()
            pl.when(z > at.z)(lambda: go_up(z).wait_send())
            pl.when(z < at.z)(lambda: go_down(z).wait_send())
            return carry

        lax.fori_loop(0, nz, body, 0)

    return start_step, diag_step, plane_step, line_step, finish


def scatter_scratch(parts, nz):
    _, _, r, c = parts.shape

    def buf(*n):
        return pltpu.VMEM((*n, c), parts.dtype)

    return [
        buf(4, nz, r), buf(4, nz, r), buf(nz, r // 2), buf(nz, r // 2),
        buf(nz, r), buf(nz, r), buf(nz, r), buf(nz, r),
        DMA((4, nz)), DMA((4, nz)), DMA((4, nz)),
        *[DMA((nz,))] * 12,
    ]


def scatter_kernel(nz, part, part_small, out, out_small, *refs):
    at = Place()
    refs = iter(refs)
    start, diag, plane, line, finish = scatter_plan(at, nz, part, out, take(refs, 23))
    small = SmallScatter(at, nz, part_small, out_small, take(refs, 4), take(refs, 4))
    greet([(at.fx, at.e), (at.fy, at.e), (at.f, at.pe)], (at, nz))
    small.stage(0)
    for s in range(nz):
        start(s)

    def body(s, carry):
        pl.when(s < nz)(lambda: diag(s))
        pl.when((s >= 1) & (s < nz + 1))(lambda: plane(s - 1))
        pl.when(s >= 2)(lambda: line(s - 2))
        for k in range(1, 5):
            pl.when(s == k)(functools.partial(small.stage, k))
        return carry

    lax.fori_loop(0, nz + 2, body, 0)
    for k in range(nz + 2, 5):
        small.stage(k)
    finish()


def scatter_all(parts, small, nz, cid):
    _, _, r, c = parts.shape
    return pl.pallas_call(
        functools.partial(scatter_kernel, nz),
        out_shape=(
            jax.ShapeDtypeStruct((r, c), jnp.float32),
            jax.ShapeDtypeStruct(small.shape[-2:], jnp.float32),
        ),
        in_specs=[pl.BlockSpec(memory_space=pl.ANY), pl.BlockSpec(memory_space=pltpu.VMEM)],
        out_specs=(pl.BlockSpec(memory_space=pltpu.VMEM),) * 2,
        scratch_shapes=[
            *scatter_scratch(parts, nz),
            *SmallScatter.scratch(nz, small.shape[-2:]),
            *SmallScatter.sems(nz),
        ],
        compiler_params=pltpu.CompilerParams(
            collective_id=cid, has_side_effects=True, vmem_limit_bytes=50 << 20
        ),
        cost_estimate=pl.CostEstimate(flops=0, bytes_accessed=240 << 20, transcendentals=0),
        name="scatter_all",
    )(parts, small)


def square_gather_kernel(own, ids, out, out_ids, xs, xr, ys, yr, fs, fr, js, jr):
    at = Place()
    half = own.shape[0] // 2
    halves = (pl.ds(0, half), pl.ds(half, half))
    peers = [(at.fx, at.e), (at.fy, at.e), (at.fd, at.e)]
    greet(peers)

    def to_x(h):
        return send(own.at[halves[h]], out.at[at.f, halves[h]], xs.at[h], xr.at[h], at.fx, at.e)

    def to_y(h):
        return send(own.at[halves[h]], out.at[at.f, halves[h]], ys.at[h], yr.at[h], at.fy, at.e)

    x_ref, y_ref = out.at[at.fx, halves[0]], out.at[at.fy, halves[1]]
    x_on = send(x_ref, x_ref, fs.at[0], fr.at[0], at.fy, at.e)
    y_on = send(y_ref, y_ref, fs.at[1], fr.at[1], at.fx, at.e)
    notes = [
        send(ids, out_ids.at[at.f], js.at[k], jr.at[k], f, e) for k, (f, e) in enumerate(peers)
    ]
    to_x(0).start()
    to_y(1).start()
    for note in notes:
        note.start()
    to_x(1).start()
    to_y(0).start()
    out[at.f] = own[...]
    out_ids[at.f] = ids[...]
    to_x(0).wait_recv()
    x_on.start()
    to_y(1).wait_recv()
    y_on.start()
    to_x(1).wait()
    to_y(0).wait()
    for note in notes:
        note.wait()
    to_x(0).wait_send()
    to_y(1).wait_send()
    x_on.wait()
    y_on.wait()


def square_gather(rows, ids, cid):
    r, c = rows.shape
    vmem = pl.BlockSpec(memory_space=pltpu.VMEM)
    return pl.pallas_call(
        square_gather_kernel,
        out_shape=(
            jax.ShapeDtypeStruct((4, r, c), rows.dtype),
            jax.ShapeDtypeStruct((4, *ids.shape), ids.dtype),
        ),
        in_specs=[vmem] * 2,
        out_specs=(vmem,) * 2,
        scratch_shapes=[DMA((2,))] * 6 + [DMA((3,))] * 2,
        compiler_params=pltpu.CompilerParams(collective_id=cid, has_side_effects=True),
        cost_estimate=pl.CostEstimate(flops=0, bytes_accessed=60 << 20, transcendentals=0),
        name="square_gather",
    )(rows, ids)


def square_scatter_kernel(part, out, xh, yh, xf, yf, ss, rs):
    at = Place()
    rows = out.shape[0]
    half = rows // 2
    lo, hi = pl.ds(0, half), pl.ds(half, half)
    greet([(at.fx, at.e), (at.fy, at.e)])

    def to_x(k, src, dst):
        return send(src, dst, ss.at[k], rs.at[k], at.fx, at.e)

    def to_y(k, src, dst):
        return send(src, dst, ss.at[k], rs.at[k], at.fy, at.e)

    copies = [
        to_x(0, part.at[at.fd, lo], xh),
        to_y(1, part.at[at.fd, hi], yh),
        to_x(2, part.at[at.fx, lo], xf.at[lo]),
        to_y(3, part.at[at.fy, hi], yf.at[hi]),
        to_x(4, yh, xf.at[hi]),
        to_y(5, xh, yf.at[lo]),
    ]
    for copy in copies[:4]:
        copy.start()
    copies[1].wait_recv()
    add_rows(yh, (0, half), [(yh, 0), (part.at[at.fx], half)])
    copies[4].start()
    copies[0].wait_recv()
    add_rows(xh, (0, half), [(xh, 0), (part.at[at.fy], 0)])
    copies[5].start()
    copies[2].wait_recv()
    copies[5].wait_recv()
    copies[3].wait_recv()
    copies[4].wait_recv()
    add_rows(out, (0, rows), [(part.at[at.f], 0), (xf, 0), (yf, 0)])
    for copy in copies:
        copy.wait_send()


def square_scatter(parts, cid):
    _, r, c = parts.shape
    vmem = pl.BlockSpec(memory_space=pltpu.VMEM)

    def buf(n):
        return pltpu.VMEM((n, c), parts.dtype)

    return pl.pallas_call(
        square_scatter_kernel,
        out_shape=jax.ShapeDtypeStruct((r, c), jnp.float32),
        in_specs=[vmem],
        out_specs=vmem,
        scratch_shapes=[buf(r // 2), buf(r // 2), buf(r), buf(r), DMA((6,)), DMA((6,))],
        compiler_params=pltpu.CompilerParams(collective_id=cid, has_side_effects=True),
        cost_estimate=pl.CostEstimate(flops=0, bytes_accessed=60 << 20, transcendentals=0),
        name="square_scatter",
    )(parts)


def square_sum_kernel(own, out, got, ss, rs):
    at = Place()
    peers = [(at.fx, at.e), (at.fy, at.e), (at.fd, at.e)]
    greet(peers)
    copies = [send(own, got.at[k], ss.at[k], rs.at[k], f, e) for k, (f, e) in enumerate(peers)]
    for copy in copies:
        copy.start()
    for copy in copies:
        copy.wait()
    out[...] = (own[...] + got[0]) + (got[1] + got[2])


def square_sum(values, cid):
    flat = values.reshape(8, -1)
    vmem = pl.BlockSpec(memory_space=pltpu.VMEM)
    return pl.pallas_call(
        square_sum_kernel,
        out_shape=jax.ShapeDtypeStruct(flat.shape, jnp.float32),
        in_specs=[vmem],
        out_specs=vmem,
        scratch_shapes=[pltpu.VMEM((3, *flat.shape), jnp.float32), DMA((3,)), DMA((3,))],
        compiler_params=pltpu.CompilerParams(collective_id=cid, has_side_effects=True),
        cost_estimate=pl.CostEstimate(flops=0, bytes_accessed=10 << 20, transcendentals=0),
        name="square_sum",
    )(flat).reshape(values.shape)


class product_plan:
    def __init__(self, inputs, outs, refs):
        self.rows, self.acts, self.grads = inputs
        self.outs = outs
        self.wide_acc, self.down_acc, self.xw, self.aw, self.load_sem, self.store_sem = refs
        self.units = self.rows.shape[0]
        self.local = self.outs[0].shape[0]
        self.per_pass = self.units // 2
        self.steps = self.per_pass * (self.local + 1)

    def loads(self, i, k, p):
        u = (i - p * self.per_pass) * 2 + k
        hidden = self.outs[0].shape[2]
        sem = self.load_sem.at[k]
        if p == self.local:
            return [
                pltpu.make_async_copy(self.grads.at[u], self.xw.at[k], sem.at[0]),
                pltpu.make_async_copy(self.acts.at[2, u], self.aw.at[k], sem.at[1]),
            ]
        cols = pl.ds(p * hidden, hidden)
        return [
            pltpu.make_async_copy(self.rows.at[u], self.xw.at[k], sem.at[0]),
            pltpu.make_async_copy(self.acts.at[0, u, :, cols], self.aw.at[k, :, pl.ds(0, hidden)], sem.at[1]),
            pltpu.make_async_copy(
                self.acts.at[1, u, :, cols], self.aw.at[k, :, pl.ds(hidden, hidden)], sem.at[2]
            ),
        ]

    def on_pass(self, i, run):
        for p in range(self.local + 1):
            pl.when((i >= p * self.per_pass) & (i < (p + 1) * self.per_pass))(functools.partial(run, p))

    def start(self):
        for k in range(2):
            for copy in self.loads(0, k, 0):
                copy.start()

        for acc in (*[self.wide_acc.at[p] for p in range(self.local)], self.down_acc):
            def body(r, carry, acc=acc):
                acc[pl.ds(r * 8, 8), :] = jnp.zeros((8, acc.shape[1]), jnp.float32)
                return carry

            lax.fori_loop(0, acc.shape[0] // 8, body, 0)

    def step(self, i):
        tile = 512

        def run(p):
            for k in range(2):
                for copy in self.loads(i, k, p):
                    copy.wait()
                a = self.aw[k]
                for t in range(self.xw.shape[2] // tile):
                    cols = pl.ds(t * tile, tile)
                    x = self.xw[k, :, cols]
                    if p == self.local:
                        self.down_acc[:, cols] += lax.dot_general(
                            a, x, TN, preferred_element_type=jnp.float32
                        )
                    else:
                        self.wide_acc[p, cols, :] += lax.dot_general(
                            x, a, TN, preferred_element_type=jnp.float32
                        )

                def more(q, k=k):
                    for copy in self.loads(i + 1, k, q):
                        copy.start()

                self.on_pass(i + 1, more)

            @pl.when(i == (p + 1) * self.per_pass - 1)
            def _():
                for copy in self.stores(p):
                    copy.start()

        self.on_pass(i, run)

    def stores(self, p):
        hidden = self.outs[0].shape[2]
        if p == self.local:
            return [pltpu.make_async_copy(self.down_acc, self.outs[2], self.store_sem.at[p, 0])]
        acc = self.wide_acc.at[p]
        return [
            pltpu.make_async_copy(
                acc.at[:, pl.ds(k * hidden, hidden)], self.outs[k].at[p], self.store_sem.at[p, k]
            )
            for k in range(2)
        ]

    def finish(self):
        for p in range(self.local + 1):
            for copy in self.stores(p):
                copy.wait()


def line_sum_kernel(nz, counts, *refs):
    at = Place()
    refs = iter(refs)
    n = len(counts)
    parts, part_small, rows_part, inputs = take(refs, n), next(refs), next(refs), take(refs, 3)
    outs, out_small, rows_out, grads = take(refs, n), next(refs), next(refs), take(refs, 3)
    begin, diag, plane, line, close = scatter_plan(at, nz, rows_part, rows_out, take(refs, 23))
    product = product_plan(inputs, grads, take(refs, 6))
    bufs = [take(refs, 5) for _ in range(n)]
    sems = [take(refs, 12) for _ in range(n)]
    own_small = next(refs)
    scatter_small = SmallScatter(at, nz, part_small, own_small, take(refs, 4), take(refs, 4))
    gather_small = SmallGather(at, nz, own_small, out_small, take(refs, 4))
    greet([(at.fx, at.e), (at.fy, at.e), (at.f, at.pe)], (at, nz))
    scatter_small.stage(0)
    total = sum(counts)
    last = nz - 1

    class Piece:
        def __init__(self, k, p):
            self.p, self.part, self.out = p, parts[k], outs[k]
            self.acc, self.pb, self.zu, self.zd, self.mine = bufs[k]
            self.sems = sems[k]
            self.r = self.acc.shape[2]

        def load(self):
            p = self.p
            return pltpu.make_async_copy(self.part.at[p, at.c], self.acc.at[p], self.sems[0].at[p])

        def to_p(self):
            p, (_, s, r, *_rest) = self.p, self.sems
            return send(self.part.at[p, 1 - at.c], self.pb.at[p], s.at[p], r.at[p], at.f, at.pe)

        def go_up(self, z):
            p, s, r = self.p, self.sems[3], self.sems[4]
            return send(self.acc.at[p, z], self.zu.at[p, z], s.at[p, z], r.at[p, z], at.f, at.e + 2)

        def go_down(self, z):
            p, s, r = self.p, self.sems[5], self.sems[6]
            return send(self.acc.at[p, z], self.zd.at[p, z], s.at[p, z], r.at[p, z], at.f, at.e - 2)

        def res(self, z, way):
            p, s, r = self.p, self.sems[7], self.sems[8]
            ref = self.out.at[p, at.c, z]
            return send(ref, ref, s.at[way, p, z], r.at[p, z], at.f, at.e + 2 - 4 * way)

        def res_p(self, z):
            p, s, r = self.p, self.sems[9], self.sems[10]
            ref = self.out.at[p, at.c, z]
            return send(ref, ref, s.at[p, z], r.at[p, z], at.f, at.pe)

        def keep(self):
            p = self.p
            return pltpu.make_async_copy(self.mine.at[p], self.out.at[p, at.c, at.z], self.sems[11].at[p])

    def piece(q, run, when=True):
        low = 0
        for k, count in enumerate(counts):
            @pl.when((q >= low) & (q < low + count) & when)
            def _(k=k, low=low):
                run(Piece(k, q - low))

            low += count

    def start(it):
        it.load().start()
        it.to_p().start()

    piece(0, start)
    begin(0)
    piece(1, start)
    product.start()

    def halve(it):
        it.load().wait()
        it.to_p().wait_recv()
        p = it.p

        def body(z, carry):
            a = it.acc.at[p, z]
            add_rows(a, (0, it.r), [(a, 0), (it.pb.at[p, z], 0)])
            return carry

        lax.fori_loop(0, nz, body, 0)

    def rise(it):
        p = it.p

        def body(i, carry):
            z = last - i

            @pl.when(z > at.z)
            def _():
                a = it.acc.at[p, z]

                @pl.when(at.z > 0)
                def _():
                    it.go_up(z).wait_recv()
                    add_rows(a, (0, it.r), [(a, 0), (it.zu.at[p, z], 0)])

                it.go_up(z).start()

            return carry

        lax.fori_loop(0, last, body, 0)

    def sink(it):
        p = it.p

        def body(z, carry):
            @pl.when(z < at.z)
            def _():
                a = it.acc.at[p, z]

                @pl.when(at.z < last)
                def _():
                    it.go_down(z).wait_recv()
                    add_rows(a, (0, it.r), [(a, 0), (it.zd.at[p, z], 0)])

                it.go_down(z).start()

            return carry

        lax.fori_loop(0, last, body, 0)

    def settle(it):
        p, z = it.p, at.z
        pl.when(z > 0)(lambda: it.go_up(z).wait_recv())
        pl.when(z < last)(lambda: it.go_down(z).wait_recv())
        a, dst = (it.acc.at[p, z], 0), it.mine.at[p]
        up, down = (it.zu.at[p, z], 0), (it.zd.at[p, z], 0)
        pl.when((z > 0) & (z < last))(lambda: add_rows(dst, (0, it.r), [a, up, down]))
        pl.when(z == 0)(lambda: add_rows(dst, (0, it.r), [a, down]))
        pl.when(z == last)(lambda: add_rows(dst, (0, it.r), [a, up]))
        it.keep().start()

    def tell(it):
        z = at.z
        it.keep().wait()
        pl.when(z < last)(lambda: it.res(z, 0).start())
        pl.when(z > 0)(lambda: it.res(z, 1).start())
        it.res_p(z).start()

    def pass_up(it, z):
        it.res(z, 0).wait_recv()
        pl.when(at.z < last)(lambda: it.res(z, 0).start())
        it.res_p(z).start()

    def pass_down(it, z):
        it.res(z, 0).wait_recv()
        pl.when(at.z > 0)(lambda: it.res(z, 1).start())
        it.res_p(z).start()

    def body(i, carry):
        piece(i + 2, start)
        s, turn = i // 5, i % 5
        pl.when((turn == 0) & (s + 1 < nz))(lambda: begin(s + 1))
        pl.when((turn == 0) & (s < nz))(lambda: diag(s))
        pl.when((turn == 2) & (s < nz))(lambda: plane(s))
        pl.when((turn == 3) & (s >= 1) & (s < nz + 1))(lambda: line(s - 1))
        piece(i, halve)
        piece(i - at.z, rise, at.z < last)
        piece(i - (last - at.z), sink, at.z > 0)
        piece(i - nz, settle)
        piece(i - nz, tell)
        for d in range(1, nz):
            piece(i - nz - d, functools.partial(pass_up, z=at.z - d), at.z >= d)
            piece(i - nz - d, functools.partial(pass_down, z=at.z + d), at.z + d <= last)
        for s in range(1, 5):
            pl.when(i == s)(functools.partial(scatter_small.stage, s))
        for s in range(5):
            pl.when(i == 5 + s)(functools.partial(gather_small.stage, s))
        product.step(i)
        return carry

    steps = max(total + 2 * nz - 1, 5 * nz + 4, product.steps)
    lax.fori_loop(0, steps, body, 0)
    product.finish()

    def finish(q, carry):
        def run(it):
            it.to_p().wait_send()

            def one(z, carry):
                pl.when(z > at.z)(lambda: it.go_up(z).wait_send())
                pl.when(z < at.z)(lambda: it.go_down(z).wait_send())
                pl.when((z <= at.z) & (at.z < last))(lambda: it.res(z, 0).wait_send())
                pl.when((z >= at.z) & (at.z > 0))(lambda: it.res(z, 1).wait_send())
                it.res_p(z).wait_send()
                it.res_p(z).wait_recv()
                return carry

            lax.fori_loop(0, nz, one, 0)

        piece(q, run)
        return carry

    lax.fori_loop(0, total, finish, 0)
    close()


def line_sum(parts, small, rows, inputs, local, nz, cid):
    counts = tuple(p.shape[0] for p in parts)
    units, unit, width = inputs[0].shape
    wide = inputs[1].shape[3]
    scratch, sems = [], []
    for p in parts:
        n, _, _, r, c = p.shape

        def buf(*lead):
            return pltpu.VMEM((*lead, r, c), p.dtype)

        scratch += [buf(n, nz), buf(n, nz), buf(n, nz), buf(n, nz), buf(n)]
        each, line = DMA((n,)), DMA((n, nz))
        sems += [each, each, each, line, line, line, line, DMA((2, n, nz)), line, line, line, each]
    hbm, vmem = pl.BlockSpec(memory_space=pl.ANY), pl.BlockSpec(memory_space=pltpu.VMEM)
    return pl.pallas_call(
        functools.partial(line_sum_kernel, nz, counts),
        out_shape=(
            *(jax.ShapeDtypeStruct(p.shape, p.dtype) for p in parts),
            jax.ShapeDtypeStruct(small.shape, jnp.float32),
            jax.ShapeDtypeStruct(rows.shape[2:], jnp.float32),
            jax.ShapeDtypeStruct((local, width, wide // local), jnp.float32),
            jax.ShapeDtypeStruct((local, width, wide // local), jnp.float32),
            jax.ShapeDtypeStruct((wide, width), jnp.float32),
        ),
        in_specs=[hbm] * len(parts) + [vmem, hbm] + [hbm] * 3,
        out_specs=(*[hbm] * len(parts), vmem, vmem, *[hbm] * 3),
        scratch_shapes=[
            *scatter_scratch(rows, nz),
            pltpu.VMEM((local, width, 2 * wide // local), jnp.float32),
            pltpu.VMEM((wide, width), jnp.float32),
            pltpu.VMEM((2, unit, width), rows.dtype),
            pltpu.VMEM((2, unit, wide), rows.dtype),
            DMA((2, 3)), DMA((local + 1, 2)),
            *scratch, *sems, pltpu.VMEM(small.shape[-2:], jnp.float32),
            *SmallScatter.scratch(nz, small.shape[-2:]), *SmallScatter.sems(nz), *SmallGather.sems(nz),
        ],
        compiler_params=pltpu.CompilerParams(
            collective_id=cid, has_side_effects=True, vmem_limit_bytes=63 << 20
        ),
        cost_estimate=pl.CostEstimate(flops=0, bytes_accessed=300 << 20, transcendentals=0),
        name="line_sum",
    )(*parts, small, rows, *inputs)


def rope_tables(seg_ids, head_dim):
    length = seg_ids.shape[0]
    ordinal = lax.iota(jnp.int32, length)
    earlier = (seg_ids[:, None] == seg_ids[None, :]) & (ordinal[None, :] < ordinal[:, None])
    places = jnp.sum(earlier.astype(jnp.int32), axis=1).astype(jnp.float32)
    half_dim = head_dim // 2
    inv_freq = rope_base ** (
        -(lax.iota(jnp.int32, half_dim).astype(jnp.float32) * (2.0 / head_dim))
    )
    angles = places[:, None] * inv_freq[None, :]
    angles = jnp.concatenate([angles, angles], axis=1)
    return (jnp.cos(angles), jnp.sin(angles))


def rotate_half(values):
    half_dim = values.shape[-1] // 2
    return jnp.concatenate([-values[..., half_dim:], values[..., :half_dim]], axis=-1)


def rotate_back(values):
    half_dim = values.shape[-1] // 2
    return jnp.concatenate([values[..., half_dim:], -values[..., :half_dim]], axis=-1)


def apply_rope(values, cosine, sine_table):
    return values * cosine[:, None, :] + rotate_half(values) * sine_table[:, None, :]


def rope_grad(grads_in, cosine, sine_table):
    return grads_in * cosine[:, None, :] + rotate_back(grads_in * sine_table[:, None, :])


def across_heads(kernel, pair_sums):
    if kernel:
        return square_sum(jnp.stack(pair_sums), kernel)
    return lax.psum((pair_sums[0], pair_sums[1]), "fsdp")


def share_rows(kernel, term_fn, own_rows):
    if kernel:
        parts = term_fn(jnp.int32(0), own_rows * lax.axis_size("fsdp"))
        return square_scatter(parts.reshape(-1, own_rows, parts.shape[1]), kernel)
    return lax.psum_scatter(
        term_fn(jnp.int32(0), own_rows * lax.axis_size("fsdp")),
        "fsdp",
        scatter_dimension=0,
        tiled=True,
    )


def to_owner(block_rows):
    return lax.all_to_all(block_rows, "expert", split_axis=0, concat_axis=0, tiled=True)


def from_owner(block_rows):
    return lax.all_to_all(block_rows, "expert", split_axis=0, concat_axis=0, tiled=True)


def shard_gather(block_rows):
    return lax.all_gather(block_rows, "fsdp", axis=0, tiled=True)


def owner_sum(term_fn, sources):
    own_rows = sources // lax.axis_size("fsdp")
    return lax.psum_scatter(
        term_fn(jnp.int32(0), own_rows * lax.axis_size("fsdp")),
        "fsdp",
        scatter_dimension=0,
        tiled=True,
    )


def head_scores(q_heads, k_heads, allowed):
    scores = jnp.einsum(
        "thd,shd->hts", q_heads, k_heads, preferred_element_type=jnp.float32
    ) * HEAD_DIM ** (-0.5)
    return jnp.where(allowed[None], scores, -1e30)


def experts_by_slot(
    second_in, second_rows, cotangent, routes, capacity, w_router, w_gate, w_up, w_down
):
    tok_count, model_width = second_rows.shape
    experts = w_router.shape[1]
    local_experts = w_gate.shape[0]
    slot_count = tok_count * TOP * 3 // (2 * experts)
    pair_count = tok_count * TOP
    zero_row = jnp.zeros((1, model_width), jnp.bfloat16)
    logits = jnp.dot(second_rows, w_router, preferred_element_type=jnp.float32)
    chosen = routes
    expert_ids = lax.iota(jnp.int32, experts)
    chosen_hot = (chosen[:, :, None] == expert_ids[None, None, :]).astype(jnp.float32)
    routed = jnp.sum(chosen_hot * logits[:, None, :], axis=2)
    gate_wts = jax.nn.softmax(routed, axis=1)
    pair_hot = chosen_hot.reshape(pair_count, experts).astype(jnp.int32)
    earlier_hits = jnp.cumsum(pair_hot, axis=0) - pair_hot
    ranking = jnp.sum(earlier_hits * pair_hot, axis=1)
    cap_pair = jnp.sum(pair_hot * capacity[None, :], axis=1)
    is_kept = ranking < cap_pair
    pair_route = chosen.reshape(pair_count)
    slot_place = jnp.where(is_kept, pair_route * slot_count + ranking, experts * slot_count)
    pair_ids = lax.iota(jnp.int32, pair_count)
    slot_pair = (
        jnp.full((experts * slot_count,), pair_count, jnp.int32)
        .at[slot_place]
        .set(pair_ids, mode="drop")
    )
    padded = jnp.concatenate([second_rows, zero_row], axis=0)
    outgoing = padded[slot_pair // TOP].reshape(experts, slot_count, model_width)
    arrived = shard_gather(to_owner(outgoing))
    gate_w, up_w, down_w = (w_gate, w_up, w_down)
    owner_rows = arrived.reshape(-1, local_experts, slot_count, model_width)
    sources = owner_rows.shape[0]
    gate_act = jnp.einsum("sjcd,jdh->sjch", owner_rows, gate_w, preferred_element_type=jnp.float32)
    up_act = jnp.einsum("sjcd,jdh->sjch", owner_rows, up_w, preferred_element_type=jnp.float32)
    sig_gate = jax.nn.sigmoid(gate_act)
    silu_gate = gate_act * sig_gate
    hidden = (silu_gate * up_act).astype(jnp.bfloat16)

    def down_term(start, length):
        return jnp.einsum("sjch,jhd->sjcd", hidden, down_w, preferred_element_type=jnp.float32)

    produced = owner_sum(down_term, sources)
    returned = from_owner(produced.astype(jnp.bfloat16).reshape(-1, slot_count, model_width))
    slot_rows = jnp.concatenate(
        [returned.reshape(experts * slot_count, model_width), zero_row], axis=0
    )
    pair_rows = slot_rows[slot_place].reshape(tok_count, TOP, model_width).astype(jnp.float32)
    kept_mask = is_kept.reshape(tok_count, TOP).astype(jnp.float32)
    gate_kept = gate_wts * kept_mask
    moe_rows = jnp.sum(gate_kept[:, :, None] * pair_rows, axis=1)
    final_rows = second_in + moe_rows
    block_output = final_rows.astype(jnp.bfloat16)
    grad_out = cotangent.astype(jnp.float32)
    grad_gate_k = jnp.sum(pair_rows * grad_out[:, None, :], axis=2) * kept_mask
    grad_routed = gate_wts * (grad_gate_k - jnp.sum(gate_wts * grad_gate_k, axis=1, keepdims=True))
    grad_logits = jnp.sum(chosen_hot * grad_routed[:, :, None], axis=1)
    router_grad = jnp.dot(second_rows.astype(jnp.float32).T, grad_logits, precision=precise)
    grad_second = jnp.dot(grad_logits, w_router.astype(jnp.float32).T, precision=precise)
    pair_grads = (
        (gate_kept[:, :, None] * grad_out[:, None, :])
        .astype(jnp.bfloat16)
        .reshape(pair_count, model_width)
    )
    pair_grads = jnp.concatenate([pair_grads, zero_row], axis=0)
    slot_grads = pair_grads[slot_pair].reshape(experts, slot_count, model_width)
    grad_blocks = shard_gather(to_owner(slot_grads)).reshape(
        -1, local_experts, slot_count, model_width
    )
    grad_hidden = jnp.einsum(
        "sjcd,jhd->sjch", grad_blocks, down_w, preferred_element_type=jnp.float32
    )
    grad_down_w = jnp.einsum(
        "sjch,sjcd->jhd", hidden, grad_blocks, preferred_element_type=jnp.float32
    )
    grad_gate_in = (grad_hidden * up_act * sig_gate * (1.0 + gate_act * (1.0 - sig_gate))).astype(
        jnp.bfloat16
    )
    grad_up_in = (grad_hidden * silu_gate).astype(jnp.bfloat16)
    grad_gate_w = jnp.einsum(
        "sjcd,sjch->jdh", owner_rows, grad_gate_in, preferred_element_type=jnp.float32
    )
    grad_up_w = jnp.einsum(
        "sjcd,sjch->jdh", owner_rows, grad_up_in, preferred_element_type=jnp.float32
    )

    def back_term(start, length):
        from_gate = jnp.einsum(
            "sjch,jdh->sjcd", grad_gate_in, gate_w, preferred_element_type=jnp.float32
        )
        from_up = jnp.einsum("sjch,jdh->sjcd", grad_up_in, up_w, preferred_element_type=jnp.float32)
        return from_gate + from_up

    grad_slots = from_owner(
        owner_sum(back_term, sources).astype(jnp.bfloat16).reshape(-1, slot_count, model_width)
    )
    back_rows = jnp.concatenate(
        [grad_slots.reshape(experts * slot_count, model_width), zero_row], axis=0
    )
    grad_second = grad_second + jnp.sum(
        back_rows[slot_place].reshape(tok_count, TOP, model_width).astype(jnp.float32), axis=1
    )
    return block_output[None], grad_second, router_grad.T, (grad_gate_w, grad_up_w, grad_down_w)


def experts_dense(
    second_in, second_rows, cotangent, routes, capacity, w_router, w_gate, w_up, w_down
):
    tok_count = second_rows.shape[0]
    experts = w_router.shape[1]
    local_experts, model_width, hidden_here = w_gate.shape
    shards = lax.axis_size("fsdp")
    owners = lax.axis_size("expert")
    wide = local_experts * hidden_here
    logits = jnp.dot(second_rows, w_router, preferred_element_type=jnp.float32)
    expert_ids = lax.iota(jnp.int32, experts)
    named = jnp.any(routes[:, :, None] == expert_ids[None, None, :], axis=1)
    before = lax.iota(jnp.int32, tok_count)[None, :] < lax.iota(jnp.int32, tok_count)[:, None]
    ranking = jnp.dot(
        before.astype(jnp.bfloat16), named.astype(jnp.bfloat16), preferred_element_type=jnp.float32
    )
    kept = named & (ranking < capacity.astype(jnp.float32)[None, :])
    kept_mask = kept.astype(jnp.float32)
    top_logit = jnp.max(jnp.where(named, logits, -jnp.inf), axis=1, keepdims=True)
    powers = jnp.where(named, jnp.exp(jnp.where(named, logits - top_logit, 0.0)), 0.0)
    gate_wts = powers / jnp.sum(powers, axis=1, keepdims=True)
    gate_kept = gate_wts * kept_mask

    grad_all = lax.all_gather(cotangent, ("fsdp", "expert"), axis=0, tiled=True)
    nz = owners // 2
    grad_all = grad_all.reshape(shards, owners, tok_count, model_width)
    rows_all, acts, terms = gather_act(
        second_rows, gate_kept.T, w_gate, w_up, w_down, grad_all, nz, 7
    )
    rows_all = rows_all.reshape(-1, model_width)
    grad_all = grad_all.reshape(-1, model_width)
    grad_gate_in, grad_up_in, weighted = acts.reshape(3, -1, wide)
    gate_w = jnp.transpose(w_gate, (1, 0, 2)).reshape(model_width, wide)
    up_w = jnp.transpose(w_up, (1, 0, 2)).reshape(model_width, wide)
    down_w = w_down.reshape(wide, model_width)
    back = (
        jnp.einsum("th,dh->td", grad_gate_in, gate_w, preferred_element_type=jnp.float32)
        + jnp.einsum("th,dh->td", grad_up_in, up_w, preferred_element_type=jnp.float32)
    ).astype(jnp.bfloat16)
    back = back.reshape(shards, owners, tok_count, model_width)
    back_rows, terms = scatter_all(back, terms, nz, 8)
    grad_gate_k = terms.T * kept_mask
    forward = jnp.dot(weighted, down_w, preferred_element_type=jnp.float32).astype(jnp.bfloat16)
    forward = forward.reshape(shards, owners, tok_count, model_width)
    grad_logits = gate_wts * (grad_gate_k - jnp.sum(gate_wts * grad_gate_k, axis=1, keepdims=True))
    router_grad = jnp.dot(grad_logits.T, second_rows.astype(jnp.float32), precision=precise)
    grad_second = jnp.dot(grad_logits, w_router.astype(jnp.float32).T, precision=precise)
    grad_second = grad_second + back_rows

    units = shards * nz
    inputs = (
        rows_all.reshape(units, -1, model_width),
        acts.reshape(3, units, -1, wide),
        grad_all.reshape(units, -1, model_width),
    )
    return forward, grad_second, router_grad, inputs


def sum_grads(narrow, gains, head_gains, rows, inputs, local, nz):
    shards, width = lax.axis_size("fsdp"), gains.shape[1]
    mine = lax.iota(jnp.int32, shards) == lax.axis_index("fsdp")
    heads_flat = jnp.pad(head_gains.reshape(-1), (0, width - head_gains.size))
    table = jnp.concatenate([gains, jnp.where(mine[:, None], heads_flat[None], 0.0)], axis=0)
    share = -(-table.size // (2 * shards * nz * 1024)) * 8
    small = jnp.pad(table.reshape(-1), (0, 2 * shards * nz * share * 128 - table.size))
    small = small.reshape(2, shards, nz, share, 128)
    parts = [g.reshape(-1, 2, nz, 16, g.shape[1]) for g in narrow]
    *sums, small, rows, gate, up, down = line_sum(parts, small, rows, inputs, local, nz, 9)
    expert_grads = (gate, up, down.reshape(local, -1, width))
    small = small.reshape(-1)[: table.size].reshape(table.shape)
    own = lax.dynamic_slice_in_dim(small, gains.shape[0] + lax.axis_index("fsdp"), 1, axis=0)
    head_gains = own[0, : head_gains.size].reshape(head_gains.shape)
    return [s.reshape(g.shape) for s, g in zip(sums, narrow)], small[: gains.shape[0]], head_gains, rows, expert_grads


def on_device(
    block_input,
    cotangent,
    w_query,
    w_key,
    w_value,
    w_output,
    q_gain,
    k_gain,
    attn_gain,
    mlp_gain,
    w_router,
    w_gate,
    w_up,
    w_down,
    segments,
    routes,
    capacity,
):
    tok_count = block_input.shape[1]
    model_width = block_input.shape[2]
    experts = w_router.shape[1]
    nz = lax.axis_size("expert") // 2
    dense = 2 * TOP >= experts and lax.axis_size("fsdp") == 4
    flat_in = block_input[0].astype(jnp.float32)
    scale_one = lax.rsqrt(jnp.mean(flat_in * flat_in, axis=1, keepdims=True) + epsilon)
    normed_one = flat_in * scale_one
    first_rows = (normed_one * attn_gain).astype(jnp.bfloat16)
    if dense:
        group_rows, group_segs = square_gather(first_rows, jnp.tile(segments, (8, 1)), 1)
        group_rows = group_rows.reshape(-1, model_width)
        group_segs = group_segs[:, 0].reshape(-1)
    else:
        group_rows, group_segs = (
            lax.all_gather(first_rows, "fsdp", axis=0, tiled=True),
            lax.all_gather(segments[0], "fsdp", axis=0, tiled=True),
        )
    group_len = group_rows.shape[0]
    heads_here = w_query.shape[1] // HEAD_DIM
    query_rows = jnp.dot(group_rows, w_query, preferred_element_type=jnp.float32)
    key_rows = jnp.dot(group_rows, w_key, preferred_element_type=jnp.float32)
    value_rows = jnp.dot(group_rows, w_value, preferred_element_type=jnp.float32).astype(
        jnp.bfloat16
    )
    square_sums = across_heads(
        dense and 2,
        (jnp.sum(query_rows * query_rows, axis=1), jnp.sum(key_rows * key_rows, axis=1))
    )
    q_scale = lax.rsqrt(square_sums[0][:, None] / model_width + epsilon)
    k_scale = lax.rsqrt(square_sums[1][:, None] / model_width + epsilon)
    cosine, sine_table = rope_tables(group_segs, HEAD_DIM)
    head_shape = (group_len, heads_here, HEAD_DIM)
    q_heads = apply_rope(
        (query_rows * q_scale * q_gain).reshape(head_shape), cosine, sine_table
    ).astype(jnp.bfloat16)
    k_heads = apply_rope(
        (key_rows * k_scale * k_gain).reshape(head_shape), cosine, sine_table
    ).astype(jnp.bfloat16)
    v_heads = value_rows.reshape(head_shape)
    ordinal = lax.iota(jnp.int32, group_len)
    allowed = (group_segs[:, None] == group_segs[None, :]) & (ordinal[None, :] <= ordinal[:, None])
    scores = head_scores(q_heads, k_heads, allowed)
    row_top = jnp.max(scores, axis=2, keepdims=True)
    log_total = row_top + jnp.log(jnp.sum(jnp.exp(scores - row_top), axis=2, keepdims=True))
    attn_weights = jnp.exp(scores - log_total)
    mixed_heads = jnp.einsum(
        "hts,shd->thd",
        attn_weights.astype(jnp.bfloat16),
        v_heads,
        preferred_element_type=jnp.float32,
    )
    attn_rows = mixed_heads.reshape(group_len, heads_here * HEAD_DIM).astype(jnp.bfloat16)

    def mixed_term(start, length):
        return jnp.dot(attn_rows, w_output, preferred_element_type=jnp.float32).astype(jnp.bfloat16)

    mixed_rows = share_rows(dense and 4, mixed_term, tok_count).astype(jnp.float32)
    second_in = flat_in + mixed_rows
    scale_two = lax.rsqrt(jnp.mean(second_in * second_in, axis=1, keepdims=True) + epsilon)
    normed_two = second_in * scale_two
    second_rows = (normed_two * mlp_gain).astype(jnp.bfloat16)
    if dense:
        block_output, grad_second, router_grad, expert_grads = experts_dense(
            second_in, second_rows, cotangent[0], routes[0], capacity, w_router, w_gate, w_up, w_down
        )
    else:
        block_output, grad_second, router_grad, expert_grads = experts_by_slot(
            second_in, second_rows, cotangent[0], routes[0], capacity, w_router, w_gate, w_up, w_down
        )
    grad_out = cotangent[0].astype(jnp.float32)
    mlp_gain_grad = jnp.sum(grad_second * normed_two, axis=0)
    grad_normed_two = grad_second * mlp_gain
    grad_mid = grad_out + scale_two * (
        grad_normed_two - normed_two * jnp.mean(grad_normed_two * normed_two, axis=1, keepdims=True)
    )
    if dense:
        group_grad, _ = square_gather(grad_mid.astype(jnp.bfloat16), jnp.tile(segments, (8, 1)), 6)
        group_grad = group_grad.reshape(-1, model_width)
    else:
        group_grad = lax.all_gather(grad_mid.astype(jnp.bfloat16), "fsdp", axis=0, tiled=True)
    out_grad = jnp.einsum("ti,td->id", attn_rows, group_grad, preferred_element_type=jnp.float32)
    grad_attn = (
        jnp.einsum("td,id->ti", group_grad, w_output, preferred_element_type=jnp.float32)
        .astype(jnp.bfloat16)
        .reshape(head_shape)
    )
    scores_again = head_scores(q_heads, k_heads, allowed)
    weights_again = jnp.exp(scores_again - log_total)
    grad_values = jnp.einsum(
        "hts,thd->shd",
        weights_again.astype(jnp.bfloat16),
        grad_attn,
        preferred_element_type=jnp.float32,
    )
    grad_weights = jnp.einsum(
        "thd,shd->hts", grad_attn, v_heads, preferred_element_type=jnp.float32
    )
    inner_sum = jnp.sum(weights_again * grad_weights, axis=2, keepdims=True)
    grad_scores = (weights_again * (grad_weights - inner_sum)).astype(jnp.bfloat16)
    grad_q_heads = jnp.einsum(
        "hts,shd->thd", grad_scores, k_heads, preferred_element_type=jnp.float32
    ) * HEAD_DIM ** (-0.5)
    grad_k_heads = jnp.einsum(
        "hts,thd->shd", grad_scores, q_heads, preferred_element_type=jnp.float32
    ) * HEAD_DIM ** (-0.5)
    grad_q_normed = rope_grad(grad_q_heads, cosine, sine_table).reshape(group_len, -1)
    grad_k_normed = rope_grad(grad_k_heads, cosine, sine_table).reshape(group_len, -1)
    q_gain_grad = jnp.sum(grad_q_normed * query_rows * q_scale, axis=0)
    k_gain_grad = jnp.sum(grad_k_normed * key_rows * k_scale, axis=0)
    inner_q = grad_q_normed * q_gain
    inner_k = grad_k_normed * k_gain
    inner_sums = across_heads(
        dense and 3,
        (jnp.sum(inner_q * query_rows, axis=1), jnp.sum(inner_k * key_rows, axis=1))
    )
    grad_query_rows = (
        q_scale
        * (inner_q - query_rows * q_scale * q_scale * (inner_sums[0][:, None] / model_width))
    ).astype(jnp.bfloat16)
    grad_key_rows = (
        k_scale * (inner_k - key_rows * k_scale * k_scale * (inner_sums[1][:, None] / model_width))
    ).astype(jnp.bfloat16)
    grad_value_rows = grad_values.reshape(group_len, -1).astype(jnp.bfloat16)
    head_grads = jnp.concatenate([grad_query_rows, grad_key_rows, grad_value_rows], axis=1)
    mixer_grad = jnp.einsum(
        "td,ti->di", group_rows, head_grads, preferred_element_type=jnp.float32
    ).astype(jnp.bfloat16)

    def input_term(start, length):
        from_q = jnp.einsum(
            "ti,di->td", grad_query_rows, w_query, preferred_element_type=jnp.float32
        )
        from_k = jnp.einsum("ti,di->td", grad_key_rows, w_key, preferred_element_type=jnp.float32)
        from_v = jnp.einsum(
            "ti,di->td", grad_value_rows, w_value, preferred_element_type=jnp.float32
        )
        return (from_q + from_k + from_v).astype(jnp.bfloat16)

    grad_first = share_rows(dense and 5, input_term, tok_count).astype(jnp.float32)
    attn_gain_grad = jnp.sum(grad_first * normed_one, axis=0)
    grad_normed_one = grad_first * attn_gain
    grad_x = grad_mid + scale_one * (
        grad_normed_one - normed_one * jnp.mean(grad_normed_one * normed_one, axis=1, keepdims=True)
    )
    narrow = (mixer_grad, out_grad.astype(jnp.bfloat16))
    gains = jnp.concatenate([attn_gain_grad[None], mlp_gain_grad[None], router_grad], axis=0)
    head_gains = jnp.stack([q_gain_grad, k_gain_grad])
    if dense:
        narrow, gains, head_gains, forward, expert_grads = sum_grads(
            narrow, gains, head_gains, block_output, expert_grads, w_gate.shape[0], nz
        )
        block_output = (second_in + forward).astype(jnp.bfloat16)[None]
    else:
        narrow = lax.psum(narrow, "expert")
        head_gains = lax.psum(head_gains, "expert")
        gains = lax.psum(gains, ("fsdp", "expert"))
    wide = tuple(jnp.split(narrow[0], 3, axis=1)) + (narrow[1],)
    mixer = tuple(g.astype(jnp.float32) for g in wide) + (head_gains[0], head_gains[1])
    return (
        block_output,
        grad_x[None],
        mixer[0],
        mixer[1],
        mixer[2],
        mixer[3],
        mixer[4],
        mixer[5],
        gains[0],
        gains[1],
        gains[2:].T,
        *expert_grads,
    )


def solution(mesh):
    placed = (
        P("expert", "fsdp", None),
        P("expert", "fsdp", None),
        P(None, "fsdp"),
        P(None, "fsdp"),
        P(None, "fsdp"),
        P("fsdp", None),
        P("fsdp"),
        P("fsdp"),
        P(),
        P(),
        P(),
        P("expert", None, "fsdp"),
        P("expert", None, "fsdp"),
        P("expert", "fsdp", None),
        P("expert", "fsdp"),
        P("expert", "fsdp", None),
        P(),
    )
    return jax.shard_map(
        on_device,
        mesh=mesh,
        in_specs=placed,
        out_specs=(
            P("expert", "fsdp", None),
            P("expert", "fsdp", None),
            P(None, "fsdp"),
            P(None, "fsdp"),
            P(None, "fsdp"),
            P("fsdp", None),
            P("fsdp"),
            P("fsdp"),
            P(),
            P(),
            P(),
            P("expert", None, "fsdp"),
            P("expert", None, "fsdp"),
            P("expert", "fsdp", None),
        ),
        check_vma=False,
    )
```

```python
import functools

import jax
import jax.numpy as jnp
from jax import lax
from jax.experimental import pallas as pl
from jax.experimental.pallas import tpu as pltpu
from jax.sharding import PartitionSpec as P

HEAD_DIM = 128
TOP = 8


epsilon = 1e-05
rope_base = 10000.0
precise = lax.Precision.HIGHEST


MESH = pl.DeviceIdType.MESH
DMA = pltpu.SemaphoreType.DMA


class Place:
    def __init__(self):
        self.f, self.e = lax.axis_index("fsdp"), lax.axis_index("expert")
        self.c, self.z = self.e % 2, self.e // 2
        self.fx = self.f + 1 - 2 * (self.f % 2)
        self.fy = (self.f + 2) % 4
        self.fd = 3 - self.f
        self.pe = self.e + 1 - 2 * self.c


def send(src, dst, send_sem, recv_sem, f, e):
    return pltpu.make_async_remote_copy(
        src_ref=src,
        dst_ref=dst,
        send_sem=send_sem,
        recv_sem=recv_sem,
        device_id={"fsdp": f, "expert": e},
        device_id_type=MESH,
    )


def greet(peers, line=None):
    barrier = pltpu.get_barrier_semaphore()

    def hello(f, e):
        pl.semaphore_signal(
            barrier, inc=1, device_id={"fsdp": f, "expert": e}, device_id_type=MESH
        )

    for f, e in peers:
        hello(f, e)
    if line is not None:
        at, nz = line
        for step in range(1, nz):
            hello(at.f, 2 * ((at.z + step) % nz) + at.c)
        pl.semaphore_wait(barrier, len(peers) + nz - 1)
    else:
        pl.semaphore_wait(barrier, len(peers))


class SmallGather:
    sems = staticmethod(
        lambda nz: [DMA((nz,)), DMA((nz,)), DMA((4,)), DMA((4,))]
    )

    def __init__(self, at, nz, own, out, sems):
        self.at, self.nz, self.own, self.out = at, nz, own, out
        self.ls, self.lr, self.ss, self.sr = sems

    def line(self, step):
        at = self.at
        z = (at.z + step) % self.nz
        back = (at.z + self.nz - step) % self.nz
        slot = self.out.at[at.c, at.f]
        to = send(self.own, slot.at[at.z], self.ls.at[step], self.lr.at[step], at.f, 2 * z + at.c)
        come = send(self.own, slot.at[back], self.ls.at[step], self.lr.at[step], at.f, 2 * z + at.c)
        return to, come

    def plane(self, i):
        at, out = self.at, self.out
        f, to_f = ((at.f, at.fx), (at.f, at.fy), (at.fx, at.fy))[i]
        slot = out.at[at.c, f]
        return send(slot, slot, self.ss.at[i], self.sr.at[i], to_f, at.e)

    def pair(self):
        at = self.at
        slot = self.out.at[at.c]
        return send(slot, slot, self.ss.at[3], self.sr.at[3], at.f, at.pe)

    def stage(self, i):
        at = self.at
        if i == 0:
            for step in range(1, self.nz):
                self.line(step)[0].start()
            self.out[at.c, at.f, at.z] = self.own[...]
        elif i == 1:
            for step in range(1, self.nz):
                self.line(step)[1].wait_recv()
            self.plane(0).start()
            self.plane(1).start()
        elif i == 2:
            self.plane(0).wait_recv()
            self.plane(2).start()
        elif i == 3:
            self.plane(1).wait_recv()
            self.plane(2).wait_recv()
            self.pair().start()
        elif i == 4:
            self.pair().wait_recv()
            self.pair().wait_send()
            for step in range(1, self.nz):
                self.line(step)[0].wait_send()
            for k in range(3):
                self.plane(k).wait_send()


class SmallScatter:
    sems = staticmethod(lambda nz: [DMA((nz,)), DMA((nz,)), DMA((4,)), DMA((4,))])
    scratch = staticmethod(
        lambda nz, shape: [
            pltpu.VMEM((4, nz, *shape), jnp.float32),
            pltpu.VMEM((4, nz, *shape), jnp.float32),
            pltpu.VMEM((3, nz, *shape), jnp.float32),
            pltpu.VMEM((nz, *shape), jnp.float32),
        ]
    )

    def __init__(self, at, nz, part, out, scratch, sems):
        self.at, self.nz, self.part, self.out = at, nz, part, out
        self.acc, self.pb, self.xy, self.zb = scratch
        self.ls, self.lr, self.ss, self.sr = sems

    def pair(self):
        at = self.at
        return send(
            self.part.at[1 - at.c], self.pb, self.ss.at[0], self.sr.at[0], at.f, at.pe
        )

    def plane(self, i):
        at = self.at
        f, to_f = ((at.fx, at.fx), (at.fd, at.fx), (at.fy, at.fy))[i]
        return send(
            self.acc.at[f], self.xy.at[i], self.ss.at[1 + i], self.sr.at[1 + i], to_f, at.e
        )

    def line(self, step):
        at = self.at
        z = (at.z + step) % self.nz
        return send(
            self.acc.at[at.f, z], self.zb.at[step], self.ls.at[step], self.lr.at[step], at.f, 2 * z + at.c
        )

    def stage(self, i):
        at, acc, xy = self.at, self.acc, self.xy
        if i == 0:
            self.pair().start()
        elif i == 1:
            self.pair().wait_recv()
            acc[...] = self.part[at.c] + self.pb[...]
            self.plane(0).start()
            self.plane(1).start()
        elif i == 2:
            self.plane(0).wait_recv()
            self.plane(1).wait_recv()
            acc[at.fy] = acc[at.fy] + xy[1]
            self.plane(2).start()
            acc[at.f] = acc[at.f] + xy[0]
        elif i == 3:
            self.plane(2).wait_recv()
            acc[at.f] = acc[at.f] + xy[2]
            for step in range(1, self.nz):
                self.line(step).start()
        elif i == 4:
            total = acc[at.f, at.z]
            for step in range(1, self.nz):
                self.line(step).wait_recv()
                total = total + self.zb[step]
            self.out[...] = total
            self.pair().wait_send()
            for k in range(3):
                self.plane(k).wait_send()
            for step in range(1, self.nz):
                self.line(step).wait_send()


def take(sequence, count):
    return [next(sequence) for _ in range(count)]


NT = (((1,), (1,)), ((), ()))
TN = (((0,), (0,)), ((), ()))


def above(a, b):
    return (a - b + 63) // 64


def near_first(at, nz, s):
    right = above(2 * at.z, nz - 1)
    alternate = at.z - right * (2 * at.z - (nz - 1))
    turn = at.z + (s + 1) // 2 * (1 - 2 * (s % 2))
    rest = s + right * (nz - 1 - 2 * s)
    return turn + above(s, 2 * alternate) * (rest - turn)


def gather_act_kernel(nz, own, own_small, w_gate, w_up, out, acts, gates, xb, ab, load_x, store, own_sem, zr, zs, xr, xs, yr, ys, dr, xf, yf, pr, ps, *small_sems):
    at = Place()
    rows, width = own.shape
    local, _, hidden = w_gate.shape
    half = rows // 2
    halves = (pl.ds(0, half), pl.ds(half, half))
    small = SmallGather(at, nz, own_small, gates, small_sems)
    greet([(at.fx, at.e), (at.fy, at.e), (at.f, at.pe)], (at, nz))
    keep = pltpu.make_async_copy(own, out.at[at.f, at.e], own_sem)
    keep.start()
    small.stage(0)
    places = (at.f, at.fx, at.fy, at.fd)

    def up(z):
        ref = out.at[at.f, 2 * z + at.c]
        return send(ref, ref, zs.at[0, z], zr.at[z], at.f, at.e + 2)

    def down(z):
        ref = out.at[at.f, 2 * z + at.c]
        return send(ref, ref, zs.at[1, z], zr.at[z], at.f, at.e - 2)

    def to_x(z, h):
        ref = out.at[at.f, 2 * z + at.c, halves[h]]
        return send(ref, ref, xs.at[h, z], xr.at[h, z], at.fx, at.e)

    def to_y(z, h):
        ref = out.at[at.f, 2 * z + at.c, halves[h]]
        return send(ref, ref, ys.at[h, z], yr.at[h, z], at.fy, at.e)

    def x_on(z):
        ref = out.at[at.fx, 2 * z + at.c, halves[0]]
        return send(ref, ref, yf.at[z], dr.at[0, z], at.fy, at.e)

    def y_on(z):
        ref = out.at[at.fy, 2 * z + at.c, halves[1]]
        return send(ref, ref, xf.at[z], dr.at[1, z], at.fx, at.e)

    def to_p(f, z, h):
        ref = out.at[f, 2 * z + at.c, halves[h]]
        return send(ref, ref, ps.at[f, z, h], pr.at[f, z, h], at.f, at.pe)

    def line_step(z):
        pl.when(z != at.z)(lambda: up(z).wait_recv())
        pl.when((z <= at.z) & (at.z < nz - 1))(lambda: up(z).start())
        pl.when((z >= at.z) & (at.z > 0))(lambda: down(z).start())
        to_x(z, 0).start()
        to_y(z, 1).start()
        to_x(z, 1).start()
        to_y(z, 0).start()
        for h in range(2):
            to_p(at.f, z, h).start()

    def plane_step(z):
        to_x(z, 0).wait_recv()
        x_on(z).start()
        to_y(z, 1).wait_recv()
        y_on(z).start()
        to_p(at.fx, z, 0).start()
        to_p(at.fy, z, 1).start()
        to_x(z, 1).wait_recv()
        to_p(at.fx, z, 1).start()
        to_y(z, 0).wait_recv()
        to_p(at.fy, z, 0).start()

    def diag_step(z):
        x_on(z).wait_recv()
        to_p(at.fd, z, 0).start()
        y_on(z).wait_recv()
        to_p(at.fd, z, 1).start()

    def load(q, z):
        return pltpu.make_async_copy(out.at[places[q], pl.ds(2 * z, 2)], xb.at[q], load_x.at[q])

    def stores(q, z):
        return [
            pltpu.make_async_copy(
                ab.at[q, k], acts.at[k, places[q], pl.ds(2 * z, 2)], store.at[q, k]
            )
            for k in range(2)
        ]

    def fetch(q, z):
        for h in range(2):
            to_p(places[q], z, h).wait_recv()
        load(q, z).start()

    def work(q, z):
        load(q, z).wait()
        x = xb[q].reshape(2 * rows, width)
        for j in range(local):
            for k, w in enumerate((w_gate, w_up)):
                g = jnp.dot(x, w[j], preferred_element_type=jnp.float32)
                ab[q, k, :, :, pl.ds(j * hidden, hidden)] = g.reshape(2, rows, hidden)
        for copy in stores(q, z):
            copy.start()

    keep.wait()

    def body(s, carry):
        def at_step(lag, run):
            pl.when((s >= lag) & (s < nz + lag))(lambda: run(near_first(at, nz, s - lag)))

        def free(q, lag):
            def run(z):
                for copy in stores(q, z):
                    copy.wait()

            at_step(lag + 1, run)

        at_step(0, line_step)
        for k in range(1, 5):
            pl.when(s == 0)(functools.partial(small.stage, k))
        at_step(1, lambda z: fetch(0, z))
        free(3, 4)
        at_step(4, lambda z: work(3, z))
        at_step(1, plane_step)
        at_step(2, lambda z: fetch(1, z))
        free(0, 1)
        at_step(1, lambda z: work(0, z))
        at_step(2, diag_step)
        at_step(2, lambda z: fetch(2, z))
        free(1, 2)
        at_step(2, lambda z: work(1, z))
        at_step(3, lambda z: fetch(3, z))
        free(2, 2)
        at_step(2, lambda z: work(2, z))
        return carry

    lax.fori_loop(0, nz + 5, body, 0)

    def finish(z, carry):
        pl.when((z <= at.z) & (at.z < nz - 1))(lambda: up(z).wait_send())
        pl.when((z >= at.z) & (at.z > 0))(lambda: down(z).wait_send())
        for h in range(2):
            to_x(z, h).wait_send()
            to_y(z, h).wait_send()
        x_on(z).wait_send()
        y_on(z).wait_send()
        for f in range(4):
            for h in range(2):
                to_p(f, z, h).wait_send()
        return carry

    lax.fori_loop(0, nz, finish, 0)


def gather_act(rows, small, w_gate, w_up, nz, cid):
    r, c = rows.shape
    local, _, hidden = w_gate.shape
    wide = local * hidden
    hbm, vmem = pl.BlockSpec(memory_space=pl.ANY), pl.BlockSpec(memory_space=pltpu.VMEM)
    bf16 = jnp.bfloat16
    return pl.pallas_call(
        functools.partial(gather_act_kernel, nz),
        out_shape=(
            jax.ShapeDtypeStruct((4, 2 * nz, r, c), bf16),
            jax.ShapeDtypeStruct((2, 4, 2 * nz, r, wide), jnp.float32),
            jax.ShapeDtypeStruct((2, 4, nz, *small.shape), jnp.float32),
        ),
        in_specs=[vmem] * 4,
        out_specs=(hbm, hbm, vmem),
        scratch_shapes=[
            pltpu.VMEM((4, 2, r, c), bf16),
            pltpu.VMEM((4, 2, 2, r, wide), jnp.float32),
            DMA((4,)), DMA((4, 2)),
            DMA(()), DMA((nz,)), DMA((2, nz)), DMA((2, nz)), DMA((2, nz)), DMA((2, nz)), DMA((2, nz)),
            DMA((2, nz)), DMA((nz,)), DMA((nz,)), DMA((4, nz, 2)), DMA((4, nz, 2)),
            *SmallGather.sems(nz),
        ],
        compiler_params=pltpu.CompilerParams(
            collective_id=cid, has_side_effects=True, vmem_limit_bytes=50 << 20
        ),
        cost_estimate=pl.CostEstimate(flops=0, bytes_accessed=240 << 20, transcendentals=0),
        name="gather_act",
    )(rows, small, w_gate, w_up)


def add_rows(dst, dst_rows, parts):
    start, count = dst_rows

    def body(i, carry):
        r = pl.multiple_of(i * 16, 16)
        total = None
        for ref, offset in parts:
            piece = ref[pl.ds(offset + r, 16), :].astype(jnp.float32)
            total = piece if total is None else total + piece
        dst[pl.ds(start + r, 16), :] = total.astype(dst.dtype)
        return carry

    lax.fori_loop(0, count // 16, body, 0)


def scatter_plan(at, nz, part, out, refs, staged=None):
    acc, pb, xh, yh, xf, yf, zu, zd, ls, pr, ps, xhs, xhr, yhs, yhr, xs, xr, ys, yr, us, ur, ds_, dr = refs
    rows = out.shape[0]
    half = rows // 2
    lo, hi = pl.ds(0, half), pl.ds(half, half)

    def place(s):
        return near_first(at, nz, nz - 1 - s)

    def load(f, z):
        return pltpu.make_async_copy(part.at[f, 2 * z + at.c], acc.at[f, z], ls.at[f, z])

    fs = (at.fd, at.fx, at.fy, at.f)

    def to_p(q, z):
        f = fs[q]
        src = staged.at[q] if staged is not None else part.at[f, 2 * z + 1 - at.c]
        return send(src, pb.at[f, z], ps.at[f, z], pr.at[f, z], at.f, at.pe)

    def ready(q, z):
        if staged is None:
            load(fs[q], z).wait()
        to_p(q, z).wait_recv()

    def start_step(s):
        z = place(s)
        for q in range(4):
            load(fs[q], z).start()
            to_p(q, z).start()

    def half_x(z):
        return send(acc.at[at.fd, z, lo], xh.at[z], xhs.at[z], xhr.at[z], at.fx, at.e)

    def half_y(z):
        return send(acc.at[at.fd, z, hi], yh.at[z], yhs.at[z], yhr.at[z], at.fy, at.e)

    def full_x(z):
        return send(acc.at[at.fx, z], xf.at[z], xs.at[z], xr.at[z], at.fx, at.e)

    def full_y(z):
        return send(acc.at[at.fy, z], yf.at[z], ys.at[z], yr.at[z], at.fy, at.e)

    def go_up(z):
        return send(acc.at[at.f, z], zu.at[z], us.at[z], ur.at[z], at.f, at.e + 2)

    def go_down(z):
        return send(acc.at[at.f, z], zd.at[z], ds_.at[z], dr.at[z], at.f, at.e - 2)

    def diag_step(s):
        z = place(s)
        ready(0, z)
        a, b = acc.at[at.fd, z], pb.at[at.fd, z]
        add_rows(a, (0, half), [(a, 0), (b, 0)])
        half_x(z).start()
        add_rows(a, (half, half), [(a, half), (b, half)])
        half_y(z).start()

    def plane_step(s):
        z = place(s)
        ready(1, z)
        a, b = acc.at[at.fx, z], pb.at[at.fx, z]
        half_y(z).wait_recv()
        add_rows(a, (0, half), [(a, 0), (b, 0)])
        add_rows(a, (half, half), [(a, half), (b, half), (yh.at[z], 0)])
        full_x(z).start()
        ready(2, z)
        half_x(z).wait_recv()
        a, b = acc.at[at.fy, z], pb.at[at.fy, z]
        add_rows(a, (0, half), [(a, 0), (b, 0), (xh.at[z], 0)])
        add_rows(a, (half, half), [(a, half), (b, half)])
        full_y(z).start()

    def line_step(s):
        z = place(s)
        ready(3, z)
        full_x(z).wait_recv()
        full_y(z).wait_recv()
        a = acc.at[at.f, z]
        four = [(a, 0), (pb.at[at.f, z], 0), (xf.at[z], 0), (yf.at[z], 0)]

        @pl.when(z > at.z)
        def _():
            @pl.when(at.z > 0)
            def _():
                go_up(z).wait_recv()
                add_rows(a, (0, rows), four + [(zu.at[z], 0)])

            pl.when(at.z == 0)(lambda: add_rows(a, (0, rows), four))
            go_up(z).start()

        @pl.when(z < at.z)
        def _():
            @pl.when(at.z < nz - 1)
            def _():
                go_down(z).wait_recv()
                add_rows(a, (0, rows), four + [(zd.at[z], 0)])

            pl.when(at.z == nz - 1)(lambda: add_rows(a, (0, rows), four))
            go_down(z).start()

        @pl.when(z == at.z)
        def _():
            add_rows(out, (0, rows), four)

            @pl.when(at.z > 0)
            def _():
                go_up(z).wait_recv()
                add_rows(out, (0, rows), [(out, 0), (zu.at[z], 0)])

            @pl.when(at.z < nz - 1)
            def _():
                go_down(z).wait_recv()
                add_rows(out, (0, rows), [(out, 0), (zd.at[z], 0)])

    def finish():
        def body(z, carry):
            for q in range(4):
                if staged is None:
                    to_p(q, z).wait_send()
            half_x(z).wait_send()
            half_y(z).wait_send()
            full_x(z).wait_send()
            full_y(z).wait_send()
            pl.when(z > at.z)(lambda: go_up(z).wait_send())
            pl.when(z < at.z)(lambda: go_down(z).wait_send())
            return carry

        lax.fori_loop(0, nz, body, 0)
        for q in range(4):
            if staged is not None:
                to_p(q, place(nz - 1)).wait_send()

    return start_step, diag_step, plane_step, line_step, finish, place, to_p


def scatter_scratch(parts, nz):
    _, _, r, c = parts.shape

    def buf(*n):
        return pltpu.VMEM((*n, c), parts.dtype)

    return [
        buf(4, nz, r), buf(4, nz, r), buf(nz, r // 2), buf(nz, r // 2),
        buf(nz, r), buf(nz, r), buf(nz, r), buf(nz, r),
        DMA((4, nz)), DMA((4, nz)), DMA((4, nz)),
        *[DMA((nz,))] * 12,
    ]


def scatter_act_kernel(nz, pre, grads, gates, w_gate, w_up, w_down, out, out_small, acts, forward, *refs):
    at = Place()
    refs = iter(refs)
    moved = take(refs, 23)
    acc = moved[0]
    pb_, cb, ab, sb, fb, terms, load_sem, store_sem, forward_sem = take(refs, 9)
    _, diag, plane, line, close, place, to_p = scatter_plan(at, nz, None, out, moved, sb)
    small = SmallScatter(at, nz, terms, out_small, take(refs, 4), take(refs, 4))
    greet([(at.fx, at.e), (at.fy, at.e), (at.f, at.pe)], (at, nz))
    rows, width = out.shape
    local, _, hidden = w_gate.shape
    experts = gates.shape[3]
    fs = (at.fd, at.fx, at.fy, at.f)
    cores = (at.c, 1 - at.c)
    first = at.e * local
    expert_row = lax.broadcasted_iota(jnp.int32, (experts, hidden), 0)
    tile = 512

    def loads(q, s):
        z, f = place(s), fs[q]
        copies = []
        for h, core in enumerate(cores):
            slot = 2 * z + core
            for k in range(2):
                copies.append(
                    pltpu.make_async_copy(pre.at[k, f, slot], pb_.at[q, k, h], load_sem.at[q, h, k])
                )
            copies.append(pltpu.make_async_copy(grads.at[f, slot], cb.at[q, h], load_sem.at[q, h, 2]))
        return copies

    def stores(q, s):
        z, f = place(s), fs[q]
        return [
            pltpu.make_async_copy(
                ab.at[q, k, h], acts.at[k, f, 2 * z + core], store_sem.at[q, h, k]
            )
            for h, core in enumerate(cores)
            for k in range(3)
        ]

    def sends(q, s):
        z, f = place(s), fs[q]
        return [
            pltpu.make_async_copy(fb.at[q, h], forward.at[f, 2 * z + core], forward_sem.at[q, h])
            for h, core in enumerate(cores)
        ]

    def act(q, s):
        z, f = place(s), fs[q]
        for copy in loads(q, s):
            copy.wait()

        @pl.when(s > 0)
        def _():
            for copy in stores(q, s - 1):
                copy.wait()

        c = cb[q].reshape(2 * rows, width)
        sums = [None, None]
        for j in range(local):
            pick = (expert_row == first + j).astype(jnp.float32)
            cols = pl.ds(j * hidden, hidden)
            dh = lax.dot_general(c, w_down[j], NT, preferred_element_type=jnp.float32)
            for h, core in enumerate(cores):
                g, u = pb_[q, 0, h, :, cols], pb_[q, 1, h, :, cols]
                d = dh[h * rows : (h + 1) * rows]
                sig = 1.0 / (1.0 + jnp.exp(-g))
                silu = g * sig
                hid = silu * u
                gate = lax.dot_general(
                    gates[core, f, z], pick, TN, precision=precise, preferred_element_type=jnp.float32
                )
                mine = lax.dot_general(
                    pick, hid * d, NT, precision=precise, preferred_element_type=jnp.float32
                )
                sums[h] = mine if sums[h] is None else sums[h] + mine
                d = d * gate
                ab[q, 0, h, :, cols] = (d * u * sig * (1.0 + g * (1.0 - sig))).astype(jnp.bfloat16)
                ab[q, 1, h, :, cols] = (d * silu).astype(jnp.bfloat16)
                ab[q, 2, h, :, cols] = (hid * gate).astype(jnp.bfloat16)
        for h, core in enumerate(cores):
            terms[core, f, z] = sums[h]
        for copy in stores(q, s):
            copy.start()

        @pl.when(s + 1 < nz)
        def _():
            for copy in loads(q, s + 1):
                copy.start()

    def back(q, s):
        z, f = place(s), fs[q]
        pl.when(s > 0)(lambda: to_p(q, place(s - 1)).wait_send())
        pieces = [
            (ab[q, k].reshape(2 * rows, local * hidden)[:, j * hidden : (j + 1) * hidden], w.at[j])
            for j in range(local)
            for k, w in enumerate((w_gate, w_up))
        ]

        def body(t, carry):
            cols = pl.ds(pl.multiple_of(t * tile, tile), tile)
            total = None
            for a, w in pieces:
                term = lax.dot_general(a, w[cols, :], NT, preferred_element_type=jnp.float32)
                total = term if total is None else total + term
            total = total.astype(jnp.bfloat16)
            acc[f, z, :, cols] = total[:rows]
            sb[q, :, cols] = total[rows:]
            return carry

        lax.fori_loop(0, width // tile, body, 0)
        to_p(q, z).start()

    def ahead(q, s):
        @pl.when(s > 0)
        def _():
            for copy in sends(q, s - 1):
                copy.wait()

        a = ab[q, 2].reshape(2 * rows, local * hidden)

        def body(t, carry):
            cols = pl.ds(pl.multiple_of(t * tile, tile), tile)
            total = None
            for j in range(local):
                term = jnp.dot(
                    a[:, j * hidden : (j + 1) * hidden],
                    w_down[j, :, cols],
                    preferred_element_type=jnp.float32,
                )
                total = term if total is None else total + term
            total = total.astype(jnp.bfloat16)
            fb[q, 0, :, cols] = total[:rows]
            fb[q, 1, :, cols] = total[rows:]
            return carry

        lax.fori_loop(0, width // tile, body, 0)
        for copy in sends(q, s):
            copy.start()

    for q in range(4):
        for copy in loads(q, 0):
            copy.start()

    def body(s, carry):
        @pl.when(s < nz)
        def _():
            last = s == nz - 1
            for q in (0, 1):
                act(q, s)
                back(q, s)
            diag(s)
            act(2, s)
            back(2, s)
            act(3, s)
            pl.when(last)(lambda: small.stage(0))
            back(3, s)
            for q in range(4):
                ahead(q, s)
            pl.when(last)(lambda: small.stage(1))
            plane(s)
            pl.when(last)(lambda: small.stage(2))

        pl.when(s == nz)(lambda: small.stage(3))
        pl.when(s >= 1)(lambda: line(s - 1))
        return carry

    lax.fori_loop(0, nz + 1, body, 0)
    small.stage(4)
    for q in range(4):
        for copy in stores(q, nz - 1) + sends(q, nz - 1):
            copy.wait()
    close()


def scatter_act(pre, grads, gates, w_gate, w_up, w_down, nz, cid):
    _, _, _, r, wide = pre.shape
    c = grads.shape[3]
    small = gates.shape[3:]
    hbm, vmem = pl.BlockSpec(memory_space=pl.ANY), pl.BlockSpec(memory_space=pltpu.VMEM)
    bf16 = jnp.bfloat16
    return pl.pallas_call(
        functools.partial(scatter_act_kernel, nz),
        out_shape=(
            jax.ShapeDtypeStruct((r, c), jnp.float32),
            jax.ShapeDtypeStruct(small, jnp.float32),
            jax.ShapeDtypeStruct((3, 4, 2 * nz, r, wide), bf16),
            jax.ShapeDtypeStruct((4, 2 * nz, r, c), bf16),
        ),
        in_specs=[hbm, hbm, vmem, vmem, vmem, vmem],
        out_specs=(vmem, vmem, hbm, hbm),
        scratch_shapes=[
            *scatter_scratch(grads, nz),
            pltpu.VMEM((4, 2, 2, r, wide), jnp.float32),
            pltpu.VMEM((4, 2, r, c), bf16),
            pltpu.VMEM((4, 3, 2, r, wide), bf16),
            pltpu.VMEM((4, r, c), bf16),
            pltpu.VMEM((4, 2, r, c), bf16),
            pltpu.VMEM((2, 4, nz, *small), jnp.float32),
            DMA((4, 2, 3)), DMA((4, 2, 3)), DMA((4, 2)),
            *SmallScatter.scratch(nz, small),
            *SmallScatter.sems(nz),
        ],
        compiler_params=pltpu.CompilerParams(
            collective_id=cid, has_side_effects=True, vmem_limit_bytes=62 << 20
        ),
        cost_estimate=pl.CostEstimate(flops=0, bytes_accessed=300 << 20, transcendentals=0),
        name="scatter_act",
    )(pre, grads, gates, w_gate, w_up, w_down)


def square_gather_kernel(own, ids, out, out_ids, xs, xr, ys, yr, fs, fr, js, jr):
    at = Place()
    half = own.shape[0] // 2
    halves = (pl.ds(0, half), pl.ds(half, half))
    peers = [(at.fx, at.e), (at.fy, at.e), (at.fd, at.e)]
    greet(peers)

    def to_x(h):
        return send(own.at[halves[h]], out.at[at.f, halves[h]], xs.at[h], xr.at[h], at.fx, at.e)

    def to_y(h):
        return send(own.at[halves[h]], out.at[at.f, halves[h]], ys.at[h], yr.at[h], at.fy, at.e)

    x_ref, y_ref = out.at[at.fx, halves[0]], out.at[at.fy, halves[1]]
    x_on = send(x_ref, x_ref, fs.at[0], fr.at[0], at.fy, at.e)
    y_on = send(y_ref, y_ref, fs.at[1], fr.at[1], at.fx, at.e)
    notes = [
        send(ids, out_ids.at[at.f], js.at[k], jr.at[k], f, e) for k, (f, e) in enumerate(peers)
    ]
    to_x(0).start()
    to_y(1).start()
    for note in notes:
        note.start()
    to_x(1).start()
    to_y(0).start()
    out[at.f] = own[...]
    out_ids[at.f] = ids[...]
    to_x(0).wait_recv()
    x_on.start()
    to_y(1).wait_recv()
    y_on.start()
    to_x(1).wait()
    to_y(0).wait()
    for note in notes:
        note.wait()
    to_x(0).wait_send()
    to_y(1).wait_send()
    x_on.wait()
    y_on.wait()


def square_gather(rows, ids, cid):
    r, c = rows.shape
    vmem = pl.BlockSpec(memory_space=pltpu.VMEM)
    return pl.pallas_call(
        square_gather_kernel,
        out_shape=(
            jax.ShapeDtypeStruct((4, r, c), rows.dtype),
            jax.ShapeDtypeStruct((4, *ids.shape), ids.dtype),
        ),
        in_specs=[vmem] * 2,
        out_specs=(vmem,) * 2,
        scratch_shapes=[DMA((2,))] * 6 + [DMA((3,))] * 2,
        compiler_params=pltpu.CompilerParams(collective_id=cid, has_side_effects=True),
        cost_estimate=pl.CostEstimate(flops=0, bytes_accessed=60 << 20, transcendentals=0),
        name="square_gather",
    )(rows, ids)


def square_scatter_kernel(part, out, xh, yh, xf, yf, ss, rs):
    at = Place()
    rows = out.shape[0]
    half = rows // 2
    lo, hi = pl.ds(0, half), pl.ds(half, half)
    greet([(at.fx, at.e), (at.fy, at.e)])

    def to_x(k, src, dst):
        return send(src, dst, ss.at[k], rs.at[k], at.fx, at.e)

    def to_y(k, src, dst):
        return send(src, dst, ss.at[k], rs.at[k], at.fy, at.e)

    copies = [
        to_x(0, part.at[at.fd, lo], xh),
        to_y(1, part.at[at.fd, hi], yh),
        to_x(2, part.at[at.fx, lo], xf.at[lo]),
        to_y(3, part.at[at.fy, hi], yf.at[hi]),
        to_x(4, yh, xf.at[hi]),
        to_y(5, xh, yf.at[lo]),
    ]
    for copy in copies[:4]:
        copy.start()
    copies[1].wait_recv()
    add_rows(yh, (0, half), [(yh, 0), (part.at[at.fx], half)])
    copies[4].start()
    copies[0].wait_recv()
    add_rows(xh, (0, half), [(xh, 0), (part.at[at.fy], 0)])
    copies[5].start()
    copies[2].wait_recv()
    copies[5].wait_recv()
    copies[3].wait_recv()
    copies[4].wait_recv()
    add_rows(out, (0, rows), [(part.at[at.f], 0), (xf, 0), (yf, 0)])
    for copy in copies:
        copy.wait_send()


def square_scatter(parts, cid):
    _, r, c = parts.shape
    vmem = pl.BlockSpec(memory_space=pltpu.VMEM)

    def buf(n):
        return pltpu.VMEM((n, c), parts.dtype)

    return pl.pallas_call(
        square_scatter_kernel,
        out_shape=jax.ShapeDtypeStruct((r, c), jnp.float32),
        in_specs=[vmem],
        out_specs=vmem,
        scratch_shapes=[buf(r // 2), buf(r // 2), buf(r), buf(r), DMA((6,)), DMA((6,))],
        compiler_params=pltpu.CompilerParams(collective_id=cid, has_side_effects=True),
        cost_estimate=pl.CostEstimate(flops=0, bytes_accessed=60 << 20, transcendentals=0),
        name="square_scatter",
    )(parts)


def square_sum_kernel(own, out, got, ss, rs):
    at = Place()
    peers = [(at.fx, at.e), (at.fy, at.e), (at.fd, at.e)]
    greet(peers)
    copies = [send(own, got.at[k], ss.at[k], rs.at[k], f, e) for k, (f, e) in enumerate(peers)]
    for copy in copies:
        copy.start()
    for copy in copies:
        copy.wait()
    out[...] = (own[...] + got[0]) + (got[1] + got[2])


def square_sum(values, cid):
    flat = values.reshape(8, -1)
    vmem = pl.BlockSpec(memory_space=pltpu.VMEM)
    return pl.pallas_call(
        square_sum_kernel,
        out_shape=jax.ShapeDtypeStruct(flat.shape, jnp.float32),
        in_specs=[vmem],
        out_specs=vmem,
        scratch_shapes=[pltpu.VMEM((3, *flat.shape), jnp.float32), DMA((3,)), DMA((3,))],
        compiler_params=pltpu.CompilerParams(collective_id=cid, has_side_effects=True),
        cost_estimate=pl.CostEstimate(flops=0, bytes_accessed=10 << 20, transcendentals=0),
        name="square_sum",
    )(flat).reshape(values.shape)


class product_plan:
    def __init__(self, inputs, outs, refs):
        self.rows, self.acts, self.grads = inputs
        self.outs = outs
        self.wide_acc, self.down_acc, self.xw, self.aw, self.load_sem, self.store_sem = refs
        self.units = self.rows.shape[0]
        self.local = self.outs[0].shape[0]
        self.per_pass = self.units // 2
        self.steps = self.per_pass * (self.local + 1)

    def loads(self, i, k, p):
        u = (i - p * self.per_pass) * 2 + k
        hidden = self.outs[0].shape[2]
        sem = self.load_sem.at[k]
        if p == self.local:
            return [
                pltpu.make_async_copy(self.grads.at[u], self.xw.at[k], sem.at[0]),
                pltpu.make_async_copy(self.acts.at[2, u], self.aw.at[k], sem.at[1]),
            ]
        cols = pl.ds(p * hidden, hidden)
        return [
            pltpu.make_async_copy(self.rows.at[u], self.xw.at[k], sem.at[0]),
            pltpu.make_async_copy(self.acts.at[0, u, :, cols], self.aw.at[k, :, pl.ds(0, hidden)], sem.at[1]),
            pltpu.make_async_copy(
                self.acts.at[1, u, :, cols], self.aw.at[k, :, pl.ds(hidden, hidden)], sem.at[2]
            ),
        ]

    def on_pass(self, i, run):
        for p in range(self.local + 1):
            pl.when((i >= p * self.per_pass) & (i < (p + 1) * self.per_pass))(functools.partial(run, p))

    def start(self):
        for k in range(2):
            for copy in self.loads(0, k, 0):
                copy.start()

        for acc in (*[self.wide_acc.at[p] for p in range(self.local)], self.down_acc):
            def body(r, carry, acc=acc):
                acc[pl.ds(r * 8, 8), :] = jnp.zeros((8, acc.shape[1]), jnp.float32)
                return carry

            lax.fori_loop(0, acc.shape[0] // 8, body, 0)

    def step(self, i):
        tile = 512

        def run(p):
            for k in range(2):
                for copy in self.loads(i, k, p):
                    copy.wait()
                a = self.aw[k]
                for t in range(self.xw.shape[2] // tile):
                    cols = pl.ds(t * tile, tile)
                    x = self.xw[k, :, cols]
                    if p == self.local:
                        self.down_acc[:, cols] += lax.dot_general(
                            a, x, TN, preferred_element_type=jnp.float32
                        )
                    else:
                        self.wide_acc[p, cols, :] += lax.dot_general(
                            x, a, TN, preferred_element_type=jnp.float32
                        )

                def more(q, k=k):
                    for copy in self.loads(i + 1, k, q):
                        copy.start()

                self.on_pass(i + 1, more)

            @pl.when(i == (p + 1) * self.per_pass - 1)
            def _():
                for copy in self.stores(p):
                    copy.start()

        self.on_pass(i, run)

    def stores(self, p):
        hidden = self.outs[0].shape[2]
        if p == self.local:
            return [pltpu.make_async_copy(self.down_acc, self.outs[2], self.store_sem.at[p, 0])]
        acc = self.wide_acc.at[p]
        return [
            pltpu.make_async_copy(
                acc.at[:, pl.ds(k * hidden, hidden)], self.outs[k].at[p], self.store_sem.at[p, k]
            )
            for k in range(2)
        ]

    def finish(self):
        for p in range(self.local + 1):
            for copy in self.stores(p):
                copy.wait()


def line_sum_kernel(nz, counts, *refs):
    at = Place()
    refs = iter(refs)
    n = len(counts)
    parts, part_small, rows_part, inputs = take(refs, n), next(refs), next(refs), take(refs, 3)
    outs, out_small, rows_out, grads = take(refs, n), next(refs), next(refs), take(refs, 3)
    begin, diag, plane, line, close, _, _ = scatter_plan(at, nz, rows_part, rows_out, take(refs, 23))
    product = product_plan(inputs, grads, take(refs, 6))
    bufs = [take(refs, 5) for _ in range(n)]
    sems = [take(refs, 12) for _ in range(n)]
    own_small = next(refs)
    scatter_small = SmallScatter(at, nz, part_small, own_small, take(refs, 4), take(refs, 4))
    gather_small = SmallGather(at, nz, own_small, out_small, take(refs, 4))
    greet([(at.fx, at.e), (at.fy, at.e), (at.f, at.pe)], (at, nz))
    scatter_small.stage(0)
    total = sum(counts)
    last = nz - 1
    lag, per = 2, 5

    class Piece:
        def __init__(self, k, p):
            self.p, self.part, self.out = p, parts[k], outs[k]
            self.acc, self.pb, self.zu, self.zd, self.mine = bufs[k]
            self.sems = sems[k]
            self.r = self.acc.shape[2]

        def load(self):
            p = self.p
            return pltpu.make_async_copy(self.part.at[p, at.c], self.acc.at[p], self.sems[0].at[p])

        def to_p(self):
            p, (_, s, r, *_rest) = self.p, self.sems
            return send(self.part.at[p, 1 - at.c], self.pb.at[p], s.at[p], r.at[p], at.f, at.pe)

        def go_up(self, z):
            p, s, r = self.p, self.sems[3], self.sems[4]
            return send(self.acc.at[p, z], self.zu.at[p, z], s.at[p, z], r.at[p, z], at.f, at.e + 2)

        def go_down(self, z):
            p, s, r = self.p, self.sems[5], self.sems[6]
            return send(self.acc.at[p, z], self.zd.at[p, z], s.at[p, z], r.at[p, z], at.f, at.e - 2)

        def res(self, z, way):
            p, s, r = self.p, self.sems[7], self.sems[8]
            ref = self.out.at[p, at.c, z]
            return send(ref, ref, s.at[way, p, z], r.at[p, z], at.f, at.e + 2 - 4 * way)

        def res_p(self, z):
            p, s, r = self.p, self.sems[9], self.sems[10]
            ref = self.out.at[p, at.c, z]
            return send(ref, ref, s.at[p, z], r.at[p, z], at.f, at.pe)

        def keep(self):
            p = self.p
            return pltpu.make_async_copy(self.mine.at[p], self.out.at[p, at.c, at.z], self.sems[11].at[p])

    def piece(q, run, when=True):
        low = 0
        for k, count in enumerate(counts):
            @pl.when((q >= low) & (q < low + count) & when)
            def _(k=k, low=low):
                run(Piece(k, q - low))

            low += count

    def start(it):
        it.load().start()
        it.to_p().start()

    piece(0, start)
    begin(0)
    piece(1, start)
    product.start()

    def halve(it):
        it.load().wait()
        it.to_p().wait_recv()
        p = it.p

        def body(z, carry):
            a = it.acc.at[p, z]
            add_rows(a, (0, it.r), [(a, 0), (it.pb.at[p, z], 0)])
            return carry

        lax.fori_loop(0, nz, body, 0)

    def rise(it):
        p = it.p

        def body(i, carry):
            z = last - i

            @pl.when(z > at.z)
            def _():
                a = it.acc.at[p, z]

                @pl.when(at.z > 0)
                def _():
                    it.go_up(z).wait_recv()
                    add_rows(a, (0, it.r), [(a, 0), (it.zu.at[p, z], 0)])

                it.go_up(z).start()

            return carry

        lax.fori_loop(0, last, body, 0)

    def sink(it):
        p = it.p

        def body(z, carry):
            @pl.when(z < at.z)
            def _():
                a = it.acc.at[p, z]

                @pl.when(at.z < last)
                def _():
                    it.go_down(z).wait_recv()
                    add_rows(a, (0, it.r), [(a, 0), (it.zd.at[p, z], 0)])

                it.go_down(z).start()

            return carry

        lax.fori_loop(0, last, body, 0)

    def settle(it):
        p, z = it.p, at.z
        pl.when(z > 0)(lambda: it.go_up(z).wait_recv())
        pl.when(z < last)(lambda: it.go_down(z).wait_recv())
        a, dst = (it.acc.at[p, z], 0), it.mine.at[p]
        up, down = (it.zu.at[p, z], 0), (it.zd.at[p, z], 0)
        pl.when((z > 0) & (z < last))(lambda: add_rows(dst, (0, it.r), [a, up, down]))
        pl.when(z == 0)(lambda: add_rows(dst, (0, it.r), [a, down]))
        pl.when(z == last)(lambda: add_rows(dst, (0, it.r), [a, up]))
        it.keep().start()

    def tell(it):
        z = at.z
        it.keep().wait()
        pl.when(z < last)(lambda: it.res(z, 0).start())
        pl.when(z > 0)(lambda: it.res(z, 1).start())
        it.res_p(z).start()

    def pass_up(it, z):
        it.res(z, 0).wait_recv()
        pl.when(at.z < last)(lambda: it.res(z, 0).start())
        it.res_p(z).start()

    def pass_down(it, z):
        it.res(z, 0).wait_recv()
        pl.when(at.z > 0)(lambda: it.res(z, 1).start())
        it.res_p(z).start()

    def body(i, carry):
        piece(i + 2, start)
        s, turn = i // per, i % per
        pl.when((turn == 0) & (s + 1 < nz))(lambda: begin(s + 1))
        pl.when((turn == 0) & (s < nz))(lambda: diag(s))
        pl.when((turn == 2) & (s < nz))(lambda: plane(s))
        pl.when((turn == 3) & (s >= 1) & (s < nz + 1))(lambda: line(s - 1))
        piece(i, halve)
        piece(i - lag * at.z, rise, at.z < last)
        piece(i - lag * (last - at.z), sink, at.z > 0)
        piece(i - lag * nz, settle)
        piece(i - lag * nz, tell)
        for d in range(1, nz):
            piece(i - lag * (nz + d), functools.partial(pass_up, z=at.z - d), at.z >= d)
            piece(i - lag * (nz + d), functools.partial(pass_down, z=at.z + d), at.z + d <= last)
        for s in range(1, 5):
            pl.when(i == s)(functools.partial(scatter_small.stage, s))
        for s in range(5):
            pl.when(i == 5 + s)(functools.partial(gather_small.stage, s))
        product.step(i)
        return carry

    steps = max(total + lag * (2 * nz - 1), per * (nz + 1), product.steps)
    lax.fori_loop(0, steps, body, 0)
    product.finish()

    def finish(q, carry):
        def run(it):
            it.to_p().wait_send()

            def one(z, carry):
                pl.when(z > at.z)(lambda: it.go_up(z).wait_send())
                pl.when(z < at.z)(lambda: it.go_down(z).wait_send())
                pl.when((z <= at.z) & (at.z < last))(lambda: it.res(z, 0).wait_send())
                pl.when((z >= at.z) & (at.z > 0))(lambda: it.res(z, 1).wait_send())
                it.res_p(z).wait_send()
                it.res_p(z).wait_recv()
                return carry

            lax.fori_loop(0, nz, one, 0)

        piece(q, run)
        return carry

    lax.fori_loop(0, total, finish, 0)
    close()


def line_sum(parts, small, rows, inputs, local, nz, cid):
    counts = tuple(p.shape[0] for p in parts)
    units, unit, width = inputs[0].shape
    wide = inputs[1].shape[3]
    scratch, sems = [], []
    for p in parts:
        n, _, _, r, c = p.shape

        def buf(*lead):
            return pltpu.VMEM((*lead, r, c), p.dtype)

        scratch += [buf(n, nz), buf(n, nz), buf(n, nz), buf(n, nz), buf(n)]
        each, line = DMA((n,)), DMA((n, nz))
        sems += [each, each, each, line, line, line, line, DMA((2, n, nz)), line, line, line, each]
    hbm, vmem = pl.BlockSpec(memory_space=pl.ANY), pl.BlockSpec(memory_space=pltpu.VMEM)
    return pl.pallas_call(
        functools.partial(line_sum_kernel, nz, counts),
        out_shape=(
            *(jax.ShapeDtypeStruct(p.shape, p.dtype) for p in parts),
            jax.ShapeDtypeStruct(small.shape, jnp.float32),
            jax.ShapeDtypeStruct(rows.shape[2:], jnp.float32),
            jax.ShapeDtypeStruct((local, width, wide // local), jnp.float32),
            jax.ShapeDtypeStruct((local, width, wide // local), jnp.float32),
            jax.ShapeDtypeStruct((wide, width), jnp.float32),
        ),
        in_specs=[hbm] * len(parts) + [vmem, hbm] + [hbm] * 3,
        out_specs=(*[hbm] * len(parts), vmem, vmem, *[hbm] * 3),
        scratch_shapes=[
            *scatter_scratch(rows, nz),
            pltpu.VMEM((local, width, 2 * wide // local), jnp.float32),
            pltpu.VMEM((wide, width), jnp.float32),
            pltpu.VMEM((2, unit, width), rows.dtype),
            pltpu.VMEM((2, unit, wide), rows.dtype),
            DMA((2, 3)), DMA((local + 1, 2)),
            *scratch, *sems, pltpu.VMEM(small.shape[-2:], jnp.float32),
            *SmallScatter.scratch(nz, small.shape[-2:]), *SmallScatter.sems(nz), *SmallGather.sems(nz),
        ],
        compiler_params=pltpu.CompilerParams(
            collective_id=cid, has_side_effects=True, vmem_limit_bytes=63 << 20
        ),
        cost_estimate=pl.CostEstimate(flops=0, bytes_accessed=300 << 20, transcendentals=0),
        name="line_sum",
    )(*parts, small, rows, *inputs)


def rope_tables(seg_ids, head_dim):
    length = seg_ids.shape[0]
    ordinal = lax.iota(jnp.int32, length)
    earlier = (seg_ids[:, None] == seg_ids[None, :]) & (ordinal[None, :] < ordinal[:, None])
    places = jnp.sum(earlier.astype(jnp.int32), axis=1).astype(jnp.float32)
    half_dim = head_dim // 2
    inv_freq = rope_base ** (
        -(lax.iota(jnp.int32, half_dim).astype(jnp.float32) * (2.0 / head_dim))
    )
    angles = places[:, None] * inv_freq[None, :]
    angles = jnp.concatenate([angles, angles], axis=1)
    return (jnp.cos(angles), jnp.sin(angles))


def rotate_half(values):
    half_dim = values.shape[-1] // 2
    return jnp.concatenate([-values[..., half_dim:], values[..., :half_dim]], axis=-1)


def rotate_back(values):
    half_dim = values.shape[-1] // 2
    return jnp.concatenate([values[..., half_dim:], -values[..., :half_dim]], axis=-1)


def apply_rope(values, cosine, sine_table):
    return values * cosine[:, None, :] + rotate_half(values) * sine_table[:, None, :]


def rope_grad(grads_in, cosine, sine_table):
    return grads_in * cosine[:, None, :] + rotate_back(grads_in * sine_table[:, None, :])


def across_heads(kernel, pair_sums):
    if kernel:
        return square_sum(jnp.stack(pair_sums), kernel)
    return lax.psum((pair_sums[0], pair_sums[1]), "fsdp")


def share_rows(kernel, term_fn, own_rows):
    if kernel:
        parts = term_fn(jnp.int32(0), own_rows * lax.axis_size("fsdp"))
        return square_scatter(parts.reshape(-1, own_rows, parts.shape[1]), kernel)
    return lax.psum_scatter(
        term_fn(jnp.int32(0), own_rows * lax.axis_size("fsdp")),
        "fsdp",
        scatter_dimension=0,
        tiled=True,
    )


def to_owner(block_rows):
    return lax.all_to_all(block_rows, "expert", split_axis=0, concat_axis=0, tiled=True)


def from_owner(block_rows):
    return lax.all_to_all(block_rows, "expert", split_axis=0, concat_axis=0, tiled=True)


def shard_gather(block_rows):
    return lax.all_gather(block_rows, "fsdp", axis=0, tiled=True)


def owner_sum(term_fn, sources):
    own_rows = sources // lax.axis_size("fsdp")
    return lax.psum_scatter(
        term_fn(jnp.int32(0), own_rows * lax.axis_size("fsdp")),
        "fsdp",
        scatter_dimension=0,
        tiled=True,
    )


def head_scores(q_heads, k_heads, allowed):
    scores = jnp.einsum(
        "thd,shd->hts", q_heads, k_heads, preferred_element_type=jnp.float32
    ) * HEAD_DIM ** (-0.5)
    return jnp.where(allowed[None], scores, -1e30)


def experts_by_slot(
    second_in, second_rows, cotangent, routes, capacity, w_router, w_gate, w_up, w_down
):
    tok_count, model_width = second_rows.shape
    experts = w_router.shape[1]
    local_experts = w_gate.shape[0]
    slot_count = tok_count * TOP * 3 // (2 * experts)
    pair_count = tok_count * TOP
    zero_row = jnp.zeros((1, model_width), jnp.bfloat16)
    logits = jnp.dot(second_rows, w_router, preferred_element_type=jnp.float32)
    chosen = routes
    expert_ids = lax.iota(jnp.int32, experts)
    chosen_hot = (chosen[:, :, None] == expert_ids[None, None, :]).astype(jnp.float32)
    routed = jnp.sum(chosen_hot * logits[:, None, :], axis=2)
    gate_wts = jax.nn.softmax(routed, axis=1)
    pair_hot = chosen_hot.reshape(pair_count, experts).astype(jnp.int32)
    earlier_hits = jnp.cumsum(pair_hot, axis=0) - pair_hot
    ranking = jnp.sum(earlier_hits * pair_hot, axis=1)
    cap_pair = jnp.sum(pair_hot * capacity[None, :], axis=1)
    is_kept = ranking < cap_pair
    pair_route = chosen.reshape(pair_count)
    slot_place = jnp.where(is_kept, pair_route * slot_count + ranking, experts * slot_count)
    pair_ids = lax.iota(jnp.int32, pair_count)
    slot_pair = (
        jnp.full((experts * slot_count,), pair_count, jnp.int32)
        .at[slot_place]
        .set(pair_ids, mode="drop")
    )
    padded = jnp.concatenate([second_rows, zero_row], axis=0)
    outgoing = padded[slot_pair // TOP].reshape(experts, slot_count, model_width)
    arrived = shard_gather(to_owner(outgoing))
    gate_w, up_w, down_w = (w_gate, w_up, w_down)
    owner_rows = arrived.reshape(-1, local_experts, slot_count, model_width)
    sources = owner_rows.shape[0]
    gate_act = jnp.einsum("sjcd,jdh->sjch", owner_rows, gate_w, preferred_element_type=jnp.float32)
    up_act = jnp.einsum("sjcd,jdh->sjch", owner_rows, up_w, preferred_element_type=jnp.float32)
    sig_gate = jax.nn.sigmoid(gate_act)
    silu_gate = gate_act * sig_gate
    hidden = (silu_gate * up_act).astype(jnp.bfloat16)

    def down_term(start, length):
        return jnp.einsum("sjch,jhd->sjcd", hidden, down_w, preferred_element_type=jnp.float32)

    produced = owner_sum(down_term, sources)
    returned = from_owner(produced.astype(jnp.bfloat16).reshape(-1, slot_count, model_width))
    slot_rows = jnp.concatenate(
        [returned.reshape(experts * slot_count, model_width), zero_row], axis=0
    )
    pair_rows = slot_rows[slot_place].reshape(tok_count, TOP, model_width).astype(jnp.float32)
    kept_mask = is_kept.reshape(tok_count, TOP).astype(jnp.float32)
    gate_kept = gate_wts * kept_mask
    moe_rows = jnp.sum(gate_kept[:, :, None] * pair_rows, axis=1)
    final_rows = second_in + moe_rows
    block_output = final_rows.astype(jnp.bfloat16)
    grad_out = cotangent.astype(jnp.float32)
    grad_gate_k = jnp.sum(pair_rows * grad_out[:, None, :], axis=2) * kept_mask
    grad_routed = gate_wts * (grad_gate_k - jnp.sum(gate_wts * grad_gate_k, axis=1, keepdims=True))
    grad_logits = jnp.sum(chosen_hot * grad_routed[:, :, None], axis=1)
    router_grad = jnp.dot(second_rows.astype(jnp.float32).T, grad_logits, precision=precise)
    grad_second = jnp.dot(grad_logits, w_router.astype(jnp.float32).T, precision=precise)
    pair_grads = (
        (gate_kept[:, :, None] * grad_out[:, None, :])
        .astype(jnp.bfloat16)
        .reshape(pair_count, model_width)
    )
    pair_grads = jnp.concatenate([pair_grads, zero_row], axis=0)
    slot_grads = pair_grads[slot_pair].reshape(experts, slot_count, model_width)
    grad_blocks = shard_gather(to_owner(slot_grads)).reshape(
        -1, local_experts, slot_count, model_width
    )
    grad_hidden = jnp.einsum(
        "sjcd,jhd->sjch", grad_blocks, down_w, preferred_element_type=jnp.float32
    )
    grad_down_w = jnp.einsum(
        "sjch,sjcd->jhd", hidden, grad_blocks, preferred_element_type=jnp.float32
    )
    grad_gate_in = (grad_hidden * up_act * sig_gate * (1.0 + gate_act * (1.0 - sig_gate))).astype(
        jnp.bfloat16
    )
    grad_up_in = (grad_hidden * silu_gate).astype(jnp.bfloat16)
    grad_gate_w = jnp.einsum(
        "sjcd,sjch->jdh", owner_rows, grad_gate_in, preferred_element_type=jnp.float32
    )
    grad_up_w = jnp.einsum(
        "sjcd,sjch->jdh", owner_rows, grad_up_in, preferred_element_type=jnp.float32
    )

    def back_term(start, length):
        from_gate = jnp.einsum(
            "sjch,jdh->sjcd", grad_gate_in, gate_w, preferred_element_type=jnp.float32
        )
        from_up = jnp.einsum("sjch,jdh->sjcd", grad_up_in, up_w, preferred_element_type=jnp.float32)
        return from_gate + from_up

    grad_slots = from_owner(
        owner_sum(back_term, sources).astype(jnp.bfloat16).reshape(-1, slot_count, model_width)
    )
    back_rows = jnp.concatenate(
        [grad_slots.reshape(experts * slot_count, model_width), zero_row], axis=0
    )
    grad_second = grad_second + jnp.sum(
        back_rows[slot_place].reshape(tok_count, TOP, model_width).astype(jnp.float32), axis=1
    )
    return block_output[None], grad_second, router_grad.T, (grad_gate_w, grad_up_w, grad_down_w)


def experts_dense(
    second_in, second_rows, cotangent, routes, capacity, w_router, w_gate, w_up, w_down
):
    tok_count = second_rows.shape[0]
    experts = w_router.shape[1]
    local_experts, model_width, hidden_here = w_gate.shape
    shards = lax.axis_size("fsdp")
    owners = lax.axis_size("expert")
    wide = local_experts * hidden_here
    logits = jnp.dot(second_rows, w_router, preferred_element_type=jnp.float32)
    expert_ids = lax.iota(jnp.int32, experts)
    named = jnp.any(routes[:, :, None] == expert_ids[None, None, :], axis=1)
    before = lax.iota(jnp.int32, tok_count)[None, :] < lax.iota(jnp.int32, tok_count)[:, None]
    ranking = jnp.dot(
        before.astype(jnp.bfloat16), named.astype(jnp.bfloat16), preferred_element_type=jnp.float32
    )
    kept = named & (ranking < capacity.astype(jnp.float32)[None, :])
    kept_mask = kept.astype(jnp.float32)
    top_logit = jnp.max(jnp.where(named, logits, -jnp.inf), axis=1, keepdims=True)
    powers = jnp.where(named, jnp.exp(jnp.where(named, logits - top_logit, 0.0)), 0.0)
    gate_wts = powers / jnp.sum(powers, axis=1, keepdims=True)
    gate_kept = gate_wts * kept_mask

    grad_all = lax.all_gather(cotangent, ("fsdp", "expert"), axis=0, tiled=True)
    nz = owners // 2
    grad_all = grad_all.reshape(shards, owners, tok_count, model_width)
    rows_all, pre, gates = gather_act(second_rows, gate_kept.T, w_gate, w_up, nz, 7)
    back_rows, terms, acts, forward = scatter_act(
        pre, grad_all, gates, w_gate, w_up, w_down, nz, 8
    )
    grad_gate_k = terms.T * kept_mask
    grad_logits = gate_wts * (grad_gate_k - jnp.sum(gate_wts * grad_gate_k, axis=1, keepdims=True))
    router_grad = jnp.dot(grad_logits.T, second_rows.astype(jnp.float32), precision=precise)
    grad_second = jnp.dot(grad_logits, w_router.astype(jnp.float32).T, precision=precise)
    grad_second = grad_second + back_rows

    units = shards * nz
    inputs = (
        rows_all.reshape(units, -1, model_width),
        acts.reshape(3, units, -1, wide),
        grad_all.reshape(units, -1, model_width),
    )
    return forward, grad_second, router_grad, inputs


def sum_grads(narrow, gains, head_gains, rows, inputs, local, nz):
    shards, width = lax.axis_size("fsdp"), gains.shape[1]
    mine = lax.iota(jnp.int32, shards) == lax.axis_index("fsdp")
    heads_flat = jnp.pad(head_gains.reshape(-1), (0, width - head_gains.size))
    table = jnp.concatenate([gains, jnp.where(mine[:, None], heads_flat[None], 0.0)], axis=0)
    share = -(-table.size // (2 * shards * nz * 1024)) * 8
    small = jnp.pad(table.reshape(-1), (0, 2 * shards * nz * share * 128 - table.size))
    small = small.reshape(2, shards, nz, share, 128)
    parts = [g.reshape(-1, 2, nz, 16, g.shape[1]) for g in narrow]
    *sums, small, rows, gate, up, down = line_sum(parts, small, rows, inputs, local, nz, 9)
    expert_grads = (gate, up, down.reshape(local, -1, width))
    small = small.reshape(-1)[: table.size].reshape(table.shape)
    own = lax.dynamic_slice_in_dim(small, gains.shape[0] + lax.axis_index("fsdp"), 1, axis=0)
    head_gains = own[0, : head_gains.size].reshape(head_gains.shape)
    return [s.reshape(g.shape) for s, g in zip(sums, narrow)], small[: gains.shape[0]], head_gains, rows, expert_grads


def on_device(
    block_input,
    cotangent,
    w_query,
    w_key,
    w_value,
    w_output,
    q_gain,
    k_gain,
    attn_gain,
    mlp_gain,
    w_router,
    w_gate,
    w_up,
    w_down,
    segments,
    routes,
    capacity,
):
    tok_count = block_input.shape[1]
    model_width = block_input.shape[2]
    experts = w_router.shape[1]
    nz = lax.axis_size("expert") // 2
    dense = 2 * TOP >= experts and lax.axis_size("fsdp") == 4
    flat_in = block_input[0].astype(jnp.float32)
    scale_one = lax.rsqrt(jnp.mean(flat_in * flat_in, axis=1, keepdims=True) + epsilon)
    normed_one = flat_in * scale_one
    first_rows = (normed_one * attn_gain).astype(jnp.bfloat16)
    if dense:
        group_rows, group_segs = square_gather(first_rows, jnp.tile(segments, (8, 1)), 1)
        group_rows = group_rows.reshape(-1, model_width)
        group_segs = group_segs[:, 0].reshape(-1)
    else:
        group_rows, group_segs = (
            lax.all_gather(first_rows, "fsdp", axis=0, tiled=True),
            lax.all_gather(segments[0], "fsdp", axis=0, tiled=True),
        )
    group_len = group_rows.shape[0]
    heads_here = w_query.shape[1] // HEAD_DIM
    query_rows = jnp.dot(group_rows, w_query, preferred_element_type=jnp.float32)
    key_rows = jnp.dot(group_rows, w_key, preferred_element_type=jnp.float32)
    value_rows = jnp.dot(group_rows, w_value, preferred_element_type=jnp.float32).astype(
        jnp.bfloat16
    )
    square_sums = across_heads(
        dense and 2,
        (jnp.sum(query_rows * query_rows, axis=1), jnp.sum(key_rows * key_rows, axis=1))
    )
    q_scale = lax.rsqrt(square_sums[0][:, None] / model_width + epsilon)
    k_scale = lax.rsqrt(square_sums[1][:, None] / model_width + epsilon)
    cosine, sine_table = rope_tables(group_segs, HEAD_DIM)
    head_shape = (group_len, heads_here, HEAD_DIM)
    q_heads = apply_rope(
        (query_rows * q_scale * q_gain).reshape(head_shape), cosine, sine_table
    ).astype(jnp.bfloat16)
    k_heads = apply_rope(
        (key_rows * k_scale * k_gain).reshape(head_shape), cosine, sine_table
    ).astype(jnp.bfloat16)
    v_heads = value_rows.reshape(head_shape)
    ordinal = lax.iota(jnp.int32, group_len)
    allowed = (group_segs[:, None] == group_segs[None, :]) & (ordinal[None, :] <= ordinal[:, None])
    scores = head_scores(q_heads, k_heads, allowed)
    row_top = jnp.max(scores, axis=2, keepdims=True)
    log_total = row_top + jnp.log(jnp.sum(jnp.exp(scores - row_top), axis=2, keepdims=True))
    attn_weights = jnp.exp(scores - log_total)
    mixed_heads = jnp.einsum(
        "hts,shd->thd",
        attn_weights.astype(jnp.bfloat16),
        v_heads,
        preferred_element_type=jnp.float32,
    )
    attn_rows = mixed_heads.reshape(group_len, heads_here * HEAD_DIM).astype(jnp.bfloat16)

    def mixed_term(start, length):
        return jnp.dot(attn_rows, w_output, preferred_element_type=jnp.float32).astype(jnp.bfloat16)

    mixed_rows = share_rows(dense and 4, mixed_term, tok_count).astype(jnp.float32)
    second_in = flat_in + mixed_rows
    scale_two = lax.rsqrt(jnp.mean(second_in * second_in, axis=1, keepdims=True) + epsilon)
    normed_two = second_in * scale_two
    second_rows = (normed_two * mlp_gain).astype(jnp.bfloat16)
    if dense:
        block_output, grad_second, router_grad, expert_grads = experts_dense(
            second_in, second_rows, cotangent[0], routes[0], capacity, w_router, w_gate, w_up, w_down
        )
    else:
        block_output, grad_second, router_grad, expert_grads = experts_by_slot(
            second_in, second_rows, cotangent[0], routes[0], capacity, w_router, w_gate, w_up, w_down
        )
    grad_out = cotangent[0].astype(jnp.float32)
    mlp_gain_grad = jnp.sum(grad_second * normed_two, axis=0)
    grad_normed_two = grad_second * mlp_gain
    grad_mid = grad_out + scale_two * (
        grad_normed_two - normed_two * jnp.mean(grad_normed_two * normed_two, axis=1, keepdims=True)
    )
    if dense:
        group_grad, _ = square_gather(grad_mid.astype(jnp.bfloat16), jnp.tile(segments, (8, 1)), 6)
        group_grad = group_grad.reshape(-1, model_width)
    else:
        group_grad = lax.all_gather(grad_mid.astype(jnp.bfloat16), "fsdp", axis=0, tiled=True)
    out_grad = jnp.einsum("ti,td->id", attn_rows, group_grad, preferred_element_type=jnp.float32)
    grad_attn = (
        jnp.einsum("td,id->ti", group_grad, w_output, preferred_element_type=jnp.float32)
        .astype(jnp.bfloat16)
        .reshape(head_shape)
    )
    scores_again = head_scores(q_heads, k_heads, allowed)
    weights_again = jnp.exp(scores_again - log_total)
    grad_values = jnp.einsum(
        "hts,thd->shd",
        weights_again.astype(jnp.bfloat16),
        grad_attn,
        preferred_element_type=jnp.float32,
    )
    grad_weights = jnp.einsum(
        "thd,shd->hts", grad_attn, v_heads, preferred_element_type=jnp.float32
    )
    inner_sum = jnp.sum(weights_again * grad_weights, axis=2, keepdims=True)
    grad_scores = (weights_again * (grad_weights - inner_sum)).astype(jnp.bfloat16)
    grad_q_heads = jnp.einsum(
        "hts,shd->thd", grad_scores, k_heads, preferred_element_type=jnp.float32
    ) * HEAD_DIM ** (-0.5)
    grad_k_heads = jnp.einsum(
        "hts,thd->shd", grad_scores, q_heads, preferred_element_type=jnp.float32
    ) * HEAD_DIM ** (-0.5)
    grad_q_normed = rope_grad(grad_q_heads, cosine, sine_table).reshape(group_len, -1)
    grad_k_normed = rope_grad(grad_k_heads, cosine, sine_table).reshape(group_len, -1)
    q_gain_grad = jnp.sum(grad_q_normed * query_rows * q_scale, axis=0)
    k_gain_grad = jnp.sum(grad_k_normed * key_rows * k_scale, axis=0)
    inner_q = grad_q_normed * q_gain
    inner_k = grad_k_normed * k_gain
    inner_sums = across_heads(
        dense and 3,
        (jnp.sum(inner_q * query_rows, axis=1), jnp.sum(inner_k * key_rows, axis=1))
    )
    grad_query_rows = (
        q_scale
        * (inner_q - query_rows * q_scale * q_scale * (inner_sums[0][:, None] / model_width))
    ).astype(jnp.bfloat16)
    grad_key_rows = (
        k_scale * (inner_k - key_rows * k_scale * k_scale * (inner_sums[1][:, None] / model_width))
    ).astype(jnp.bfloat16)
    grad_value_rows = grad_values.reshape(group_len, -1).astype(jnp.bfloat16)
    head_grads = jnp.concatenate([grad_query_rows, grad_key_rows, grad_value_rows], axis=1)
    mixer_grad = jnp.einsum(
        "td,ti->di", group_rows, head_grads, preferred_element_type=jnp.float32
    ).astype(jnp.bfloat16)

    def input_term(start, length):
        from_q = jnp.einsum(
            "ti,di->td", grad_query_rows, w_query, preferred_element_type=jnp.float32
        )
        from_k = jnp.einsum("ti,di->td", grad_key_rows, w_key, preferred_element_type=jnp.float32)
        from_v = jnp.einsum(
            "ti,di->td", grad_value_rows, w_value, preferred_element_type=jnp.float32
        )
        return (from_q + from_k + from_v).astype(jnp.bfloat16)

    grad_first = share_rows(dense and 5, input_term, tok_count).astype(jnp.float32)
    attn_gain_grad = jnp.sum(grad_first * normed_one, axis=0)
    grad_normed_one = grad_first * attn_gain
    grad_x = grad_mid + scale_one * (
        grad_normed_one - normed_one * jnp.mean(grad_normed_one * normed_one, axis=1, keepdims=True)
    )
    narrow = (mixer_grad, out_grad.astype(jnp.bfloat16))
    gains = jnp.concatenate([attn_gain_grad[None], mlp_gain_grad[None], router_grad], axis=0)
    head_gains = jnp.stack([q_gain_grad, k_gain_grad])
    if dense:
        narrow, gains, head_gains, forward, expert_grads = sum_grads(
            narrow, gains, head_gains, block_output, expert_grads, w_gate.shape[0], nz
        )
        block_output = (second_in + forward).astype(jnp.bfloat16)[None]
    else:
        narrow = lax.psum(narrow, "expert")
        head_gains = lax.psum(head_gains, "expert")
        gains = lax.psum(gains, ("fsdp", "expert"))
    wide = tuple(jnp.split(narrow[0], 3, axis=1)) + (narrow[1],)
    mixer = tuple(g.astype(jnp.float32) for g in wide) + (head_gains[0], head_gains[1])
    return (
        block_output,
        grad_x[None],
        mixer[0],
        mixer[1],
        mixer[2],
        mixer[3],
        mixer[4],
        mixer[5],
        gains[0],
        gains[1],
        gains[2:].T,
        *expert_grads,
    )


def solution(mesh):
    placed = (
        P("expert", "fsdp", None),
        P("expert", "fsdp", None),
        P(None, "fsdp"),
        P(None, "fsdp"),
        P(None, "fsdp"),
        P("fsdp", None),
        P("fsdp"),
        P("fsdp"),
        P(),
        P(),
        P(),
        P("expert", None, "fsdp"),
        P("expert", None, "fsdp"),
        P("expert", "fsdp", None),
        P("expert", "fsdp"),
        P("expert", "fsdp", None),
        P(),
    )
    return jax.shard_map(
        on_device,
        mesh=mesh,
        in_specs=placed,
        out_specs=(
            P("expert", "fsdp", None),
            P("expert", "fsdp", None),
            P(None, "fsdp"),
            P(None, "fsdp"),
            P(None, "fsdp"),
            P("fsdp", None),
            P("fsdp"),
            P("fsdp"),
            P(),
            P(),
            P(),
            P("expert", None, "fsdp"),
            P("expert", None, "fsdp"),
            P("expert", "fsdp", None),
        ),
        check_vma=False,
    )
```

```python
import functools

import jax
import jax.numpy as jnp
from jax import lax
from jax.experimental import pallas as pl
from jax.experimental.pallas import tpu as pltpu
from jax.sharding import PartitionSpec as P

HEAD_DIM = 128
TOP = 8


epsilon = 1e-05
rope_base = 10000.0
precise = lax.Precision.HIGHEST


MESH = pl.DeviceIdType.MESH
DMA = pltpu.SemaphoreType.DMA


class Place:
    def __init__(self):
        self.f, self.e = lax.axis_index("fsdp"), lax.axis_index("expert")
        self.c, self.z = self.e % 2, self.e // 2
        self.fx = self.f + 1 - 2 * (self.f % 2)
        self.fy = (self.f + 2) % 4
        self.fd = 3 - self.f
        self.pe = self.e + 1 - 2 * self.c


def send(src, dst, send_sem, recv_sem, f, e):
    return pltpu.make_async_remote_copy(
        src_ref=src,
        dst_ref=dst,
        send_sem=send_sem,
        recv_sem=recv_sem,
        device_id={"fsdp": f, "expert": e},
        device_id_type=MESH,
    )


def greet(peers, line=None):
    barrier = pltpu.get_barrier_semaphore()

    def hello(f, e):
        pl.semaphore_signal(
            barrier, inc=1, device_id={"fsdp": f, "expert": e}, device_id_type=MESH
        )

    for f, e in peers:
        hello(f, e)
    if line is not None:
        at, nz = line
        for step in range(1, nz):
            hello(at.f, 2 * ((at.z + step) % nz) + at.c)
        pl.semaphore_wait(barrier, len(peers) + nz - 1)
    else:
        pl.semaphore_wait(barrier, len(peers))


class SmallGather:
    sems = staticmethod(
        lambda nz: [DMA((nz,)), DMA((nz,)), DMA((4,)), DMA((4,))]
    )

    def __init__(self, at, nz, own, out, sems):
        self.at, self.nz, self.own, self.out = at, nz, own, out
        self.ls, self.lr, self.ss, self.sr = sems

    def line(self, step):
        at = self.at
        z = (at.z + step) % self.nz
        back = (at.z + self.nz - step) % self.nz
        slot = self.out.at[at.c, at.f]
        to = send(self.own, slot.at[at.z], self.ls.at[step], self.lr.at[step], at.f, 2 * z + at.c)
        come = send(self.own, slot.at[back], self.ls.at[step], self.lr.at[step], at.f, 2 * z + at.c)
        return to, come

    def plane(self, i):
        at, out = self.at, self.out
        f, to_f = ((at.f, at.fx), (at.f, at.fy), (at.fx, at.fy))[i]
        slot = out.at[at.c, f]
        return send(slot, slot, self.ss.at[i], self.sr.at[i], to_f, at.e)

    def pair(self):
        at = self.at
        slot = self.out.at[at.c]
        return send(slot, slot, self.ss.at[3], self.sr.at[3], at.f, at.pe)

    def stage(self, i):
        at = self.at
        if i == 0:
            for step in range(1, self.nz):
                self.line(step)[0].start()
            self.out[at.c, at.f, at.z] = self.own[...]
        elif i == 1:
            for step in range(1, self.nz):
                self.line(step)[1].wait_recv()
            self.plane(0).start()
            self.plane(1).start()
        elif i == 2:
            self.plane(0).wait_recv()
            self.plane(2).start()
        elif i == 3:
            self.plane(1).wait_recv()
            self.plane(2).wait_recv()
            self.pair().start()
        elif i == 4:
            self.pair().wait_recv()
            self.pair().wait_send()
            for step in range(1, self.nz):
                self.line(step)[0].wait_send()
            for k in range(3):
                self.plane(k).wait_send()


class SmallScatter:
    sems = staticmethod(lambda nz: [DMA((nz,)), DMA((nz,)), DMA((4,)), DMA((4,))])
    scratch = staticmethod(
        lambda nz, shape: [
            pltpu.VMEM((4, nz, *shape), jnp.float32),
            pltpu.VMEM((4, nz, *shape), jnp.float32),
            pltpu.VMEM((3, nz, *shape), jnp.float32),
            pltpu.VMEM((nz, *shape), jnp.float32),
        ]
    )

    def __init__(self, at, nz, part, out, scratch, sems):
        self.at, self.nz, self.part, self.out = at, nz, part, out
        self.acc, self.pb, self.xy, self.zb = scratch
        self.ls, self.lr, self.ss, self.sr = sems

    def pair(self):
        at = self.at
        return send(
            self.part.at[1 - at.c], self.pb, self.ss.at[0], self.sr.at[0], at.f, at.pe
        )

    def plane(self, i):
        at = self.at
        f, to_f = ((at.fx, at.fx), (at.fd, at.fx), (at.fy, at.fy))[i]
        return send(
            self.acc.at[f], self.xy.at[i], self.ss.at[1 + i], self.sr.at[1 + i], to_f, at.e
        )

    def line(self, step):
        at = self.at
        z = (at.z + step) % self.nz
        return send(
            self.acc.at[at.f, z], self.zb.at[step], self.ls.at[step], self.lr.at[step], at.f, 2 * z + at.c
        )

    def stage(self, i):
        at, acc, xy = self.at, self.acc, self.xy
        if i == 0:
            self.pair().start()
        elif i == 1:
            self.pair().wait_recv()
            acc[...] = self.part[at.c] + self.pb[...]
            self.plane(0).start()
            self.plane(1).start()
        elif i == 2:
            self.plane(0).wait_recv()
            self.plane(1).wait_recv()
            acc[at.fy] = acc[at.fy] + xy[1]
            self.plane(2).start()
            acc[at.f] = acc[at.f] + xy[0]
        elif i == 3:
            self.plane(2).wait_recv()
            acc[at.f] = acc[at.f] + xy[2]
            for step in range(1, self.nz):
                self.line(step).start()
        elif i == 4:
            total = acc[at.f, at.z]
            for step in range(1, self.nz):
                self.line(step).wait_recv()
                total = total + self.zb[step]
            self.out[...] = total
            self.pair().wait_send()
            for k in range(3):
                self.plane(k).wait_send()
            for step in range(1, self.nz):
                self.line(step).wait_send()


def take(sequence, count):
    return [next(sequence) for _ in range(count)]


NT = (((1,), (1,)), ((), ()))
TN = (((0,), (0,)), ((), ()))


def halves_of(x):
    high = x.astype(jnp.bfloat16)
    return high, (x - high.astype(jnp.float32)).astype(jnp.bfloat16)


def spread(blocks, first, hidden, wide):
    experts = blocks[0].shape[0]
    high, low = halves_of(jnp.concatenate(blocks, axis=1))
    row = lax.broadcasted_iota(jnp.int32, (2 * experts, wide), 0) % experts
    col = lax.broadcasted_iota(jnp.int32, (2 * experts, wide), 1) // hidden
    pick = (row == first + col).astype(jnp.float32).astype(jnp.bfloat16)
    both = jnp.concatenate([high.astype(jnp.float32), low.astype(jnp.float32)], axis=0)
    return lax.dot_general(
        both.astype(jnp.bfloat16), pick, TN, preferred_element_type=jnp.float32
    )


def above(a, b):
    return (a - b + 63) // 64


def near_first(at, nz, s):
    right = above(2 * at.z, nz - 1)
    alternate = at.z - right * (2 * at.z - (nz - 1))
    turn = at.z + (s + 1) // 2 * (1 - 2 * (s % 2))
    rest = s + right * (nz - 1 - 2 * s)
    return turn + above(s, 2 * alternate) * (rest - turn)


def gather_act_kernel(nz, own, own_small, w_gate, w_up, w_down, out, acts, weighted, forward, gates, xb, ab, hb, fb, load_x, store, own_sem, zr, zs, xr, xs, yr, ys, dr, xf, yf, pr, ps, *small_sems):
    at = Place()
    rows, width = own.shape
    local, _, hidden = w_gate.shape
    half = rows // 2
    halves = (pl.ds(0, half), pl.ds(half, half))
    small = SmallGather(at, nz, own_small, gates, small_sems)
    greet([(at.fx, at.e), (at.fy, at.e), (at.f, at.pe)], (at, nz))
    keep = pltpu.make_async_copy(own, out.at[at.f, at.e], own_sem)
    keep.start()
    small.stage(0)
    places = (at.f, at.fx, at.fy, at.fd)
    first = at.e * w_gate.shape[0]

    def up(z):
        ref = out.at[at.f, 2 * z + at.c]
        return send(ref, ref, zs.at[0, z], zr.at[z], at.f, at.e + 2)

    def down(z):
        ref = out.at[at.f, 2 * z + at.c]
        return send(ref, ref, zs.at[1, z], zr.at[z], at.f, at.e - 2)

    def to_x(z, h):
        ref = out.at[at.f, 2 * z + at.c, halves[h]]
        return send(ref, ref, xs.at[h, z], xr.at[h, z], at.fx, at.e)

    def to_y(z, h):
        ref = out.at[at.f, 2 * z + at.c, halves[h]]
        return send(ref, ref, ys.at[h, z], yr.at[h, z], at.fy, at.e)

    def x_on(z):
        ref = out.at[at.fx, 2 * z + at.c, halves[0]]
        return send(ref, ref, yf.at[z], dr.at[0, z], at.fy, at.e)

    def y_on(z):
        ref = out.at[at.fy, 2 * z + at.c, halves[1]]
        return send(ref, ref, xf.at[z], dr.at[1, z], at.fx, at.e)

    def to_p(f, z, h):
        ref = out.at[f, 2 * z + at.c, halves[h]]
        return send(ref, ref, ps.at[f, z, h], pr.at[f, z, h], at.f, at.pe)

    def line_step(z):
        pl.when(z != at.z)(lambda: up(z).wait_recv())
        pl.when((z <= at.z) & (at.z < nz - 1))(lambda: up(z).start())
        pl.when((z >= at.z) & (at.z > 0))(lambda: down(z).start())
        to_x(z, 0).start()
        to_y(z, 1).start()
        to_x(z, 1).start()
        to_y(z, 0).start()
        for h in range(2):
            to_p(at.f, z, h).start()

    def plane_step(z):
        to_x(z, 0).wait_recv()
        x_on(z).start()
        to_y(z, 1).wait_recv()
        y_on(z).start()
        to_p(at.fx, z, 0).start()
        to_p(at.fy, z, 1).start()
        to_x(z, 1).wait_recv()
        to_p(at.fx, z, 1).start()
        to_y(z, 0).wait_recv()
        to_p(at.fy, z, 0).start()

    def diag_step(z):
        x_on(z).wait_recv()
        to_p(at.fd, z, 0).start()
        y_on(z).wait_recv()
        to_p(at.fd, z, 1).start()

    def load(q, z):
        return pltpu.make_async_copy(out.at[places[q], pl.ds(2 * z, 2)], xb.at[q], load_x.at[q])

    def stores(q, z):
        pair, f = pl.ds(2 * z, 2), places[q]
        return [
            *(
                pltpu.make_async_copy(ab.at[q, k], acts.at[k, f, pair], store.at[q, k])
                for k in range(3)
            ),
            pltpu.make_async_copy(hb.at[q], weighted.at[f, pair], store.at[q, 3]),
            pltpu.make_async_copy(fb.at[q], forward.at[f, pair], store.at[q, 4]),
        ]

    def fetch(q, z):
        for h in range(2):
            to_p(places[q], z, h).wait_recv()
        load(q, z).start()

    def work(q, z):
        load(q, z).wait()
        f = places[q]
        x = xb[q].reshape(2 * rows, width)
        gate_all = spread([gates[0, f, z], gates[1, f, z]], first, hidden, local * hidden)
        for j in range(local):
            cols = pl.ds(j * hidden, hidden)
            g_all = jnp.dot(x, w_gate[j], preferred_element_type=jnp.float32)
            u_all = jnp.dot(x, w_up[j], preferred_element_type=jnp.float32)
            for h in range(2):
                g, u = g_all[h * rows : (h + 1) * rows], u_all[h * rows : (h + 1) * rows]
                gate = gate_all[h * rows : (h + 1) * rows, j * hidden : (j + 1) * hidden]
                sig = 1.0 / (1.0 + jnp.exp(-g))
                silu = g * sig
                hid = silu * u
                ab[q, 0, h, :, cols] = u * sig * (1.0 + g * (1.0 - sig))
                ab[q, 1, h, :, cols] = silu
                ab[q, 2, h, :, cols] = hid
                hb[q, h, :, cols] = (hid * gate).astype(jnp.bfloat16)
        a = hb[q].reshape(2 * rows, local * hidden)

        def body(t, carry):
            cols = pl.ds(pl.multiple_of(t * 512, 512), 512)
            total = jnp.dot(a, w_down[:, cols], preferred_element_type=jnp.float32)
            fb[q, :, :, cols] = total.astype(jnp.bfloat16).reshape(2, rows, 512)
            return carry

        lax.fori_loop(0, width // 512, body, 0)
        for copy in stores(q, z):
            copy.start()

    keep.wait()

    def body(s, carry):
        def at_step(lag, run):
            pl.when((s >= lag) & (s < nz + lag))(lambda: run(near_first(at, nz, s - lag)))

        def free(q, lag):
            def run(z):
                for copy in stores(q, z):
                    copy.wait()

            at_step(lag + 1, run)

        at_step(0, line_step)
        for k in range(1, 5):
            pl.when(s == 0)(functools.partial(small.stage, k))
        at_step(1, lambda z: fetch(0, z))
        free(3, 4)
        at_step(4, lambda z: work(3, z))
        at_step(1, plane_step)
        at_step(2, lambda z: fetch(1, z))
        free(0, 1)
        at_step(1, lambda z: work(0, z))
        at_step(2, diag_step)
        at_step(2, lambda z: fetch(2, z))
        free(1, 2)
        at_step(2, lambda z: work(1, z))
        at_step(3, lambda z: fetch(3, z))
        free(2, 2)
        at_step(2, lambda z: work(2, z))
        return carry

    lax.fori_loop(0, nz + 5, body, 0)

    def finish(z, carry):
        pl.when((z <= at.z) & (at.z < nz - 1))(lambda: up(z).wait_send())
        pl.when((z >= at.z) & (at.z > 0))(lambda: down(z).wait_send())
        for h in range(2):
            to_x(z, h).wait_send()
            to_y(z, h).wait_send()
        x_on(z).wait_send()
        y_on(z).wait_send()
        for f in range(4):
            for h in range(2):
                to_p(f, z, h).wait_send()
        return carry

    lax.fori_loop(0, nz, finish, 0)


def gather_act(rows, small, w_gate, w_up, w_down, nz, cid):
    r, c = rows.shape
    local, _, hidden = w_gate.shape
    wide = local * hidden
    hbm, vmem = pl.BlockSpec(memory_space=pl.ANY), pl.BlockSpec(memory_space=pltpu.VMEM)
    bf16 = jnp.bfloat16
    return pl.pallas_call(
        functools.partial(gather_act_kernel, nz),
        out_shape=(
            jax.ShapeDtypeStruct((4, 2 * nz, r, c), bf16),
            jax.ShapeDtypeStruct((3, 4, 2 * nz, r, wide), jnp.float32),
            jax.ShapeDtypeStruct((4, 2 * nz, r, wide), bf16),
            jax.ShapeDtypeStruct((4, 2 * nz, r, c), bf16),
            jax.ShapeDtypeStruct((2, 4, nz, *small.shape), jnp.float32),
        ),
        in_specs=[vmem] * 5,
        out_specs=(hbm, hbm, hbm, hbm, vmem),
        scratch_shapes=[
            pltpu.VMEM((4, 2, r, c), bf16),
            pltpu.VMEM((4, 3, 2, r, wide), jnp.float32),
            pltpu.VMEM((4, 2, r, wide), bf16),
            pltpu.VMEM((4, 2, r, c), bf16),
            DMA((4,)), DMA((4, 5)),
            DMA(()), DMA((nz,)), DMA((2, nz)), DMA((2, nz)), DMA((2, nz)), DMA((2, nz)), DMA((2, nz)),
            DMA((2, nz)), DMA((nz,)), DMA((nz,)), DMA((4, nz, 2)), DMA((4, nz, 2)),
            *SmallGather.sems(nz),
        ],
        compiler_params=pltpu.CompilerParams(
            collective_id=cid, has_side_effects=True, vmem_limit_bytes=50 << 20
        ),
        cost_estimate=pl.CostEstimate(flops=0, bytes_accessed=240 << 20, transcendentals=0),
        name="gather_act",
    )(rows, small, w_gate, w_up, w_down.reshape(wide, c))


def add_rows(dst, dst_rows, parts):
    start, count = dst_rows

    def body(i, carry):
        r = pl.multiple_of(i * 16, 16)
        total = None
        for ref, offset in parts:
            piece = ref[pl.ds(offset + r, 16), :].astype(jnp.float32)
            total = piece if total is None else total + piece
        dst[pl.ds(start + r, 16), :] = total.astype(dst.dtype)
        return carry

    lax.fori_loop(0, count // 16, body, 0)


def scatter_plan(at, nz, part, out, refs, staged=None, split=1):
    acc, pb, xh, yh, xf, yf, zu, zd, ls, pr, ps, xhs, xhr, yhs, yhr, xs, xr, ys, yr, us, ur, ds_, dr = refs
    rows = out.shape[0]
    half = rows // 2
    lo, hi = pl.ds(0, half), pl.ds(half, half)

    def place(s):
        return near_first(at, nz, nz - 1 - s)

    def load(f, z):
        return pltpu.make_async_copy(part.at[f, 2 * z + at.c], acc.at[f, z], ls.at[f, z])

    fs = (at.fd, at.fx, at.fy, at.f)

    def to_p(q, z):
        f = fs[q]
        src = staged.at[q] if staged is not None else part.at[f, 2 * z + 1 - at.c]
        return send(src, pb.at[f, z], ps.at[f, z], pr.at[f, z], at.f, at.pe)

    def ready(q, z):
        if staged is None:
            load(fs[q], z).wait()
        to_p(q, z).wait_recv()

    def start_step(s):
        z = place(s)
        for q in range(4):
            load(fs[q], z).start()
            to_p(q, z).start()

    def half_x(z):
        return send(acc.at[at.fd, z, lo], xh.at[z], xhs.at[z], xhr.at[z], at.fx, at.e)

    def half_y(z):
        return send(acc.at[at.fd, z, hi], yh.at[z], yhs.at[z], yhr.at[z], at.fy, at.e)

    def full_x(z):
        return send(acc.at[at.fx, z], xf.at[z], xs.at[z], xr.at[z], at.fx, at.e)

    def full_y(z):
        return send(acc.at[at.fy, z], yf.at[z], ys.at[z], yr.at[z], at.fy, at.e)

    count = rows // split

    def go_up(z, k):
        cut = pl.ds(k * count, count)
        return send(acc.at[at.f, z, cut], zu.at[z, cut], us.at[z, k], ur.at[z, k], at.f, at.e + 2)

    def go_down(z, k):
        cut = pl.ds(k * count, count)
        return send(acc.at[at.f, z, cut], zd.at[z, cut], ds_.at[z, k], dr.at[z, k], at.f, at.e - 2)

    def diag_step(s):
        z = place(s)
        ready(0, z)
        a, b = acc.at[at.fd, z], pb.at[at.fd, z]
        add_rows(a, (0, half), [(a, 0), (b, 0)])
        half_x(z).start()
        add_rows(a, (half, half), [(a, half), (b, half)])
        half_y(z).start()

    def plane_step(s):
        z = place(s)
        ready(1, z)
        a, b = acc.at[at.fx, z], pb.at[at.fx, z]
        half_y(z).wait_recv()
        add_rows(a, (0, half), [(a, 0), (b, 0)])
        add_rows(a, (half, half), [(a, half), (b, half), (yh.at[z], 0)])
        full_x(z).start()
        ready(2, z)
        half_x(z).wait_recv()
        a, b = acc.at[at.fy, z], pb.at[at.fy, z]
        add_rows(a, (0, half), [(a, 0), (b, 0), (xh.at[z], 0)])
        add_rows(a, (half, half), [(a, half), (b, half)])
        full_y(z).start()

    def line_step(s, k=0):
        z = place(s)
        if k == 0:
            ready(3, z)
            full_x(z).wait_recv()
            full_y(z).wait_recv()
        r = k * count
        a = acc.at[at.f, z]
        four = [(a, r), (pb.at[at.f, z], r), (xf.at[z], r), (yf.at[z], r)]

        @pl.when(z > at.z)
        def _():
            @pl.when(at.z > 0)
            def _():
                go_up(z, k).wait_recv()
                add_rows(a, (r, count), four + [(zu.at[z], r)])

            pl.when(at.z == 0)(lambda: add_rows(a, (r, count), four))
            go_up(z, k).start()

        @pl.when(z < at.z)
        def _():
            @pl.when(at.z < nz - 1)
            def _():
                go_down(z, k).wait_recv()
                add_rows(a, (r, count), four + [(zd.at[z], r)])

            pl.when(at.z == nz - 1)(lambda: add_rows(a, (r, count), four))
            go_down(z, k).start()

        @pl.when(z == at.z)
        def _():
            add_rows(out, (r, count), four)

            @pl.when(at.z > 0)
            def _():
                go_up(z, k).wait_recv()
                add_rows(out, (r, count), [(out, r), (zu.at[z], r)])

            @pl.when(at.z < nz - 1)
            def _():
                go_down(z, k).wait_recv()
                add_rows(out, (r, count), [(out, r), (zd.at[z], r)])

    def finish():
        def body(z, carry):
            for q in range(4):
                if staged is None:
                    to_p(q, z).wait_send()
            half_x(z).wait_send()
            half_y(z).wait_send()
            full_x(z).wait_send()
            full_y(z).wait_send()
            for k in range(split):
                pl.when(z > at.z)(functools.partial(lambda k: go_up(z, k).wait_send(), k))
                pl.when(z < at.z)(functools.partial(lambda k: go_down(z, k).wait_send(), k))
            return carry

        lax.fori_loop(0, nz, body, 0)
        for q in range(4):
            if staged is not None:
                to_p(q, place(nz - 1)).wait_send()

    return start_step, diag_step, plane_step, line_step, finish, place, to_p


def scatter_scratch(parts, nz):
    _, _, r, c = parts.shape

    def buf(*n):
        return pltpu.VMEM((*n, c), parts.dtype)

    return [
        buf(4, nz, r), buf(4, nz, r), buf(nz, r // 2), buf(nz, r // 2),
        buf(nz, r), buf(nz, r), buf(nz, r), buf(nz, r),
        DMA((4, nz)), DMA((4, nz)), DMA((4, nz)),
        *[DMA((nz,))] * 8,
        *[DMA((nz, 4))] * 4,
    ]


def scatter_act_kernel(nz, pre, grads, gates, w_gate, w_up, w_down, out, out_small, acts, *refs):
    at = Place()
    refs = iter(refs)
    moved = take(refs, 23)
    acc = moved[0]
    pb_, cb, ab, sb, terms, load_sem, store_sem = take(refs, 7)
    _, diag, plane, line, close, place, to_p = scatter_plan(at, nz, None, out, moved, sb)
    small = SmallScatter(at, nz, terms, out_small, take(refs, 4), take(refs, 4))
    greet([(at.fx, at.e), (at.fy, at.e), (at.f, at.pe)], (at, nz))
    rows, width = out.shape
    local, _, hidden = w_gate.shape
    experts = gates.shape[3]
    fs = (at.fd, at.fx, at.fy, at.f)
    cores = (at.c, 1 - at.c)
    first = at.e * local
    expert_row = lax.broadcasted_iota(jnp.int32, (experts, hidden), 0)
    tile = 512

    def loads(q, s):
        z, f = place(s), fs[q]
        copies = []
        for h, core in enumerate(cores):
            slot = 2 * z + core
            for k in range(3):
                copies.append(
                    pltpu.make_async_copy(pre.at[k, f, slot], pb_.at[q, k, h], load_sem.at[q, h, k])
                )
            copies.append(pltpu.make_async_copy(grads.at[f, slot], cb.at[q, h], load_sem.at[q, h, 3]))
        return copies

    def stores(q, s):
        z, f = place(s), fs[q]
        return [
            pltpu.make_async_copy(
                ab.at[q, k, h], acts.at[k, f, 2 * z + core], store_sem.at[q, h, k]
            )
            for h, core in enumerate(cores)
            for k in range(2)
        ]

    def act(q, s):
        z, f = place(s), fs[q]
        for copy in loads(q, s):
            copy.wait()

        @pl.when(s > 0)
        def _():
            for copy in stores(q, s - 1):
                copy.wait()

        c = cb[q].reshape(2 * rows, width)
        gate_all = spread([gates[core, f, z] for core in cores], first, hidden, local * hidden)
        sums = [None, None]
        for j in range(local):
            pick = (expert_row == first + j).astype(jnp.float32).astype(jnp.bfloat16)
            cols = pl.ds(j * hidden, hidden)
            dh = lax.dot_general(c, w_down[j], NT, preferred_element_type=jnp.float32)
            for h, core in enumerate(cores):
                d = dh[h * rows : (h + 1) * rows]
                gate = gate_all[h * rows : (h + 1) * rows, j * hidden : (j + 1) * hidden]
                for part in halves_of(pb_[q, 2, h, :, cols] * d):
                    mine = lax.dot_general(pick, part, NT, preferred_element_type=jnp.float32)
                    sums[h] = mine if sums[h] is None else sums[h] + mine
                d = d * gate
                ab[q, 0, h, :, cols] = (d * pb_[q, 0, h, :, cols]).astype(jnp.bfloat16)
                ab[q, 1, h, :, cols] = (d * pb_[q, 1, h, :, cols]).astype(jnp.bfloat16)
        for h, core in enumerate(cores):
            terms[core, f, z] = sums[h]
        for copy in stores(q, s):
            copy.start()

        @pl.when(s + 1 < nz)
        def _():
            for copy in loads(q, s + 1):
                copy.start()

    def back(q, s):
        z, f = place(s), fs[q]
        pl.when(s > 0)(lambda: to_p(q, place(s - 1)).wait_send())
        pieces = [
            (ab[q, k].reshape(2 * rows, local * hidden)[:, j * hidden : (j + 1) * hidden], w.at[j])
            for j in range(local)
            for k, w in enumerate((w_gate, w_up))
        ]

        def body(t, carry):
            cols = pl.ds(pl.multiple_of(t * tile, tile), tile)
            total = None
            for a, w in pieces:
                term = lax.dot_general(a, w[cols, :], NT, preferred_element_type=jnp.float32)
                total = term if total is None else total + term
            total = total.astype(jnp.bfloat16)
            acc[f, z, :, cols] = total[:rows]
            sb[q, :, cols] = total[rows:]
            return carry

        lax.fori_loop(0, width // tile, body, 0)
        to_p(q, z).start()

    for q in range(4):
        for copy in loads(q, 0):
            copy.start()

    def body(s, carry):
        @pl.when(s < nz)
        def _():
            last = s == nz - 1
            for q in (0, 1):
                act(q, s)
                back(q, s)
            diag(s)
            act(2, s)
            back(2, s)
            act(3, s)
            pl.when(last)(lambda: small.stage(0))
            back(3, s)
            pl.when(last)(lambda: small.stage(1))
            plane(s)
            pl.when(last)(lambda: small.stage(2))

        pl.when(s == nz)(lambda: small.stage(3))
        pl.when(s >= 1)(lambda: line(s - 1))
        return carry

    lax.fori_loop(0, nz + 1, body, 0)
    small.stage(4)
    for q in range(4):
        for copy in stores(q, nz - 1):
            copy.wait()
    close()


def scatter_act(pre, grads, gates, w_gate, w_up, w_down, nz, cid):
    _, _, _, r, wide = pre.shape
    c = grads.shape[3]
    small = gates.shape[3:]
    hbm, vmem = pl.BlockSpec(memory_space=pl.ANY), pl.BlockSpec(memory_space=pltpu.VMEM)
    bf16 = jnp.bfloat16
    return pl.pallas_call(
        functools.partial(scatter_act_kernel, nz),
        out_shape=(
            jax.ShapeDtypeStruct((r, c), jnp.float32),
            jax.ShapeDtypeStruct(small, jnp.float32),
            jax.ShapeDtypeStruct((2, 4, 2 * nz, r, wide), bf16),
        ),
        in_specs=[hbm, hbm, vmem, vmem, vmem, vmem],
        out_specs=(vmem, vmem, hbm),
        scratch_shapes=[
            *scatter_scratch(grads, nz),
            pltpu.VMEM((4, 3, 2, r, wide), jnp.float32),
            pltpu.VMEM((4, 2, r, c), bf16),
            pltpu.VMEM((4, 2, 2, r, wide), bf16),
            pltpu.VMEM((4, r, c), bf16),
            pltpu.VMEM((2, 4, nz, *small), jnp.float32),
            DMA((4, 2, 4)), DMA((4, 2, 2)),
            *SmallScatter.scratch(nz, small),
            *SmallScatter.sems(nz),
        ],
        compiler_params=pltpu.CompilerParams(
            collective_id=cid, has_side_effects=True, vmem_limit_bytes=62 << 20
        ),
        cost_estimate=pl.CostEstimate(flops=0, bytes_accessed=300 << 20, transcendentals=0),
        name="scatter_act",
    )(pre, grads, gates, w_gate, w_up, w_down)


def square_gather_kernel(own, ids, out, out_ids, xs, xr, ys, yr, fs, fr, js, jr):
    at = Place()
    half = own.shape[0] // 2
    halves = (pl.ds(0, half), pl.ds(half, half))
    peers = [(at.fx, at.e), (at.fy, at.e), (at.fd, at.e)]
    greet(peers)

    def to_x(h):
        return send(own.at[halves[h]], out.at[at.f, halves[h]], xs.at[h], xr.at[h], at.fx, at.e)

    def to_y(h):
        return send(own.at[halves[h]], out.at[at.f, halves[h]], ys.at[h], yr.at[h], at.fy, at.e)

    x_ref, y_ref = out.at[at.fx, halves[0]], out.at[at.fy, halves[1]]
    x_on = send(x_ref, x_ref, fs.at[0], fr.at[0], at.fy, at.e)
    y_on = send(y_ref, y_ref, fs.at[1], fr.at[1], at.fx, at.e)
    notes = [
        send(ids, out_ids.at[at.f], js.at[k], jr.at[k], f, e) for k, (f, e) in enumerate(peers)
    ]
    to_x(0).start()
    to_y(1).start()
    for note in notes:
        note.start()
    to_x(1).start()
    to_y(0).start()
    out[at.f] = own[...]
    out_ids[at.f] = ids[...]
    to_x(0).wait_recv()
    x_on.start()
    to_y(1).wait_recv()
    y_on.start()
    to_x(1).wait()
    to_y(0).wait()
    for note in notes:
        note.wait()
    to_x(0).wait_send()
    to_y(1).wait_send()
    x_on.wait()
    y_on.wait()


def square_gather(rows, ids, cid):
    r, c = rows.shape
    vmem = pl.BlockSpec(memory_space=pltpu.VMEM)
    return pl.pallas_call(
        square_gather_kernel,
        out_shape=(
            jax.ShapeDtypeStruct((4, r, c), rows.dtype),
            jax.ShapeDtypeStruct((4, *ids.shape), ids.dtype),
        ),
        in_specs=[vmem] * 2,
        out_specs=(vmem,) * 2,
        scratch_shapes=[DMA((2,))] * 6 + [DMA((3,))] * 2,
        compiler_params=pltpu.CompilerParams(collective_id=cid, has_side_effects=True),
        cost_estimate=pl.CostEstimate(flops=0, bytes_accessed=60 << 20, transcendentals=0),
        name="square_gather",
    )(rows, ids)


def square_scatter_kernel(part, out, xh, yh, xf, yf, ss, rs):
    at = Place()
    rows = out.shape[0]
    half = rows // 2
    lo, hi = pl.ds(0, half), pl.ds(half, half)
    greet([(at.fx, at.e), (at.fy, at.e)])

    def to_x(k, src, dst):
        return send(src, dst, ss.at[k], rs.at[k], at.fx, at.e)

    def to_y(k, src, dst):
        return send(src, dst, ss.at[k], rs.at[k], at.fy, at.e)

    copies = [
        to_x(0, part.at[at.fd, lo], xh),
        to_y(1, part.at[at.fd, hi], yh),
        to_x(2, part.at[at.fx, lo], xf.at[lo]),
        to_y(3, part.at[at.fy, hi], yf.at[hi]),
        to_x(4, yh, xf.at[hi]),
        to_y(5, xh, yf.at[lo]),
    ]
    for copy in copies[:4]:
        copy.start()
    copies[1].wait_recv()
    add_rows(yh, (0, half), [(yh, 0), (part.at[at.fx], half)])
    copies[4].start()
    copies[0].wait_recv()
    add_rows(xh, (0, half), [(xh, 0), (part.at[at.fy], 0)])
    copies[5].start()
    copies[2].wait_recv()
    copies[5].wait_recv()
    copies[3].wait_recv()
    copies[4].wait_recv()
    add_rows(out, (0, rows), [(part.at[at.f], 0), (xf, 0), (yf, 0)])
    for copy in copies:
        copy.wait_send()


def square_scatter(parts, cid):
    _, r, c = parts.shape
    vmem = pl.BlockSpec(memory_space=pltpu.VMEM)

    def buf(n):
        return pltpu.VMEM((n, c), parts.dtype)

    return pl.pallas_call(
        square_scatter_kernel,
        out_shape=jax.ShapeDtypeStruct((r, c), jnp.float32),
        in_specs=[vmem],
        out_specs=vmem,
        scratch_shapes=[buf(r // 2), buf(r // 2), buf(r), buf(r), DMA((6,)), DMA((6,))],
        compiler_params=pltpu.CompilerParams(collective_id=cid, has_side_effects=True),
        cost_estimate=pl.CostEstimate(flops=0, bytes_accessed=60 << 20, transcendentals=0),
        name="square_scatter",
    )(parts)


def square_sum_kernel(own, out, got, ss, rs):
    at = Place()
    peers = [(at.fx, at.e), (at.fy, at.e), (at.fd, at.e)]
    greet(peers)
    copies = [send(own, got.at[k], ss.at[k], rs.at[k], f, e) for k, (f, e) in enumerate(peers)]
    for copy in copies:
        copy.start()
    for copy in copies:
        copy.wait()
    out[...] = (own[...] + got[0]) + (got[1] + got[2])


def square_sum(values, cid):
    flat = values.reshape(8, -1)
    vmem = pl.BlockSpec(memory_space=pltpu.VMEM)
    return pl.pallas_call(
        square_sum_kernel,
        out_shape=jax.ShapeDtypeStruct(flat.shape, jnp.float32),
        in_specs=[vmem],
        out_specs=vmem,
        scratch_shapes=[pltpu.VMEM((3, *flat.shape), jnp.float32), DMA((3,)), DMA((3,))],
        compiler_params=pltpu.CompilerParams(collective_id=cid, has_side_effects=True),
        cost_estimate=pl.CostEstimate(flops=0, bytes_accessed=10 << 20, transcendentals=0),
        name="square_sum",
    )(flat).reshape(values.shape)


class product_plan:
    def __init__(self, inputs, outs, refs):
        self.rows, self.acts, self.weighted, self.grads = inputs
        self.outs = outs
        self.acc, self.xw, self.aw, self.load_sem, self.store_sem = refs
        self.tile = self.acc.shape[2]
        self.units = self.rows.shape[0]
        self.local = self.outs[0].shape[0]
        self.per_pass = self.units // 2
        self.steps = self.per_pass * (self.local + 1)

    def loads(self, i, k, p):
        u = (i - p * self.per_pass) * 2 + k
        hidden = self.outs[0].shape[2]
        sem = self.load_sem.at[k]
        if p == self.local:
            return [
                pltpu.make_async_copy(self.grads.at[u], self.xw.at[k], sem.at[0]),
                pltpu.make_async_copy(self.weighted.at[u], self.aw.at[k], sem.at[1]),
            ]
        cols = pl.ds(p * hidden, hidden)
        return [
            pltpu.make_async_copy(self.rows.at[u], self.xw.at[k], sem.at[0]),
            pltpu.make_async_copy(self.acts.at[0, u, :, cols], self.aw.at[k, :, pl.ds(0, hidden)], sem.at[1]),
            pltpu.make_async_copy(
                self.acts.at[1, u, :, cols], self.aw.at[k, :, pl.ds(hidden, hidden)], sem.at[2]
            ),
        ]

    def on_pass(self, i, run):
        for p in range(self.local + 1):
            pl.when((i >= p * self.per_pass) & (i < (p + 1) * self.per_pass))(functools.partial(run, p))

    def start(self):
        for k in range(2):
            for copy in self.loads(0, k, 0):
                copy.start()

        for p in range(self.local):
            self.clear(p)

    def clear(self, p):
        def body(r, carry):
            self.acc[p, pl.ds(r * 8, 8), :] = jnp.zeros((8, self.tile), jnp.float32)
            return carry

        lax.fori_loop(0, self.acc.shape[1] // 8, body, 0)

    def step(self, i):
        tile = self.tile

        def run(p):
            if p == self.local:

                @pl.when(i == p * self.per_pass)
                def _():
                    for copy in self.stores(0):
                        copy.wait()
                    self.clear(0)

            for k in range(2):
                for copy in self.loads(i, k, p):
                    copy.wait()
                a = self.aw[k]
                for t in range(self.xw.shape[2] // tile):
                    cols = pl.ds(t * tile, tile)
                    x = self.xw[k, :, cols]
                    if p == self.local:
                        self.acc[0, cols, :] += lax.dot_general(
                            a, x, TN, preferred_element_type=jnp.float32
                        )
                    else:
                        self.acc[p, cols, :] += lax.dot_general(
                            x, a, TN, preferred_element_type=jnp.float32
                        )

                def more(q, k=k):
                    for copy in self.loads(i + 1, k, q):
                        copy.start()

                self.on_pass(i + 1, more)

            @pl.when(i == (p + 1) * self.per_pass - 1)
            def _():
                for copy in self.stores(p):
                    copy.start()

        self.on_pass(i, run)

    def stores(self, p):
        hidden = self.outs[0].shape[2]
        if p == self.local:
            cuts = [pl.ds(k * self.tile, self.tile) for k in range(self.outs[2].shape[1] // self.tile)]
            return [
                pltpu.make_async_copy(
                    self.acc.at[0, cut], self.outs[2].at[:, cut], self.store_sem.at[p, k]
                )
                for k, cut in enumerate(cuts)
            ]
        acc = self.acc.at[p]
        return [
            pltpu.make_async_copy(
                acc.at[:, pl.ds(k * hidden, hidden)], self.outs[k].at[p], self.store_sem.at[p, k]
            )
            for k in range(2)
        ]

    def finish(self):
        for p in range(1, self.local + 1):
            for copy in self.stores(p):
                copy.wait()


class SquareScatter:
    def __init__(self, at, part, normed, out, table, refs):
        self.part, self.normed, self.out, self.table = part, normed, out, table
        self.xh, self.yh, self.xf, self.yf, self.px, self.py, self.pf, ss, rs, ls = refs
        half = self.xh.shape[0]
        lo, hi = pl.ds(0, half), pl.ds(half, half)

        def to_x(k, src, dst):
            return send(src, dst, ss.at[k], rs.at[k], at.fx, at.e)

        def to_y(k, src, dst):
            return send(src, dst, ss.at[k], rs.at[k], at.fy, at.e)

        self.copies = [
            to_x(0, part.at[at.fd, lo], self.xh),
            to_y(1, part.at[at.fd, hi], self.yh),
            to_x(2, part.at[at.fx, lo], self.xf.at[lo]),
            to_y(3, part.at[at.fy, hi], self.yf.at[hi]),
            to_x(4, self.yh, self.xf.at[hi]),
            to_y(5, self.xh, self.yf.at[lo]),
        ]
        self.loads = [
            pltpu.make_async_copy(part.at[at.fx, hi], self.px, ls.at[0]),
            pltpu.make_async_copy(part.at[at.fy, lo], self.py, ls.at[1]),
            pltpu.make_async_copy(part.at[at.f], self.pf, ls.at[2]),
        ]

    def stage(self, i):
        copies, half, rows = self.copies, self.xh.shape[0], self.out.shape[0]
        if i == 0:
            for copy in copies[:4] + self.loads:
                copy.start()
        elif i == 1:
            for copy in self.loads:
                copy.wait()
            copies[1].wait_recv()
            add_rows(self.yh, (0, half), [(self.yh, 0), (self.px, 0)])
            copies[4].start()
            copies[0].wait_recv()
            add_rows(self.xh, (0, half), [(self.xh, 0), (self.py, 0)])
            copies[5].start()
        elif i == 2:
            for copy in copies[2:]:
                copy.wait_recv()
            add_rows(self.out, (0, rows), [(self.pf, 0), (self.xf, 0), (self.yf, 0)])

            def body(r, total):
                cut = pl.ds(pl.multiple_of(r * 16, 16), 16)
                both = self.out[cut, :] * self.normed[cut, :].astype(jnp.float32)
                return total + both[:8] + both[8:]

            total = lax.fori_loop(0, rows // 16, body, jnp.zeros((8, self.out.shape[1]), jnp.float32))
            total = jnp.sum(total, axis=0, keepdims=True)
            for k in range(self.table.shape[3]):
                self.table[0, 0, 0, k : k + 1, :] = total[:, k * 128 : (k + 1) * 128]
            for copy in copies:
                copy.wait_send()


def line_sum_kernel(nz, counts, *refs):
    at = Place()
    refs = iter(refs)
    n = len(counts)
    parts, table_in, rows_part, inputs = take(refs, n), next(refs), next(refs), take(refs, 4)
    first_part, normed = take(refs, 2)
    outs, out_small, rows_out, grads = take(refs, n), next(refs), next(refs), take(refs, 3)
    first_out, part_small = take(refs, 2)
    square = SquareScatter(at, first_part, normed, first_out, part_small, take(refs, 10))
    begin, diag, plane, line, close, _, _ = scatter_plan(
        at, nz, rows_part, rows_out, take(refs, 23), split=2
    )
    product = product_plan(inputs, grads, take(refs, 5))
    bufs = [take(refs, 5) for _ in range(n)]
    sems = [take(refs, 12) for _ in range(n)]
    own_small = next(refs)
    scatter_small = SmallScatter(at, nz, part_small, own_small, take(refs, 4), take(refs, 4))
    gather_small = SmallGather(at, nz, own_small, out_small, take(refs, 4))
    greet([(at.fx, at.e), (at.fy, at.e), (at.f, at.pe)], (at, nz))
    square.stage(0)
    part_small[...] = table_in[...]
    total = sum(counts)
    last = nz - 1
    lag, per = 2, 5

    class Piece:
        def __init__(self, k, p):
            self.p, self.part, self.out = p, parts[k], outs[k]
            self.acc, self.pb, self.zu, self.zd, self.mine = bufs[k]
            self.sems = sems[k]
            self.r = self.acc.shape[2]

        def load(self):
            p = self.p
            return pltpu.make_async_copy(self.part.at[p, at.c], self.acc.at[p], self.sems[0].at[p])

        def to_p(self):
            p, (_, s, r, *_rest) = self.p, self.sems
            return send(self.part.at[p, 1 - at.c], self.pb.at[p], s.at[p], r.at[p], at.f, at.pe)

        def go_up(self, z):
            p, s, r = self.p, self.sems[3], self.sems[4]
            return send(self.acc.at[p, z], self.zu.at[p, z], s.at[p, z], r.at[p, z], at.f, at.e + 2)

        def go_down(self, z):
            p, s, r = self.p, self.sems[5], self.sems[6]
            return send(self.acc.at[p, z], self.zd.at[p, z], s.at[p, z], r.at[p, z], at.f, at.e - 2)

        def res(self, z, way):
            p, s, r = self.p, self.sems[7], self.sems[8]
            ref = self.out.at[p, at.c, z]
            return send(ref, ref, s.at[way, p, z], r.at[p, z], at.f, at.e + 2 - 4 * way)

        def res_p(self, z):
            p, s, r = self.p, self.sems[9], self.sems[10]
            ref = self.out.at[p, at.c, z]
            return send(ref, ref, s.at[p, z], r.at[p, z], at.f, at.pe)

        def keep(self):
            p = self.p
            return pltpu.make_async_copy(self.mine.at[p], self.out.at[p, at.c, at.z], self.sems[11].at[p])

    def piece(q, run, when=True):
        low = 0
        for k, count in enumerate(counts):
            @pl.when((q >= low) & (q < low + count) & when)
            def _(k=k, low=low):
                run(Piece(k, q - low))

            low += count

    def start(it):
        it.load().start()
        it.to_p().start()

    piece(0, start)
    begin(0)
    piece(1, start)
    product.start()

    def halve(it):
        it.load().wait()
        it.to_p().wait_recv()
        p = it.p

        def body(z, carry):
            a = it.acc.at[p, z]
            add_rows(a, (0, it.r), [(a, 0), (it.pb.at[p, z], 0)])
            return carry

        lax.fori_loop(0, nz, body, 0)

    def rise(it):
        p = it.p

        def body(i, carry):
            z = last - i

            @pl.when(z > at.z)
            def _():
                a = it.acc.at[p, z]

                @pl.when(at.z > 0)
                def _():
                    it.go_up(z).wait_recv()
                    add_rows(a, (0, it.r), [(a, 0), (it.zu.at[p, z], 0)])

                it.go_up(z).start()

            return carry

        lax.fori_loop(0, last, body, 0)

    def sink(it):
        p = it.p

        def body(z, carry):
            @pl.when(z < at.z)
            def _():
                a = it.acc.at[p, z]

                @pl.when(at.z < last)
                def _():
                    it.go_down(z).wait_recv()
                    add_rows(a, (0, it.r), [(a, 0), (it.zd.at[p, z], 0)])

                it.go_down(z).start()

            return carry

        lax.fori_loop(0, last, body, 0)

    def settle(it):
        p, z = it.p, at.z
        pl.when(z > 0)(lambda: it.go_up(z).wait_recv())
        pl.when(z < last)(lambda: it.go_down(z).wait_recv())
        a, dst = (it.acc.at[p, z], 0), it.mine.at[p]
        up, down = (it.zu.at[p, z], 0), (it.zd.at[p, z], 0)
        pl.when((z > 0) & (z < last))(lambda: add_rows(dst, (0, it.r), [a, up, down]))
        pl.when(z == 0)(lambda: add_rows(dst, (0, it.r), [a, down]))
        pl.when(z == last)(lambda: add_rows(dst, (0, it.r), [a, up]))
        it.keep().start()

    def tell(it):
        z = at.z
        it.keep().wait()
        pl.when(z < last)(lambda: it.res(z, 0).start())
        pl.when(z > 0)(lambda: it.res(z, 1).start())
        it.res_p(z).start()

    def pass_up(it, z):
        it.res(z, 0).wait_recv()
        pl.when(at.z < last)(lambda: it.res(z, 0).start())
        it.res_p(z).start()

    def pass_down(it, z):
        it.res(z, 0).wait_recv()
        pl.when(at.z > 0)(lambda: it.res(z, 1).start())
        it.res_p(z).start()

    def body(i, carry):
        piece(i + 2, start)
        s, turn = i // per, i % per
        pl.when((turn == 0) & (s + 1 < nz))(lambda: begin(s + 1))
        pl.when((turn == 0) & (s < nz))(lambda: diag(s))
        pl.when((turn == 2) & (s < nz))(lambda: plane(s))
        pl.when((turn == 3) & (s >= 1) & (s < nz + 1))(lambda: line(s - 1, 0))
        pl.when((turn == 0) & (s >= 2) & (s < nz + 2))(lambda: line(s - 2, 1))
        piece(i, halve)
        piece(i - lag * at.z, rise, at.z < last)
        piece(i - lag * (last - at.z), sink, at.z > 0)
        piece(i - lag * nz, settle)
        piece(i - lag * nz, tell)
        for d in range(1, nz):
            piece(i - lag * (nz + d), functools.partial(pass_up, z=at.z - d), at.z >= d)
            piece(i - lag * (nz + d), functools.partial(pass_down, z=at.z + d), at.z + d <= last)
        for k, at_step in ((1, 1), (2, 5)):
            pl.when(i == at_step)(functools.partial(square.stage, k))
        for k in range(5):
            pl.when(i == 6 + k)(functools.partial(scatter_small.stage, k))
            pl.when(i == 11 + k)(functools.partial(gather_small.stage, k))
        product.step(i)
        return carry

    steps = max(total + lag * (2 * nz - 1), per * (nz + 2), product.steps)
    lax.fori_loop(0, steps, body, 0)
    product.finish()

    def finish(q, carry):
        def run(it):
            it.to_p().wait_send()

            def one(z, carry):
                pl.when(z > at.z)(lambda: it.go_up(z).wait_send())
                pl.when(z < at.z)(lambda: it.go_down(z).wait_send())
                pl.when((z <= at.z) & (at.z < last))(lambda: it.res(z, 0).wait_send())
                pl.when((z >= at.z) & (at.z > 0))(lambda: it.res(z, 1).wait_send())
                it.res_p(z).wait_send()
                it.res_p(z).wait_recv()
                return carry

            lax.fori_loop(0, nz, one, 0)

        piece(q, run)
        return carry

    lax.fori_loop(0, total, finish, 0)
    close()


def line_sum(parts, small, rows, inputs, first, normed, local, nz, cid):
    counts = tuple(p.shape[0] for p in parts)
    units, unit, width = inputs[0].shape
    wide = inputs[1].shape[3]
    scratch, sems = [], []
    for p in parts:
        n, _, _, r, c = p.shape

        def buf(*lead):
            return pltpu.VMEM((*lead, r, c), p.dtype)

        scratch += [buf(n, nz), buf(n, nz), buf(n, nz), buf(n, nz), buf(n)]
        each, line = DMA((n,)), DMA((n, nz))
        sems += [each, each, each, line, line, line, line, DMA((2, n, nz)), line, line, line, each]
    hbm, vmem = pl.BlockSpec(memory_space=pl.ANY), pl.BlockSpec(memory_space=pltpu.VMEM)
    _, r, c = first.shape
    bf16 = jnp.bfloat16
    assert small.shape[3] * small.shape[4] == c
    return pl.pallas_call(
        functools.partial(line_sum_kernel, nz, counts),
        out_shape=(
            *(jax.ShapeDtypeStruct(p.shape, p.dtype) for p in parts),
            jax.ShapeDtypeStruct(small.shape, jnp.float32),
            jax.ShapeDtypeStruct(rows.shape[2:], jnp.float32),
            jax.ShapeDtypeStruct((local, width, wide // local), jnp.float32),
            jax.ShapeDtypeStruct((local, width, wide // local), jnp.float32),
            jax.ShapeDtypeStruct((wide, width), jnp.float32),
            jax.ShapeDtypeStruct(first.shape[1:], jnp.float32),
        ),
        in_specs=[hbm] * len(parts) + [vmem, hbm] + [hbm] * len(inputs) + [hbm, vmem],
        out_specs=(*[hbm] * len(parts), vmem, vmem, *[hbm] * 3, vmem),
        scratch_shapes=[
            pltpu.VMEM(small.shape, jnp.float32),
            pltpu.VMEM((r // 2, c), bf16), pltpu.VMEM((r // 2, c), bf16),
            pltpu.VMEM((r, c), bf16), pltpu.VMEM((r, c), bf16),
            pltpu.VMEM((r // 2, c), bf16), pltpu.VMEM((r // 2, c), bf16), pltpu.VMEM((r, c), bf16),
            DMA((6,)), DMA((6,)), DMA((3,)),
            *scatter_scratch(rows, nz),
            pltpu.VMEM((local, width, 2 * wide // local), jnp.float32),
            pltpu.VMEM((2, unit, width), rows.dtype),
            pltpu.VMEM((2, unit, wide), rows.dtype),
            DMA((2, 3)), DMA((local + 1, 4)),
            *scratch, *sems, pltpu.VMEM(small.shape[-2:], jnp.float32),
            *SmallScatter.scratch(nz, small.shape[-2:]), *SmallScatter.sems(nz), *SmallGather.sems(nz),
        ],
        compiler_params=pltpu.CompilerParams(
            collective_id=cid, has_side_effects=True, vmem_limit_bytes=63 << 20
        ),
        cost_estimate=pl.CostEstimate(flops=0, bytes_accessed=300 << 20, transcendentals=0),
        name="line_sum",
    )(*parts, small, rows, *inputs, first, normed)


def rope_tables(seg_ids, head_dim):
    length = seg_ids.shape[0]
    ordinal = lax.iota(jnp.int32, length)
    earlier = (seg_ids[:, None] == seg_ids[None, :]) & (ordinal[None, :] < ordinal[:, None])
    places = jnp.sum(earlier.astype(jnp.int32), axis=1).astype(jnp.float32)
    half_dim = head_dim // 2
    inv_freq = rope_base ** (
        -(lax.iota(jnp.int32, half_dim).astype(jnp.float32) * (2.0 / head_dim))
    )
    angles = places[:, None] * inv_freq[None, :]
    angles = jnp.concatenate([angles, angles], axis=1)
    return (jnp.cos(angles), jnp.sin(angles))


def rotate_half(values):
    half_dim = values.shape[-1] // 2
    return jnp.concatenate([-values[..., half_dim:], values[..., :half_dim]], axis=-1)


def rotate_back(values):
    half_dim = values.shape[-1] // 2
    return jnp.concatenate([values[..., half_dim:], -values[..., :half_dim]], axis=-1)


def apply_rope(values, cosine, sine_table):
    return values * cosine[:, None, :] + rotate_half(values) * sine_table[:, None, :]


def rope_grad(grads_in, cosine, sine_table):
    return grads_in * cosine[:, None, :] + rotate_back(grads_in * sine_table[:, None, :])


def across_heads(kernel, pair_sums):
    if kernel:
        return square_sum(jnp.stack(pair_sums), kernel)
    return lax.psum((pair_sums[0], pair_sums[1]), "fsdp")


def share_rows(term_fn, own_rows, kernel=0):
    if kernel:
        parts = term_fn(jnp.int32(0), own_rows * lax.axis_size("fsdp"))
        return square_scatter(parts.reshape(-1, own_rows, parts.shape[1]), kernel)
    return lax.psum_scatter(
        term_fn(jnp.int32(0), own_rows * lax.axis_size("fsdp")),
        "fsdp",
        scatter_dimension=0,
        tiled=True,
    )


def to_owner(block_rows):
    return lax.all_to_all(block_rows, "expert", split_axis=0, concat_axis=0, tiled=True)


def from_owner(block_rows):
    return lax.all_to_all(block_rows, "expert", split_axis=0, concat_axis=0, tiled=True)


def shard_gather(block_rows):
    return lax.all_gather(block_rows, "fsdp", axis=0, tiled=True)


def owner_sum(term_fn, sources):
    own_rows = sources // lax.axis_size("fsdp")
    return lax.psum_scatter(
        term_fn(jnp.int32(0), own_rows * lax.axis_size("fsdp")),
        "fsdp",
        scatter_dimension=0,
        tiled=True,
    )


def head_scores(q_heads, k_heads, allowed):
    scores = jnp.einsum(
        "thd,shd->hts", q_heads, k_heads, preferred_element_type=jnp.float32
    ) * HEAD_DIM ** (-0.5)
    return jnp.where(allowed[None], scores, -1e30)


def experts_by_slot(
    second_in, second_rows, cotangent, routes, capacity, w_router, w_gate, w_up, w_down
):
    tok_count, model_width = second_rows.shape
    experts = w_router.shape[1]
    local_experts = w_gate.shape[0]
    slot_count = tok_count * TOP * 3 // (2 * experts)
    pair_count = tok_count * TOP
    zero_row = jnp.zeros((1, model_width), jnp.bfloat16)
    logits = jnp.dot(second_rows, w_router, preferred_element_type=jnp.float32)
    chosen = routes
    expert_ids = lax.iota(jnp.int32, experts)
    chosen_hot = (chosen[:, :, None] == expert_ids[None, None, :]).astype(jnp.float32)
    routed = jnp.sum(chosen_hot * logits[:, None, :], axis=2)
    gate_wts = jax.nn.softmax(routed, axis=1)
    pair_hot = chosen_hot.reshape(pair_count, experts).astype(jnp.int32)
    earlier_hits = jnp.cumsum(pair_hot, axis=0) - pair_hot
    ranking = jnp.sum(earlier_hits * pair_hot, axis=1)
    cap_pair = jnp.sum(pair_hot * capacity[None, :], axis=1)
    is_kept = ranking < cap_pair
    pair_route = chosen.reshape(pair_count)
    slot_place = jnp.where(is_kept, pair_route * slot_count + ranking, experts * slot_count)
    pair_ids = lax.iota(jnp.int32, pair_count)
    slot_pair = (
        jnp.full((experts * slot_count,), pair_count, jnp.int32)
        .at[slot_place]
        .set(pair_ids, mode="drop")
    )
    padded = jnp.concatenate([second_rows, zero_row], axis=0)
    outgoing = padded[slot_pair // TOP].reshape(experts, slot_count, model_width)
    arrived = shard_gather(to_owner(outgoing))
    gate_w, up_w, down_w = (w_gate, w_up, w_down)
    owner_rows = arrived.reshape(-1, local_experts, slot_count, model_width)
    sources = owner_rows.shape[0]
    gate_act = jnp.einsum("sjcd,jdh->sjch", owner_rows, gate_w, preferred_element_type=jnp.float32)
    up_act = jnp.einsum("sjcd,jdh->sjch", owner_rows, up_w, preferred_element_type=jnp.float32)
    sig_gate = jax.nn.sigmoid(gate_act)
    silu_gate = gate_act * sig_gate
    hidden = (silu_gate * up_act).astype(jnp.bfloat16)

    def down_term(start, length):
        return jnp.einsum("sjch,jhd->sjcd", hidden, down_w, preferred_element_type=jnp.float32)

    produced = owner_sum(down_term, sources)
    returned = from_owner(produced.astype(jnp.bfloat16).reshape(-1, slot_count, model_width))
    slot_rows = jnp.concatenate(
        [returned.reshape(experts * slot_count, model_width), zero_row], axis=0
    )
    pair_rows = slot_rows[slot_place].reshape(tok_count, TOP, model_width).astype(jnp.float32)
    kept_mask = is_kept.reshape(tok_count, TOP).astype(jnp.float32)
    gate_kept = gate_wts * kept_mask
    moe_rows = jnp.sum(gate_kept[:, :, None] * pair_rows, axis=1)
    final_rows = second_in + moe_rows
    block_output = final_rows.astype(jnp.bfloat16)
    grad_out = cotangent.astype(jnp.float32)
    grad_gate_k = jnp.sum(pair_rows * grad_out[:, None, :], axis=2) * kept_mask
    grad_routed = gate_wts * (grad_gate_k - jnp.sum(gate_wts * grad_gate_k, axis=1, keepdims=True))
    grad_logits = jnp.sum(chosen_hot * grad_routed[:, :, None], axis=1)
    router_grad = jnp.dot(second_rows.astype(jnp.float32).T, grad_logits, precision=precise)
    grad_second = jnp.dot(grad_logits, w_router.astype(jnp.float32).T, precision=precise)
    pair_grads = (
        (gate_kept[:, :, None] * grad_out[:, None, :])
        .astype(jnp.bfloat16)
        .reshape(pair_count, model_width)
    )
    pair_grads = jnp.concatenate([pair_grads, zero_row], axis=0)
    slot_grads = pair_grads[slot_pair].reshape(experts, slot_count, model_width)
    grad_blocks = shard_gather(to_owner(slot_grads)).reshape(
        -1, local_experts, slot_count, model_width
    )
    grad_hidden = jnp.einsum(
        "sjcd,jhd->sjch", grad_blocks, down_w, preferred_element_type=jnp.float32
    )
    grad_down_w = jnp.einsum(
        "sjch,sjcd->jhd", hidden, grad_blocks, preferred_element_type=jnp.float32
    )
    grad_gate_in = (grad_hidden * up_act * sig_gate * (1.0 + gate_act * (1.0 - sig_gate))).astype(
        jnp.bfloat16
    )
    grad_up_in = (grad_hidden * silu_gate).astype(jnp.bfloat16)
    grad_gate_w = jnp.einsum(
        "sjcd,sjch->jdh", owner_rows, grad_gate_in, preferred_element_type=jnp.float32
    )
    grad_up_w = jnp.einsum(
        "sjcd,sjch->jdh", owner_rows, grad_up_in, preferred_element_type=jnp.float32
    )

    def back_term(start, length):
        from_gate = jnp.einsum(
            "sjch,jdh->sjcd", grad_gate_in, gate_w, preferred_element_type=jnp.float32
        )
        from_up = jnp.einsum("sjch,jdh->sjcd", grad_up_in, up_w, preferred_element_type=jnp.float32)
        return from_gate + from_up

    grad_slots = from_owner(
        owner_sum(back_term, sources).astype(jnp.bfloat16).reshape(-1, slot_count, model_width)
    )
    back_rows = jnp.concatenate(
        [grad_slots.reshape(experts * slot_count, model_width), zero_row], axis=0
    )
    grad_second = grad_second + jnp.sum(
        back_rows[slot_place].reshape(tok_count, TOP, model_width).astype(jnp.float32), axis=1
    )
    return block_output[None], grad_second, router_grad.T, (grad_gate_w, grad_up_w, grad_down_w)


def experts_dense(
    second_in, second_rows, cotangent, routes, capacity, w_router, w_gate, w_up, w_down
):
    tok_count = second_rows.shape[0]
    experts = w_router.shape[1]
    local_experts, model_width, hidden_here = w_gate.shape
    shards = lax.axis_size("fsdp")
    owners = lax.axis_size("expert")
    wide = local_experts * hidden_here
    logits = jnp.dot(second_rows, w_router, preferred_element_type=jnp.float32)
    expert_ids = lax.iota(jnp.int32, experts)
    named = jnp.any(routes[:, :, None] == expert_ids[None, None, :], axis=1)
    before = lax.iota(jnp.int32, tok_count)[None, :] < lax.iota(jnp.int32, tok_count)[:, None]
    ranking = jnp.dot(
        before.astype(jnp.bfloat16), named.astype(jnp.bfloat16), preferred_element_type=jnp.float32
    )
    kept = named & (ranking < capacity.astype(jnp.float32)[None, :])
    kept_mask = kept.astype(jnp.float32)
    top_logit = jnp.max(jnp.where(named, logits, -jnp.inf), axis=1, keepdims=True)
    powers = jnp.where(named, jnp.exp(jnp.where(named, logits - top_logit, 0.0)), 0.0)
    gate_wts = powers / jnp.sum(powers, axis=1, keepdims=True)
    gate_kept = gate_wts * kept_mask

    grad_all = lax.all_gather(cotangent, ("fsdp", "expert"), axis=0, tiled=True)
    nz = owners // 2
    grad_all = grad_all.reshape(shards, owners, tok_count, model_width)
    rows_all, pre, weighted, forward, gates = gather_act(
        second_rows, gate_kept.T, w_gate, w_up, w_down, nz, 7
    )
    back_rows, terms, acts = scatter_act(pre, grad_all, gates, w_gate, w_up, w_down, nz, 8)
    grad_gate_k = terms.T * kept_mask
    grad_logits = gate_wts * (grad_gate_k - jnp.sum(gate_wts * grad_gate_k, axis=1, keepdims=True))
    router_grad = jnp.dot(grad_logits.T, second_rows.astype(jnp.float32), precision=precise)
    grad_second = jnp.dot(grad_logits, w_router.astype(jnp.float32).T, precision=precise)
    grad_second = grad_second + back_rows

    units = shards * nz
    inputs = (
        rows_all.reshape(units, -1, model_width),
        acts.reshape(2, units, -1, wide),
        weighted.reshape(units, -1, wide),
        grad_all.reshape(units, -1, model_width),
    )
    return forward, grad_second, router_grad, inputs


def sum_grads(narrow, gains, head_gains, rows, inputs, first, normed, local, nz):
    shards, width = lax.axis_size("fsdp"), gains.shape[1]
    mine = lax.iota(jnp.int32, shards) == lax.axis_index("fsdp")
    heads_flat = jnp.pad(head_gains.reshape(-1), (0, width - head_gains.size))
    table = jnp.concatenate([gains, jnp.where(mine[:, None], heads_flat[None], 0.0)], axis=0)
    share = -(-table.size // (2 * shards * nz * 1024)) * 8
    small = jnp.pad(table.reshape(-1), (0, 2 * shards * nz * share * 128 - table.size))
    small = small.reshape(2, shards, nz, share, 128)
    parts = [g.reshape(-1, 2, nz, 16, g.shape[1]) for g in narrow]
    first = first.reshape(shards, -1, width)
    *sums, small, rows, gate, up, down, first = line_sum(
        parts, small, rows, inputs, first, normed.astype(jnp.bfloat16), local, nz, 9
    )
    expert_grads = (gate, up, down.reshape(local, -1, width))
    small = small.reshape(-1)[: table.size].reshape(table.shape)
    own = lax.dynamic_slice_in_dim(small, gains.shape[0] + lax.axis_index("fsdp"), 1, axis=0)
    head_gains = own[0, : head_gains.size].reshape(head_gains.shape)
    return [s.reshape(g.shape) for s, g in zip(sums, narrow)], small[: gains.shape[0]], head_gains, rows, expert_grads, first


def on_device(
    block_input,
    cotangent,
    w_query,
    w_key,
    w_value,
    w_output,
    q_gain,
    k_gain,
    attn_gain,
    mlp_gain,
    w_router,
    w_gate,
    w_up,
    w_down,
    segments,
    routes,
    capacity,
):
    tok_count = block_input.shape[1]
    model_width = block_input.shape[2]
    experts = w_router.shape[1]
    nz = lax.axis_size("expert") // 2
    dense = 2 * TOP >= experts and lax.axis_size("fsdp") == 4
    flat_in = block_input[0].astype(jnp.float32)
    scale_one = lax.rsqrt(jnp.mean(flat_in * flat_in, axis=1, keepdims=True) + epsilon)
    normed_one = flat_in * scale_one
    first_rows = (normed_one * attn_gain).astype(jnp.bfloat16)
    if dense:
        group_rows, group_segs = square_gather(first_rows, jnp.tile(segments, (8, 1)), 1)
        group_rows = group_rows.reshape(-1, model_width)
        group_segs = group_segs[:, 0].reshape(-1)
    else:
        group_rows, group_segs = (
            lax.all_gather(first_rows, "fsdp", axis=0, tiled=True),
            lax.all_gather(segments[0], "fsdp", axis=0, tiled=True),
        )
    group_len = group_rows.shape[0]
    heads_here = w_query.shape[1] // HEAD_DIM
    query_rows = jnp.dot(group_rows, w_query, preferred_element_type=jnp.float32)
    key_rows = jnp.dot(group_rows, w_key, preferred_element_type=jnp.float32)
    value_rows = jnp.dot(group_rows, w_value, preferred_element_type=jnp.float32).astype(
        jnp.bfloat16
    )
    square_sums = across_heads(
        dense and 2,
        (jnp.sum(query_rows * query_rows, axis=1), jnp.sum(key_rows * key_rows, axis=1))
    )
    q_scale = lax.rsqrt(square_sums[0][:, None] / model_width + epsilon)
    k_scale = lax.rsqrt(square_sums[1][:, None] / model_width + epsilon)
    cosine, sine_table = rope_tables(group_segs, HEAD_DIM)
    head_shape = (group_len, heads_here, HEAD_DIM)
    q_heads = apply_rope(
        (query_rows * q_scale * q_gain).reshape(head_shape), cosine, sine_table
    ).astype(jnp.bfloat16)
    k_heads = apply_rope(
        (key_rows * k_scale * k_gain).reshape(head_shape), cosine, sine_table
    ).astype(jnp.bfloat16)
    v_heads = value_rows.reshape(head_shape)
    ordinal = lax.iota(jnp.int32, group_len)
    allowed = (group_segs[:, None] == group_segs[None, :]) & (ordinal[None, :] <= ordinal[:, None])
    scores = head_scores(q_heads, k_heads, allowed)
    row_top = jnp.max(scores, axis=2, keepdims=True)
    log_total = row_top + jnp.log(jnp.sum(jnp.exp(scores - row_top), axis=2, keepdims=True))
    attn_weights = jnp.exp(scores - log_total)
    mixed_heads = jnp.einsum(
        "hts,shd->thd",
        attn_weights.astype(jnp.bfloat16),
        v_heads,
        preferred_element_type=jnp.float32,
    )
    attn_rows = mixed_heads.reshape(group_len, heads_here * HEAD_DIM).astype(jnp.bfloat16)

    def mixed_term(start, length):
        return jnp.dot(attn_rows, w_output, preferred_element_type=jnp.float32).astype(jnp.bfloat16)

    mixed_rows = share_rows(mixed_term, tok_count, dense and 4).astype(jnp.float32)
    second_in = flat_in + mixed_rows
    scale_two = lax.rsqrt(jnp.mean(second_in * second_in, axis=1, keepdims=True) + epsilon)
    normed_two = second_in * scale_two
    second_rows = (normed_two * mlp_gain).astype(jnp.bfloat16)
    if dense:
        block_output, grad_second, router_grad, expert_grads = experts_dense(
            second_in, second_rows, cotangent[0], routes[0], capacity, w_router, w_gate, w_up, w_down
        )
    else:
        block_output, grad_second, router_grad, expert_grads = experts_by_slot(
            second_in, second_rows, cotangent[0], routes[0], capacity, w_router, w_gate, w_up, w_down
        )
    grad_out = cotangent[0].astype(jnp.float32)
    mlp_gain_grad = jnp.sum(grad_second * normed_two, axis=0)
    grad_normed_two = grad_second * mlp_gain
    grad_mid = grad_out + scale_two * (
        grad_normed_two - normed_two * jnp.mean(grad_normed_two * normed_two, axis=1, keepdims=True)
    )
    if dense:
        group_grad, _ = square_gather(grad_mid.astype(jnp.bfloat16), jnp.tile(segments, (8, 1)), 6)
        group_grad = group_grad.reshape(-1, model_width)
    else:
        group_grad = lax.all_gather(grad_mid.astype(jnp.bfloat16), "fsdp", axis=0, tiled=True)
    out_grad = jnp.einsum("ti,td->id", attn_rows, group_grad, preferred_element_type=jnp.float32)
    grad_attn = (
        jnp.einsum("td,id->ti", group_grad, w_output, preferred_element_type=jnp.float32)
        .astype(jnp.bfloat16)
        .reshape(head_shape)
    )
    scores_again = head_scores(q_heads, k_heads, allowed)
    weights_again = jnp.exp(scores_again - log_total)
    grad_values = jnp.einsum(
        "hts,thd->shd",
        weights_again.astype(jnp.bfloat16),
        grad_attn,
        preferred_element_type=jnp.float32,
    )
    grad_weights = jnp.einsum(
        "thd,shd->hts", grad_attn, v_heads, preferred_element_type=jnp.float32
    )
    inner_sum = jnp.sum(weights_again * grad_weights, axis=2, keepdims=True)
    grad_scores = (weights_again * (grad_weights - inner_sum)).astype(jnp.bfloat16)
    grad_q_heads = jnp.einsum(
        "hts,shd->thd", grad_scores, k_heads, preferred_element_type=jnp.float32
    ) * HEAD_DIM ** (-0.5)
    grad_k_heads = jnp.einsum(
        "hts,thd->shd", grad_scores, q_heads, preferred_element_type=jnp.float32
    ) * HEAD_DIM ** (-0.5)
    grad_q_normed = rope_grad(grad_q_heads, cosine, sine_table).reshape(group_len, -1)
    grad_k_normed = rope_grad(grad_k_heads, cosine, sine_table).reshape(group_len, -1)
    q_gain_grad = jnp.sum(grad_q_normed * query_rows * q_scale, axis=0)
    k_gain_grad = jnp.sum(grad_k_normed * key_rows * k_scale, axis=0)
    inner_q = grad_q_normed * q_gain
    inner_k = grad_k_normed * k_gain
    inner_sums = across_heads(
        dense and 3,
        (jnp.sum(inner_q * query_rows, axis=1), jnp.sum(inner_k * key_rows, axis=1))
    )
    grad_query_rows = (
        q_scale
        * (inner_q - query_rows * q_scale * q_scale * (inner_sums[0][:, None] / model_width))
    ).astype(jnp.bfloat16)
    grad_key_rows = (
        k_scale * (inner_k - key_rows * k_scale * k_scale * (inner_sums[1][:, None] / model_width))
    ).astype(jnp.bfloat16)
    grad_value_rows = grad_values.reshape(group_len, -1).astype(jnp.bfloat16)
    head_grads = jnp.concatenate([grad_query_rows, grad_key_rows, grad_value_rows], axis=1)
    mixer_grad = jnp.einsum(
        "td,ti->di", group_rows, head_grads, preferred_element_type=jnp.float32
    ).astype(jnp.bfloat16)

    def input_term(start, length):
        from_q = jnp.einsum(
            "ti,di->td", grad_query_rows, w_query, preferred_element_type=jnp.float32
        )
        from_k = jnp.einsum("ti,di->td", grad_key_rows, w_key, preferred_element_type=jnp.float32)
        from_v = jnp.einsum(
            "ti,di->td", grad_value_rows, w_value, preferred_element_type=jnp.float32
        )
        return (from_q + from_k + from_v).astype(jnp.bfloat16)

    if dense:
        attn_gain_grad = jnp.zeros_like(mlp_gain_grad)
    else:
        grad_first = share_rows(input_term, tok_count).astype(jnp.float32)
        attn_gain_grad = jnp.sum(grad_first * normed_one, axis=0)
    narrow = (mixer_grad, out_grad.astype(jnp.bfloat16))
    gains = jnp.concatenate([attn_gain_grad[None], mlp_gain_grad[None], router_grad], axis=0)
    head_gains = jnp.stack([q_gain_grad, k_gain_grad])
    if dense:
        first = input_term(jnp.int32(0), group_len)
        narrow, gains, head_gains, forward, expert_grads, grad_first = sum_grads(
            narrow, gains, head_gains, block_output, expert_grads, first, normed_one, w_gate.shape[0], nz
        )
        block_output = (second_in + forward).astype(jnp.bfloat16)[None]
    else:
        narrow = lax.psum(narrow, "expert")
        head_gains = lax.psum(head_gains, "expert")
        gains = lax.psum(gains, ("fsdp", "expert"))
    grad_normed_one = grad_first * attn_gain
    grad_x = grad_mid + scale_one * (
        grad_normed_one - normed_one * jnp.mean(grad_normed_one * normed_one, axis=1, keepdims=True)
    )
    wide = tuple(jnp.split(narrow[0], 3, axis=1)) + (narrow[1],)
    mixer = tuple(g.astype(jnp.float32) for g in wide) + (head_gains[0], head_gains[1])
    return (
        block_output,
        grad_x[None],
        mixer[0],
        mixer[1],
        mixer[2],
        mixer[3],
        mixer[4],
        mixer[5],
        gains[0],
        gains[1],
        gains[2:].T,
        *expert_grads,
    )


def solution(mesh):
    placed = (
        P("expert", "fsdp", None),
        P("expert", "fsdp", None),
        P(None, "fsdp"),
        P(None, "fsdp"),
        P(None, "fsdp"),
        P("fsdp", None),
        P("fsdp"),
        P("fsdp"),
        P(),
        P(),
        P(),
        P("expert", None, "fsdp"),
        P("expert", None, "fsdp"),
        P("expert", "fsdp", None),
        P("expert", "fsdp"),
        P("expert", "fsdp", None),
        P(),
    )
    return jax.shard_map(
        on_device,
        mesh=mesh,
        in_specs=placed,
        out_specs=(
            P("expert", "fsdp", None),
            P("expert", "fsdp", None),
            P(None, "fsdp"),
            P(None, "fsdp"),
            P(None, "fsdp"),
            P("fsdp", None),
            P("fsdp"),
            P("fsdp"),
            P(),
            P(),
            P(),
            P("expert", None, "fsdp"),
            P("expert", None, "fsdp"),
            P("expert", "fsdp", None),
        ),
        check_vma=False,
    )
```

```python
import functools

import jax
import jax.numpy as jnp
from jax import lax
from jax.experimental import pallas as pl
from jax.experimental.pallas import tpu as pltpu
from jax.sharding import PartitionSpec as P

HEAD_DIM = 128
TOP = 8


epsilon = 1e-05
rope_base = 10000.0
precise = lax.Precision.HIGHEST


MESH = pl.DeviceIdType.MESH
DMA = pltpu.SemaphoreType.DMA


class Place:
    def __init__(self):
        self.f, self.e = lax.axis_index("fsdp"), lax.axis_index("expert")
        self.c, self.z = self.e % 2, self.e // 2
        self.fx = self.f + 1 - 2 * (self.f % 2)
        self.fy = (self.f + 2) % 4
        self.fd = 3 - self.f
        self.pe = self.e + 1 - 2 * self.c


def send(src, dst, send_sem, recv_sem, f, e):
    return pltpu.make_async_remote_copy(
        src_ref=src,
        dst_ref=dst,
        send_sem=send_sem,
        recv_sem=recv_sem,
        device_id={"fsdp": f, "expert": e},
        device_id_type=MESH,
    )


def greet(peers, line=None):
    barrier = pltpu.get_barrier_semaphore()

    def hello(f, e):
        pl.semaphore_signal(
            barrier, inc=1, device_id={"fsdp": f, "expert": e}, device_id_type=MESH
        )

    for f, e in peers:
        hello(f, e)
    if line is not None:
        at, nz = line
        for step in range(1, nz):
            hello(at.f, 2 * ((at.z + step) % nz) + at.c)
        pl.semaphore_wait(barrier, len(peers) + nz - 1)
    else:
        pl.semaphore_wait(barrier, len(peers))


class SmallGather:
    sems = staticmethod(
        lambda nz: [DMA((nz,)), DMA((nz,)), DMA((4,)), DMA((4,))]
    )

    def __init__(self, at, nz, own, out, sems):
        self.at, self.nz, self.own, self.out = at, nz, own, out
        self.ls, self.lr, self.ss, self.sr = sems

    def line(self, step):
        at = self.at
        z = (at.z + step) % self.nz
        back = (at.z + self.nz - step) % self.nz
        slot = self.out.at[at.c, at.f]
        to = send(self.own, slot.at[at.z], self.ls.at[step], self.lr.at[step], at.f, 2 * z + at.c)
        come = send(self.own, slot.at[back], self.ls.at[step], self.lr.at[step], at.f, 2 * z + at.c)
        return to, come

    def plane(self, i):
        at, out = self.at, self.out
        f, to_f = ((at.f, at.fx), (at.f, at.fy), (at.fx, at.fy))[i]
        slot = out.at[at.c, f]
        return send(slot, slot, self.ss.at[i], self.sr.at[i], to_f, at.e)

    def pair(self):
        at = self.at
        slot = self.out.at[at.c]
        return send(slot, slot, self.ss.at[3], self.sr.at[3], at.f, at.pe)

    def stage(self, i):
        at = self.at
        if i == 0:
            for step in range(1, self.nz):
                self.line(step)[0].start()
            self.out[at.c, at.f, at.z] = self.own[...]
        elif i == 1:
            for step in range(1, self.nz):
                self.line(step)[1].wait_recv()
            self.plane(0).start()
            self.plane(1).start()
        elif i == 2:
            self.plane(0).wait_recv()
            self.plane(2).start()
        elif i == 3:
            self.plane(1).wait_recv()
            self.plane(2).wait_recv()
            self.pair().start()
        elif i == 4:
            self.pair().wait_recv()
            self.pair().wait_send()
            for step in range(1, self.nz):
                self.line(step)[0].wait_send()
            for k in range(3):
                self.plane(k).wait_send()


class SmallScatter:
    sems = staticmethod(lambda nz: [DMA((nz,)), DMA((nz,)), DMA((4,)), DMA((4,))])
    scratch = staticmethod(
        lambda nz, shape: [
            pltpu.VMEM((4, nz, *shape), jnp.float32),
            pltpu.VMEM((4, nz, *shape), jnp.float32),
            pltpu.VMEM((3, nz, *shape), jnp.float32),
            pltpu.VMEM((nz, *shape), jnp.float32),
        ]
    )

    def __init__(self, at, nz, part, out, scratch, sems):
        self.at, self.nz, self.part, self.out = at, nz, part, out
        self.acc, self.pb, self.xy, self.zb = scratch
        self.ls, self.lr, self.ss, self.sr = sems

    def pair(self):
        at = self.at
        return send(
            self.part.at[1 - at.c], self.pb, self.ss.at[0], self.sr.at[0], at.f, at.pe
        )

    def plane(self, i):
        at = self.at
        f, to_f = ((at.fx, at.fx), (at.fd, at.fx), (at.fy, at.fy))[i]
        return send(
            self.acc.at[f], self.xy.at[i], self.ss.at[1 + i], self.sr.at[1 + i], to_f, at.e
        )

    def line(self, step):
        at = self.at
        z = (at.z + step) % self.nz
        return send(
            self.acc.at[at.f, z], self.zb.at[step], self.ls.at[step], self.lr.at[step], at.f, 2 * z + at.c
        )

    def stage(self, i):
        at, acc, xy = self.at, self.acc, self.xy
        if i == 0:
            self.pair().start()
        elif i == 1:
            self.pair().wait_recv()
            acc[...] = self.part[at.c] + self.pb[...]
            self.plane(0).start()
            self.plane(1).start()
        elif i == 2:
            self.plane(0).wait_recv()
            self.plane(1).wait_recv()
            acc[at.fy] = acc[at.fy] + xy[1]
            self.plane(2).start()
            acc[at.f] = acc[at.f] + xy[0]
        elif i == 3:
            self.plane(2).wait_recv()
            acc[at.f] = acc[at.f] + xy[2]
            for step in range(1, self.nz):
                self.line(step).start()
        elif i == 4:
            total = acc[at.f, at.z]
            for step in range(1, self.nz):
                self.line(step).wait_recv()
                total = total + self.zb[step]
            self.out[...] = total
            self.pair().wait_send()
            for k in range(3):
                self.plane(k).wait_send()
            for step in range(1, self.nz):
                self.line(step).wait_send()


def take(sequence, count):
    return [next(sequence) for _ in range(count)]


NT = (((1,), (1,)), ((), ()))
TN = (((0,), (0,)), ((), ()))


def halves_of(x):
    high = x.astype(jnp.bfloat16)
    return high, (x - high.astype(jnp.float32)).astype(jnp.bfloat16)


def spread(blocks, first, hidden, wide):
    experts = blocks[0].shape[0]
    high, low = halves_of(jnp.concatenate(blocks, axis=1))
    row = lax.broadcasted_iota(jnp.int32, (2 * experts, wide), 0) % experts
    col = lax.broadcasted_iota(jnp.int32, (2 * experts, wide), 1) // hidden
    pick = (row == first + col).astype(jnp.float32).astype(jnp.bfloat16)
    both = jnp.concatenate([high.astype(jnp.float32), low.astype(jnp.float32)], axis=0)
    return lax.dot_general(
        both.astype(jnp.bfloat16), pick, TN, preferred_element_type=jnp.float32
    )


def above(a, b):
    return (a - b + 63) // 64


def near_first(at, nz, s):
    right = above(2 * at.z, nz - 1)
    alternate = at.z - right * (2 * at.z - (nz - 1))
    turn = at.z + (s + 1) // 2 * (1 - 2 * (s % 2))
    rest = s + right * (nz - 1 - 2 * s)
    return turn + above(s, 2 * alternate) * (rest - turn)


def gather_act_kernel(nz, own, own_small, w_gate, w_up, w_down, out, acts, weighted, forward, gates, xb, ab, hb, fb, load_x, store, own_sem, zr, zs, xr, xs, yr, ys, dr, xf, yf, pr, ps, *small_sems):
    at = Place()
    rows, width = own.shape
    local, _, hidden = w_gate.shape
    half = rows // 2
    halves = (pl.ds(0, half), pl.ds(half, half))
    small = SmallGather(at, nz, own_small, gates, small_sems)
    greet([(at.fx, at.e), (at.fy, at.e), (at.f, at.pe)], (at, nz))
    keep = pltpu.make_async_copy(own, out.at[at.f, at.e], own_sem)
    keep.start()
    small.stage(0)
    places = (at.f, at.fx, at.fy, at.fd)
    first = at.e * w_gate.shape[0]

    def up(z):
        ref = out.at[at.f, 2 * z + at.c]
        return send(ref, ref, zs.at[0, z], zr.at[z], at.f, at.e + 2)

    def down(z):
        ref = out.at[at.f, 2 * z + at.c]
        return send(ref, ref, zs.at[1, z], zr.at[z], at.f, at.e - 2)

    def to_x(z, h):
        ref = out.at[at.f, 2 * z + at.c, halves[h]]
        return send(ref, ref, xs.at[h, z], xr.at[h, z], at.fx, at.e)

    def to_y(z, h):
        ref = out.at[at.f, 2 * z + at.c, halves[h]]
        return send(ref, ref, ys.at[h, z], yr.at[h, z], at.fy, at.e)

    def x_on(z):
        ref = out.at[at.fx, 2 * z + at.c, halves[0]]
        return send(ref, ref, yf.at[z], dr.at[0, z], at.fy, at.e)

    def y_on(z):
        ref = out.at[at.fy, 2 * z + at.c, halves[1]]
        return send(ref, ref, xf.at[z], dr.at[1, z], at.fx, at.e)

    def to_p(f, z, h):
        ref = out.at[f, 2 * z + at.c, halves[h]]
        return send(ref, ref, ps.at[f, z, h], pr.at[f, z, h], at.f, at.pe)

    def line_step(z):
        pl.when(z != at.z)(lambda: up(z).wait_recv())
        pl.when((z <= at.z) & (at.z < nz - 1))(lambda: up(z).start())
        pl.when((z >= at.z) & (at.z > 0))(lambda: down(z).start())
        to_x(z, 0).start()
        to_y(z, 1).start()
        to_x(z, 1).start()
        to_y(z, 0).start()
        for h in range(2):
            to_p(at.f, z, h).start()

    def plane_step(z):
        to_x(z, 0).wait_recv()
        x_on(z).start()
        to_y(z, 1).wait_recv()
        y_on(z).start()
        to_p(at.fx, z, 0).start()
        to_p(at.fy, z, 1).start()
        to_x(z, 1).wait_recv()
        to_p(at.fx, z, 1).start()
        to_y(z, 0).wait_recv()
        to_p(at.fy, z, 0).start()

    def diag_step(z):
        x_on(z).wait_recv()
        to_p(at.fd, z, 0).start()
        y_on(z).wait_recv()
        to_p(at.fd, z, 1).start()

    def load(q, z):
        return pltpu.make_async_copy(out.at[places[q], pl.ds(2 * z, 2)], xb.at[q], load_x.at[q])

    def stores(q, z):
        pair, f = pl.ds(2 * z, 2), places[q]
        return [
            *(
                pltpu.make_async_copy(ab.at[q, k], acts.at[k, f, pair], store.at[q, k])
                for k in range(3)
            ),
            pltpu.make_async_copy(hb.at[q], weighted.at[f, pair], store.at[q, 3]),
            pltpu.make_async_copy(fb.at[q], forward.at[f, pair], store.at[q, 4]),
        ]

    def fetch(q, z):
        for h in range(2):
            to_p(places[q], z, h).wait_recv()
        load(q, z).start()

    def work(q, z):
        load(q, z).wait()
        f = places[q]
        x = xb[q].reshape(2 * rows, width)
        gate_all = spread([gates[0, f, z], gates[1, f, z]], first, hidden, local * hidden)
        for j in range(local):
            cols = pl.ds(j * hidden, hidden)
            g_all = jnp.dot(x, w_gate[j], preferred_element_type=jnp.float32)
            u_all = jnp.dot(x, w_up[j], preferred_element_type=jnp.float32)
            for h in range(2):
                g, u = g_all[h * rows : (h + 1) * rows], u_all[h * rows : (h + 1) * rows]
                gate = gate_all[h * rows : (h + 1) * rows, j * hidden : (j + 1) * hidden]
                sig = 1.0 / (1.0 + jnp.exp(-g))
                silu = g * sig
                hid = silu * u
                ab[q, 0, h, :, cols] = u * sig * (1.0 + g * (1.0 - sig))
                ab[q, 1, h, :, cols] = silu
                ab[q, 2, h, :, cols] = hid
                hb[q, h, :, cols] = (hid * gate).astype(jnp.bfloat16)
        a = hb[q].reshape(2 * rows, local * hidden)

        def body(t, carry):
            cols = pl.ds(pl.multiple_of(t * 512, 512), 512)
            total = jnp.dot(a, w_down[:, cols], preferred_element_type=jnp.float32)
            fb[q, :, :, cols] = total.astype(jnp.bfloat16).reshape(2, rows, 512)
            return carry

        lax.fori_loop(0, width // 512, body, 0)
        for copy in stores(q, z):
            copy.start()

    keep.wait()

    def body(s, carry):
        def at_step(lag, run):
            pl.when((s >= lag) & (s < nz + lag))(lambda: run(near_first(at, nz, s - lag)))

        def free(q, lag):
            def run(z):
                for copy in stores(q, z):
                    copy.wait()

            at_step(lag + 1, run)

        at_step(0, line_step)
        for k in range(1, 5):
            pl.when(s == 0)(functools.partial(small.stage, k))
        at_step(1, lambda z: fetch(0, z))
        free(3, 4)
        at_step(4, lambda z: work(3, z))
        at_step(1, plane_step)
        at_step(2, lambda z: fetch(1, z))
        free(0, 1)
        at_step(1, lambda z: work(0, z))
        at_step(2, diag_step)
        at_step(2, lambda z: fetch(2, z))
        free(1, 2)
        at_step(2, lambda z: work(1, z))
        at_step(3, lambda z: fetch(3, z))
        free(2, 2)
        at_step(2, lambda z: work(2, z))
        return carry

    lax.fori_loop(0, nz + 5, body, 0)

    def finish(z, carry):
        pl.when((z <= at.z) & (at.z < nz - 1))(lambda: up(z).wait_send())
        pl.when((z >= at.z) & (at.z > 0))(lambda: down(z).wait_send())
        for h in range(2):
            to_x(z, h).wait_send()
            to_y(z, h).wait_send()
        x_on(z).wait_send()
        y_on(z).wait_send()
        for f in range(4):
            for h in range(2):
                to_p(f, z, h).wait_send()
        return carry

    lax.fori_loop(0, nz, finish, 0)


def gather_act(rows, small, w_gate, w_up, w_down, nz, cid):
    r, c = rows.shape
    local, _, hidden = w_gate.shape
    wide = local * hidden
    hbm, vmem = pl.BlockSpec(memory_space=pl.ANY), pl.BlockSpec(memory_space=pltpu.VMEM)
    bf16 = jnp.bfloat16
    return pl.pallas_call(
        functools.partial(gather_act_kernel, nz),
        out_shape=(
            jax.ShapeDtypeStruct((4, 2 * nz, r, c), bf16),
            jax.ShapeDtypeStruct((3, 4, 2 * nz, r, wide), jnp.float32),
            jax.ShapeDtypeStruct((4, 2 * nz, r, wide), bf16),
            jax.ShapeDtypeStruct((4, 2 * nz, r, c), bf16),
            jax.ShapeDtypeStruct((2, 4, nz, *small.shape), jnp.float32),
        ),
        in_specs=[vmem] * 5,
        out_specs=(hbm, hbm, hbm, hbm, vmem),
        scratch_shapes=[
            pltpu.VMEM((4, 2, r, c), bf16),
            pltpu.VMEM((4, 3, 2, r, wide), jnp.float32),
            pltpu.VMEM((4, 2, r, wide), bf16),
            pltpu.VMEM((4, 2, r, c), bf16),
            DMA((4,)), DMA((4, 5)),
            DMA(()), DMA((nz,)), DMA((2, nz)), DMA((2, nz)), DMA((2, nz)), DMA((2, nz)), DMA((2, nz)),
            DMA((2, nz)), DMA((nz,)), DMA((nz,)), DMA((4, nz, 2)), DMA((4, nz, 2)),
            *SmallGather.sems(nz),
        ],
        compiler_params=pltpu.CompilerParams(
            collective_id=cid, has_side_effects=True, vmem_limit_bytes=50 << 20
        ),
        cost_estimate=pl.CostEstimate(flops=0, bytes_accessed=240 << 20, transcendentals=0),
        name="gather_act",
    )(rows, small, w_gate, w_up, w_down.reshape(wide, c))


def add_rows(dst, dst_rows, parts):
    start, count = dst_rows

    def body(i, carry):
        r = pl.multiple_of(i * 16, 16)
        total = None
        for ref, offset in parts:
            piece = ref[pl.ds(offset + r, 16), :].astype(jnp.float32)
            total = piece if total is None else total + piece
        dst[pl.ds(start + r, 16), :] = total.astype(dst.dtype)
        return carry

    lax.fori_loop(0, count // 16, body, 0)


def scatter_plan(at, nz, part, out, refs, staged=None, split=1):
    acc, pb, xh, yh, xf, yf, zu, zd, ls, pr, ps, xhs, xhr, yhs, yhr, xs, xr, ys, yr, us, ur, ds_, dr = refs
    rows = out.shape[0]
    half = rows // 2
    lo, hi = pl.ds(0, half), pl.ds(half, half)

    def place(s):
        return near_first(at, nz, nz - 1 - s)

    def load(f, z):
        return pltpu.make_async_copy(part.at[f, 2 * z + at.c], acc.at[f, z], ls.at[f, z])

    fs = (at.fd, at.fx, at.fy, at.f)

    def to_p(q, z):
        f = fs[q]
        src = staged.at[q] if staged is not None else part.at[f, 2 * z + 1 - at.c]
        return send(src, pb.at[f, z], ps.at[f, z], pr.at[f, z], at.f, at.pe)

    def ready(q, z):
        if staged is None:
            load(fs[q], z).wait()
        to_p(q, z).wait_recv()

    def start_step(s):
        z = place(s)
        for q in range(4):
            load(fs[q], z).start()
            to_p(q, z).start()

    def half_x(z):
        return send(acc.at[at.fd, z, lo], xh.at[z], xhs.at[z], xhr.at[z], at.fx, at.e)

    def half_y(z):
        return send(acc.at[at.fd, z, hi], yh.at[z], yhs.at[z], yhr.at[z], at.fy, at.e)

    def full_x(z):
        return send(acc.at[at.fx, z], xf.at[z], xs.at[z], xr.at[z], at.fx, at.e)

    def full_y(z):
        return send(acc.at[at.fy, z], yf.at[z], ys.at[z], yr.at[z], at.fy, at.e)

    count = rows // split

    def go_up(z, k):
        cut = pl.ds(k * count, count)
        return send(acc.at[at.f, z, cut], zu.at[z, cut], us.at[z, k], ur.at[z, k], at.f, at.e + 2)

    def go_down(z, k):
        cut = pl.ds(k * count, count)
        return send(acc.at[at.f, z, cut], zd.at[z, cut], ds_.at[z, k], dr.at[z, k], at.f, at.e - 2)

    def diag_step(s):
        z = place(s)
        ready(0, z)
        a, b = acc.at[at.fd, z], pb.at[at.fd, z]
        add_rows(a, (0, half), [(a, 0), (b, 0)])
        half_x(z).start()
        add_rows(a, (half, half), [(a, half), (b, half)])
        half_y(z).start()

    def plane_step(s):
        z = place(s)
        ready(1, z)
        a, b = acc.at[at.fx, z], pb.at[at.fx, z]
        half_y(z).wait_recv()
        add_rows(a, (0, half), [(a, 0), (b, 0)])
        add_rows(a, (half, half), [(a, half), (b, half), (yh.at[z], 0)])
        full_x(z).start()
        ready(2, z)
        half_x(z).wait_recv()
        a, b = acc.at[at.fy, z], pb.at[at.fy, z]
        add_rows(a, (0, half), [(a, 0), (b, 0), (xh.at[z], 0)])
        add_rows(a, (half, half), [(a, half), (b, half)])
        full_y(z).start()

    def line_step(s, k=0):
        z = place(s)
        if k == 0:
            ready(3, z)
            full_x(z).wait_recv()
            full_y(z).wait_recv()
        r = k * count
        a = acc.at[at.f, z]
        four = [(a, r), (pb.at[at.f, z], r), (xf.at[z], r), (yf.at[z], r)]

        @pl.when(z > at.z)
        def _():
            @pl.when(at.z > 0)
            def _():
                go_up(z, k).wait_recv()
                add_rows(a, (r, count), four + [(zu.at[z], r)])

            pl.when(at.z == 0)(lambda: add_rows(a, (r, count), four))
            go_up(z, k).start()

        @pl.when(z < at.z)
        def _():
            @pl.when(at.z < nz - 1)
            def _():
                go_down(z, k).wait_recv()
                add_rows(a, (r, count), four + [(zd.at[z], r)])

            pl.when(at.z == nz - 1)(lambda: add_rows(a, (r, count), four))
            go_down(z, k).start()

        @pl.when(z == at.z)
        def _():
            add_rows(out, (r, count), four)

            @pl.when(at.z > 0)
            def _():
                go_up(z, k).wait_recv()
                add_rows(out, (r, count), [(out, r), (zu.at[z], r)])

            @pl.when(at.z < nz - 1)
            def _():
                go_down(z, k).wait_recv()
                add_rows(out, (r, count), [(out, r), (zd.at[z], r)])

    def finish():
        def body(z, carry):
            for q in range(4):
                if staged is None:
                    to_p(q, z).wait_send()
            half_x(z).wait_send()
            half_y(z).wait_send()
            full_x(z).wait_send()
            full_y(z).wait_send()
            for k in range(split):
                pl.when(z > at.z)(functools.partial(lambda k: go_up(z, k).wait_send(), k))
                pl.when(z < at.z)(functools.partial(lambda k: go_down(z, k).wait_send(), k))
            return carry

        lax.fori_loop(0, nz, body, 0)
        for q in range(4):
            if staged is not None:
                to_p(q, place(nz - 1)).wait_send()

    return start_step, diag_step, plane_step, line_step, finish, place, to_p


def scatter_scratch(parts, nz):
    _, _, r, c = parts.shape

    def buf(*n):
        return pltpu.VMEM((*n, c), parts.dtype)

    return [
        buf(4, nz, r), buf(4, nz, r), buf(nz, r // 2), buf(nz, r // 2),
        buf(nz, r), buf(nz, r), buf(nz, r), buf(nz, r),
        DMA((4, nz)), DMA((4, nz)), DMA((4, nz)),
        *[DMA((nz,))] * 8,
        *[DMA((nz, 4))] * 4,
    ]


def scatter_act_kernel(nz, pre, grads, gates, w_gate, w_up, w_down, out, out_small, acts, *refs):
    at = Place()
    refs = iter(refs)
    moved = take(refs, 23)
    acc = moved[0]
    pb_, cb, ab, sb, terms, load_sem, store_sem = take(refs, 7)
    _, diag, plane, line, close, place, to_p = scatter_plan(at, nz, None, out, moved, sb)
    small = SmallScatter(at, nz, terms, out_small, take(refs, 4), take(refs, 4))
    greet([(at.fx, at.e), (at.fy, at.e), (at.f, at.pe)], (at, nz))
    rows, width = out.shape
    local, _, hidden = w_gate.shape
    experts = gates.shape[3]
    fs = (at.fd, at.fx, at.fy, at.f)
    cores = (at.c, 1 - at.c)
    first = at.e * local
    expert_row = lax.broadcasted_iota(jnp.int32, (experts, hidden), 0)
    tile = 512

    def loads(q, s):
        z, f = place(s), fs[q]
        copies = []
        for h, core in enumerate(cores):
            slot = 2 * z + core
            for k in range(3):
                copies.append(
                    pltpu.make_async_copy(pre.at[k, f, slot], pb_.at[q, k, h], load_sem.at[q, h, k])
                )
            copies.append(pltpu.make_async_copy(grads.at[f, slot], cb.at[q, h], load_sem.at[q, h, 3]))
        return copies

    def stores(q, s):
        z, f = place(s), fs[q]
        return [
            pltpu.make_async_copy(
                ab.at[q, k, h], acts.at[k, f, 2 * z + core], store_sem.at[q, h, k]
            )
            for h, core in enumerate(cores)
            for k in range(2)
        ]

    def act(q, s):
        z, f = place(s), fs[q]
        for copy in loads(q, s):
            copy.wait()

        @pl.when(s > 0)
        def _():
            for copy in stores(q, s - 1):
                copy.wait()

        c = cb[q].reshape(2 * rows, width)
        gate_all = spread([gates[core, f, z] for core in cores], first, hidden, local * hidden)
        sums = [None, None]
        for j in range(local):
            pick = (expert_row == first + j).astype(jnp.float32).astype(jnp.bfloat16)
            cols = pl.ds(j * hidden, hidden)
            dh = lax.dot_general(c, w_down[j], NT, preferred_element_type=jnp.float32)
            for h, core in enumerate(cores):
                d = dh[h * rows : (h + 1) * rows]
                gate = gate_all[h * rows : (h + 1) * rows, j * hidden : (j + 1) * hidden]
                for part in halves_of(pb_[q, 2, h, :, cols] * d):
                    mine = lax.dot_general(pick, part, NT, preferred_element_type=jnp.float32)
                    sums[h] = mine if sums[h] is None else sums[h] + mine
                d = d * gate
                ab[q, 0, h, :, cols] = (d * pb_[q, 0, h, :, cols]).astype(jnp.bfloat16)
                ab[q, 1, h, :, cols] = (d * pb_[q, 1, h, :, cols]).astype(jnp.bfloat16)
        for h, core in enumerate(cores):
            terms[core, f, z] = sums[h]
        for copy in stores(q, s):
            copy.start()

        @pl.when(s + 1 < nz)
        def _():
            for copy in loads(q, s + 1):
                copy.start()

    def back(q, s):
        z, f = place(s), fs[q]
        pl.when(s > 0)(lambda: to_p(q, place(s - 1)).wait_send())
        pieces = [
            (ab[q, k].reshape(2 * rows, local * hidden)[:, j * hidden : (j + 1) * hidden], w.at[j])
            for j in range(local)
            for k, w in enumerate((w_gate, w_up))
        ]

        def body(t, carry):
            cols = pl.ds(pl.multiple_of(t * tile, tile), tile)
            total = None
            for a, w in pieces:
                term = lax.dot_general(a, w[cols, :], NT, preferred_element_type=jnp.float32)
                total = term if total is None else total + term
            total = total.astype(jnp.bfloat16)
            acc[f, z, :, cols] = total[:rows]
            sb[q, :, cols] = total[rows:]
            return carry

        lax.fori_loop(0, width // tile, body, 0)
        to_p(q, z).start()

    for q in range(4):
        for copy in loads(q, 0):
            copy.start()

    def body(s, carry):
        @pl.when(s < nz)
        def _():
            last = s == nz - 1
            for q in (0, 1):
                act(q, s)
                back(q, s)
            diag(s)
            act(2, s)
            back(2, s)
            act(3, s)
            pl.when(last)(lambda: small.stage(0))
            back(3, s)
            pl.when(last)(lambda: small.stage(1))
            plane(s)
            pl.when(last)(lambda: small.stage(2))

        pl.when(s == nz)(lambda: small.stage(3))
        pl.when(s >= 1)(lambda: line(s - 1))
        return carry

    lax.fori_loop(0, nz + 1, body, 0)
    small.stage(4)
    for q in range(4):
        for copy in stores(q, nz - 1):
            copy.wait()
    close()


def scatter_act(pre, grads, gates, w_gate, w_up, w_down, nz, cid):
    _, _, _, r, wide = pre.shape
    c = grads.shape[3]
    small = gates.shape[3:]
    hbm, vmem = pl.BlockSpec(memory_space=pl.ANY), pl.BlockSpec(memory_space=pltpu.VMEM)
    bf16 = jnp.bfloat16
    return pl.pallas_call(
        functools.partial(scatter_act_kernel, nz),
        out_shape=(
            jax.ShapeDtypeStruct((r, c), jnp.float32),
            jax.ShapeDtypeStruct(small, jnp.float32),
            jax.ShapeDtypeStruct((2, 4, 2 * nz, r, wide), bf16),
        ),
        in_specs=[hbm, hbm, vmem, vmem, vmem, vmem],
        out_specs=(vmem, vmem, hbm),
        scratch_shapes=[
            *scatter_scratch(grads, nz),
            pltpu.VMEM((4, 3, 2, r, wide), jnp.float32),
            pltpu.VMEM((4, 2, r, c), bf16),
            pltpu.VMEM((4, 2, 2, r, wide), bf16),
            pltpu.VMEM((4, r, c), bf16),
            pltpu.VMEM((2, 4, nz, *small), jnp.float32),
            DMA((4, 2, 4)), DMA((4, 2, 2)),
            *SmallScatter.scratch(nz, small),
            *SmallScatter.sems(nz),
        ],
        compiler_params=pltpu.CompilerParams(
            collective_id=cid, has_side_effects=True, vmem_limit_bytes=62 << 20
        ),
        cost_estimate=pl.CostEstimate(flops=0, bytes_accessed=300 << 20, transcendentals=0),
        name="scatter_act",
    )(pre, grads, gates, w_gate, w_up, w_down)


def square_gather_kernel(own, ids, out, out_ids, xs, xr, ys, yr, fs, fr, js, jr):
    at = Place()
    half = own.shape[0] // 2
    halves = (pl.ds(0, half), pl.ds(half, half))
    peers = [(at.fx, at.e), (at.fy, at.e), (at.fd, at.e)]
    greet(peers)

    def to_x(h):
        return send(own.at[halves[h]], out.at[at.f, halves[h]], xs.at[h], xr.at[h], at.fx, at.e)

    def to_y(h):
        return send(own.at[halves[h]], out.at[at.f, halves[h]], ys.at[h], yr.at[h], at.fy, at.e)

    x_ref, y_ref = out.at[at.fx, halves[0]], out.at[at.fy, halves[1]]
    x_on = send(x_ref, x_ref, fs.at[0], fr.at[0], at.fy, at.e)
    y_on = send(y_ref, y_ref, fs.at[1], fr.at[1], at.fx, at.e)
    notes = [
        send(ids, out_ids.at[at.f], js.at[k], jr.at[k], f, e) for k, (f, e) in enumerate(peers)
    ]
    to_x(0).start()
    to_y(1).start()
    for note in notes:
        note.start()
    to_x(1).start()
    to_y(0).start()
    out[at.f] = own[...]
    out_ids[at.f] = ids[...]
    to_x(0).wait_recv()
    x_on.start()
    to_y(1).wait_recv()
    y_on.start()
    to_x(1).wait()
    to_y(0).wait()
    for note in notes:
        note.wait()
    to_x(0).wait_send()
    to_y(1).wait_send()
    x_on.wait()
    y_on.wait()


def square_gather(rows, ids, cid):
    r, c = rows.shape
    vmem = pl.BlockSpec(memory_space=pltpu.VMEM)
    return pl.pallas_call(
        square_gather_kernel,
        out_shape=(
            jax.ShapeDtypeStruct((4, r, c), rows.dtype),
            jax.ShapeDtypeStruct((4, *ids.shape), ids.dtype),
        ),
        in_specs=[vmem] * 2,
        out_specs=(vmem,) * 2,
        scratch_shapes=[DMA((2,))] * 6 + [DMA((3,))] * 2,
        compiler_params=pltpu.CompilerParams(collective_id=cid, has_side_effects=True),
        cost_estimate=pl.CostEstimate(flops=0, bytes_accessed=60 << 20, transcendentals=0),
        name="square_gather",
    )(rows, ids)


def square_scatter_kernel(part, out, xh, yh, xf, yf, ss, rs):
    at = Place()
    rows = out.shape[0]
    half = rows // 2
    lo, hi = pl.ds(0, half), pl.ds(half, half)
    greet([(at.fx, at.e), (at.fy, at.e)])

    def to_x(k, src, dst):
        return send(src, dst, ss.at[k], rs.at[k], at.fx, at.e)

    def to_y(k, src, dst):
        return send(src, dst, ss.at[k], rs.at[k], at.fy, at.e)

    copies = [
        to_x(0, part.at[at.fd, lo], xh),
        to_y(1, part.at[at.fd, hi], yh),
        to_x(2, part.at[at.fx, lo], xf.at[lo]),
        to_y(3, part.at[at.fy, hi], yf.at[hi]),
        to_x(4, yh, xf.at[hi]),
        to_y(5, xh, yf.at[lo]),
    ]
    for copy in copies[:4]:
        copy.start()
    copies[1].wait_recv()
    add_rows(yh, (0, half), [(yh, 0), (part.at[at.fx], half)])
    copies[4].start()
    copies[0].wait_recv()
    add_rows(xh, (0, half), [(xh, 0), (part.at[at.fy], 0)])
    copies[5].start()
    copies[2].wait_recv()
    copies[5].wait_recv()
    copies[3].wait_recv()
    copies[4].wait_recv()
    add_rows(out, (0, rows), [(part.at[at.f], 0), (xf, 0), (yf, 0)])
    for copy in copies:
        copy.wait_send()


def square_scatter(parts, cid):
    _, r, c = parts.shape
    vmem = pl.BlockSpec(memory_space=pltpu.VMEM)

    def buf(n):
        return pltpu.VMEM((n, c), parts.dtype)

    return pl.pallas_call(
        square_scatter_kernel,
        out_shape=jax.ShapeDtypeStruct((r, c), jnp.float32),
        in_specs=[vmem],
        out_specs=vmem,
        scratch_shapes=[buf(r // 2), buf(r // 2), buf(r), buf(r), DMA((6,)), DMA((6,))],
        compiler_params=pltpu.CompilerParams(collective_id=cid, has_side_effects=True),
        cost_estimate=pl.CostEstimate(flops=0, bytes_accessed=60 << 20, transcendentals=0),
        name="square_scatter",
    )(parts)


def square_sum_kernel(own, out, got, ss, rs):
    at = Place()
    peers = [(at.fx, at.e), (at.fy, at.e), (at.fd, at.e)]
    greet(peers)
    copies = [send(own, got.at[k], ss.at[k], rs.at[k], f, e) for k, (f, e) in enumerate(peers)]
    for copy in copies:
        copy.start()
    for copy in copies:
        copy.wait()
    out[...] = (own[...] + got[0]) + (got[1] + got[2])


def square_sum(values, cid):
    flat = values.reshape(8, -1)
    vmem = pl.BlockSpec(memory_space=pltpu.VMEM)
    return pl.pallas_call(
        square_sum_kernel,
        out_shape=jax.ShapeDtypeStruct(flat.shape, jnp.float32),
        in_specs=[vmem],
        out_specs=vmem,
        scratch_shapes=[pltpu.VMEM((3, *flat.shape), jnp.float32), DMA((3,)), DMA((3,))],
        compiler_params=pltpu.CompilerParams(collective_id=cid, has_side_effects=True),
        cost_estimate=pl.CostEstimate(flops=0, bytes_accessed=10 << 20, transcendentals=0),
        name="square_sum",
    )(flat).reshape(values.shape)


class product_plan:
    def __init__(self, inputs, outs, refs):
        self.rows, self.acts, self.weighted, self.grads = inputs
        self.outs = outs
        self.acc, self.xw, self.aw, self.load_sem, self.store_sem = refs
        self.tile = self.acc.shape[2]
        self.units = self.rows.shape[0]
        self.local = self.outs[0].shape[0]
        self.per_pass = self.units // 2
        self.steps = self.per_pass * (self.local + 1)

    def loads(self, i, k, p):
        u = (i - p * self.per_pass) * 2 + k
        hidden = self.outs[0].shape[2]
        sem = self.load_sem.at[k]
        if p == self.local:
            return [
                pltpu.make_async_copy(self.grads.at[u], self.xw.at[k], sem.at[0]),
                pltpu.make_async_copy(self.weighted.at[u], self.aw.at[k], sem.at[1]),
            ]
        cols = pl.ds(p * hidden, hidden)
        return [
            pltpu.make_async_copy(self.rows.at[u], self.xw.at[k], sem.at[0]),
            pltpu.make_async_copy(self.acts.at[0, u, :, cols], self.aw.at[k, :, pl.ds(0, hidden)], sem.at[1]),
            pltpu.make_async_copy(
                self.acts.at[1, u, :, cols], self.aw.at[k, :, pl.ds(hidden, hidden)], sem.at[2]
            ),
        ]

    def on_pass(self, i, run):
        for p in range(self.local + 1):
            pl.when((i >= p * self.per_pass) & (i < (p + 1) * self.per_pass))(functools.partial(run, p))

    def start(self):
        for k in range(2):
            for copy in self.loads(0, k, 0):
                copy.start()

        for p in range(self.local):
            self.clear(p)

    def clear(self, p):
        def body(r, carry):
            self.acc[p, pl.ds(r * 8, 8), :] = jnp.zeros((8, self.tile), jnp.float32)
            return carry

        lax.fori_loop(0, self.acc.shape[1] // 8, body, 0)

    def step(self, i):
        tile = self.tile

        def run(p):
            if p == self.local:

                @pl.when(i == p * self.per_pass)
                def _():
                    for copy in self.stores(0):
                        copy.wait()
                    self.clear(0)

            for k in range(2):
                for copy in self.loads(i, k, p):
                    copy.wait()
                a = self.aw[k]
                for t in range(self.xw.shape[2] // tile):
                    cols = pl.ds(t * tile, tile)
                    x = self.xw[k, :, cols]
                    if p == self.local:
                        self.acc[0, cols, :] += lax.dot_general(
                            a, x, TN, preferred_element_type=jnp.float32
                        )
                    else:
                        self.acc[p, cols, :] += lax.dot_general(
                            x, a, TN, preferred_element_type=jnp.float32
                        )

                def more(q, k=k):
                    for copy in self.loads(i + 1, k, q):
                        copy.start()

                self.on_pass(i + 1, more)

            @pl.when(i == (p + 1) * self.per_pass - 1)
            def _():
                for copy in self.stores(p):
                    copy.start()

        self.on_pass(i, run)

    def stores(self, p):
        hidden = self.outs[0].shape[2]
        if p == self.local:
            cuts = [pl.ds(k * self.tile, self.tile) for k in range(self.outs[2].shape[1] // self.tile)]
            return [
                pltpu.make_async_copy(
                    self.acc.at[0, cut], self.outs[2].at[:, cut], self.store_sem.at[p, k]
                )
                for k, cut in enumerate(cuts)
            ]
        acc = self.acc.at[p]
        return [
            pltpu.make_async_copy(
                acc.at[:, pl.ds(k * hidden, hidden)], self.outs[k].at[p], self.store_sem.at[p, k]
            )
            for k in range(2)
        ]

    def finish(self):
        for p in range(1, self.local + 1):
            for copy in self.stores(p):
                copy.wait()


class SquareScatter:
    def __init__(self, at, part, normed, out, table, refs):
        self.part, self.normed, self.out, self.table = part, normed, out, table
        self.xh, self.yh, self.xf, self.yf, self.px, self.py, self.pf, ss, rs, ls = refs
        half = self.xh.shape[0]
        lo, hi = pl.ds(0, half), pl.ds(half, half)

        def to_x(k, src, dst):
            return send(src, dst, ss.at[k], rs.at[k], at.fx, at.e)

        def to_y(k, src, dst):
            return send(src, dst, ss.at[k], rs.at[k], at.fy, at.e)

        self.copies = [
            to_x(0, part.at[at.fd, lo], self.xh),
            to_y(1, part.at[at.fd, hi], self.yh),
            to_x(2, part.at[at.fx, lo], self.xf.at[lo]),
            to_y(3, part.at[at.fy, hi], self.yf.at[hi]),
            to_x(4, self.yh, self.xf.at[hi]),
            to_y(5, self.xh, self.yf.at[lo]),
        ]
        self.loads = [
            pltpu.make_async_copy(part.at[at.fx, hi], self.px, ls.at[0]),
            pltpu.make_async_copy(part.at[at.fy, lo], self.py, ls.at[1]),
            pltpu.make_async_copy(part.at[at.f], self.pf, ls.at[2]),
        ]

    def stage(self, i):
        copies, half, rows = self.copies, self.xh.shape[0], self.out.shape[0]
        if i == 0:
            for copy in copies[:4] + self.loads:
                copy.start()
        elif i == 1:
            for copy in self.loads:
                copy.wait()
            copies[1].wait_recv()
            add_rows(self.yh, (0, half), [(self.yh, 0), (self.px, 0)])
            copies[4].start()
            copies[0].wait_recv()
            add_rows(self.xh, (0, half), [(self.xh, 0), (self.py, 0)])
            copies[5].start()
        elif i == 2:
            for copy in copies[2:]:
                copy.wait_recv()
            add_rows(self.out, (0, rows), [(self.pf, 0), (self.xf, 0), (self.yf, 0)])

            def body(r, total):
                cut = pl.ds(pl.multiple_of(r * 16, 16), 16)
                both = self.out[cut, :] * self.normed[cut, :].astype(jnp.float32)
                return total + both[:8] + both[8:]

            total = lax.fori_loop(0, rows // 16, body, jnp.zeros((8, self.out.shape[1]), jnp.float32))
            total = jnp.sum(total, axis=0, keepdims=True)
            for k in range(self.table.shape[3]):
                self.table[0, 0, 0, k : k + 1, :] = total[:, k * 128 : (k + 1) * 128]
            for copy in copies:
                copy.wait_send()


def line_sum_kernel(nz, counts, *refs):
    at = Place()
    refs = iter(refs)
    n = len(counts)
    parts, table_in, rows_part, inputs = take(refs, n), next(refs), next(refs), take(refs, 4)
    first_part, normed = take(refs, 2)
    outs, out_small, rows_out, grads = take(refs, n), next(refs), next(refs), take(refs, 3)
    first_out, part_small = take(refs, 2)
    square = SquareScatter(at, first_part, normed, first_out, part_small, take(refs, 10))
    begin, diag, plane, line, close, _, _ = scatter_plan(
        at, nz, rows_part, rows_out, take(refs, 23), split=2
    )
    product = product_plan(inputs, grads, take(refs, 5))
    bufs = [take(refs, 5) for _ in range(n)]
    sems = [take(refs, 12) for _ in range(n)]
    own_small = next(refs)
    scatter_small = SmallScatter(at, nz, part_small, own_small, take(refs, 4), take(refs, 4))
    gather_small = SmallGather(at, nz, own_small, out_small, take(refs, 4))
    greet([(at.fx, at.e), (at.fy, at.e), (at.f, at.pe)], (at, nz))
    square.stage(0)
    part_small[...] = table_in[...]
    total = sum(counts)
    last = nz - 1
    lag, per = 1, 5

    class Piece:
        def __init__(self, k, p):
            self.p, self.part, self.out = p, parts[k], outs[k]
            self.acc, self.pb, self.zu, self.zd, self.mine = bufs[k]
            self.sems = sems[k]
            self.r = self.acc.shape[2]

        def load(self):
            p = self.p
            return pltpu.make_async_copy(self.part.at[p, at.c], self.acc.at[p], self.sems[0].at[p])

        def to_p(self):
            p, (_, s, r, *_rest) = self.p, self.sems
            return send(self.part.at[p, 1 - at.c], self.pb.at[p], s.at[p], r.at[p], at.f, at.pe)

        def go_up(self, z):
            p, s, r = self.p, self.sems[3], self.sems[4]
            return send(self.acc.at[p, z], self.zu.at[p, z], s.at[p, z], r.at[p, z], at.f, at.e + 2)

        def go_down(self, z):
            p, s, r = self.p, self.sems[5], self.sems[6]
            return send(self.acc.at[p, z], self.zd.at[p, z], s.at[p, z], r.at[p, z], at.f, at.e - 2)

        def res(self, z, way):
            p, s, r = self.p, self.sems[7], self.sems[8]
            ref = self.out.at[p, at.c, z]
            return send(ref, ref, s.at[way, p, z], r.at[p, z], at.f, at.e + 2 - 4 * way)

        def res_p(self, z):
            p, s, r = self.p, self.sems[9], self.sems[10]
            ref = self.out.at[p, at.c, z]
            return send(ref, ref, s.at[p, z], r.at[p, z], at.f, at.pe)

        def keep(self):
            p = self.p
            return pltpu.make_async_copy(self.mine.at[p], self.out.at[p, at.c, at.z], self.sems[11].at[p])

    def piece(q, run, when=True):
        low = 0
        for k, count in enumerate(counts):
            @pl.when((q >= low) & (q < low + count) & when)
            def _(k=k, low=low):
                run(Piece(k, q - low))

            low += count

    def start(it):
        it.load().start()
        it.to_p().start()

    piece(0, start)
    begin(0)
    piece(1, start)
    product.start()

    def halve(it):
        it.load().wait()
        it.to_p().wait_recv()
        p = it.p

        def body(z, carry):
            a = it.acc.at[p, z]
            add_rows(a, (0, it.r), [(a, 0), (it.pb.at[p, z], 0)])
            return carry

        lax.fori_loop(0, nz, body, 0)

    def rise(it):
        p = it.p

        def body(i, carry):
            z = last - i

            @pl.when(z > at.z)
            def _():
                a = it.acc.at[p, z]

                @pl.when(at.z > 0)
                def _():
                    it.go_up(z).wait_recv()
                    add_rows(a, (0, it.r), [(a, 0), (it.zu.at[p, z], 0)])

                it.go_up(z).start()

            return carry

        lax.fori_loop(0, last, body, 0)

    def sink(it):
        p = it.p

        def body(z, carry):
            @pl.when(z < at.z)
            def _():
                a = it.acc.at[p, z]

                @pl.when(at.z < last)
                def _():
                    it.go_down(z).wait_recv()
                    add_rows(a, (0, it.r), [(a, 0), (it.zd.at[p, z], 0)])

                it.go_down(z).start()

            return carry

        lax.fori_loop(0, last, body, 0)

    def settle(it):
        p, z = it.p, at.z
        pl.when(z > 0)(lambda: it.go_up(z).wait_recv())
        pl.when(z < last)(lambda: it.go_down(z).wait_recv())
        a, dst = (it.acc.at[p, z], 0), it.mine.at[p]
        up, down = (it.zu.at[p, z], 0), (it.zd.at[p, z], 0)
        pl.when((z > 0) & (z < last))(lambda: add_rows(dst, (0, it.r), [a, up, down]))
        pl.when(z == 0)(lambda: add_rows(dst, (0, it.r), [a, down]))
        pl.when(z == last)(lambda: add_rows(dst, (0, it.r), [a, up]))
        it.keep().start()

    def tell(it):
        z = at.z
        it.keep().wait()
        pl.when(z < last)(lambda: it.res(z, 0).start())
        pl.when(z > 0)(lambda: it.res(z, 1).start())
        it.res_p(z).start()

    def pass_up(it, z):
        it.res(z, 0).wait_recv()
        pl.when(at.z < last)(lambda: it.res(z, 0).start())
        it.res_p(z).start()

    def pass_down(it, z):
        it.res(z, 0).wait_recv()
        pl.when(at.z > 0)(lambda: it.res(z, 1).start())
        it.res_p(z).start()

    def body(i, carry):
        piece(i + 2, start)
        s, turn = i // per, i % per
        pl.when((turn == 0) & (s + 1 < nz))(lambda: begin(s + 1))
        pl.when((turn == 0) & (s < nz))(lambda: diag(s))
        pl.when((turn == 2) & (s < nz))(lambda: plane(s))
        pl.when((turn == 3) & (s >= 1) & (s < nz + 1))(lambda: line(s - 1, 0))
        pl.when((turn == 0) & (s >= 2) & (s < nz + 2))(lambda: line(s - 2, 1))
        piece(i, halve)
        piece(i - lag * at.z, rise, at.z < last)
        piece(i - lag * (last - at.z), sink, at.z > 0)
        piece(i - lag * nz, settle)
        piece(i - lag * nz, tell)
        for d in range(1, nz):
            piece(i - lag * (nz + d), functools.partial(pass_up, z=at.z - d), at.z >= d)
            piece(i - lag * (nz + d), functools.partial(pass_down, z=at.z + d), at.z + d <= last)
        for k, at_step in ((1, 1), (2, 5)):
            pl.when(i == at_step)(functools.partial(square.stage, k))
        for k in range(5):
            pl.when(i == 6 + k)(functools.partial(scatter_small.stage, k))
            pl.when(i == 11 + k)(functools.partial(gather_small.stage, k))
        product.step(i)
        return carry

    steps = max(total + lag * (2 * nz - 1), per * (nz + 2), product.steps)
    lax.fori_loop(0, steps, body, 0)
    product.finish()

    def finish(q, carry):
        def run(it):
            it.to_p().wait_send()

            def one(z, carry):
                pl.when(z > at.z)(lambda: it.go_up(z).wait_send())
                pl.when(z < at.z)(lambda: it.go_down(z).wait_send())
                pl.when((z <= at.z) & (at.z < last))(lambda: it.res(z, 0).wait_send())
                pl.when((z >= at.z) & (at.z > 0))(lambda: it.res(z, 1).wait_send())
                it.res_p(z).wait_send()
                it.res_p(z).wait_recv()
                return carry

            lax.fori_loop(0, nz, one, 0)

        piece(q, run)
        return carry

    lax.fori_loop(0, total, finish, 0)
    close()


def line_sum(parts, small, rows, inputs, first, normed, local, nz, cid):
    counts = tuple(p.shape[0] for p in parts)
    units, unit, width = inputs[0].shape
    wide = inputs[1].shape[3]
    scratch, sems = [], []
    for p in parts:
        n, _, _, r, c = p.shape

        def buf(*lead):
            return pltpu.VMEM((*lead, r, c), p.dtype)

        scratch += [buf(n, nz), buf(n, nz), buf(n, nz), buf(n, nz), buf(n)]
        each, line = DMA((n,)), DMA((n, nz))
        sems += [each, each, each, line, line, line, line, DMA((2, n, nz)), line, line, line, each]
    hbm, vmem = pl.BlockSpec(memory_space=pl.ANY), pl.BlockSpec(memory_space=pltpu.VMEM)
    _, r, c = first.shape
    bf16 = jnp.bfloat16
    assert small.shape[3] * small.shape[4] == c
    return pl.pallas_call(
        functools.partial(line_sum_kernel, nz, counts),
        out_shape=(
            *(jax.ShapeDtypeStruct(p.shape, p.dtype) for p in parts),
            jax.ShapeDtypeStruct(small.shape, jnp.float32),
            jax.ShapeDtypeStruct(rows.shape[2:], jnp.float32),
            jax.ShapeDtypeStruct((local, width, wide // local), jnp.float32),
            jax.ShapeDtypeStruct((local, width, wide // local), jnp.float32),
            jax.ShapeDtypeStruct((wide, width), jnp.float32),
            jax.ShapeDtypeStruct(first.shape[1:], jnp.float32),
        ),
        in_specs=[hbm] * len(parts) + [vmem, hbm] + [hbm] * len(inputs) + [hbm, vmem],
        out_specs=(*[hbm] * len(parts), vmem, vmem, *[hbm] * 3, vmem),
        scratch_shapes=[
            pltpu.VMEM(small.shape, jnp.float32),
            pltpu.VMEM((r // 2, c), bf16), pltpu.VMEM((r // 2, c), bf16),
            pltpu.VMEM((r, c), bf16), pltpu.VMEM((r, c), bf16),
            pltpu.VMEM((r // 2, c), bf16), pltpu.VMEM((r // 2, c), bf16), pltpu.VMEM((r, c), bf16),
            DMA((6,)), DMA((6,)), DMA((3,)),
            *scatter_scratch(rows, nz),
            pltpu.VMEM((local, width, 2 * wide // local), jnp.float32),
            pltpu.VMEM((2, unit, width), rows.dtype),
            pltpu.VMEM((2, unit, wide), rows.dtype),
            DMA((2, 3)), DMA((local + 1, 4)),
            *scratch, *sems, pltpu.VMEM(small.shape[-2:], jnp.float32),
            *SmallScatter.scratch(nz, small.shape[-2:]), *SmallScatter.sems(nz), *SmallGather.sems(nz),
        ],
        compiler_params=pltpu.CompilerParams(
            collective_id=cid, has_side_effects=True, vmem_limit_bytes=63 << 20
        ),
        cost_estimate=pl.CostEstimate(flops=0, bytes_accessed=300 << 20, transcendentals=0),
        name="line_sum",
    )(*parts, small, rows, *inputs, first, normed)


def rope_tables(seg_ids, head_dim):
    length = seg_ids.shape[0]
    ordinal = lax.iota(jnp.int32, length)
    earlier = (seg_ids[:, None] == seg_ids[None, :]) & (ordinal[None, :] < ordinal[:, None])
    places = jnp.sum(earlier.astype(jnp.int32), axis=1).astype(jnp.float32)
    half_dim = head_dim // 2
    inv_freq = rope_base ** (
        -(lax.iota(jnp.int32, half_dim).astype(jnp.float32) * (2.0 / head_dim))
    )
    angles = places[:, None] * inv_freq[None, :]
    angles = jnp.concatenate([angles, angles], axis=1)
    return (jnp.cos(angles), jnp.sin(angles))


def rotate_half(values):
    half_dim = values.shape[-1] // 2
    return jnp.concatenate([-values[..., half_dim:], values[..., :half_dim]], axis=-1)


def rotate_back(values):
    half_dim = values.shape[-1] // 2
    return jnp.concatenate([values[..., half_dim:], -values[..., :half_dim]], axis=-1)


def apply_rope(values, cosine, sine_table):
    return values * cosine[:, None, :] + rotate_half(values) * sine_table[:, None, :]


def rope_grad(grads_in, cosine, sine_table):
    return grads_in * cosine[:, None, :] + rotate_back(grads_in * sine_table[:, None, :])


def across_heads(kernel, pair_sums):
    if kernel:
        return square_sum(jnp.stack(pair_sums), kernel)
    return lax.psum((pair_sums[0], pair_sums[1]), "fsdp")


def share_rows(term_fn, own_rows, kernel=0):
    if kernel:
        parts = term_fn(jnp.int32(0), own_rows * lax.axis_size("fsdp"))
        return square_scatter(parts.reshape(-1, own_rows, parts.shape[1]), kernel)
    return lax.psum_scatter(
        term_fn(jnp.int32(0), own_rows * lax.axis_size("fsdp")),
        "fsdp",
        scatter_dimension=0,
        tiled=True,
    )


def to_owner(block_rows):
    return lax.all_to_all(block_rows, "expert", split_axis=0, concat_axis=0, tiled=True)


def from_owner(block_rows):
    return lax.all_to_all(block_rows, "expert", split_axis=0, concat_axis=0, tiled=True)


def shard_gather(block_rows):
    return lax.all_gather(block_rows, "fsdp", axis=0, tiled=True)


def owner_sum(term_fn, sources):
    own_rows = sources // lax.axis_size("fsdp")
    return lax.psum_scatter(
        term_fn(jnp.int32(0), own_rows * lax.axis_size("fsdp")),
        "fsdp",
        scatter_dimension=0,
        tiled=True,
    )


def head_scores(q_heads, k_heads, allowed):
    scores = jnp.einsum(
        "thd,shd->hts", q_heads, k_heads, preferred_element_type=jnp.float32
    ) * HEAD_DIM ** (-0.5)
    return jnp.where(allowed[None], scores, -1e30)


def experts_by_slot(
    second_in, second_rows, cotangent, routes, capacity, w_router, w_gate, w_up, w_down
):
    tok_count, model_width = second_rows.shape
    experts = w_router.shape[1]
    local_experts = w_gate.shape[0]
    slot_count = tok_count * TOP * 3 // (2 * experts)
    pair_count = tok_count * TOP
    zero_row = jnp.zeros((1, model_width), jnp.bfloat16)
    logits = jnp.dot(second_rows, w_router, preferred_element_type=jnp.float32)
    chosen = routes
    expert_ids = lax.iota(jnp.int32, experts)
    chosen_hot = (chosen[:, :, None] == expert_ids[None, None, :]).astype(jnp.float32)
    routed = jnp.sum(chosen_hot * logits[:, None, :], axis=2)
    gate_wts = jax.nn.softmax(routed, axis=1)
    pair_hot = chosen_hot.reshape(pair_count, experts).astype(jnp.int32)
    earlier_hits = jnp.cumsum(pair_hot, axis=0) - pair_hot
    ranking = jnp.sum(earlier_hits * pair_hot, axis=1)
    cap_pair = jnp.sum(pair_hot * capacity[None, :], axis=1)
    is_kept = ranking < cap_pair
    pair_route = chosen.reshape(pair_count)
    slot_place = jnp.where(is_kept, pair_route * slot_count + ranking, experts * slot_count)
    pair_ids = lax.iota(jnp.int32, pair_count)
    slot_pair = (
        jnp.full((experts * slot_count,), pair_count, jnp.int32)
        .at[slot_place]
        .set(pair_ids, mode="drop")
    )
    padded = jnp.concatenate([second_rows, zero_row], axis=0)
    outgoing = padded[slot_pair // TOP].reshape(experts, slot_count, model_width)
    arrived = shard_gather(to_owner(outgoing))
    gate_w, up_w, down_w = (w_gate, w_up, w_down)
    owner_rows = arrived.reshape(-1, local_experts, slot_count, model_width)
    sources = owner_rows.shape[0]
    gate_act = jnp.einsum("sjcd,jdh->sjch", owner_rows, gate_w, preferred_element_type=jnp.float32)
    up_act = jnp.einsum("sjcd,jdh->sjch", owner_rows, up_w, preferred_element_type=jnp.float32)
    sig_gate = jax.nn.sigmoid(gate_act)
    silu_gate = gate_act * sig_gate
    hidden = (silu_gate * up_act).astype(jnp.bfloat16)

    def down_term(start, length):
        return jnp.einsum("sjch,jhd->sjcd", hidden, down_w, preferred_element_type=jnp.float32)

    produced = owner_sum(down_term, sources)
    returned = from_owner(produced.astype(jnp.bfloat16).reshape(-1, slot_count, model_width))
    slot_rows = jnp.concatenate(
        [returned.reshape(experts * slot_count, model_width), zero_row], axis=0
    )
    pair_rows = slot_rows[slot_place].reshape(tok_count, TOP, model_width).astype(jnp.float32)
    kept_mask = is_kept.reshape(tok_count, TOP).astype(jnp.float32)
    gate_kept = gate_wts * kept_mask
    moe_rows = jnp.sum(gate_kept[:, :, None] * pair_rows, axis=1)
    final_rows = second_in + moe_rows
    block_output = final_rows.astype(jnp.bfloat16)
    grad_out = cotangent.astype(jnp.float32)
    grad_gate_k = jnp.sum(pair_rows * grad_out[:, None, :], axis=2) * kept_mask
    grad_routed = gate_wts * (grad_gate_k - jnp.sum(gate_wts * grad_gate_k, axis=1, keepdims=True))
    grad_logits = jnp.sum(chosen_hot * grad_routed[:, :, None], axis=1)
    router_grad = jnp.dot(second_rows.astype(jnp.float32).T, grad_logits, precision=precise)
    grad_second = jnp.dot(grad_logits, w_router.astype(jnp.float32).T, precision=precise)
    pair_grads = (
        (gate_kept[:, :, None] * grad_out[:, None, :])
        .astype(jnp.bfloat16)
        .reshape(pair_count, model_width)
    )
    pair_grads = jnp.concatenate([pair_grads, zero_row], axis=0)
    slot_grads = pair_grads[slot_pair].reshape(experts, slot_count, model_width)
    grad_blocks = shard_gather(to_owner(slot_grads)).reshape(
        -1, local_experts, slot_count, model_width
    )
    grad_hidden = jnp.einsum(
        "sjcd,jhd->sjch", grad_blocks, down_w, preferred_element_type=jnp.float32
    )
    grad_down_w = jnp.einsum(
        "sjch,sjcd->jhd", hidden, grad_blocks, preferred_element_type=jnp.float32
    )
    grad_gate_in = (grad_hidden * up_act * sig_gate * (1.0 + gate_act * (1.0 - sig_gate))).astype(
        jnp.bfloat16
    )
    grad_up_in = (grad_hidden * silu_gate).astype(jnp.bfloat16)
    grad_gate_w = jnp.einsum(
        "sjcd,sjch->jdh", owner_rows, grad_gate_in, preferred_element_type=jnp.float32
    )
    grad_up_w = jnp.einsum(
        "sjcd,sjch->jdh", owner_rows, grad_up_in, preferred_element_type=jnp.float32
    )

    def back_term(start, length):
        from_gate = jnp.einsum(
            "sjch,jdh->sjcd", grad_gate_in, gate_w, preferred_element_type=jnp.float32
        )
        from_up = jnp.einsum("sjch,jdh->sjcd", grad_up_in, up_w, preferred_element_type=jnp.float32)
        return from_gate + from_up

    grad_slots = from_owner(
        owner_sum(back_term, sources).astype(jnp.bfloat16).reshape(-1, slot_count, model_width)
    )
    back_rows = jnp.concatenate(
        [grad_slots.reshape(experts * slot_count, model_width), zero_row], axis=0
    )
    grad_second = grad_second + jnp.sum(
        back_rows[slot_place].reshape(tok_count, TOP, model_width).astype(jnp.float32), axis=1
    )
    return block_output[None], grad_second, router_grad.T, (grad_gate_w, grad_up_w, grad_down_w)


def experts_dense(
    second_in, second_rows, cotangent, routes, capacity, w_router, w_gate, w_up, w_down
):
    tok_count = second_rows.shape[0]
    experts = w_router.shape[1]
    local_experts, model_width, hidden_here = w_gate.shape
    shards = lax.axis_size("fsdp")
    owners = lax.axis_size("expert")
    wide = local_experts * hidden_here
    logits = jnp.dot(second_rows, w_router, preferred_element_type=jnp.float32)
    expert_ids = lax.iota(jnp.int32, experts)
    named = jnp.any(routes[:, :, None] == expert_ids[None, None, :], axis=1)
    before = lax.iota(jnp.int32, tok_count)[None, :] < lax.iota(jnp.int32, tok_count)[:, None]
    ranking = jnp.dot(
        before.astype(jnp.bfloat16), named.astype(jnp.bfloat16), preferred_element_type=jnp.float32
    )
    kept = named & (ranking < capacity.astype(jnp.float32)[None, :])
    kept_mask = kept.astype(jnp.float32)
    top_logit = jnp.max(jnp.where(named, logits, -jnp.inf), axis=1, keepdims=True)
    powers = jnp.where(named, jnp.exp(jnp.where(named, logits - top_logit, 0.0)), 0.0)
    gate_wts = powers / jnp.sum(powers, axis=1, keepdims=True)
    gate_kept = gate_wts * kept_mask

    grad_all = lax.all_gather(cotangent, ("fsdp", "expert"), axis=0, tiled=True)
    nz = owners // 2
    grad_all = grad_all.reshape(shards, owners, tok_count, model_width)
    rows_all, pre, weighted, forward, gates = gather_act(
        second_rows, gate_kept.T, w_gate, w_up, w_down, nz, 7
    )
    back_rows, terms, acts = scatter_act(pre, grad_all, gates, w_gate, w_up, w_down, nz, 8)
    grad_gate_k = terms.T * kept_mask
    grad_logits = gate_wts * (grad_gate_k - jnp.sum(gate_wts * grad_gate_k, axis=1, keepdims=True))
    router_grad = jnp.dot(grad_logits.T, second_rows.astype(jnp.float32), precision=precise)
    grad_second = jnp.dot(grad_logits, w_router.astype(jnp.float32).T, precision=precise)
    grad_second = grad_second + back_rows

    units = shards * nz
    inputs = (
        rows_all.reshape(units, -1, model_width),
        acts.reshape(2, units, -1, wide),
        weighted.reshape(units, -1, wide),
        grad_all.reshape(units, -1, model_width),
    )
    return forward, grad_second, router_grad, inputs


def sum_grads(narrow, gains, head_gains, rows, inputs, first, normed, local, nz):
    shards, width = lax.axis_size("fsdp"), gains.shape[1]
    mine = lax.iota(jnp.int32, shards) == lax.axis_index("fsdp")
    heads_flat = jnp.pad(head_gains.reshape(-1), (0, width - head_gains.size))
    table = jnp.concatenate([gains, jnp.where(mine[:, None], heads_flat[None], 0.0)], axis=0)
    share = -(-table.size // (2 * shards * nz * 1024)) * 8
    small = jnp.pad(table.reshape(-1), (0, 2 * shards * nz * share * 128 - table.size))
    small = small.reshape(2, shards, nz, share, 128)
    parts = [g.reshape(-1, 2, nz, 32, g.shape[1]) for g in narrow]
    first = first.reshape(shards, -1, width)
    *sums, small, rows, gate, up, down, first = line_sum(
        parts, small, rows, inputs, first, normed.astype(jnp.bfloat16), local, nz, 9
    )
    expert_grads = (gate, up, down.reshape(local, -1, width))
    small = small.reshape(-1)[: table.size].reshape(table.shape)
    own = lax.dynamic_slice_in_dim(small, gains.shape[0] + lax.axis_index("fsdp"), 1, axis=0)
    head_gains = own[0, : head_gains.size].reshape(head_gains.shape)
    return [s.reshape(g.shape) for s, g in zip(sums, narrow)], small[: gains.shape[0]], head_gains, rows, expert_grads, first


def on_device(
    block_input,
    cotangent,
    w_query,
    w_key,
    w_value,
    w_output,
    q_gain,
    k_gain,
    attn_gain,
    mlp_gain,
    w_router,
    w_gate,
    w_up,
    w_down,
    segments,
    routes,
    capacity,
):
    tok_count = block_input.shape[1]
    model_width = block_input.shape[2]
    experts = w_router.shape[1]
    nz = lax.axis_size("expert") // 2
    dense = 2 * TOP >= experts and lax.axis_size("fsdp") == 4
    flat_in = block_input[0].astype(jnp.float32)
    scale_one = lax.rsqrt(jnp.mean(flat_in * flat_in, axis=1, keepdims=True) + epsilon)
    normed_one = flat_in * scale_one
    first_rows = (normed_one * attn_gain).astype(jnp.bfloat16)
    if dense:
        group_rows, group_segs = square_gather(first_rows, jnp.tile(segments, (8, 1)), 1)
        group_rows = group_rows.reshape(-1, model_width)
        group_segs = group_segs[:, 0].reshape(-1)
    else:
        group_rows, group_segs = (
            lax.all_gather(first_rows, "fsdp", axis=0, tiled=True),
            lax.all_gather(segments[0], "fsdp", axis=0, tiled=True),
        )
    group_len = group_rows.shape[0]
    heads_here = w_query.shape[1] // HEAD_DIM
    query_rows = jnp.dot(group_rows, w_query, preferred_element_type=jnp.float32)
    key_rows = jnp.dot(group_rows, w_key, preferred_element_type=jnp.float32)
    value_rows = jnp.dot(group_rows, w_value, preferred_element_type=jnp.float32).astype(
        jnp.bfloat16
    )
    square_sums = across_heads(
        dense and 2,
        (jnp.sum(query_rows * query_rows, axis=1), jnp.sum(key_rows * key_rows, axis=1))
    )
    q_scale = lax.rsqrt(square_sums[0][:, None] / model_width + epsilon)
    k_scale = lax.rsqrt(square_sums[1][:, None] / model_width + epsilon)
    cosine, sine_table = rope_tables(group_segs, HEAD_DIM)
    head_shape = (group_len, heads_here, HEAD_DIM)
    q_heads = apply_rope(
        (query_rows * q_scale * q_gain).reshape(head_shape), cosine, sine_table
    ).astype(jnp.bfloat16)
    k_heads = apply_rope(
        (key_rows * k_scale * k_gain).reshape(head_shape), cosine, sine_table
    ).astype(jnp.bfloat16)
    v_heads = value_rows.reshape(head_shape)
    ordinal = lax.iota(jnp.int32, group_len)
    allowed = (group_segs[:, None] == group_segs[None, :]) & (ordinal[None, :] <= ordinal[:, None])
    scores = head_scores(q_heads, k_heads, allowed)
    row_top = jnp.max(scores, axis=2, keepdims=True)
    log_total = row_top + jnp.log(jnp.sum(jnp.exp(scores - row_top), axis=2, keepdims=True))
    attn_weights = jnp.exp(scores - log_total)
    mixed_heads = jnp.einsum(
        "hts,shd->thd",
        attn_weights.astype(jnp.bfloat16),
        v_heads,
        preferred_element_type=jnp.float32,
    )
    attn_rows = mixed_heads.reshape(group_len, heads_here * HEAD_DIM).astype(jnp.bfloat16)

    def mixed_term(start, length):
        return jnp.dot(attn_rows, w_output, preferred_element_type=jnp.float32).astype(jnp.bfloat16)

    mixed_rows = share_rows(mixed_term, tok_count, dense and 4).astype(jnp.float32)
    second_in = flat_in + mixed_rows
    scale_two = lax.rsqrt(jnp.mean(second_in * second_in, axis=1, keepdims=True) + epsilon)
    normed_two = second_in * scale_two
    second_rows = (normed_two * mlp_gain).astype(jnp.bfloat16)
    if dense:
        block_output, grad_second, router_grad, expert_grads = experts_dense(
            second_in, second_rows, cotangent[0], routes[0], capacity, w_router, w_gate, w_up, w_down
        )
    else:
        block_output, grad_second, router_grad, expert_grads = experts_by_slot(
            second_in, second_rows, cotangent[0], routes[0], capacity, w_router, w_gate, w_up, w_down
        )
    grad_out = cotangent[0].astype(jnp.float32)
    mlp_gain_grad = jnp.sum(grad_second * normed_two, axis=0)
    grad_normed_two = grad_second * mlp_gain
    grad_mid = grad_out + scale_two * (
        grad_normed_two - normed_two * jnp.mean(grad_normed_two * normed_two, axis=1, keepdims=True)
    )
    if dense:
        group_grad, _ = square_gather(grad_mid.astype(jnp.bfloat16), jnp.tile(segments, (8, 1)), 6)
        group_grad = group_grad.reshape(-1, model_width)
    else:
        group_grad = lax.all_gather(grad_mid.astype(jnp.bfloat16), "fsdp", axis=0, tiled=True)
    out_grad = jnp.einsum("ti,td->id", attn_rows, group_grad, preferred_element_type=jnp.float32)
    grad_attn = (
        jnp.einsum("td,id->ti", group_grad, w_output, preferred_element_type=jnp.float32)
        .astype(jnp.bfloat16)
        .reshape(head_shape)
    )
    scores_again = head_scores(q_heads, k_heads, allowed)
    weights_again = jnp.exp(scores_again - log_total)
    grad_values = jnp.einsum(
        "hts,thd->shd",
        weights_again.astype(jnp.bfloat16),
        grad_attn,
        preferred_element_type=jnp.float32,
    )
    grad_weights = jnp.einsum(
        "thd,shd->hts", grad_attn, v_heads, preferred_element_type=jnp.float32
    )
    inner_sum = jnp.sum(weights_again * grad_weights, axis=2, keepdims=True)
    grad_scores = (weights_again * (grad_weights - inner_sum)).astype(jnp.bfloat16)
    grad_q_heads = jnp.einsum(
        "hts,shd->thd", grad_scores, k_heads, preferred_element_type=jnp.float32
    ) * HEAD_DIM ** (-0.5)
    grad_k_heads = jnp.einsum(
        "hts,thd->shd", grad_scores, q_heads, preferred_element_type=jnp.float32
    ) * HEAD_DIM ** (-0.5)
    grad_q_normed = rope_grad(grad_q_heads, cosine, sine_table).reshape(group_len, -1)
    grad_k_normed = rope_grad(grad_k_heads, cosine, sine_table).reshape(group_len, -1)
    q_gain_grad = jnp.sum(grad_q_normed * query_rows * q_scale, axis=0)
    k_gain_grad = jnp.sum(grad_k_normed * key_rows * k_scale, axis=0)
    inner_q = grad_q_normed * q_gain
    inner_k = grad_k_normed * k_gain
    inner_sums = across_heads(
        dense and 3,
        (jnp.sum(inner_q * query_rows, axis=1), jnp.sum(inner_k * key_rows, axis=1))
    )
    grad_query_rows = (
        q_scale
        * (inner_q - query_rows * q_scale * q_scale * (inner_sums[0][:, None] / model_width))
    ).astype(jnp.bfloat16)
    grad_key_rows = (
        k_scale * (inner_k - key_rows * k_scale * k_scale * (inner_sums[1][:, None] / model_width))
    ).astype(jnp.bfloat16)
    grad_value_rows = grad_values.reshape(group_len, -1).astype(jnp.bfloat16)
    head_grads = jnp.concatenate([grad_query_rows, grad_key_rows, grad_value_rows], axis=1)
    mixer_grad = jnp.einsum(
        "td,ti->di", group_rows, head_grads, preferred_element_type=jnp.float32
    ).astype(jnp.bfloat16)

    def input_term(start, length):
        from_q = jnp.einsum(
            "ti,di->td", grad_query_rows, w_query, preferred_element_type=jnp.float32
        )
        from_k = jnp.einsum("ti,di->td", grad_key_rows, w_key, preferred_element_type=jnp.float32)
        from_v = jnp.einsum(
            "ti,di->td", grad_value_rows, w_value, preferred_element_type=jnp.float32
        )
        return (from_q + from_k + from_v).astype(jnp.bfloat16)

    if dense:
        attn_gain_grad = jnp.zeros_like(mlp_gain_grad)
    else:
        grad_first = share_rows(input_term, tok_count).astype(jnp.float32)
        attn_gain_grad = jnp.sum(grad_first * normed_one, axis=0)
    narrow = (mixer_grad, out_grad.astype(jnp.bfloat16))
    gains = jnp.concatenate([attn_gain_grad[None], mlp_gain_grad[None], router_grad], axis=0)
    head_gains = jnp.stack([q_gain_grad, k_gain_grad])
    if dense:
        first = input_term(jnp.int32(0), group_len)
        narrow, gains, head_gains, forward, expert_grads, grad_first = sum_grads(
            narrow, gains, head_gains, block_output, expert_grads, first, normed_one, w_gate.shape[0], nz
        )
        block_output = (second_in + forward).astype(jnp.bfloat16)[None]
    else:
        narrow = lax.psum(narrow, "expert")
        head_gains = lax.psum(head_gains, "expert")
        gains = lax.psum(gains, ("fsdp", "expert"))
    grad_normed_one = grad_first * attn_gain
    grad_x = grad_mid + scale_one * (
        grad_normed_one - normed_one * jnp.mean(grad_normed_one * normed_one, axis=1, keepdims=True)
    )
    wide = tuple(jnp.split(narrow[0], 3, axis=1)) + (narrow[1],)
    mixer = tuple(g.astype(jnp.float32) for g in wide) + (head_gains[0], head_gains[1])
    return (
        block_output,
        grad_x[None],
        mixer[0],
        mixer[1],
        mixer[2],
        mixer[3],
        mixer[4],
        mixer[5],
        gains[0],
        gains[1],
        gains[2:].T,
        *expert_grads,
    )


def solution(mesh):
    placed = (
        P("expert", "fsdp", None),
        P("expert", "fsdp", None),
        P(None, "fsdp"),
        P(None, "fsdp"),
        P(None, "fsdp"),
        P("fsdp", None),
        P("fsdp"),
        P("fsdp"),
        P(),
        P(),
        P(),
        P("expert", None, "fsdp"),
        P("expert", None, "fsdp"),
        P("expert", "fsdp", None),
        P("expert", "fsdp"),
        P("expert", "fsdp", None),
        P(),
    )
    return jax.shard_map(
        on_device,
        mesh=mesh,
        in_specs=placed,
        out_specs=(
            P("expert", "fsdp", None),
            P("expert", "fsdp", None),
            P(None, "fsdp"),
            P(None, "fsdp"),
            P(None, "fsdp"),
            P("fsdp", None),
            P("fsdp"),
            P("fsdp"),
            P(),
            P(),
            P(),
            P("expert", None, "fsdp"),
            P("expert", None, "fsdp"),
            P("expert", "fsdp", None),
        ),
        check_vma=False,
    )
```

```python
import functools

import jax
import jax.numpy as jnp
from jax import lax
from jax.experimental import pallas as pl
from jax.experimental.pallas import tpu as pltpu
from jax.sharding import PartitionSpec as P

HEAD_DIM = 128
TOP = 8


epsilon = 1e-05
rope_base = 10000.0
precise = lax.Precision.HIGHEST


MESH = pl.DeviceIdType.MESH
DMA = pltpu.SemaphoreType.DMA


class Place:
    def __init__(self):
        self.f, self.e = lax.axis_index("fsdp"), lax.axis_index("expert")
        self.c, self.z = self.e % 2, self.e // 2
        self.fx = self.f + 1 - 2 * (self.f % 2)
        self.fy = (self.f + 2) % 4
        self.fd = 3 - self.f
        self.pe = self.e + 1 - 2 * self.c


def send(src, dst, send_sem, recv_sem, f, e):
    return pltpu.make_async_remote_copy(
        src_ref=src,
        dst_ref=dst,
        send_sem=send_sem,
        recv_sem=recv_sem,
        device_id={"fsdp": f, "expert": e},
        device_id_type=MESH,
    )


def greet(peers, line=None):
    barrier = pltpu.get_barrier_semaphore()

    def hello(f, e):
        pl.semaphore_signal(
            barrier, inc=1, device_id={"fsdp": f, "expert": e}, device_id_type=MESH
        )

    for f, e in peers:
        hello(f, e)
    if line is not None:
        at, nz = line
        for step in range(1, nz):
            hello(at.f, 2 * ((at.z + step) % nz) + at.c)
        pl.semaphore_wait(barrier, len(peers) + nz - 1)
    else:
        pl.semaphore_wait(barrier, len(peers))


class SmallGather:
    sems = staticmethod(
        lambda nz: [DMA((nz,)), DMA((nz,)), DMA((4,)), DMA((4,))]
    )

    def __init__(self, at, nz, own, out, sems):
        self.at, self.nz, self.own, self.out = at, nz, own, out
        self.ls, self.lr, self.ss, self.sr = sems

    def line(self, step):
        at = self.at
        z = (at.z + step) % self.nz
        back = (at.z + self.nz - step) % self.nz
        slot = self.out.at[at.c, at.f]
        to = send(self.own, slot.at[at.z], self.ls.at[step], self.lr.at[step], at.f, 2 * z + at.c)
        come = send(self.own, slot.at[back], self.ls.at[step], self.lr.at[step], at.f, 2 * z + at.c)
        return to, come

    def plane(self, i):
        at, out = self.at, self.out
        f, to_f = ((at.f, at.fx), (at.f, at.fy), (at.fx, at.fy))[i]
        slot = out.at[at.c, f]
        return send(slot, slot, self.ss.at[i], self.sr.at[i], to_f, at.e)

    def pair(self):
        at = self.at
        slot = self.out.at[at.c]
        return send(slot, slot, self.ss.at[3], self.sr.at[3], at.f, at.pe)

    def stage(self, i):
        at = self.at
        if i == 0:
            for step in range(1, self.nz):
                self.line(step)[0].start()
            self.out[at.c, at.f, at.z] = self.own[...]
        elif i == 1:
            for step in range(1, self.nz):
                self.line(step)[1].wait_recv()
            self.plane(0).start()
            self.plane(1).start()
        elif i == 2:
            self.plane(0).wait_recv()
            self.plane(2).start()
        elif i == 3:
            self.plane(1).wait_recv()
            self.plane(2).wait_recv()
            self.pair().start()
        elif i == 4:
            self.pair().wait_recv()
            self.pair().wait_send()
            for step in range(1, self.nz):
                self.line(step)[0].wait_send()
            for k in range(3):
                self.plane(k).wait_send()


class SmallScatter:
    sems = staticmethod(lambda nz: [DMA((nz,)), DMA((nz,)), DMA((4,)), DMA((4,))])
    scratch = staticmethod(
        lambda nz, shape: [
            pltpu.VMEM((4, nz, *shape), jnp.float32),
            pltpu.VMEM((4, nz, *shape), jnp.float32),
            pltpu.VMEM((3, nz, *shape), jnp.float32),
            pltpu.VMEM((nz, *shape), jnp.float32),
        ]
    )

    def __init__(self, at, nz, part, out, scratch, sems):
        self.at, self.nz, self.part, self.out = at, nz, part, out
        self.acc, self.pb, self.xy, self.zb = scratch
        self.ls, self.lr, self.ss, self.sr = sems

    def pair(self):
        at = self.at
        return send(
            self.part.at[1 - at.c], self.pb, self.ss.at[0], self.sr.at[0], at.f, at.pe
        )

    def plane(self, i):
        at = self.at
        f, to_f = ((at.fx, at.fx), (at.fd, at.fx), (at.fy, at.fy))[i]
        return send(
            self.acc.at[f], self.xy.at[i], self.ss.at[1 + i], self.sr.at[1 + i], to_f, at.e
        )

    def line(self, step):
        at = self.at
        z = (at.z + step) % self.nz
        return send(
            self.acc.at[at.f, z], self.zb.at[step], self.ls.at[step], self.lr.at[step], at.f, 2 * z + at.c
        )

    def stage(self, i):
        at, acc, xy = self.at, self.acc, self.xy
        if i == 0:
            self.pair().start()
        elif i == 1:
            self.pair().wait_recv()
            acc[...] = self.part[at.c] + self.pb[...]
            self.plane(0).start()
            self.plane(1).start()
        elif i == 2:
            self.plane(0).wait_recv()
            self.plane(1).wait_recv()
            acc[at.fy] = acc[at.fy] + xy[1]
            self.plane(2).start()
            acc[at.f] = acc[at.f] + xy[0]
        elif i == 3:
            self.plane(2).wait_recv()
            acc[at.f] = acc[at.f] + xy[2]
            for step in range(1, self.nz):
                self.line(step).start()
        elif i == 4:
            total = acc[at.f, at.z]
            for step in range(1, self.nz):
                self.line(step).wait_recv()
                total = total + self.zb[step]
            self.out[...] = total
            self.pair().wait_send()
            for k in range(3):
                self.plane(k).wait_send()
            for step in range(1, self.nz):
                self.line(step).wait_send()


def take(sequence, count):
    return [next(sequence) for _ in range(count)]


NT = (((1,), (1,)), ((), ()))
TN = (((0,), (0,)), ((), ()))


def halves_of(x):
    high = x.astype(jnp.bfloat16)
    return high, (x - high.astype(jnp.float32)).astype(jnp.bfloat16)


def spread(blocks, first, hidden, wide):
    experts = blocks[0].shape[0]
    high, low = halves_of(jnp.concatenate(blocks, axis=1))
    row = lax.broadcasted_iota(jnp.int32, (2 * experts, wide), 0) % experts
    col = lax.broadcasted_iota(jnp.int32, (2 * experts, wide), 1) // hidden
    pick = (row == first + col).astype(jnp.float32).astype(jnp.bfloat16)
    both = jnp.concatenate([high.astype(jnp.float32), low.astype(jnp.float32)], axis=0)
    return lax.dot_general(
        both.astype(jnp.bfloat16), pick, TN, preferred_element_type=jnp.float32
    )


def above(a, b):
    return (a - b + 63) // 64


def near_first(at, nz, s):
    right = above(2 * at.z, nz - 1)
    alternate = at.z - right * (2 * at.z - (nz - 1))
    turn = at.z + (s + 1) // 2 * (1 - 2 * (s % 2))
    rest = s + right * (nz - 1 - 2 * s)
    return turn + above(s, 2 * alternate) * (rest - turn)


def gather_act_kernel(nz, own, own_small, w_gate, w_up, w_down, out, acts, weighted, forward, gates, xb, ab, hb, fb, load_x, store, own_sem, zr, zs, xr, xs, yr, ys, dr, xf, yf, pr, ps, *small_sems):
    at = Place()
    rows, width = own.shape
    local, _, hidden = w_gate.shape
    half = rows // 2
    halves = (pl.ds(0, half), pl.ds(half, half))
    small = SmallGather(at, nz, own_small, gates, small_sems)
    greet([(at.fx, at.e), (at.fy, at.e), (at.f, at.pe)], (at, nz))
    keep = pltpu.make_async_copy(own, out.at[at.f, at.e], own_sem)
    keep.start()
    small.stage(0)
    places = (at.f, at.fx, at.fy, at.fd)
    first = at.e * w_gate.shape[0]

    def up(z):
        ref = out.at[at.f, 2 * z + at.c]
        return send(ref, ref, zs.at[0, z], zr.at[z], at.f, at.e + 2)

    def down(z):
        ref = out.at[at.f, 2 * z + at.c]
        return send(ref, ref, zs.at[1, z], zr.at[z], at.f, at.e - 2)

    def to_x(z, h):
        ref = out.at[at.f, 2 * z + at.c, halves[h]]
        return send(ref, ref, xs.at[h, z], xr.at[h, z], at.fx, at.e)

    def to_y(z, h):
        ref = out.at[at.f, 2 * z + at.c, halves[h]]
        return send(ref, ref, ys.at[h, z], yr.at[h, z], at.fy, at.e)

    def x_on(z):
        ref = out.at[at.fx, 2 * z + at.c, halves[0]]
        return send(ref, ref, yf.at[z], dr.at[0, z], at.fy, at.e)

    def y_on(z):
        ref = out.at[at.fy, 2 * z + at.c, halves[1]]
        return send(ref, ref, xf.at[z], dr.at[1, z], at.fx, at.e)

    def to_p(f, z, h):
        ref = out.at[f, 2 * z + at.c, halves[h]]
        return send(ref, ref, ps.at[f, z, h], pr.at[f, z, h], at.f, at.pe)

    def line_step(z):
        pl.when(z != at.z)(lambda: up(z).wait_recv())
        pl.when((z <= at.z) & (at.z < nz - 1))(lambda: up(z).start())
        pl.when((z >= at.z) & (at.z > 0))(lambda: down(z).start())
        to_x(z, 0).start()
        to_y(z, 1).start()
        to_x(z, 1).start()
        to_y(z, 0).start()
        for h in range(2):
            to_p(at.f, z, h).start()

    def plane_step(z):
        to_x(z, 0).wait_recv()
        x_on(z).start()
        to_y(z, 1).wait_recv()
        y_on(z).start()
        to_p(at.fx, z, 0).start()
        to_p(at.fy, z, 1).start()
        to_x(z, 1).wait_recv()
        to_p(at.fx, z, 1).start()
        to_y(z, 0).wait_recv()
        to_p(at.fy, z, 0).start()

    def diag_step(z):
        x_on(z).wait_recv()
        to_p(at.fd, z, 0).start()
        y_on(z).wait_recv()
        to_p(at.fd, z, 1).start()

    def load(q, z):
        return pltpu.make_async_copy(out.at[places[q], pl.ds(2 * z, 2)], xb.at[q], load_x.at[q])

    def stores(q, z):
        pair, f = pl.ds(2 * z, 2), places[q]
        return [
            *(
                pltpu.make_async_copy(ab.at[q, k], acts.at[k, f, pair], store.at[q, k])
                for k in range(3)
            ),
            pltpu.make_async_copy(hb.at[q], weighted.at[f, pair], store.at[q, 3]),
            pltpu.make_async_copy(fb.at[q], forward.at[f, pair], store.at[q, 4]),
        ]

    def fetch(q, z):
        for h in range(2):
            to_p(places[q], z, h).wait_recv()
        load(q, z).start()

    def work(q, z):
        load(q, z).wait()
        f = places[q]
        x = xb[q].reshape(2 * rows, width)
        gate_all = spread([gates[0, f, z], gates[1, f, z]], first, hidden, local * hidden)
        for j in range(local):
            cols = pl.ds(j * hidden, hidden)
            g_all = jnp.dot(x, w_gate[j], preferred_element_type=jnp.float32)
            u_all = jnp.dot(x, w_up[j], preferred_element_type=jnp.float32)
            for h in range(2):
                g, u = g_all[h * rows : (h + 1) * rows], u_all[h * rows : (h + 1) * rows]
                gate = gate_all[h * rows : (h + 1) * rows, j * hidden : (j + 1) * hidden]
                sig = 1.0 / (1.0 + jnp.exp(-g))
                silu = g * sig
                hid = silu * u
                ab[q, 0, h, :, cols] = u * sig * (1.0 + g * (1.0 - sig))
                ab[q, 1, h, :, cols] = silu
                ab[q, 2, h, :, cols] = hid
                hb[q, h, :, cols] = (hid * gate).astype(jnp.bfloat16)
        a = hb[q].reshape(2 * rows, local * hidden)

        def body(t, carry):
            cols = pl.ds(pl.multiple_of(t * 512, 512), 512)
            total = jnp.dot(a, w_down[:, cols], preferred_element_type=jnp.float32)
            fb[q, :, :, cols] = total.astype(jnp.bfloat16).reshape(2, rows, 512)
            return carry

        lax.fori_loop(0, width // 512, body, 0)
        for copy in stores(q, z):
            copy.start()

    keep.wait()

    def body(s, carry):
        def at_step(lag, run):
            pl.when((s >= lag) & (s < nz + lag))(lambda: run(near_first(at, nz, s - lag)))

        def free(q, lag):
            def run(z):
                for copy in stores(q, z):
                    copy.wait()

            at_step(lag + 1, run)

        at_step(0, line_step)
        for k in range(1, 5):
            pl.when(s == 0)(functools.partial(small.stage, k))
        at_step(1, lambda z: fetch(0, z))
        free(3, 4)
        at_step(4, lambda z: work(3, z))
        at_step(1, plane_step)
        at_step(2, lambda z: fetch(1, z))
        free(0, 1)
        at_step(1, lambda z: work(0, z))
        at_step(2, diag_step)
        at_step(2, lambda z: fetch(2, z))
        free(1, 2)
        at_step(2, lambda z: work(1, z))
        at_step(3, lambda z: fetch(3, z))
        free(2, 2)
        at_step(2, lambda z: work(2, z))
        return carry

    lax.fori_loop(0, nz + 5, body, 0)

    def finish(z, carry):
        pl.when((z <= at.z) & (at.z < nz - 1))(lambda: up(z).wait_send())
        pl.when((z >= at.z) & (at.z > 0))(lambda: down(z).wait_send())
        for h in range(2):
            to_x(z, h).wait_send()
            to_y(z, h).wait_send()
        x_on(z).wait_send()
        y_on(z).wait_send()
        for f in range(4):
            for h in range(2):
                to_p(f, z, h).wait_send()
        return carry

    lax.fori_loop(0, nz, finish, 0)


def gather_act(rows, small, w_gate, w_up, w_down, nz, cid):
    r, c = rows.shape
    local, _, hidden = w_gate.shape
    wide = local * hidden
    hbm, vmem = pl.BlockSpec(memory_space=pl.ANY), pl.BlockSpec(memory_space=pltpu.VMEM)
    bf16 = jnp.bfloat16
    return pl.pallas_call(
        functools.partial(gather_act_kernel, nz),
        out_shape=(
            jax.ShapeDtypeStruct((4, 2 * nz, r, c), bf16),
            jax.ShapeDtypeStruct((3, 4, 2 * nz, r, wide), jnp.float32),
            jax.ShapeDtypeStruct((4, 2 * nz, r, wide), bf16),
            jax.ShapeDtypeStruct((4, 2 * nz, r, c), bf16),
            jax.ShapeDtypeStruct((2, 4, nz, *small.shape), jnp.float32),
        ),
        in_specs=[vmem] * 5,
        out_specs=(hbm, hbm, hbm, hbm, vmem),
        scratch_shapes=[
            pltpu.VMEM((4, 2, r, c), bf16),
            pltpu.VMEM((4, 3, 2, r, wide), jnp.float32),
            pltpu.VMEM((4, 2, r, wide), bf16),
            pltpu.VMEM((4, 2, r, c), bf16),
            DMA((4,)), DMA((4, 5)),
            DMA(()), DMA((nz,)), DMA((2, nz)), DMA((2, nz)), DMA((2, nz)), DMA((2, nz)), DMA((2, nz)),
            DMA((2, nz)), DMA((nz,)), DMA((nz,)), DMA((4, nz, 2)), DMA((4, nz, 2)),
            *SmallGather.sems(nz),
        ],
        compiler_params=pltpu.CompilerParams(
            collective_id=cid, has_side_effects=True, vmem_limit_bytes=50 << 20
        ),
        cost_estimate=pl.CostEstimate(flops=0, bytes_accessed=240 << 20, transcendentals=0),
        name="gather_act",
    )(rows, small, w_gate, w_up, w_down.reshape(wide, c))


def add_rows(dst, dst_rows, parts):
    start, count = dst_rows

    def body(i, carry):
        r = pl.multiple_of(i * 16, 16)
        total = None
        for ref, offset in parts:
            piece = ref[pl.ds(offset + r, 16), :].astype(jnp.float32)
            total = piece if total is None else total + piece
        dst[pl.ds(start + r, 16), :] = total.astype(dst.dtype)
        return carry

    lax.fori_loop(0, count // 16, body, 0)


def scatter_plan(at, nz, part, out, refs, staged=None, split=1):
    acc, pb, xh, yh, xf, yf, zu, zd, ls, pr, ps, xhs, xhr, yhs, yhr, xs, xr, ys, yr, us, ur, ds_, dr = refs
    rows = out.shape[0]
    half = rows // 2
    lo, hi = pl.ds(0, half), pl.ds(half, half)

    def place(s):
        return near_first(at, nz, nz - 1 - s)

    def load(f, z):
        return pltpu.make_async_copy(part.at[f, 2 * z + at.c], acc.at[f, z], ls.at[f, z])

    fs = (at.fd, at.fx, at.fy, at.f)

    def to_p(q, z):
        f = fs[q]
        src = staged.at[q] if staged is not None else part.at[f, 2 * z + 1 - at.c]
        return send(src, pb.at[f, z], ps.at[f, z], pr.at[f, z], at.f, at.pe)

    def ready(q, z):
        if staged is None:
            load(fs[q], z).wait()
        to_p(q, z).wait_recv()

    def start_step(s):
        z = place(s)
        for q in range(4):
            load(fs[q], z).start()
            to_p(q, z).start()

    def half_x(z):
        return send(acc.at[at.fd, z, lo], xh.at[z], xhs.at[z], xhr.at[z], at.fx, at.e)

    def half_y(z):
        return send(acc.at[at.fd, z, hi], yh.at[z], yhs.at[z], yhr.at[z], at.fy, at.e)

    def full_x(z):
        return send(acc.at[at.fx, z], xf.at[z], xs.at[z], xr.at[z], at.fx, at.e)

    def full_y(z):
        return send(acc.at[at.fy, z], yf.at[z], ys.at[z], yr.at[z], at.fy, at.e)

    count = rows // split

    def go_up(z, k):
        cut = pl.ds(k * count, count)
        return send(acc.at[at.f, z, cut], zu.at[z, cut], us.at[z, k], ur.at[z, k], at.f, at.e + 2)

    def go_down(z, k):
        cut = pl.ds(k * count, count)
        return send(acc.at[at.f, z, cut], zd.at[z, cut], ds_.at[z, k], dr.at[z, k], at.f, at.e - 2)

    def diag_step(s):
        z = place(s)
        ready(0, z)
        a, b = acc.at[at.fd, z], pb.at[at.fd, z]
        add_rows(a, (0, half), [(a, 0), (b, 0)])
        half_x(z).start()
        add_rows(a, (half, half), [(a, half), (b, half)])
        half_y(z).start()

    def plane_step(s):
        z = place(s)
        ready(1, z)
        a, b = acc.at[at.fx, z], pb.at[at.fx, z]
        half_y(z).wait_recv()
        add_rows(a, (0, half), [(a, 0), (b, 0)])
        add_rows(a, (half, half), [(a, half), (b, half), (yh.at[z], 0)])
        full_x(z).start()
        ready(2, z)
        half_x(z).wait_recv()
        a, b = acc.at[at.fy, z], pb.at[at.fy, z]
        add_rows(a, (0, half), [(a, 0), (b, 0), (xh.at[z], 0)])
        add_rows(a, (half, half), [(a, half), (b, half)])
        full_y(z).start()

    def line_step(s, k=0):
        z = place(s)
        if k == 0:
            ready(3, z)
            full_x(z).wait_recv()
            full_y(z).wait_recv()
        r = k * count
        a = acc.at[at.f, z]
        four = [(a, r), (pb.at[at.f, z], r), (xf.at[z], r), (yf.at[z], r)]

        @pl.when(z > at.z)
        def _():
            @pl.when(at.z > 0)
            def _():
                go_up(z, k).wait_recv()
                add_rows(a, (r, count), four + [(zu.at[z], r)])

            pl.when(at.z == 0)(lambda: add_rows(a, (r, count), four))
            go_up(z, k).start()

        @pl.when(z < at.z)
        def _():
            @pl.when(at.z < nz - 1)
            def _():
                go_down(z, k).wait_recv()
                add_rows(a, (r, count), four + [(zd.at[z], r)])

            pl.when(at.z == nz - 1)(lambda: add_rows(a, (r, count), four))
            go_down(z, k).start()

        @pl.when(z == at.z)
        def _():
            add_rows(out, (r, count), four)

            @pl.when(at.z > 0)
            def _():
                go_up(z, k).wait_recv()
                add_rows(out, (r, count), [(out, r), (zu.at[z], r)])

            @pl.when(at.z < nz - 1)
            def _():
                go_down(z, k).wait_recv()
                add_rows(out, (r, count), [(out, r), (zd.at[z], r)])

    def finish():
        def body(z, carry):
            for q in range(4):
                if staged is None:
                    to_p(q, z).wait_send()
            half_x(z).wait_send()
            half_y(z).wait_send()
            full_x(z).wait_send()
            full_y(z).wait_send()
            for k in range(split):
                pl.when(z > at.z)(functools.partial(lambda k: go_up(z, k).wait_send(), k))
                pl.when(z < at.z)(functools.partial(lambda k: go_down(z, k).wait_send(), k))
            return carry

        lax.fori_loop(0, nz, body, 0)
        for q in range(4):
            if staged is not None:
                to_p(q, place(nz - 1)).wait_send()

    return start_step, diag_step, plane_step, line_step, finish, place, to_p


def scatter_scratch(parts, nz):
    _, _, r, c = parts.shape

    def buf(*n):
        return pltpu.VMEM((*n, c), parts.dtype)

    return [
        buf(4, nz, r), buf(4, nz, r), buf(nz, r // 2), buf(nz, r // 2),
        buf(nz, r), buf(nz, r), buf(nz, r), buf(nz, r),
        DMA((4, nz)), DMA((4, nz)), DMA((4, nz)),
        *[DMA((nz,))] * 8,
        *[DMA((nz, 4))] * 4,
    ]


def scatter_act_kernel(nz, pre, grads, gates, w_gate, w_up, w_down, out, out_small, acts, *refs):
    at = Place()
    refs = iter(refs)
    moved = take(refs, 23)
    acc = moved[0]
    pb_, cb, ab, sb, terms, load_sem, store_sem = take(refs, 7)
    _, diag, plane, line, close, place, to_p = scatter_plan(at, nz, None, out, moved, sb)
    small = SmallScatter(at, nz, terms, out_small, take(refs, 4), take(refs, 4))
    greet([(at.fx, at.e), (at.fy, at.e), (at.f, at.pe)], (at, nz))
    rows, width = out.shape
    local, _, hidden = w_gate.shape
    experts = gates.shape[3]
    fs = (at.fd, at.fx, at.fy, at.f)
    cores = (at.c, 1 - at.c)
    first = at.e * local
    expert_row = lax.broadcasted_iota(jnp.int32, (experts, hidden), 0)
    tile = 512

    def loads(q, s):
        z, f = place(s), fs[q]
        copies = []
        for h, core in enumerate(cores):
            slot = 2 * z + core
            for k in range(3):
                copies.append(
                    pltpu.make_async_copy(pre.at[k, f, slot], pb_.at[q, k, h], load_sem.at[q, h, k])
                )
            copies.append(pltpu.make_async_copy(grads.at[f, slot], cb.at[q, h], load_sem.at[q, h, 3]))
        return copies

    def stores(q, s):
        z, f = place(s), fs[q]
        return [
            pltpu.make_async_copy(
                ab.at[q, k, h], acts.at[k, f, 2 * z + core], store_sem.at[q, h, k]
            )
            for h, core in enumerate(cores)
            for k in range(2)
        ]

    def act(q, s):
        z, f = place(s), fs[q]
        for copy in loads(q, s):
            copy.wait()

        @pl.when(s > 0)
        def _():
            for copy in stores(q, s - 1):
                copy.wait()

        c = cb[q].reshape(2 * rows, width)
        gate_all = spread([gates[core, f, z] for core in cores], first, hidden, local * hidden)
        sums = [None, None]
        for j in range(local):
            pick = (expert_row == first + j).astype(jnp.float32).astype(jnp.bfloat16)
            cols = pl.ds(j * hidden, hidden)
            dh = lax.dot_general(c, w_down[j], NT, preferred_element_type=jnp.float32)
            for h, core in enumerate(cores):
                d = dh[h * rows : (h + 1) * rows]
                gate = gate_all[h * rows : (h + 1) * rows, j * hidden : (j + 1) * hidden]
                for part in halves_of(pb_[q, 2, h, :, cols] * d):
                    mine = lax.dot_general(pick, part, NT, preferred_element_type=jnp.float32)
                    sums[h] = mine if sums[h] is None else sums[h] + mine
                d = d * gate
                ab[q, 0, h, :, cols] = (d * pb_[q, 0, h, :, cols]).astype(jnp.bfloat16)
                ab[q, 1, h, :, cols] = (d * pb_[q, 1, h, :, cols]).astype(jnp.bfloat16)
        for h, core in enumerate(cores):
            terms[core, f, z] = sums[h]
        for copy in stores(q, s):
            copy.start()

        @pl.when(s + 1 < nz)
        def _():
            for copy in loads(q, s + 1):
                copy.start()

    def back(q, s):
        z, f = place(s), fs[q]
        pl.when(s > 0)(lambda: to_p(q, place(s - 1)).wait_send())
        pieces = [
            (ab[q, k].reshape(2 * rows, local * hidden)[:, j * hidden : (j + 1) * hidden], w.at[j])
            for j in range(local)
            for k, w in enumerate((w_gate, w_up))
        ]

        def body(t, carry):
            cols = pl.ds(pl.multiple_of(t * tile, tile), tile)
            total = None
            for a, w in pieces:
                term = lax.dot_general(a, w[cols, :], NT, preferred_element_type=jnp.float32)
                total = term if total is None else total + term
            total = total.astype(jnp.bfloat16)
            acc[f, z, :, cols] = total[:rows]
            sb[q, :, cols] = total[rows:]
            return carry

        lax.fori_loop(0, width // tile, body, 0)
        to_p(q, z).start()

    for q in range(4):
        for copy in loads(q, 0):
            copy.start()

    def body(s, carry):
        @pl.when(s < nz)
        def _():
            last = s == nz - 1
            for q in (0, 1):
                act(q, s)
                back(q, s)
            diag(s)
            act(2, s)
            back(2, s)
            act(3, s)
            pl.when(last)(lambda: small.stage(0))
            back(3, s)
            pl.when(last)(lambda: small.stage(1))
            plane(s)
            pl.when(last)(lambda: small.stage(2))

        pl.when(s == nz)(lambda: small.stage(3))
        pl.when(s >= 1)(lambda: line(s - 1))
        return carry

    lax.fori_loop(0, nz + 1, body, 0)
    small.stage(4)
    for q in range(4):
        for copy in stores(q, nz - 1):
            copy.wait()
    close()


def scatter_act(pre, grads, gates, w_gate, w_up, w_down, nz, cid):
    _, _, _, r, wide = pre.shape
    c = grads.shape[3]
    small = gates.shape[3:]
    hbm, vmem = pl.BlockSpec(memory_space=pl.ANY), pl.BlockSpec(memory_space=pltpu.VMEM)
    bf16 = jnp.bfloat16
    return pl.pallas_call(
        functools.partial(scatter_act_kernel, nz),
        out_shape=(
            jax.ShapeDtypeStruct((r, c), jnp.float32),
            jax.ShapeDtypeStruct(small, jnp.float32),
            jax.ShapeDtypeStruct((2, 4, 2 * nz, r, wide), bf16),
        ),
        in_specs=[hbm, hbm, vmem, vmem, vmem, vmem],
        out_specs=(vmem, vmem, hbm),
        scratch_shapes=[
            *scatter_scratch(grads, nz),
            pltpu.VMEM((4, 3, 2, r, wide), jnp.float32),
            pltpu.VMEM((4, 2, r, c), bf16),
            pltpu.VMEM((4, 2, 2, r, wide), bf16),
            pltpu.VMEM((4, r, c), bf16),
            pltpu.VMEM((2, 4, nz, *small), jnp.float32),
            DMA((4, 2, 4)), DMA((4, 2, 2)),
            *SmallScatter.scratch(nz, small),
            *SmallScatter.sems(nz),
        ],
        compiler_params=pltpu.CompilerParams(
            collective_id=cid, has_side_effects=True, vmem_limit_bytes=62 << 20
        ),
        cost_estimate=pl.CostEstimate(flops=0, bytes_accessed=300 << 20, transcendentals=0),
        name="scatter_act",
    )(pre, grads, gates, w_gate, w_up, w_down)


def square_gather_kernel(own, ids, out, out_ids, xs, xr, ys, yr, fs, fr, js, jr):
    at = Place()
    half = own.shape[0] // 2
    halves = (pl.ds(0, half), pl.ds(half, half))
    peers = [(at.fx, at.e), (at.fy, at.e), (at.fd, at.e)]
    greet(peers)

    def to_x(h):
        return send(own.at[halves[h]], out.at[at.f, halves[h]], xs.at[h], xr.at[h], at.fx, at.e)

    def to_y(h):
        return send(own.at[halves[h]], out.at[at.f, halves[h]], ys.at[h], yr.at[h], at.fy, at.e)

    x_ref, y_ref = out.at[at.fx, halves[0]], out.at[at.fy, halves[1]]
    x_on = send(x_ref, x_ref, fs.at[0], fr.at[0], at.fy, at.e)
    y_on = send(y_ref, y_ref, fs.at[1], fr.at[1], at.fx, at.e)
    notes = [
        send(ids, out_ids.at[at.f], js.at[k], jr.at[k], f, e) for k, (f, e) in enumerate(peers)
    ]
    to_x(0).start()
    to_y(1).start()
    for note in notes:
        note.start()
    to_x(1).start()
    to_y(0).start()
    out[at.f] = own[...]
    out_ids[at.f] = ids[...]
    to_x(0).wait_recv()
    x_on.start()
    to_y(1).wait_recv()
    y_on.start()
    to_x(1).wait()
    to_y(0).wait()
    for note in notes:
        note.wait()
    to_x(0).wait_send()
    to_y(1).wait_send()
    x_on.wait()
    y_on.wait()


def square_gather(rows, ids, cid):
    r, c = rows.shape
    vmem = pl.BlockSpec(memory_space=pltpu.VMEM)
    return pl.pallas_call(
        square_gather_kernel,
        out_shape=(
            jax.ShapeDtypeStruct((4, r, c), rows.dtype),
            jax.ShapeDtypeStruct((4, *ids.shape), ids.dtype),
        ),
        in_specs=[vmem] * 2,
        out_specs=(vmem,) * 2,
        scratch_shapes=[DMA((2,))] * 6 + [DMA((3,))] * 2,
        compiler_params=pltpu.CompilerParams(collective_id=cid, has_side_effects=True),
        cost_estimate=pl.CostEstimate(flops=0, bytes_accessed=60 << 20, transcendentals=0),
        name="square_gather",
    )(rows, ids)


def square_scatter_kernel(part, out, xh, yh, xf, yf, ss, rs):
    at = Place()
    rows = out.shape[0]
    half = rows // 2
    lo, hi = pl.ds(0, half), pl.ds(half, half)
    greet([(at.fx, at.e), (at.fy, at.e)])

    def to_x(k, src, dst):
        return send(src, dst, ss.at[k], rs.at[k], at.fx, at.e)

    def to_y(k, src, dst):
        return send(src, dst, ss.at[k], rs.at[k], at.fy, at.e)

    copies = [
        to_x(0, part.at[at.fd, lo], xh),
        to_y(1, part.at[at.fd, hi], yh),
        to_x(2, part.at[at.fx, lo], xf.at[lo]),
        to_y(3, part.at[at.fy, hi], yf.at[hi]),
        to_x(4, yh, xf.at[hi]),
        to_y(5, xh, yf.at[lo]),
    ]
    for copy in copies[:4]:
        copy.start()
    copies[1].wait_recv()
    add_rows(yh, (0, half), [(yh, 0), (part.at[at.fx], half)])
    copies[4].start()
    copies[0].wait_recv()
    add_rows(xh, (0, half), [(xh, 0), (part.at[at.fy], 0)])
    copies[5].start()
    copies[2].wait_recv()
    copies[5].wait_recv()
    copies[3].wait_recv()
    copies[4].wait_recv()
    add_rows(out, (0, rows), [(part.at[at.f], 0), (xf, 0), (yf, 0)])
    for copy in copies:
        copy.wait_send()


def square_scatter(parts, cid):
    _, r, c = parts.shape
    vmem = pl.BlockSpec(memory_space=pltpu.VMEM)

    def buf(n):
        return pltpu.VMEM((n, c), parts.dtype)

    return pl.pallas_call(
        square_scatter_kernel,
        out_shape=jax.ShapeDtypeStruct((r, c), jnp.float32),
        in_specs=[vmem],
        out_specs=vmem,
        scratch_shapes=[buf(r // 2), buf(r // 2), buf(r), buf(r), DMA((6,)), DMA((6,))],
        compiler_params=pltpu.CompilerParams(collective_id=cid, has_side_effects=True),
        cost_estimate=pl.CostEstimate(flops=0, bytes_accessed=60 << 20, transcendentals=0),
        name="square_scatter",
    )(parts)


def square_sum_kernel(own, out, got, ss, rs):
    at = Place()
    peers = [(at.fx, at.e), (at.fy, at.e), (at.fd, at.e)]
    greet(peers)
    copies = [send(own, got.at[k], ss.at[k], rs.at[k], f, e) for k, (f, e) in enumerate(peers)]
    for copy in copies:
        copy.start()
    for copy in copies:
        copy.wait()
    out[...] = (own[...] + got[0]) + (got[1] + got[2])


def square_sum(values, cid):
    flat = values.reshape(8, -1)
    vmem = pl.BlockSpec(memory_space=pltpu.VMEM)
    return pl.pallas_call(
        square_sum_kernel,
        out_shape=jax.ShapeDtypeStruct(flat.shape, jnp.float32),
        in_specs=[vmem],
        out_specs=vmem,
        scratch_shapes=[pltpu.VMEM((3, *flat.shape), jnp.float32), DMA((3,)), DMA((3,))],
        compiler_params=pltpu.CompilerParams(collective_id=cid, has_side_effects=True),
        cost_estimate=pl.CostEstimate(flops=0, bytes_accessed=10 << 20, transcendentals=0),
        name="square_sum",
    )(flat).reshape(values.shape)


class product_plan:
    def __init__(self, inputs, outs, refs):
        self.rows, self.acts, self.weighted, self.grads = inputs
        self.outs = outs
        self.acc, self.xw, self.aw, self.load_sem, self.store_sem = refs
        self.tile = self.acc.shape[2]
        self.units = self.rows.shape[0]
        self.local = self.outs[0].shape[0]
        self.per_pass = self.units // 2
        self.steps = self.per_pass * (self.local + 1)

    def loads(self, i, k, p):
        u = (i - p * self.per_pass) * 2 + k
        hidden = self.outs[0].shape[2]
        sem = self.load_sem.at[k]
        if p == self.local:
            return [
                pltpu.make_async_copy(self.grads.at[u], self.xw.at[k], sem.at[0]),
                pltpu.make_async_copy(self.weighted.at[u], self.aw.at[k], sem.at[1]),
            ]
        cols = pl.ds(p * hidden, hidden)
        return [
            pltpu.make_async_copy(self.rows.at[u], self.xw.at[k], sem.at[0]),
            pltpu.make_async_copy(self.acts.at[0, u, :, cols], self.aw.at[k, :, pl.ds(0, hidden)], sem.at[1]),
            pltpu.make_async_copy(
                self.acts.at[1, u, :, cols], self.aw.at[k, :, pl.ds(hidden, hidden)], sem.at[2]
            ),
        ]

    def on_pass(self, i, run):
        for p in range(self.local + 1):
            pl.when((i >= p * self.per_pass) & (i < (p + 1) * self.per_pass))(functools.partial(run, p))

    def start(self):
        for k in range(2):
            for copy in self.loads(0, k, 0):
                copy.start()

        for p in range(self.local):
            self.clear(p)

    def clear(self, p):
        def body(r, carry):
            self.acc[p, pl.ds(r * 8, 8), :] = jnp.zeros((8, self.tile), jnp.float32)
            return carry

        lax.fori_loop(0, self.acc.shape[1] // 8, body, 0)

    def step(self, i):
        tile = self.tile

        def run(p):
            if p == self.local:

                @pl.when(i == p * self.per_pass)
                def _():
                    for copy in self.stores(0):
                        copy.wait()
                    self.clear(0)

            for k in range(2):
                for copy in self.loads(i, k, p):
                    copy.wait()
                a = self.aw[k]
                for t in range(self.xw.shape[2] // tile):
                    cols = pl.ds(t * tile, tile)
                    x = self.xw[k, :, cols]
                    if p == self.local:
                        self.acc[0, cols, :] += lax.dot_general(
                            a, x, TN, preferred_element_type=jnp.float32
                        )
                    else:
                        self.acc[p, cols, :] += lax.dot_general(
                            x, a, TN, preferred_element_type=jnp.float32
                        )

                def more(q, k=k):
                    for copy in self.loads(i + 1, k, q):
                        copy.start()

                self.on_pass(i + 1, more)

            @pl.when(i == (p + 1) * self.per_pass - 1)
            def _():
                for copy in self.stores(p):
                    copy.start()

        self.on_pass(i, run)

    def stores(self, p):
        hidden = self.outs[0].shape[2]
        if p == self.local:
            cuts = [pl.ds(k * self.tile, self.tile) for k in range(self.outs[2].shape[1] // self.tile)]
            return [
                pltpu.make_async_copy(
                    self.acc.at[0, cut], self.outs[2].at[:, cut], self.store_sem.at[p, k]
                )
                for k, cut in enumerate(cuts)
            ]
        acc = self.acc.at[p]
        return [
            pltpu.make_async_copy(
                acc.at[:, pl.ds(k * hidden, hidden)], self.outs[k].at[p], self.store_sem.at[p, k]
            )
            for k in range(2)
        ]

    def finish(self):
        for p in range(1, self.local + 1):
            for copy in self.stores(p):
                copy.wait()


class SquareScatter:
    def __init__(self, at, part, normed, out, table, refs):
        self.part, self.normed, self.out, self.table = part, normed, out, table
        self.xh, self.yh, self.xf, self.yf, self.px, self.py, self.pf, ss, rs, ls = refs
        half = self.xh.shape[0]
        lo, hi = pl.ds(0, half), pl.ds(half, half)

        def to_x(k, src, dst):
            return send(src, dst, ss.at[k], rs.at[k], at.fx, at.e)

        def to_y(k, src, dst):
            return send(src, dst, ss.at[k], rs.at[k], at.fy, at.e)

        self.copies = [
            to_x(0, part.at[at.fd, lo], self.xh),
            to_y(1, part.at[at.fd, hi], self.yh),
            to_x(2, part.at[at.fx, lo], self.xf.at[lo]),
            to_y(3, part.at[at.fy, hi], self.yf.at[hi]),
            to_x(4, self.yh, self.xf.at[hi]),
            to_y(5, self.xh, self.yf.at[lo]),
        ]
        self.loads = [
            pltpu.make_async_copy(part.at[at.fx, hi], self.px, ls.at[0]),
            pltpu.make_async_copy(part.at[at.fy, lo], self.py, ls.at[1]),
            pltpu.make_async_copy(part.at[at.f], self.pf, ls.at[2]),
        ]

    def stage(self, i):
        copies, half, rows = self.copies, self.xh.shape[0], self.out.shape[0]
        if i == 0:
            for copy in copies[:4] + self.loads:
                copy.start()
        elif i == 1:
            for copy in self.loads:
                copy.wait()
            copies[1].wait_recv()
            add_rows(self.yh, (0, half), [(self.yh, 0), (self.px, 0)])
            copies[4].start()
            copies[0].wait_recv()
            add_rows(self.xh, (0, half), [(self.xh, 0), (self.py, 0)])
            copies[5].start()
        elif i == 2:
            for copy in copies[2:]:
                copy.wait_recv()
            add_rows(self.out, (0, rows), [(self.pf, 0), (self.xf, 0), (self.yf, 0)])

            def body(r, total):
                cut = pl.ds(pl.multiple_of(r * 16, 16), 16)
                both = self.out[cut, :] * self.normed[cut, :].astype(jnp.float32)
                return total + both[:8] + both[8:]

            total = lax.fori_loop(0, rows // 16, body, jnp.zeros((8, self.out.shape[1]), jnp.float32))
            total = jnp.sum(total, axis=0, keepdims=True)
            for k in range(self.table.shape[3]):
                self.table[0, 0, 0, k : k + 1, :] = total[:, k * 128 : (k + 1) * 128]
            for copy in copies:
                copy.wait_send()


def line_sum_kernel(nz, counts, *refs):
    at = Place()
    refs = iter(refs)
    n = len(counts)
    parts, table_in, rows_part, inputs = take(refs, n), next(refs), next(refs), take(refs, 4)
    first_part, normed = take(refs, 2)
    outs, out_small, rows_out, grads = take(refs, n), next(refs), next(refs), take(refs, 3)
    first_out, part_small = take(refs, 2)
    square = SquareScatter(at, first_part, normed, first_out, part_small, take(refs, 10))
    begin, diag, plane, line, close, _, _ = scatter_plan(
        at, nz, rows_part, rows_out, take(refs, 23), split=2
    )
    product = product_plan(inputs, grads, take(refs, 5))
    bufs = [take(refs, 5) for _ in range(n)]
    sems = [take(refs, 12) for _ in range(n)]
    own_small = next(refs)
    scatter_small = SmallScatter(at, nz, part_small, own_small, take(refs, 4), take(refs, 4))
    gather_small = SmallGather(at, nz, own_small, out_small, take(refs, 4))
    greet([(at.fx, at.e), (at.fy, at.e), (at.f, at.pe)], (at, nz))
    square.stage(0)
    part_small[...] = table_in[...]
    total = sum(counts)
    last = nz - 1
    lag, per = 1, 5

    class Piece:
        def __init__(self, k, p):
            self.p, self.part, self.out = p, parts[k], outs[k]
            self.acc, self.pb, self.zu, self.zd, self.mine = bufs[k]
            self.sems = sems[k]
            self.r = self.acc.shape[2]

        def load(self):
            p = self.p
            return pltpu.make_async_copy(self.part.at[p, at.c], self.acc.at[p], self.sems[0].at[p])

        def to_p(self):
            p, (_, s, r, *_rest) = self.p, self.sems
            return send(self.part.at[p, 1 - at.c], self.pb.at[p], s.at[p], r.at[p], at.f, at.pe)

        def go_up(self, z):
            p, s, r = self.p, self.sems[3], self.sems[4]
            return send(self.acc.at[p, z], self.zu.at[p, z], s.at[p, z], r.at[p, z], at.f, at.e + 2)

        def go_down(self, z):
            p, s, r = self.p, self.sems[5], self.sems[6]
            return send(self.acc.at[p, z], self.zd.at[p, z], s.at[p, z], r.at[p, z], at.f, at.e - 2)

        def res(self, z, way):
            p, s, r = self.p, self.sems[7], self.sems[8]
            ref = self.out.at[p, at.c, z]
            return send(ref, ref, s.at[way, p, z], r.at[p, z], at.f, at.e + 2 - 4 * way)

        def res_p(self, z):
            p, s, r = self.p, self.sems[9], self.sems[10]
            ref = self.out.at[p, at.c, z]
            return send(ref, ref, s.at[p, z], r.at[p, z], at.f, at.pe)

        def keep(self):
            p = self.p
            return pltpu.make_async_copy(self.mine.at[p], self.out.at[p, at.c, at.z], self.sems[11].at[p])

    def piece(q, run, when=True):
        low = 0
        for k, count in enumerate(counts):
            @pl.when((q >= low) & (q < low + count) & when)
            def _(k=k, low=low):
                run(Piece(k, q - low))

            low += count

    def start(it):
        it.load().start()
        it.to_p().start()

    piece(0, start)
    begin(0)
    piece(1, start)
    product.start()

    def halve(it):
        it.load().wait()
        it.to_p().wait_recv()
        p = it.p

        def body(z, carry):
            a = it.acc.at[p, z]
            add_rows(a, (0, it.r), [(a, 0), (it.pb.at[p, z], 0)])
            return carry

        lax.fori_loop(0, nz, body, 0)

    def rise(it):
        p = it.p

        def body(i, carry):
            z = last - i

            @pl.when(z > at.z)
            def _():
                a = it.acc.at[p, z]

                @pl.when(at.z > 0)
                def _():
                    it.go_up(z).wait_recv()
                    add_rows(a, (0, it.r), [(a, 0), (it.zu.at[p, z], 0)])

                it.go_up(z).start()

            return carry

        lax.fori_loop(0, last, body, 0)

    def sink(it):
        p = it.p

        def body(z, carry):
            @pl.when(z < at.z)
            def _():
                a = it.acc.at[p, z]

                @pl.when(at.z < last)
                def _():
                    it.go_down(z).wait_recv()
                    add_rows(a, (0, it.r), [(a, 0), (it.zd.at[p, z], 0)])

                it.go_down(z).start()

            return carry

        lax.fori_loop(0, last, body, 0)

    def settle(it):
        p, z = it.p, at.z
        pl.when(z > 0)(lambda: it.go_up(z).wait_recv())
        pl.when(z < last)(lambda: it.go_down(z).wait_recv())
        a, dst = (it.acc.at[p, z], 0), it.mine.at[p]
        up, down = (it.zu.at[p, z], 0), (it.zd.at[p, z], 0)
        pl.when((z > 0) & (z < last))(lambda: add_rows(dst, (0, it.r), [a, up, down]))
        pl.when(z == 0)(lambda: add_rows(dst, (0, it.r), [a, down]))
        pl.when(z == last)(lambda: add_rows(dst, (0, it.r), [a, up]))
        it.keep().start()

    def tell(it):
        z = at.z
        it.keep().wait()
        pl.when(z < last)(lambda: it.res(z, 0).start())
        pl.when(z > 0)(lambda: it.res(z, 1).start())
        it.res_p(z).start()

    def pass_up(it, z):
        it.res(z, 0).wait_recv()
        pl.when(at.z < last)(lambda: it.res(z, 0).start())
        it.res_p(z).start()

    def pass_down(it, z):
        it.res(z, 0).wait_recv()
        pl.when(at.z > 0)(lambda: it.res(z, 1).start())
        it.res_p(z).start()

    def body(i, carry):
        piece(i + 2, start)
        s, turn = i // per, i % per
        pl.when((turn == 0) & (s + 1 < nz))(lambda: begin(s + 1))
        pl.when((turn == 0) & (s < nz))(lambda: diag(s))
        pl.when((turn == 2) & (s < nz))(lambda: plane(s))
        pl.when((turn == 3) & (s >= 1) & (s < nz + 1))(lambda: line(s - 1, 0))
        pl.when((turn == 0) & (s >= 2) & (s < nz + 2))(lambda: line(s - 2, 1))
        piece(i, halve)
        piece(i - lag * at.z, rise, at.z < last)
        piece(i - lag * (last - at.z), sink, at.z > 0)
        piece(i - lag * nz, settle)
        piece(i - lag * nz, tell)
        for d in range(1, nz):
            piece(i - lag * (nz + d), functools.partial(pass_up, z=at.z - d), at.z >= d)
            piece(i - lag * (nz + d), functools.partial(pass_down, z=at.z + d), at.z + d <= last)
        for k, at_step in ((1, 1), (2, 5)):
            pl.when(i == at_step)(functools.partial(square.stage, k))
        for k in range(5):
            pl.when(i == 6 + k)(functools.partial(scatter_small.stage, k))
            pl.when(i == 11 + k)(functools.partial(gather_small.stage, k))
        product.step(i)
        return carry

    steps = max(total + lag * (2 * nz - 1), per * (nz + 2), product.steps)
    lax.fori_loop(0, steps, body, 0)
    product.finish()

    def finish(q, carry):
        def run(it):
            it.to_p().wait_send()

            def one(z, carry):
                pl.when(z > at.z)(lambda: it.go_up(z).wait_send())
                pl.when(z < at.z)(lambda: it.go_down(z).wait_send())
                pl.when((z <= at.z) & (at.z < last))(lambda: it.res(z, 0).wait_send())
                pl.when((z >= at.z) & (at.z > 0))(lambda: it.res(z, 1).wait_send())
                it.res_p(z).wait_send()
                it.res_p(z).wait_recv()
                return carry

            lax.fori_loop(0, nz, one, 0)

        piece(q, run)
        return carry

    lax.fori_loop(0, total, finish, 0)
    close()


def line_sum(parts, small, rows, inputs, first, normed, local, nz, cid):
    counts = tuple(p.shape[0] for p in parts)
    units, unit, width = inputs[0].shape
    wide = inputs[1].shape[3]
    scratch, sems = [], []
    for p in parts:
        n, _, _, r, c = p.shape

        def buf(*lead):
            return pltpu.VMEM((*lead, r, c), p.dtype)

        scratch += [buf(n, nz), buf(n, nz), buf(n, nz), buf(n, nz), buf(n)]
        each, line = DMA((n,)), DMA((n, nz))
        sems += [each, each, each, line, line, line, line, DMA((2, n, nz)), line, line, line, each]
    hbm, vmem = pl.BlockSpec(memory_space=pl.ANY), pl.BlockSpec(memory_space=pltpu.VMEM)
    _, r, c = first.shape
    bf16 = jnp.bfloat16
    assert small.shape[3] * small.shape[4] == c
    return pl.pallas_call(
        functools.partial(line_sum_kernel, nz, counts),
        out_shape=(
            *(jax.ShapeDtypeStruct(p.shape, p.dtype) for p in parts),
            jax.ShapeDtypeStruct(small.shape, jnp.float32),
            jax.ShapeDtypeStruct(rows.shape[2:], jnp.float32),
            jax.ShapeDtypeStruct((local, width, wide // local), jnp.float32),
            jax.ShapeDtypeStruct((local, width, wide // local), jnp.float32),
            jax.ShapeDtypeStruct((wide, width), jnp.float32),
            jax.ShapeDtypeStruct(first.shape[1:], jnp.float32),
        ),
        in_specs=[hbm] * len(parts) + [vmem, hbm] + [hbm] * len(inputs) + [hbm, vmem],
        out_specs=(*[hbm] * len(parts), vmem, vmem, *[hbm] * 3, vmem),
        scratch_shapes=[
            pltpu.VMEM(small.shape, jnp.float32),
            pltpu.VMEM((r // 2, c), bf16), pltpu.VMEM((r // 2, c), bf16),
            pltpu.VMEM((r, c), bf16), pltpu.VMEM((r, c), bf16),
            pltpu.VMEM((r // 2, c), bf16), pltpu.VMEM((r // 2, c), bf16), pltpu.VMEM((r, c), bf16),
            DMA((6,)), DMA((6,)), DMA((3,)),
            *scatter_scratch(rows, nz),
            pltpu.VMEM((local, width, 2 * wide // local), jnp.float32),
            pltpu.VMEM((2, unit, width), rows.dtype),
            pltpu.VMEM((2, unit, wide), rows.dtype),
            DMA((2, 3)), DMA((local + 1, 4)),
            *scratch, *sems, pltpu.VMEM(small.shape[-2:], jnp.float32),
            *SmallScatter.scratch(nz, small.shape[-2:]), *SmallScatter.sems(nz), *SmallGather.sems(nz),
        ],
        compiler_params=pltpu.CompilerParams(
            collective_id=cid, has_side_effects=True, vmem_limit_bytes=63 << 20
        ),
        cost_estimate=pl.CostEstimate(flops=0, bytes_accessed=300 << 20, transcendentals=0),
        name="line_sum",
    )(*parts, small, rows, *inputs, first, normed)


def rope_tables(seg_ids, head_dim):
    length = seg_ids.shape[0]
    ordinal = lax.iota(jnp.int32, length)
    earlier = (seg_ids[:, None] == seg_ids[None, :]) & (ordinal[None, :] < ordinal[:, None])
    places = jnp.sum(earlier.astype(jnp.int32), axis=1).astype(jnp.float32)
    half_dim = head_dim // 2
    inv_freq = rope_base ** (
        -(lax.iota(jnp.int32, half_dim).astype(jnp.float32) * (2.0 / head_dim))
    )
    angles = places[:, None] * inv_freq[None, :]
    angles = jnp.concatenate([angles, angles], axis=1)
    return (jnp.cos(angles), jnp.sin(angles))


def rotate_half(values):
    half_dim = values.shape[-1] // 2
    return jnp.concatenate([-values[..., half_dim:], values[..., :half_dim]], axis=-1)


def rotate_back(values):
    half_dim = values.shape[-1] // 2
    return jnp.concatenate([values[..., half_dim:], -values[..., :half_dim]], axis=-1)


def apply_rope(values, cosine, sine_table):
    return values * cosine[:, None, :] + rotate_half(values) * sine_table[:, None, :]


def rope_grad(grads_in, cosine, sine_table):
    return grads_in * cosine[:, None, :] + rotate_back(grads_in * sine_table[:, None, :])


def across_heads(kernel, pair_sums):
    if kernel:
        return square_sum(jnp.stack(pair_sums), kernel)
    return lax.psum((pair_sums[0], pair_sums[1]), "fsdp")


def share_rows(term_fn, own_rows, kernel=0):
    if kernel:
        parts = term_fn(jnp.int32(0), own_rows * lax.axis_size("fsdp"))
        return square_scatter(parts.reshape(-1, own_rows, parts.shape[1]), kernel)
    return lax.psum_scatter(
        term_fn(jnp.int32(0), own_rows * lax.axis_size("fsdp")),
        "fsdp",
        scatter_dimension=0,
        tiled=True,
    )


def to_owner(block_rows):
    return lax.all_to_all(block_rows, "expert", split_axis=0, concat_axis=0, tiled=True)


def from_owner(block_rows):
    return lax.all_to_all(block_rows, "expert", split_axis=0, concat_axis=0, tiled=True)


def shard_gather(block_rows):
    return lax.all_gather(block_rows, "fsdp", axis=0, tiled=True)


def owner_sum(term_fn, sources):
    own_rows = sources // lax.axis_size("fsdp")
    return lax.psum_scatter(
        term_fn(jnp.int32(0), own_rows * lax.axis_size("fsdp")),
        "fsdp",
        scatter_dimension=0,
        tiled=True,
    )


def head_scores(q_heads, k_heads, allowed):
    scores = jnp.einsum(
        "thd,shd->hts", q_heads, k_heads, preferred_element_type=jnp.float32
    ) * HEAD_DIM ** (-0.5)
    return jnp.where(allowed[None], scores, -1e30)


def experts_by_slot(
    second_in, second_rows, cotangent, routes, capacity, w_router, w_gate, w_up, w_down
):
    tok_count, model_width = second_rows.shape
    experts = w_router.shape[1]
    local_experts = w_gate.shape[0]
    slot_count = tok_count * TOP * 3 // (2 * experts)
    pair_count = tok_count * TOP
    zero_row = jnp.zeros((1, model_width), jnp.bfloat16)
    logits = jnp.dot(second_rows, w_router, preferred_element_type=jnp.float32)
    chosen = routes
    expert_ids = lax.iota(jnp.int32, experts)
    chosen_hot = (chosen[:, :, None] == expert_ids[None, None, :]).astype(jnp.float32)
    routed = jnp.sum(chosen_hot * logits[:, None, :], axis=2)
    gate_wts = jax.nn.softmax(routed, axis=1)
    pair_hot = chosen_hot.reshape(pair_count, experts).astype(jnp.int32)
    earlier_hits = jnp.cumsum(pair_hot, axis=0) - pair_hot
    ranking = jnp.sum(earlier_hits * pair_hot, axis=1)
    cap_pair = jnp.sum(pair_hot * capacity[None, :], axis=1)
    is_kept = ranking < cap_pair
    pair_route = chosen.reshape(pair_count)
    slot_place = jnp.where(is_kept, pair_route * slot_count + ranking, experts * slot_count)
    pair_ids = lax.iota(jnp.int32, pair_count)
    slot_pair = (
        jnp.full((experts * slot_count,), pair_count, jnp.int32)
        .at[slot_place]
        .set(pair_ids, mode="drop")
    )
    padded = jnp.concatenate([second_rows, zero_row], axis=0)
    outgoing = padded[slot_pair // TOP].reshape(experts, slot_count, model_width)
    arrived = shard_gather(to_owner(outgoing))
    gate_w, up_w, down_w = (w_gate, w_up, w_down)
    owner_rows = arrived.reshape(-1, local_experts, slot_count, model_width)
    sources = owner_rows.shape[0]
    gate_act = jnp.einsum("sjcd,jdh->sjch", owner_rows, gate_w, preferred_element_type=jnp.float32)
    up_act = jnp.einsum("sjcd,jdh->sjch", owner_rows, up_w, preferred_element_type=jnp.float32)
    sig_gate = jax.nn.sigmoid(gate_act)
    silu_gate = gate_act * sig_gate
    hidden = (silu_gate * up_act).astype(jnp.bfloat16)

    def down_term(start, length):
        return jnp.einsum("sjch,jhd->sjcd", hidden, down_w, preferred_element_type=jnp.float32)

    produced = owner_sum(down_term, sources)
    returned = from_owner(produced.astype(jnp.bfloat16).reshape(-1, slot_count, model_width))
    slot_rows = jnp.concatenate(
        [returned.reshape(experts * slot_count, model_width), zero_row], axis=0
    )
    pair_rows = slot_rows[slot_place].reshape(tok_count, TOP, model_width).astype(jnp.float32)
    kept_mask = is_kept.reshape(tok_count, TOP).astype(jnp.float32)
    gate_kept = gate_wts * kept_mask
    moe_rows = jnp.sum(gate_kept[:, :, None] * pair_rows, axis=1)
    final_rows = second_in + moe_rows
    block_output = final_rows.astype(jnp.bfloat16)
    grad_out = cotangent.astype(jnp.float32)
    grad_gate_k = jnp.sum(pair_rows * grad_out[:, None, :], axis=2) * kept_mask
    grad_routed = gate_wts * (grad_gate_k - jnp.sum(gate_wts * grad_gate_k, axis=1, keepdims=True))
    grad_logits = jnp.sum(chosen_hot * grad_routed[:, :, None], axis=1)
    router_grad = jnp.dot(second_rows.astype(jnp.float32).T, grad_logits, precision=precise)
    grad_second = jnp.dot(grad_logits, w_router.astype(jnp.float32).T, precision=precise)
    pair_grads = (
        (gate_kept[:, :, None] * grad_out[:, None, :])
        .astype(jnp.bfloat16)
        .reshape(pair_count, model_width)
    )
    pair_grads = jnp.concatenate([pair_grads, zero_row], axis=0)
    slot_grads = pair_grads[slot_pair].reshape(experts, slot_count, model_width)
    grad_blocks = shard_gather(to_owner(slot_grads)).reshape(
        -1, local_experts, slot_count, model_width
    )
    grad_hidden = jnp.einsum(
        "sjcd,jhd->sjch", grad_blocks, down_w, preferred_element_type=jnp.float32
    )
    grad_down_w = jnp.einsum(
        "sjch,sjcd->jhd", hidden, grad_blocks, preferred_element_type=jnp.float32
    )
    grad_gate_in = (grad_hidden * up_act * sig_gate * (1.0 + gate_act * (1.0 - sig_gate))).astype(
        jnp.bfloat16
    )
    grad_up_in = (grad_hidden * silu_gate).astype(jnp.bfloat16)
    grad_gate_w = jnp.einsum(
        "sjcd,sjch->jdh", owner_rows, grad_gate_in, preferred_element_type=jnp.float32
    )
    grad_up_w = jnp.einsum(
        "sjcd,sjch->jdh", owner_rows, grad_up_in, preferred_element_type=jnp.float32
    )

    def back_term(start, length):
        from_gate = jnp.einsum(
            "sjch,jdh->sjcd", grad_gate_in, gate_w, preferred_element_type=jnp.float32
        )
        from_up = jnp.einsum("sjch,jdh->sjcd", grad_up_in, up_w, preferred_element_type=jnp.float32)
        return from_gate + from_up

    grad_slots = from_owner(
        owner_sum(back_term, sources).astype(jnp.bfloat16).reshape(-1, slot_count, model_width)
    )
    back_rows = jnp.concatenate(
        [grad_slots.reshape(experts * slot_count, model_width), zero_row], axis=0
    )
    grad_second = grad_second + jnp.sum(
        back_rows[slot_place].reshape(tok_count, TOP, model_width).astype(jnp.float32), axis=1
    )
    return block_output[None], grad_second, router_grad.T, (grad_gate_w, grad_up_w, grad_down_w)


def experts_dense(
    second_in, second_rows, cotangent, routes, capacity, w_router, w_gate, w_up, w_down
):
    tok_count = second_rows.shape[0]
    experts = w_router.shape[1]
    local_experts, model_width, hidden_here = w_gate.shape
    shards = lax.axis_size("fsdp")
    owners = lax.axis_size("expert")
    wide = local_experts * hidden_here
    logits = jnp.dot(second_rows, w_router, preferred_element_type=jnp.float32)
    expert_ids = lax.iota(jnp.int32, experts)
    named = jnp.any(routes[:, :, None] == expert_ids[None, None, :], axis=1)
    before = lax.iota(jnp.int32, tok_count)[None, :] < lax.iota(jnp.int32, tok_count)[:, None]
    ranking = jnp.dot(
        before.astype(jnp.bfloat16), named.astype(jnp.bfloat16), preferred_element_type=jnp.float32
    )
    kept = named & (ranking < capacity.astype(jnp.float32)[None, :])
    kept_mask = kept.astype(jnp.float32)
    top_logit = jnp.max(jnp.where(named, logits, -jnp.inf), axis=1, keepdims=True)
    powers = jnp.where(named, jnp.exp(jnp.where(named, logits - top_logit, 0.0)), 0.0)
    gate_wts = powers / jnp.sum(powers, axis=1, keepdims=True)
    gate_kept = gate_wts * kept_mask

    grad_all = lax.all_gather(cotangent, ("fsdp", "expert"), axis=0, tiled=True)
    nz = owners // 2
    grad_all = grad_all.reshape(shards, owners, tok_count, model_width)
    rows_all, pre, weighted, forward, gates = gather_act(
        second_rows, gate_kept.T, w_gate, w_up, w_down, nz, 7
    )
    back_rows, terms, acts = scatter_act(pre, grad_all, gates, w_gate, w_up, w_down, nz, 8)
    grad_gate_k = terms.T * kept_mask
    grad_logits = gate_wts * (grad_gate_k - jnp.sum(gate_wts * grad_gate_k, axis=1, keepdims=True))
    router_grad = jnp.dot(grad_logits.T, second_rows.astype(jnp.float32), precision=precise)
    grad_second = jnp.dot(grad_logits, w_router.astype(jnp.float32).T, precision=precise)
    grad_second = grad_second + back_rows

    units = shards * nz
    inputs = (
        rows_all.reshape(units, -1, model_width),
        acts.reshape(2, units, -1, wide),
        weighted.reshape(units, -1, wide),
        grad_all.reshape(units, -1, model_width),
    )
    return forward, grad_second, router_grad, inputs


def sum_grads(narrow, gains, head_gains, rows, inputs, first, normed, local, nz):
    shards, width = lax.axis_size("fsdp"), gains.shape[1]
    mine = lax.iota(jnp.int32, shards) == lax.axis_index("fsdp")
    heads_flat = jnp.pad(head_gains.reshape(-1), (0, width - head_gains.size))
    table = jnp.concatenate([gains, jnp.where(mine[:, None], heads_flat[None], 0.0)], axis=0)
    share = -(-table.size // (2 * shards * nz * 1024)) * 8
    small = jnp.pad(table.reshape(-1), (0, 2 * shards * nz * share * 128 - table.size))
    small = small.reshape(2, shards, nz, share, 128)
    parts = [g.reshape(-1, 2, nz, 32, g.shape[1]) for g in narrow]
    first = first.reshape(shards, -1, width)
    *sums, small, rows, gate, up, down, first = line_sum(
        parts, small, rows, inputs, first, normed.astype(jnp.bfloat16), local, nz, 9
    )
    expert_grads = (gate, up, down.reshape(local, -1, width))
    small = small.reshape(-1)[: table.size].reshape(table.shape)
    own = lax.dynamic_slice_in_dim(small, gains.shape[0] + lax.axis_index("fsdp"), 1, axis=0)
    head_gains = own[0, : head_gains.size].reshape(head_gains.shape)
    return [s.reshape(g.shape) for s, g in zip(sums, narrow)], small[: gains.shape[0]], head_gains, rows, expert_grads, first


def on_device(
    block_input,
    cotangent,
    w_query,
    w_key,
    w_value,
    w_output,
    q_gain,
    k_gain,
    attn_gain,
    mlp_gain,
    w_router,
    w_gate,
    w_up,
    w_down,
    segments,
    routes,
    capacity,
):
    tok_count = block_input.shape[1]
    model_width = block_input.shape[2]
    experts = w_router.shape[1]
    nz = lax.axis_size("expert") // 2
    dense = 2 * TOP >= experts and lax.axis_size("fsdp") == 4
    flat_in = block_input[0].astype(jnp.float32)
    scale_one = lax.rsqrt(jnp.mean(flat_in * flat_in, axis=1, keepdims=True) + epsilon)
    normed_one = flat_in * scale_one
    first_rows = (normed_one * attn_gain).astype(jnp.bfloat16)
    if dense:
        group_rows, group_segs = square_gather(first_rows, jnp.tile(segments, (8, 1)), 1)
        group_rows = group_rows.reshape(-1, model_width)
        group_segs = group_segs[:, 0].reshape(-1)
    else:
        group_rows, group_segs = (
            lax.all_gather(first_rows, "fsdp", axis=0, tiled=True),
            lax.all_gather(segments[0], "fsdp", axis=0, tiled=True),
        )
    group_len = group_rows.shape[0]
    heads_here = w_query.shape[1] // HEAD_DIM
    query_rows = jnp.dot(group_rows, w_query, preferred_element_type=jnp.float32)
    key_rows = jnp.dot(group_rows, w_key, preferred_element_type=jnp.float32)
    value_rows = jnp.dot(group_rows, w_value, preferred_element_type=jnp.float32).astype(
        jnp.bfloat16
    )
    square_sums = across_heads(
        dense and 2,
        (jnp.sum(query_rows * query_rows, axis=1), jnp.sum(key_rows * key_rows, axis=1))
    )
    q_scale = lax.rsqrt(square_sums[0][:, None] / model_width + epsilon)
    k_scale = lax.rsqrt(square_sums[1][:, None] / model_width + epsilon)
    cosine, sine_table = rope_tables(group_segs, HEAD_DIM)
    head_shape = (group_len, heads_here, HEAD_DIM)
    q_heads = apply_rope(
        (query_rows * q_scale * q_gain).reshape(head_shape), cosine, sine_table
    ).astype(jnp.bfloat16)
    k_heads = apply_rope(
        (key_rows * k_scale * k_gain).reshape(head_shape), cosine, sine_table
    ).astype(jnp.bfloat16)
    v_heads = value_rows.reshape(head_shape)
    ordinal = lax.iota(jnp.int32, group_len)
    allowed = (group_segs[:, None] == group_segs[None, :]) & (ordinal[None, :] <= ordinal[:, None])
    scores = head_scores(q_heads, k_heads, allowed)
    row_top = jnp.max(scores, axis=2, keepdims=True)
    log_total = row_top + jnp.log(jnp.sum(jnp.exp(scores - row_top), axis=2, keepdims=True))
    attn_weights = jnp.exp(scores - log_total)
    mixed_heads = jnp.einsum(
        "hts,shd->thd",
        attn_weights.astype(jnp.bfloat16),
        v_heads,
        preferred_element_type=jnp.float32,
    )
    attn_rows = mixed_heads.reshape(group_len, heads_here * HEAD_DIM).astype(jnp.bfloat16)

    def mixed_term(start, length):
        return jnp.dot(attn_rows, w_output, preferred_element_type=jnp.float32).astype(jnp.bfloat16)

    mixed_rows = share_rows(mixed_term, tok_count, dense and 4).astype(jnp.float32)
    second_in = flat_in + mixed_rows
    scale_two = lax.rsqrt(jnp.mean(second_in * second_in, axis=1, keepdims=True) + epsilon)
    normed_two = second_in * scale_two
    second_rows = (normed_two * mlp_gain).astype(jnp.bfloat16)
    if dense:
        block_output, grad_second, router_grad, expert_grads = experts_dense(
            second_in, second_rows, cotangent[0], routes[0], capacity, w_router, w_gate, w_up, w_down
        )
    else:
        block_output, grad_second, router_grad, expert_grads = experts_by_slot(
            second_in, second_rows, cotangent[0], routes[0], capacity, w_router, w_gate, w_up, w_down
        )
    grad_out = cotangent[0].astype(jnp.float32)
    mlp_gain_grad = jnp.sum(grad_second * normed_two, axis=0)
    grad_normed_two = grad_second * mlp_gain
    grad_mid = grad_out + scale_two * (
        grad_normed_two - normed_two * jnp.mean(grad_normed_two * normed_two, axis=1, keepdims=True)
    )
    if dense:
        group_grad, _ = square_gather(grad_mid.astype(jnp.bfloat16), jnp.tile(segments, (8, 1)), 6)
        group_grad = group_grad.reshape(-1, model_width)
    else:
        group_grad = lax.all_gather(grad_mid.astype(jnp.bfloat16), "fsdp", axis=0, tiled=True)
    out_grad = jnp.einsum("ti,td->id", attn_rows, group_grad, preferred_element_type=jnp.float32)
    grad_attn = (
        jnp.einsum("td,id->ti", group_grad, w_output, preferred_element_type=jnp.float32)
        .astype(jnp.bfloat16)
        .reshape(head_shape)
    )
    scores_again = head_scores(q_heads, k_heads, allowed)
    weights_again = jnp.exp(scores_again - log_total)
    grad_values = jnp.einsum(
        "hts,thd->shd",
        weights_again.astype(jnp.bfloat16),
        grad_attn,
        preferred_element_type=jnp.float32,
    )
    grad_weights = jnp.einsum(
        "thd,shd->hts", grad_attn, v_heads, preferred_element_type=jnp.float32
    )
    inner_sum = jnp.sum(weights_again * grad_weights, axis=2, keepdims=True)
    grad_scores = (weights_again * (grad_weights - inner_sum)).astype(jnp.bfloat16)
    grad_q_heads = jnp.einsum(
        "hts,shd->thd", grad_scores, k_heads, preferred_element_type=jnp.float32
    ) * HEAD_DIM ** (-0.5)
    grad_k_heads = jnp.einsum(
        "hts,thd->shd", grad_scores, q_heads, preferred_element_type=jnp.float32
    ) * HEAD_DIM ** (-0.5)
    grad_q_normed = rope_grad(grad_q_heads, cosine, sine_table).reshape(group_len, -1)
    grad_k_normed = rope_grad(grad_k_heads, cosine, sine_table).reshape(group_len, -1)
    q_gain_grad = jnp.sum(grad_q_normed * query_rows * q_scale, axis=0)
    k_gain_grad = jnp.sum(grad_k_normed * key_rows * k_scale, axis=0)
    inner_q = grad_q_normed * q_gain
    inner_k = grad_k_normed * k_gain
    inner_sums = across_heads(
        dense and 3,
        (jnp.sum(inner_q * query_rows, axis=1), jnp.sum(inner_k * key_rows, axis=1))
    )
    grad_query_rows = (
        q_scale
        * (inner_q - query_rows * q_scale * q_scale * (inner_sums[0][:, None] / model_width))
    ).astype(jnp.bfloat16)
    grad_key_rows = (
        k_scale * (inner_k - key_rows * k_scale * k_scale * (inner_sums[1][:, None] / model_width))
    ).astype(jnp.bfloat16)
    grad_value_rows = grad_values.reshape(group_len, -1).astype(jnp.bfloat16)
    head_grads = jnp.concatenate([grad_query_rows, grad_key_rows, grad_value_rows], axis=1)
    mixer_grad = jnp.einsum(
        "td,ti->di", group_rows, head_grads, preferred_element_type=jnp.float32
    ).astype(jnp.bfloat16)

    def input_term(start, length):
        head_w = jnp.concatenate([w_query, w_key, w_value], axis=1)
        return jnp.einsum(
            "ti,di->td", head_grads, head_w, preferred_element_type=jnp.float32
        ).astype(jnp.bfloat16)

    if dense:
        attn_gain_grad = jnp.zeros_like(mlp_gain_grad)
    else:
        grad_first = share_rows(input_term, tok_count).astype(jnp.float32)
        attn_gain_grad = jnp.sum(grad_first * normed_one, axis=0)
    narrow = (mixer_grad, out_grad.astype(jnp.bfloat16))
    gains = jnp.concatenate([attn_gain_grad[None], mlp_gain_grad[None], router_grad], axis=0)
    head_gains = jnp.stack([q_gain_grad, k_gain_grad])
    if dense:
        first = input_term(jnp.int32(0), group_len)
        narrow, gains, head_gains, forward, expert_grads, grad_first = sum_grads(
            narrow, gains, head_gains, block_output, expert_grads, first, normed_one, w_gate.shape[0], nz
        )
        block_output = (second_in + forward).astype(jnp.bfloat16)[None]
    else:
        narrow = lax.psum(narrow, "expert")
        head_gains = lax.psum(head_gains, "expert")
        gains = lax.psum(gains, ("fsdp", "expert"))
    grad_normed_one = grad_first * attn_gain
    grad_x = grad_mid + scale_one * (
        grad_normed_one - normed_one * jnp.mean(grad_normed_one * normed_one, axis=1, keepdims=True)
    )
    wide = tuple(jnp.split(narrow[0], 3, axis=1)) + (narrow[1],)
    mixer = tuple(g.astype(jnp.float32) for g in wide) + (head_gains[0], head_gains[1])
    return (
        block_output,
        grad_x[None],
        mixer[0],
        mixer[1],
        mixer[2],
        mixer[3],
        mixer[4],
        mixer[5],
        gains[0],
        gains[1],
        gains[2:].T,
        *expert_grads,
    )


def solution(mesh):
    placed = (
        P("expert", "fsdp", None),
        P("expert", "fsdp", None),
        P(None, "fsdp"),
        P(None, "fsdp"),
        P(None, "fsdp"),
        P("fsdp", None),
        P("fsdp"),
        P("fsdp"),
        P(),
        P(),
        P(),
        P("expert", None, "fsdp"),
        P("expert", None, "fsdp"),
        P("expert", "fsdp", None),
        P("expert", "fsdp"),
        P("expert", "fsdp", None),
        P(),
    )
    return jax.shard_map(
        on_device,
        mesh=mesh,
        in_specs=placed,
        out_specs=(
            P("expert", "fsdp", None),
            P("expert", "fsdp", None),
            P(None, "fsdp"),
            P(None, "fsdp"),
            P(None, "fsdp"),
            P("fsdp", None),
            P("fsdp"),
            P("fsdp"),
            P(),
            P(),
            P(),
            P("expert", None, "fsdp"),
            P("expert", None, "fsdp"),
            P("expert", "fsdp", None),
        ),
        check_vma=False,
    )
```
